32 devices in a mesh: rep: 8 (over y, x, core), shard: 4 (over z).
Axes of the slice: x: 2, y: 2, z: 4, core: 2. Of those that a mesh axis runs over, the one named last changes fastest.
Arguments:
- tokens: bfloat16 [32, 512, 2048], P(('rep', 'shard')), may hold values from -6 to 6
- segments: int32 [32, 512], P(('rep', 'shard')), may hold values from 0 to 7, never falling along the last dimension, each value on 1 to 256 neighbouring positions
- cotangent: bfloat16 [32, 512, 2048], P(('rep', 'shard')), may hold values from -6 to 6
- gain: float32 [2048], P('shard'), may hold values from 0.5 to 1.5
- w_query: float32 [2048, 1024], P('shard'), may hold values from -0.125 to 0.125
- w_key: float32 [2048, 256], P('shard'), may hold values from -0.125 to 0.125
- w_value: float32 [2048, 256], P('shard'), may hold values from -0.125 to 0.125
- w_outproj: float32 [1024, 2048], P('shard'), may hold values from -0.75 to 0.75
- moment_gain: float32 [2048], P('shard'), may hold values from -160 to 160
- moment_query: float32 [2048, 1024], P('shard'), may hold values from -224 to 224
- moment_key: float32 [2048, 256], P('shard'), may hold values from -224 to 224
- moment_value: float32 [2048, 256], P('shard'), may hold values from -384 to 384
- moment_outproj: float32 [1024, 2048], P('shard'), may hold values from -40 to 40
Outputs:
- output: bfloat16 [32, 512, 2048], P(('rep', 'shard'))
- grad_input: bfloat16 [32, 512, 2048], P(('rep', 'shard'))
- grad_gain: float32 [2048], P('shard')
- grad_query: float32 [2048, 1024], P('shard')
- grad_key: float32 [2048, 256], P('shard')
- grad_value: float32 [2048, 256], P('shard')
- grad_outproj: float32 [1024, 2048], P('shard')
- gain_next: float32 [2048], P('shard')
- query_next: float32 [2048, 1024], P('shard', 'rep')
- key_next: float32 [2048, 256], P('shard', 'rep')
- value_next: float32 [2048, 256], P('shard', 'rep')
- outproj_next: float32 [1024, 2048], P('shard', 'rep')
- moment_gain_next: float32 [2048], P('shard')
- moment_query_next: float32 [2048, 1024], P('shard')
- moment_key_next: float32 [2048, 256], P('shard')
- moment_value_next: float32 [2048, 256], P('shard')
- moment_outproj_next: float32 [1024, 2048], P('shard')
The draws below stay inside these ranges and needn't reach their ends.
Inputs may be any that keep to these rules, and one draw needn't show every extreme that they name: `segments`: within a sequence ids never fall; every one of the 8 ids appears, each document has 1 to 256 tokens, and one has exactly 256.
All inputs are finite; a program needn't handle non-finite values.
Results may differ from the reference program's by a relative error of at most 0.012.
The reference program's roundings to bfloat16 on the way count: a program that leaves them out, or rounds other values in their place, can miss the bound.
Values may be sent and summed in bfloat16 or wider, within the bound.
A program may use at most 320 MiB of HBM per device.

```python
import math
import jax
import jax.numpy as jnp
import numpy as np
from jax import lax

D = 2048
QUERY_HEADS = 16
KEY_VALUE_HEADS = 4
HEAD_SIZE = 64
SEQ = 512
DOCS = 8
QUERY_FEATURES = 1024
KEY_FEATURES = 256
SEQS = 32
TOKENS = 16384


def block_levels(stream_key, extent, cuts, least, top_value):
    level = 1.0
    for dim, blocks in cuts:
        draws = jax.random.uniform(jax.random.fold_in(jax.random.fold_in(stream_key, 6), dim), (blocks,), jnp.float32, least / len(cuts), top_value / len(cuts))
        level = level * jnp.repeat(jnp.exp(draws), extent[dim] // blocks).reshape((-1,) + (1,) * (len(extent) - 1 - dim))
    return level


def length_profile(count, total, reach, skew):
    weights = [(1 << 20) // math.isqrt(standing ** skew) + 1 for standing in range(2, count + 1)]
    rest, given = total - reach - (count - 1), [1] * (count - 1)
    while rest > 0:
        candidates = [i for i in range(count - 1) if given[i] < reach]
        pool, budget = sum([weights[i] for i in candidates]), rest
        for i in candidates:
            extra = min(reach - given[i], max(1, budget * weights[i] // pool), rest)
            given[i] = given[i] + extra
            rest = rest - extra
    return np.array([reach] + given)


def ragged_sizes(key, count, total, limit, slope):
    if count == 2:
        one = jax.random.randint(key, (), max(1, total - limit), min(limit, total - 1) + 1)
        return jnp.stack([one, total - one])
    lengths = jnp.asarray(length_profile(count, total, limit, slope), jnp.int32)
    pairs = (count - 1) // 2
    donor, sink = lengths[1:1 + 2 * pairs:2], lengths[2:2 + 2 * pairs:2]
    room = jnp.minimum(donor - 1, limit - sink)
    shifted = jax.random.randint(jax.random.fold_in(key, 1), (pairs,), 0, 1 << 20) % (room + 1)
    lengths = lengths.at[1:1 + 2 * pairs:2].set(donor - shifted).at[2:2 + 2 * pairs:2].set(sink + shifted)
    return lengths[jax.random.permutation(jax.random.fold_in(key, 2), count)]


def scatter_about(stream_key, extent, spread, limit, pieces=(), kind=jnp.bfloat16):
    level = block_levels(stream_key, extent, pieces, -0.22, 0.18) if pieces else 1.0
    result = jax.random.normal(stream_key, extent, jnp.float32) * spread * level
    return jnp.minimum(jnp.maximum(result, -limit), limit).astype(kind)


def setup_inputs(seed: int = 0) -> dict:
    keys = jax.random.split(jax.random.key(seed), 14)
    return {
        "tokens": scatter_about(keys[0], (SEQS, SEQ, D), 1.0, 6.0, ((0, 32),)),
        "segments": jax.vmap(lambda own: jnp.searchsorted(jnp.cumsum(ragged_sizes(own, DOCS, SEQ, SEQ // 2, 2)), jnp.arange(SEQ), side="right"))(jax.random.split(keys[1], SEQS)).reshape((SEQS, SEQ)).astype(jnp.int32),
        "cotangent": scatter_about(keys[2], (SEQS, SEQ, D), 1.0, 6.0, ((0, 32),)),
        "gain": jnp.clip(1.0 + 0.1 * jax.random.normal(keys[3], (D,), jnp.float32), 0.5, 1.5),
        "w_query": scatter_about(keys[4], (D, QUERY_FEATURES), D ** -0.5, 0.125, ((0, 4),), jnp.float32),
        "w_key": scatter_about(keys[5], (D, KEY_FEATURES), D ** -0.5, 0.125, ((0, 4),), jnp.float32),
        "w_value": scatter_about(keys[6], (D, KEY_FEATURES), D ** -0.5, 0.125, ((0, 4),), jnp.float32),
        "w_outproj": scatter_about(keys[7], (QUERY_FEATURES, D), (QUERY_FEATURES // 16) ** -0.5, 0.75, ((0, 4),), jnp.float32),
        "moment_gain": scatter_about(keys[8], (D,), (0.2 * TOKENS ** 0.5), 160.0, ((0, 4),), jnp.float32),
        "moment_query": scatter_about(keys[9], (D, QUERY_FEATURES), (0.3 * TOKENS ** 0.5), 224.0, ((0, 4),), jnp.float32),
        "moment_key": scatter_about(keys[10], (D, KEY_FEATURES), (0.3 * TOKENS ** 0.5), 224.0, ((0, 4),), jnp.float32),
        "moment_value": scatter_about(keys[11], (D, KEY_FEATURES), (0.5 * TOKENS ** 0.5), 384.0, ((0, 4),), jnp.float32),
        "moment_outproj": scatter_about(keys[12], (QUERY_FEATURES, D), (0.05 * TOKENS ** 0.5), 40.0, ((0, 4),), jnp.float32),
    }


norm_eps = 1e-05
rope_base = 500000.0
coef_a = 3.4445
coef_b = -4.775
coef_c = 2.0315
decay = 0.95
muon_rate = 0.02
gain_rate = 0.2

def positions_of(seq_segments):
    sequence_length = seq_segments.shape[0]
    token_index = jnp.arange(sequence_length, dtype=jnp.int32)
    before = jnp.concatenate([seq_segments[:1] - 1, seq_segments[:-1]])
    starts = jnp.where(seq_segments != before, token_index, jnp.zeros_like(token_index))
    return token_index - lax.cummax(starts, axis=0)

def rope_tables(seq_segments, head_dim):
    position = positions_of(seq_segments).astype(jnp.float32)
    half_dim = head_dim // 2
    frequency = rope_base ** (-2.0 * jnp.arange(half_dim, dtype=jnp.float32) / head_dim)
    angles = position[:, None] * frequency[None, :]
    return (jnp.cos(angles)[:, None, :], jnp.sin(angles)[:, None, :])

def apply_rotary(values, cosine_table, sine_table):
    half_dim = values.shape[-1] // 2
    front_half = values[..., :half_dim]
    back_half = values[..., half_dim:]
    return jnp.concatenate([front_half * cosine_table - back_half * sine_table, back_half * cosine_table + front_half * sine_table], -1)

def unrotate(gradient, cosine_table, sine_table):
    half_dim = gradient.shape[-1] // 2
    front_half = gradient[..., :half_dim]
    back_half = gradient[..., half_dim:]
    return jnp.concatenate([front_half * cosine_table + back_half * sine_table, back_half * cosine_table - front_half * sine_table], -1)

def contract_rows(left, right):
    return lax.dot_general(left, right, (((0,), (0,)), ((), ())), preferred_element_type=jnp.float32)

def contract_cols(left, right):
    return lax.dot_general(left, right, (((1,), (1,)), ((), ())), preferred_element_type=jnp.float32)

def head_forward(q_head, k_head, v_head, allowed, score_scale):
    scores = jnp.einsum('qgd,kd->gqk', q_head.astype(jnp.float32), k_head.astype(jnp.float32)) * score_scale
    exponent = jnp.where(allowed[None], jnp.exp(scores), jnp.zeros_like(scores))
    denom_sum = lax.optimization_barrier(jnp.sum(exponent, -1, keepdims=True))
    probabilities = (exponent / denom_sum).astype(jnp.bfloat16)
    attended = jnp.einsum('gqk,kd->qgd', probabilities.astype(jnp.float32), v_head.astype(jnp.float32))
    return (attended, jnp.log(denom_sum))

def head_backward(q_head, k_head, v_head, log_sum, grad_head, allowed, score_scale):
    scores = jnp.einsum('qgd,kd->gqk', q_head.astype(jnp.float32), k_head.astype(jnp.float32)) * score_scale
    recomputed = jnp.where(allowed[None], jnp.exp(scores - log_sum), jnp.zeros_like(scores))
    rounded = recomputed.astype(jnp.bfloat16)
    value_grad = jnp.einsum('gqk,qgd->kd', rounded.astype(jnp.float32), grad_head.astype(jnp.float32))
    prob_grad = jnp.einsum('qgd,kd->gqk', grad_head.astype(jnp.float32), v_head.astype(jnp.float32))
    row_inner = lax.optimization_barrier(jnp.sum(recomputed * prob_grad, -1, keepdims=True))
    score_grad = (recomputed * (prob_grad - row_inner) * score_scale).astype(jnp.bfloat16)
    query_grad = jnp.einsum('gqk,kd->qgd', score_grad.astype(jnp.float32), k_head.astype(jnp.float32))
    key_grad = jnp.einsum('gqk,qgd->kd', score_grad.astype(jnp.float32), q_head.astype(jnp.float32))
    return (query_grad, key_grad, value_grad)

def sequence_pass(seq_tokens, seq_segments, seq_cotangent, w_in, gain_cast, w_out):
    sequence_length = seq_tokens.shape[0]
    group_width = QUERY_HEADS // KEY_VALUE_HEADS
    score_scale = 1.0 / math.sqrt(HEAD_SIZE)
    tok_float = seq_tokens.astype(jnp.float32)
    inv_rms = lax.rsqrt(lax.optimization_barrier(jnp.mean(tok_float * tok_float, -1, keepdims=True)) + norm_eps)
    normed = tok_float * inv_rms
    norm_bf = (normed * gain_cast).astype(jnp.bfloat16)
    projected_rows = jnp.dot(norm_bf, w_in, preferred_element_type=jnp.float32)
    cosine_table, sine_table = rope_tables(seq_segments, HEAD_SIZE)
    query_rows = apply_rotary(projected_rows[:, :QUERY_FEATURES].reshape(sequence_length, QUERY_HEADS, HEAD_SIZE), cosine_table, sine_table).astype(jnp.bfloat16)
    rotated_keys = apply_rotary(projected_rows[:, QUERY_FEATURES:QUERY_FEATURES + KEY_FEATURES].reshape(sequence_length, KEY_VALUE_HEADS, HEAD_SIZE), cosine_table, sine_table).astype(jnp.bfloat16)
    values_bfloat = projected_rows[:, QUERY_FEATURES + KEY_FEATURES:].reshape(sequence_length, KEY_VALUE_HEADS, HEAD_SIZE).astype(jnp.bfloat16)
    token_index = jnp.arange(sequence_length, dtype=jnp.int32)
    allowed = (token_index[None, :] <= token_index[:, None]) & (seq_segments[None, :] == seq_segments[:, None])
    query_head_rows = query_rows.reshape(sequence_length, KEY_VALUE_HEADS, group_width, HEAD_SIZE).transpose(1, 0, 2, 3)
    k_heads = rotated_keys.transpose(1, 0, 2)
    v_heads = values_bfloat.transpose(1, 0, 2)
    attended, log_sum = lax.map(lambda blocks: head_forward(blocks[0], blocks[1], blocks[2], allowed, score_scale), (query_head_rows, k_heads, v_heads))
    attn_bf = attended.transpose(1, 0, 2, 3).reshape(sequence_length, QUERY_FEATURES).astype(jnp.bfloat16)
    output = (tok_float + jnp.dot(attn_bf, w_out, preferred_element_type=jnp.float32)).astype(jnp.bfloat16)
    outproj_part = contract_rows(attn_bf, seq_cotangent)
    attention_gradient = contract_cols(seq_cotangent, w_out).astype(jnp.bfloat16)
    head_gradients = attention_gradient.reshape(sequence_length, KEY_VALUE_HEADS, group_width, HEAD_SIZE).transpose(1, 0, 2, 3)
    query_grad, key_grad, value_grad = lax.map(lambda blocks: head_backward(blocks[0], blocks[1], blocks[2], blocks[3], blocks[4], allowed, score_scale), (query_head_rows, k_heads, v_heads, log_sum, head_gradients))
    query_grad = unrotate(query_grad.transpose(1, 0, 2, 3).reshape(sequence_length, QUERY_HEADS, HEAD_SIZE), cosine_table, sine_table)
    key_grad = unrotate(key_grad.transpose(1, 0, 2), cosine_table, sine_table)
    grad_qkv = jnp.concatenate([query_grad.reshape(sequence_length, QUERY_FEATURES), key_grad.reshape(sequence_length, KEY_FEATURES), value_grad.transpose(1, 0, 2).reshape(sequence_length, KEY_FEATURES)], 1).astype(jnp.bfloat16)
    in_part = contract_rows(norm_bf, grad_qkv)
    grad_normed = contract_cols(grad_qkv, w_in)
    gain_part = lax.optimization_barrier(jnp.sum(grad_normed * normed, 0))
    grad_hat = grad_normed * gain_cast
    grad_tokens = (seq_cotangent.astype(jnp.float32) + inv_rms * (grad_hat - normed * lax.optimization_barrier(jnp.mean(grad_hat * normed, -1, keepdims=True)))).astype(jnp.bfloat16)
    return (output, grad_tokens, in_part, gain_part, outproj_part)

def orthogonalize(matrix):
    is_tall = matrix.shape[0] > matrix.shape[1]
    iterate = matrix.T if is_tall else matrix
    iterate = iterate / (jnp.sqrt(jnp.sum(iterate * iterate)) + 1e-06)
    for sweep in range(5):
        square = jnp.dot(iterate, iterate.T, precision=lax.Precision.HIGHEST)
        polynomial = coef_b * square + coef_c * jnp.dot(square, square, precision=lax.Precision.HIGHEST)
        iterate = coef_a * iterate + jnp.dot(polynomial, iterate, precision=lax.Precision.HIGHEST)
    return iterate.T if is_tall else iterate

def reference(tokens, segments, cotangent, gain, w_query, w_key, w_value, w_outproj, moment_gain, moment_query, moment_key, moment_value, moment_outproj):
    w_in = jnp.concatenate([w_query, w_key, w_value], 1).astype(jnp.bfloat16)
    gain_cast = lax.optimization_barrier(gain.astype(jnp.bfloat16)).astype(jnp.float32)
    w_out = w_outproj.astype(jnp.bfloat16)

    def step(running, blocks):
        output, grad_tokens, in_part, gain_part, outproj_part = sequence_pass(blocks[0], blocks[1], blocks[2], w_in, gain_cast, w_out)
        return ((running[0] + in_part, running[1] + gain_part, running[2] + outproj_part), (output, grad_tokens))
    zeros_init = (jnp.zeros((D, QUERY_FEATURES + 2 * KEY_FEATURES), jnp.float32), jnp.zeros((D,), jnp.float32), jnp.zeros((QUERY_FEATURES, D), jnp.float32))
    sums, stacked = lax.scan(step, zeros_init, (tokens, segments, cotangent))
    grad_in, grad_gain, grad_outproj = sums
    outputs, grad_input = stacked
    grad_query = grad_in[:, :QUERY_FEATURES]
    grad_key = grad_in[:, QUERY_FEATURES:QUERY_FEATURES + KEY_FEATURES]
    grad_value = grad_in[:, QUERY_FEATURES + KEY_FEATURES:]
    moment_gain_next = decay * moment_gain + grad_gain
    moment_query_next = decay * moment_query + grad_query
    moment_key_next = decay * moment_key + grad_key
    moment_value_next = decay * moment_value + grad_value
    moment_outproj_next = decay * moment_outproj + grad_outproj
    gain_next = gain - gain_rate / math.sqrt(TOKENS) * moment_gain_next
    query_next = w_query - muon_rate * math.sqrt(max(w_query.shape)) * orthogonalize(moment_query_next)
    key_next = w_key - muon_rate * math.sqrt(max(w_key.shape)) * orthogonalize(moment_key_next)
    value_next = w_value - muon_rate * math.sqrt(max(w_value.shape)) * orthogonalize(moment_value_next)
    outproj_next = w_outproj - muon_rate * math.sqrt(max(w_outproj.shape)) * orthogonalize(moment_outproj_next)
    return (outputs, grad_input, grad_gain, grad_query, grad_key, grad_value, grad_outproj, gain_next, query_next, key_next, value_next, outproj_next, moment_gain_next, moment_query_next, moment_key_next, moment_value_next, moment_outproj_next)
```

```python
import functools
import math

import jax
import jax.numpy as jnp
from jax import lax
from jax.experimental import pallas as pl
from jax.experimental.pallas import tpu as pltpu
from jax.sharding import PartitionSpec as P

MESH = pl.DeviceIdType.MESH


class Links:
    def __init__(self, n_rep, n_shard):
        self.n_bits = n_rep.bit_length() - 1
        self.n_shard = n_shard
        self.rep = lax.axis_index("rep")
        self.shard = lax.axis_index("shard")
        self.bits = [lax.rem(lax.div(self.rep, 1 << b), 2) for b in range(self.n_bits)]
        far = list(range(1, self.n_bits))
        self.orders = (far, far[::-1])

    def flip(self, bit):
        return self.rep + (1 << bit) * (1 - 2 * self.bits[bit])

    def barrier(self, line):
        sem = pltpu.get_barrier_semaphore()
        count = self.n_bits
        for b in range(self.n_bits):
            pl.semaphore_signal(sem, 1, device_id=(self.flip(b), self.shard), device_id_type=MESH)
        if line:
            for step in (-1, 1):
                there = self.shard + step
                inside = jnp.logical_and(there >= 0, there < self.n_shard)

                @pl.when(inside)
                def _():
                    pl.semaphore_signal(sem, 1, device_id=(self.rep, there), device_id_type=MESH)

                count = count + inside.astype(jnp.int32)
        else:
            for k in range(1, self.n_shard):
                there = lax.rem(self.shard + k, self.n_shard)
                pl.semaphore_signal(sem, 1, device_id=(self.rep, there), device_id_type=MESH)
            count = count + self.n_shard - 1
        pl.semaphore_wait(sem, count)

    def where(self, fixed, free=()):
        return tuple(
            slice(None) if b in free else fixed.get(b, self.bits[b])
            for b in reversed(range(self.n_bits))
        )


def halves(ref):
    cols = ref.shape[-1]
    return (pl.ds(0, cols // 2), pl.ds(cols // 2, cols // 2))


def spread(links, full, q, half, step, send, recv):
    order = links.orders[half] + [0]
    bit, done = order[step], order[:step]
    view = full.at[(q, *links.where({}, done), slice(None), halves(full)[half])]
    return pltpu.make_async_remote_copy(
        view, view, send, recv, device_id=(links.flip(bit), links.shard), device_id_type=MESH
    )


def gather_kernel(n_rep, n_shard, n_arrays, *refs):
    local, row = refs[:n_arrays], refs[n_arrays]
    full, row_full = refs[n_arrays + 1 : 2 * n_arrays + 1], refs[2 * n_arrays + 1]
    keep_sem, line_send, line_recv, plane_send, plane_recv, row_send, row_recv = refs[2 * n_arrays + 2 :]
    links = Links(n_rep, n_shard)
    me = links.shard
    links.barrier(True)
    row_full[me] = row[...]

    def row_line(way, k):
        q, side = me - way * k, (way + 1) // 2
        return pltpu.make_async_remote_copy(
            row if k == 0 else row_full.at[q], row_full.at[q], row_send.at[side, k], row_recv.at[side, k],
            device_id=(links.rep, me + way), device_id_type=MESH,
        )

    def row_came(way, k):
        here, side = row_full.at[me - way * (k + 1)], (way + 1) // 2
        return pltpu.make_async_remote_copy(
            here, here, row_send.at[side, k], row_recv.at[side, k], device_id=(links.rep, me), device_id_type=MESH
        )
    keeps = [pltpu.make_async_copy(local[a], full[a].at[me], keep_sem.at[a]) for a in range(n_arrays)]

    def line(a, way, k):
        q = me - way * k
        here = links.where({})
        src = local[a].at[here] if k == 0 else full[a].at[(q, *here)]
        side = (way + 1) // 2
        return pltpu.make_async_remote_copy(
            src, full[a].at[(q, *here)], line_send.at[a, side, k], line_recv.at[a, side, k],
            device_id=(links.rep, me + way), device_id_type=MESH,
        )

    def came(a, way, k):
        q = me - way * (k + 1)
        here = full[a].at[(q, *links.where({}))]
        side = (way + 1) // 2
        return pltpu.make_async_remote_copy(
            here, here, line_send.at[a, side, k], line_recv.at[a, side, k],
            device_id=(links.rep, me), device_id_type=MESH,
        )

    def goes(way, k):
        q, there = me - way * k, me + way
        return (q >= 0) & (q < n_shard) & (there >= 0) & (there < n_shard)

    def comes(way, k):
        q = me - way * (k + 1)
        return (q >= 0) & (q < n_shard)

    ways = (1, -1)
    n_steps = links.n_bits
    for way in ways:
        @pl.when(goes(way, 0))
        def _():
            row_line(way, 0).start()
    for a in range(n_arrays):
        for way in ways:
            @pl.when(goes(way, 0))
            def _():
                line(a, way, 0).start()
    for keep in keeps:
        keep.start()

    def plane(a, way, k, half, step):
        q = me - way * (k + 1)
        side = (way + 1) // 2
        return spread(links, full[a], q, half, step,
                      plane_send.at[a, side, k, half, step], plane_recv.at[a, side, k, half, step])

    items = [(a, k) for a in range(n_arrays) for k in range(n_shard - 1)]
    for t in range(len(items) + n_steps):
        for i, (a, k) in enumerate(items):
            step = t - i
            if step < 0 or step > n_steps:
                continue
            for way in ways:
                @pl.when(comes(way, k))
                def _():
                    if step == 0 and a == 0:
                        row_came(way, k).wait_recv()
                        if k + 1 < n_shard - 1:
                            @pl.when(goes(way, k + 1))
                            def _():
                                row_line(way, k + 1).start()
                    if step == 0:
                        came(a, way, k).wait_recv()
                        if k + 1 < n_shard - 1:
                            @pl.when(goes(way, k + 1))
                            def _():
                                line(a, way, k + 1).start()
                    else:
                        for half in range(2):
                            plane(a, way, k, half, step - 1).wait_recv()
                    if step < n_steps:
                        for half in range(2):
                            plane(a, way, k, half, step).start()
    for keep in keeps:
        keep.wait()
    for way in ways:
        for k in range(n_shard - 1):
            @pl.when(goes(way, k))
            def _():
                row_line(way, k).wait_send()
    for a in range(n_arrays):
        for way in ways:
            for k in range(n_shard - 1):
                @pl.when(goes(way, k))
                def _():
                    line(a, way, k).wait_send()

                @pl.when(comes(way, k))
                def _():
                    for half in range(2):
                        for step in range(n_steps):
                            plane(a, way, k, half, step).wait_send()


def gather_all(blocks, row, n_rep, n_shard, collective_id):
    n_bits = n_rep.bit_length() - 1
    n = len(blocks)
    shaped = [b.reshape((2,) * n_bits + (b.shape[0] // n_rep, b.shape[1])) for b in blocks]
    steps = max(n_shard - 1, 1)
    out = pl.pallas_call(
        functools.partial(gather_kernel, n_rep, n_shard, n),
        out_shape=[jax.ShapeDtypeStruct((n_shard,) + s.shape, s.dtype) for s in shaped]
        + [jax.ShapeDtypeStruct((n_shard, 1) + row.shape, row.dtype)],
        in_specs=[pl.BlockSpec(memory_space=pltpu.VMEM)] * (n + 1),
        out_specs=[pl.BlockSpec(memory_space=pl.ANY)] * n + [pl.BlockSpec(memory_space=pltpu.VMEM)],
        scratch_shapes=[
            pltpu.SemaphoreType.DMA((n,)),
            pltpu.SemaphoreType.DMA((n, 2, steps)),
            pltpu.SemaphoreType.DMA((n, 2, steps)),
            pltpu.SemaphoreType.DMA((n, 2, steps, 2, n_bits)),
            pltpu.SemaphoreType.DMA((n, 2, steps, 2, n_bits)),
            pltpu.SemaphoreType.DMA((2, steps)),
            pltpu.SemaphoreType.DMA((2, steps)),
        ],
        compiler_params=pltpu.CompilerParams(collective_id=collective_id, has_side_effects=True),
        name="gather_all",
    )(*shaped, row[None])
    return [o.reshape(n_shard * b.shape[0], b.shape[1]) for o, b in zip(out, blocks)] + [out[n].reshape(-1)]


F32 = jnp.float32


class Sems:
    def __init__(self, send, recv):
        self.send, self.recv, self.names = send, recv, {}

    def pair(self, *name):
        i = self.names.setdefault(name, len(self.names))
        return self.send.at[i], self.recv.at[i]


def reduce_kernel(n_rep, n_shard, decay, n_sems, *refs):
    parts, gain, moments = refs[0:2], refs[2], refs[3:5]
    sums, wholes, gain_out = refs[5:7], refs[7:9], refs[9]
    rest = list(refs[10:])
    nb = n_rep.bit_length() - 1
    bufs = [[rest.pop(0) for _ in range(nb)] for _ in range(2)]
    zbuf = [rest.pop(0) for _ in range(2)]
    gpiece = [rest.pop(0) for _ in range(2)]
    mpiece = [rest.pop(0) for _ in range(2)]
    gacc, gcome, gz = rest.pop(0), rest.pop(0), rest.pop(0)
    keep_sem = rest.pop(0)
    sems = Sems(rest.pop(0), rest.pop(0))
    links = Links(n_rep, n_shard)
    me = links.shard
    links.barrier(False)

    def remote(src, dst, name, rep, shard):
        send, recv = sems.pair(*name)
        return pltpu.make_async_remote_copy(src, dst, send, recv, device_id=(rep, shard), device_id_type=MESH)

    def dest(k):
        return lax.rem(me + 1 + k, n_shard)

    def order(half):
        return [0] + links.orders[half]

    def pick(half, step, bit_value, fixed_lead):
        o = order(half)
        remaining = sorted(o[step:], reverse=True)
        return fixed_lead + tuple(bit_value if b == o[step] else slice(None) for b in remaining)

    def send_reduce(a, k, half, step):
        d, o = dest(k), order(half)
        bit = o[step]
        src = parts[a] if step == 0 else bufs[a][step - 1]
        cols = slice(None) if step == 0 else halves(parts[a])[half]
        view = src.at[pick(half, step, 1 - links.bits[bit], (d,)) + (slice(None), cols)]
        into = bufs[a][step].at[(d,) + (slice(None),) * (nb - step) + (cols,)]
        return remote(view, into, ("r", a, k, half, step), links.flip(bit), me)

    def add_reduce(a, k, half, step):
        d, o = dest(k), order(half)
        src = parts[a] if step == 0 else bufs[a][step - 1]
        n_left = nb - 1 - step
        cols = slice(None) if step == 0 else halves(parts[a])[half]
        mine = links.bits[o[step]]
        remaining = sorted(o[step:], reverse=True)

        def one(i, c):
            left = {}
            rest_bits = [b for b in remaining if b != o[step]]
            for pos, b in enumerate(rest_bits):
                left[b] = lax.rem(lax.div(i, 1 << (len(rest_bits) - 1 - pos)), 2)
            here = tuple(left[b] for b in rest_bits)
            there = tuple(mine if b == o[step] else left[b] for b in remaining)
            x = src[(d,) + there + (slice(None), cols)].astype(F32)
            y = bufs[a][step][(d,) + here + (slice(None), cols)].astype(F32)
            bufs[a][step][(d,) + here + (slice(None), cols)] = (x + y).astype(jnp.bfloat16)
            return c

        if n_left == 0:
            one(0, 0)
        else:
            lax.fori_loop(0, 1 << n_left, one, 0)

    def send_line(a, k):
        d = dest(k)
        return remote(bufs[a][nb - 1].at[d], zbuf[a].at[me], ("z", a, k), links.rep, d)

    def wait_line(a, k):
        q = lax.rem(me + n_shard - 1 - k, n_shard)
        return remote(zbuf[a].at[q], zbuf[a].at[q], ("z", a, k), links.rep, me)

    for a in (1, 0):
        for k in range(n_shard):
            send_reduce(a, k, 0, 0).start()

    def gain_send(b):
        return remote(gacc, gcome.at[b], ("gain", b), links.flip(b), me)

    def gain_line(k):
        d = dest(k)
        return remote(gacc.at[d], gz.at[me], ("gainz", k), links.rep, d)

    gacc[...] = gain[...]
    gain_send(0).start()

    def gain_step(b):
        gain_send(b).wait()
        gacc[...] = gacc[...] + gcome[b]
        if b + 1 < nb:
            gain_send(b + 1).start()
        else:
            for k in range(n_shard - 1):
                gain_line(k).start()

    def gain_end():
        acc = gacc[me]
        for k in range(n_shard - 1):
            gain_line(k).wait_send()
            q = lax.rem(me + n_shard - 1 - k, n_shard)
            remote(gz.at[q], gz.at[q], ("gainz", k), links.rep, me).wait_recv()
        for q in range(n_shard):
            acc = jnp.where(me == q, acc, acc + gz[q])
        gain_out[...] = acc

    here = links.where({})

    def g_step(a, half, step):
        o = links.orders[half] + [0]
        bit, done = o[step], o[:step]
        cols = halves(parts[a])[half]
        into = sums[a].at[links.where({}, done) + (slice(None), cols)]
        src = gpiece[a].at[:, cols] if step == 0 else into
        return remote(src, into, ("g", a, half, step), links.flip(bit), me)

    def keep(a, i):
        return pltpu.make_async_copy(gpiece[a], sums[a].at[here], keep_sem.at[a])

    def line(a, way, k):
        q = me - way * k
        at = wholes[a].at[(q,) + here]
        src = mpiece[a] if k == 0 else at
        return remote(src, at, ("l", a, way, k), links.rep, me + way)

    def came(a, way, k):
        at = wholes[a].at[(me - way * (k + 1),) + here]
        return remote(at, at, ("l", a, way, k), links.rep, me)

    def goes(way, k):
        q, there = me - way * k, me + way
        return (q >= 0) & (q < n_shard) & (there >= 0) & (there < n_shard)

    def comes(way, k):
        q = me - way * (k + 1)
        return (q >= 0) & (q < n_shard)

    def plane(a, way, k, half, step):
        o = links.orders[half] + [0]
        bit, done = o[step], o[:step]
        view = wholes[a].at[(me - way * (k + 1),) + links.where({}, done) + (slice(None), halves(parts[a])[half])]
        return remote(view, view, ("p", a, way, k, half, step), links.flip(bit), me)

    ways = (1, -1)

    def finish(a):
        for k in range(n_shard - 1):
            wait_line(a, k).wait_recv()
        acc = bufs[a][nb - 1][me].astype(F32)
        for k in range(n_shard - 1):
            acc = acc + zbuf[a][lax.rem(me + n_shard - 1 - k, n_shard)].astype(F32)
        g = acc.astype(jnp.bfloat16)
        gpiece[a][...] = g
        mpiece[a][...] = (decay * moments[a][...] + g.astype(F32)).astype(jnp.bfloat16)
        for way in ways:
            @pl.when(goes(way, 0))
            def _():
                line(a, way, 0).start()
        for half in range(2):
            g_step(a, half, 0).start()
        keep(a, 0).start()

    def gather_event(a, i, step):
        if i == 0:
            if step == 0:
                keep(a, 0).wait()
            if step < nb:
                for half in range(2):
                    g_step(a, half, step).wait_recv()
                    if step + 1 < nb:
                        g_step(a, half, step + 1).start()
            return
        k = i - 1
        for way in ways:
            @pl.when(comes(way, k))
            def _():
                if step == 0:
                    came(a, way, k).wait_recv()
                    if k + 1 < n_shard - 1:
                        @pl.when(goes(way, k + 1))
                        def _():
                            line(a, way, k + 1).start()
                else:
                    for half in range(2):
                        plane(a, way, k, half, step - 1).wait_recv()
                if step < nb:
                    for half in range(2):
                        plane(a, way, k, half, step).start()

    def reduce_event(a, k, step):
        for half in range(1 if step == 0 else 2):
            send_reduce(a, k, half, step).wait_recv()
            add_reduce(a, k, half, step)
            if step == 0 and nb > 1:
                send_reduce(a, k, 0, 1).start()
                send_reduce(a, k, 1, 1).start()
            elif step + 1 < nb:
                send_reduce(a, k, half, step + 1).start()
        if step == nb - 1 and k < n_shard - 1:
            send_line(a, k).start()

    events = []
    chunks = [(a, k) for a in (1, 0) for k in range(n_shard)]
    for t in range(len(chunks) + nb):
        if t < nb:
            events.append(functools.partial(gain_step, t))
        for step in reversed(range(nb)):
            i = t - step
            if 0 <= i < len(chunks):
                events.append(functools.partial(reduce_event, *chunks[i], step))
        if t == n_shard + nb:
            events.append(functools.partial(finish, 1))
            events.append(gain_end)
        i = t - n_shard - nb - 1
        if i >= 0:
            for j in range(n_shard):
                step = i - j
                if 0 <= step <= nb:
                    events.append(functools.partial(gather_event, 1, j, step))
    done_t = len(chunks) + nb - n_shard - nb - 1
    events.append(functools.partial(finish, 0))
    for t in range(n_shard + nb + 1):
        for a in (1, 0):
            i = t + (done_t if a == 1 else 0)
            for j in range(n_shard):
                step = i - j
                if 0 <= step <= nb:
                    events.append(functools.partial(gather_event, a, j, step))
    for event in events:
        event()

    for a in (1, 0):
        for k in range(n_shard):
            for step in range(nb):
                for half in range(1 if step == 0 else 2):
                    send_reduce(a, k, half, step).wait_send()
            if k < n_shard - 1:
                send_line(a, k).wait_send()
        for half in range(2):
            for step in range(nb):
                g_step(a, half, step).wait_send()
        for way in ways:
            for k in range(n_shard - 1):
                @pl.when(goes(way, k))
                def _():
                    line(a, way, k).wait_send()

                @pl.when(comes(way, k))
                def _():
                    for half in range(2):
                        for step in range(nb):
                            plane(a, way, k, half, step).wait_send()
    assert len(sems.names) <= n_sems, len(sems.names)


def reduce_and_gather(parts, gain_part, moment_pieces, decay, n_rep, n_shard, collective_id):
    nb = n_rep.bit_length() - 1
    bits = (2,) * nb
    b16 = jnp.bfloat16
    shaped = [p.reshape((n_shard,) + bits + (p.shape[0] // n_shard // n_rep, p.shape[1])) for p in parts]
    pieces = [s.shape[-2:] for s in shaped]
    own = gain_part.shape[0] // n_shard
    gain3 = gain_part.reshape(n_shard, 1, own)
    vmem, any_ = pl.BlockSpec(memory_space=pltpu.VMEM), pl.BlockSpec(memory_space=pl.ANY)
    scratch = []
    for p in pieces:
        for j in range(nb):
            scratch.append(pltpu.VMEM((n_shard,) + (2,) * (nb - 1 - j) + p, b16))
    scratch += [pltpu.VMEM((n_shard,) + p, b16) for p in pieces]
    scratch += [pltpu.VMEM(p, b16) for p in pieces] * 2
    scratch += [pltpu.VMEM(gain3.shape, F32), pltpu.VMEM((nb,) + gain3.shape, F32), pltpu.VMEM(gain3.shape, F32)]
    n_sems = 2 * (n_shard * (1 + 2 * (nb - 1)) + (n_shard - 1) + 2 * nb + 2 * (n_shard - 1) * (1 + 2 * nb)) + nb + n_shard
    scratch += [pltpu.SemaphoreType.DMA((2,)), pltpu.SemaphoreType.DMA((n_sems,)), pltpu.SemaphoreType.DMA((n_sems,))]
    out = pl.pallas_call(
        functools.partial(reduce_kernel, n_rep, n_shard, decay, n_sems),
        out_shape=[jax.ShapeDtypeStruct(bits + p, b16) for p in pieces]
        + [jax.ShapeDtypeStruct(s.shape, b16) for s in shaped]
        + [jax.ShapeDtypeStruct((1, own), F32)],
        in_specs=[vmem] * 5,
        out_specs=[any_] * 4 + [vmem],
        scratch_shapes=scratch,
        compiler_params=pltpu.CompilerParams(
            collective_id=collective_id, has_side_effects=True, vmem_limit_bytes=60 << 20
        ),
        name="reduce_and_gather",
    )(*shaped, gain3, *moment_pieces)
    g = [o.reshape(n_rep * p[0], p[1]) for o, p in zip(out[:2], pieces)]
    m = [o.reshape(q.shape) for o, q in zip(out[2:4], parts)]
    return g, m, out[4].reshape(own)


coef_a = 3.4445
coef_b = -4.775
coef_c = 2.0315
SWEEPS = 5


def nt(left, right):
    return lax.dot_general(left, right, (((1,), (1,)), ((), ())), preferred_element_type=jnp.float32)


def tn(left, right):
    return lax.dot_general(left, right, (((0,), (0,)), ((), ())), preferred_element_type=jnp.float32)


def mm(left, right):
    return jnp.dot(left, right, preferred_element_type=jnp.float32)


def eye(n):
    return lax.broadcasted_iota(jnp.int32, (n, n), 0) == lax.broadcasted_iota(jnp.int32, (n, n), 1)


def total(x):
    return jnp.sum(jnp.sum(x, axis=1, keepdims=True), axis=0, keepdims=True)


class Iterate:
    def __init__(self, e, ebf, k, kbf, h, hbf, fbf, tile, rows):
        self.e, self.ebf, self.k, self.kbf, self.h, self.hbf, self.fbf = e, ebf, k, kbf, h, hbf, fbf
        self.n = e.shape[0]
        self.tile = min(tile, self.n)
        self.rows = min(rows, self.n)

    def blocks(self, body):
        nr, nc = self.n // self.rows, self.n // self.tile

        def one(i, carry):
            j, r = lax.div(i, nr), lax.rem(i, nr)
            body(pl.ds(pl.multiple_of(r * self.rows, self.rows), self.rows),
                 pl.ds(pl.multiple_of(j * self.tile, self.tile), self.tile))
            return carry

        if nr * nc == 1:
            one(0, 0)
        else:
            lax.fori_loop(0, nr * nc, one, 0)

    def diagonals(self, body, init):
        def one(i, carry):
            d = pl.ds(pl.multiple_of(i * self.tile, self.tile), self.tile)
            return body(d, carry)

        if self.n == self.tile:
            return one(0, init)
        return lax.fori_loop(0, self.n // self.tile, one, init)

    def trace(self, ref):
        mask = eye(self.tile)
        zero = jnp.zeros((1, 1), jnp.float32)
        return self.diagonals(lambda d, c: c + total(jnp.where(mask, ref[d, d], 0.0)), zero)

    def centre(self, s):
        shift = self.trace(self.e) * (1.0 / self.n)
        mask = eye(self.tile)

        def one(d, c):
            moved = self.e[d, d] - jnp.where(mask, shift, 0.0)
            self.e[d, d] = moved
            self.ebf[d, d] = moved.astype(jnp.bfloat16)
            return c

        self.diagonals(one, 0)
        return s + shift

    def start(self, gram):
        def block(r, c):
            self.e[r, c] = gram(r, c)

        self.blocks(block)
        norm = jnp.sqrt(self.trace(self.e)) + 1e-06
        scale = 1.0 / (norm * norm)

        def scaled(r, c):
            x = self.e[r, c] * scale
            self.e[r, c] = x
            self.ebf[r, c] = x.astype(jnp.bfloat16)

        self.blocks(scaled)
        return self.centre(jnp.zeros((1, 1), jnp.float32)), 1.0 / norm

    def polynomial(self, s):
        p0 = coef_a + s * (coef_b + coef_c * s)
        p1 = coef_b + 2.0 * coef_c * s

        def block(r, c):
            f = p1 * self.e[r, c] + coef_c * mm(self.ebf[r, :], self.ebf[:, c])
            self.fbf[r, c] = f.astype(jnp.bfloat16)

        self.blocks(block)
        return p0

    def first(self):
        def block(r, c):
            f = self.fbf[r, c]
            self.h[r, c] = f.astype(jnp.float32)
            self.hbf[r, c] = f

        self.blocks(block)

    def grow(self, p0, q):
        def block(r, c):
            new = p0 * self.h[r, c] + q * self.fbf[r, c].astype(jnp.float32) + mm(self.fbf[r, :], self.hbf[:, c])
            self.k[r, c] = new

        self.blocks(block)

        def back(r, c):
            new = self.k[r, c]
            self.h[r, c] = new
            self.hbf[r, c] = new.astype(jnp.bfloat16)

        self.blocks(back)

    def advance(self, p0, s):
        def inner(r, c):
            new = p0 * self.e[r, c] + s * self.fbf[r, c].astype(jnp.float32) + mm(self.fbf[r, :], self.ebf[:, c])
            self.k[r, c] = new
            self.kbf[r, c] = new.astype(jnp.bfloat16)

        self.blocks(inner)
        beta = p0 * s

        def outer(r, c):
            new = p0 * self.k[r, c] + beta * self.fbf[r, c].astype(jnp.float32) + mm(self.fbf[r, :], self.kbf[:, c])
            self.e[r, c] = new
            self.ebf[r, c] = new.astype(jnp.bfloat16)

        self.blocks(outer)
        return self.centre(p0 * beta)


def muon_kernel(wide, m_in, m_out, h_out, hs_out, scal, x, *scratch):
    big = Iterate(*scratch[:7], tile=256, rows=512)
    small = Iterate(*scratch[7:], tile=256, rows=256)
    core = lax.rem(lax.axis_index("rep"), 2)
    n, ns = big.n, small.n

    @pl.when(core == 0)
    def _():
        def turn(i, c):
            r = pl.ds(pl.multiple_of(i * 256, 256), 256)
            x[:, r] = m_in[r, pl.ds(0, n)].T
            return c

        lax.fori_loop(0, wide // 256, turn, 0)

    @pl.when(core != 0)
    def _():
        def take(i, c):
            r = pl.ds(pl.multiple_of(i * 128, 128), 128)
            x[r, :] = m_out[r, :]
            return c

        lax.fori_loop(0, n // 128, take, 0)

    s, inv = big.start(lambda r, c: nt(x[r, :], x[c, :]))
    mine = m_in.at[:, pl.ds(pl.multiple_of(n + core * ns, 128), ns)]
    ss, sinv = small.start(lambda r, c: tn(mine[:, r], mine[:, c]))

    def sweep(it, carry):
        s, q, ss, sq = carry
        p0, sp0 = big.polynomial(s), small.polynomial(ss)

        @pl.when(it == 0)
        def _():
            big.first()
            small.first()

        @pl.when(it > 0)
        def _():
            big.grow(p0, q)
            small.grow(sp0, sq)

        q, sq = p0 * q, sp0 * sq
        s, ss = lax.cond(
            it < SWEEPS - 1,
            lambda: (big.advance(p0, s), small.advance(sp0, ss)),
            lambda: (s, ss),
        )
        return s, q, ss, sq

    one = jnp.ones((1, 1), jnp.float32)
    s, q, ss, sq = lax.fori_loop(0, SWEEPS, sweep, (s, one, ss, one))
    h_out[...] = big.hbf[...]
    hs_out[...] = small.hbf[...]
    row = lax.broadcasted_iota(jnp.int32, (8, 128), 0)
    scal[...] = jnp.where(row == 0, q * inv, jnp.where(row == 1, inv, jnp.where(row == 2, sq * sinv, sinv)))


def muon(m_in, m_out, kv):
    wide, n = m_in.shape[0], m_out.shape[0]
    sets = []
    for d in (n, kv):
        f32, b16 = pltpu.VMEM((d, d), jnp.float32), pltpu.VMEM((d, d), jnp.bfloat16)
        sets += [f32, b16, f32, b16, f32, b16, b16]
    vmem = pl.BlockSpec(memory_space=pltpu.VMEM)
    return pl.pallas_call(
        functools.partial(muon_kernel, wide),
        out_shape=[
            jax.ShapeDtypeStruct((n, n), jnp.bfloat16),
            jax.ShapeDtypeStruct((kv, kv), jnp.bfloat16),
            jax.ShapeDtypeStruct((8, 128), jnp.float32),
        ],
        in_specs=[vmem] * 2,
        out_specs=[vmem] * 3,
        scratch_shapes=[pltpu.VMEM((n, wide), jnp.bfloat16)] + sets,
        compiler_params=pltpu.CompilerParams(vmem_limit_bytes=60 << 20),
        name="muon",
    )(m_in, m_out)


HEAD_SIZE = 64

norm_eps = 1e-05
rope_base = 500000.0
decay = 0.95
muon_rate = 0.02
gain_rate = 0.2


def positions_of(seq_segments):
    sequence_length = seq_segments.shape[0]
    token_index = jnp.arange(sequence_length, dtype=jnp.int32)
    before = jnp.concatenate([seq_segments[:1] - 1, seq_segments[:-1]])
    starts = jnp.where(seq_segments != before, token_index, jnp.zeros_like(token_index))
    return token_index - lax.cummax(starts, axis=0)


def rope_tables(seq_segments, head_dim):
    position = positions_of(seq_segments).astype(jnp.float32)
    half_dim = head_dim // 2
    frequency = rope_base ** (-2.0 * jnp.arange(half_dim, dtype=jnp.float32) / head_dim)
    angles = position[:, None] * frequency[None, :]
    return (jnp.cos(angles)[:, None, :], jnp.sin(angles)[:, None, :])


def apply_rotary(values, cosine_table, sine_table):
    half_dim = values.shape[-1] // 2
    front_half = values[..., :half_dim]
    back_half = values[..., half_dim:]
    return jnp.concatenate(
        [
            front_half * cosine_table - back_half * sine_table,
            back_half * cosine_table + front_half * sine_table,
        ],
        -1,
    )


def contract_rows(left, right, dtype=jnp.float32):
    return lax.dot_general(left, right, (((0,), (0,)), ((), ())), preferred_element_type=jnp.float32).astype(dtype)


def contract_cols(left, right):
    return lax.dot_general(left, right, (((1,), (1,)), ((), ())), preferred_element_type=jnp.float32)


def head_forward(q_head, k_head, v_head, allowed, score_scale):
    scores = jnp.einsum("qgd,kd->gqk", q_head, k_head, preferred_element_type=jnp.float32) * score_scale
    exponent = jnp.where(allowed[None], jnp.exp(scores), jnp.zeros_like(scores))
    denom_sum = jnp.sum(exponent, -1, keepdims=True)
    probabilities = (exponent / denom_sum).astype(jnp.bfloat16)
    attended = jnp.einsum("gqk,kd->qgd", probabilities, v_head, preferred_element_type=jnp.float32)
    return (attended, jnp.log(denom_sum))


def head_backward(q_head, k_head, v_head, log_sum, grad_head, allowed, score_scale):
    scores = jnp.einsum("qgd,kd->gqk", q_head, k_head, preferred_element_type=jnp.float32) * score_scale
    recomputed = jnp.where(allowed[None], jnp.exp(scores - log_sum), jnp.zeros_like(scores))
    rounded = recomputed.astype(jnp.bfloat16)
    value_grad = jnp.einsum("gqk,qgd->kd", rounded, grad_head, preferred_element_type=jnp.float32)
    prob_grad = jnp.einsum("qgd,kd->gqk", grad_head, v_head, preferred_element_type=jnp.float32)
    row_inner = jnp.sum(recomputed * prob_grad, -1, keepdims=True)
    score_grad = (recomputed * (prob_grad - row_inner) * score_scale).astype(jnp.bfloat16)
    query_grad = jnp.einsum("gqk,kd->qgd", score_grad, k_head, preferred_element_type=jnp.float32)
    key_grad = jnp.einsum("gqk,qgd->kd", score_grad, q_head, preferred_element_type=jnp.float32)
    return (query_grad, key_grad, value_grad)


def attention(query_rows, rotated_keys, values_bfloat, dattn_of, allowed, score_scale):
    sequence_length, query_heads = query_rows.shape[:2]
    kv_heads = rotated_keys.shape[1]
    group_width = query_heads // kv_heads
    query_width = query_heads * HEAD_SIZE
    query_head_rows = query_rows.reshape(sequence_length, kv_heads, group_width, HEAD_SIZE).transpose(1, 0, 2, 3)
    k_heads = rotated_keys.transpose(1, 0, 2)
    v_heads = values_bfloat.transpose(1, 0, 2)
    attended, log_sum = lax.map(
        lambda blocks: head_forward(blocks[0], blocks[1], blocks[2], allowed, score_scale),
        (query_head_rows, k_heads, v_heads),
    )
    attn_bf = attended.transpose(1, 0, 2, 3).reshape(sequence_length, query_width).astype(jnp.bfloat16)
    head_gradients = dattn_of().reshape(sequence_length, kv_heads, group_width, HEAD_SIZE).transpose(1, 0, 2, 3)
    query_grad, key_grad, value_grad = lax.map(
        lambda blocks: head_backward(blocks[0], blocks[1], blocks[2], blocks[3], blocks[4], allowed, score_scale),
        (query_head_rows, k_heads, v_heads, log_sum, head_gradients),
    )
    return (
        attn_bf,
        query_grad.transpose(1, 0, 2, 3).reshape(sequence_length, query_heads, HEAD_SIZE),
        key_grad.transpose(1, 0, 2),
        value_grad.transpose(1, 0, 2),
    )


def rows_of(matrix, index, count):
    return lax.dynamic_slice_in_dim(matrix, index * count, count, 0)


def cols_of(matrix, index, count):
    return lax.dynamic_slice_in_dim(matrix, index * count, count, 1)


def on_device(
    tokens,
    segments,
    cotangent,
    gain,
    w_query,
    w_key,
    w_value,
    w_outproj,
    moment_gain,
    moment_query,
    moment_key,
    moment_value,
    moment_outproj,
):
    n_rep = lax.axis_size("rep")
    n_shard = lax.axis_size("shard")
    rep_index = lax.axis_index("rep")
    shard_index = lax.axis_index("shard")
    sequence_length = tokens.shape[1]
    query_width = w_query.shape[1]
    kv_width = w_key.shape[1]
    query_heads = query_width // HEAD_SIZE
    kv_heads = kv_width // HEAD_SIZE
    score_scale = 1.0 / math.sqrt(HEAD_SIZE)
    total_tokens = tokens.shape[0] * sequence_length * n_rep * n_shard
    seq_tokens = tokens[0]
    seq_segments = segments[0]
    seq_cotangent = cotangent[0]
    b16, f32 = jnp.bfloat16, jnp.float32
    w_in_bf = jnp.concatenate([w_query, w_key, w_value], 1).astype(b16)
    w_out_bf = w_outproj.astype(b16)
    w_in_all, w_out_all, gain_all = gather_all(
        [w_in_bf, w_out_bf], gain.astype(b16).astype(f32), n_rep, n_shard, 0
    )
    tok_float = seq_tokens.astype(f32)
    inv_rms = lax.rsqrt(jnp.mean(tok_float * tok_float, -1, keepdims=True) + norm_eps)
    normed = tok_float * inv_rms
    norm_bf = (normed * gain_all).astype(b16)
    projected_rows = jnp.dot(norm_bf, w_in_all, preferred_element_type=f32)
    cosine_table, sine_table = rope_tables(seq_segments, HEAD_SIZE)
    query_rows = apply_rotary(
        projected_rows[:, :query_width].reshape(sequence_length, query_heads, HEAD_SIZE), cosine_table, sine_table
    ).astype(b16)
    rotated_keys = apply_rotary(
        projected_rows[:, query_width : query_width + kv_width].reshape(sequence_length, kv_heads, HEAD_SIZE),
        cosine_table,
        sine_table,
    ).astype(b16)
    values_bfloat = projected_rows[:, query_width + kv_width :].reshape(sequence_length, kv_heads, HEAD_SIZE).astype(b16)
    token_index = jnp.arange(sequence_length, dtype=jnp.int32)
    allowed = (token_index[None, :] <= token_index[:, None]) & (seq_segments[None, :] == seq_segments[:, None])
    attn_bf, query_grad, key_grad, value_grad = attention(
        query_rows,
        rotated_keys,
        values_bfloat,
        lambda: contract_cols(seq_cotangent, w_out_all).astype(b16),
        allowed,
        score_scale,
    )
    branch_out = jnp.dot(attn_bf, w_out_all, preferred_element_type=f32)
    result = (tok_float + branch_out).astype(b16)
    part_outproj = contract_rows(attn_bf, seq_cotangent, b16)
    grad_qkv = jnp.concatenate(
        [
            apply_rotary(query_grad, cosine_table, -sine_table).reshape(sequence_length, query_width),
            apply_rotary(key_grad, cosine_table, -sine_table).reshape(sequence_length, kv_width),
            value_grad.reshape(sequence_length, kv_width),
        ],
        1,
    ).astype(b16)
    part_in = contract_rows(norm_bf, grad_qkv, b16)
    grad_normed = contract_cols(grad_qkv, w_in_all)
    part_gain = jnp.sum(grad_normed * normed, 0)
    grad_hat = grad_normed * gain_all
    grad_tokens = (
        seq_cotangent.astype(f32) + inv_rms * (grad_hat - normed * jnp.mean(grad_hat * normed, -1, keepdims=True))
    ).astype(b16)
    return finish(
        result, grad_tokens, part_in, part_outproj, part_gain, total_tokens, gain, (w_query, w_key, w_value, w_outproj),
        moment_gain, (moment_query, moment_key, moment_value, moment_outproj),
    )


def finish(result, grad_tokens, part_in, part_outproj, part_gain, total_tokens, gain, weights, moment_gain, moments):
    n_rep, n_shard = lax.axis_size("rep"), lax.axis_size("shard")
    rep_index, shard_index = lax.axis_index("rep"), lax.axis_index("shard")
    b16, f32 = jnp.bfloat16, jnp.float32
    w_query, w_key, w_value, w_outproj = weights
    query_width, kv_width = w_query.shape[1], w_key.shape[1]
    in_piece = jnp.concatenate([rows_of(m, rep_index, m.shape[0] // n_rep) for m in moments[:3]], 1)
    out_piece = rows_of(moments[3], rep_index, moments[3].shape[0] // n_rep)
    (sum_in, sum_out), (m_in, m_out), grad_gain = reduce_and_gather(
        [part_in, part_outproj], part_gain, [in_piece, out_piece], decay, n_rep, n_shard, 1
    )
    grads = [
        sum_in[:, :query_width].astype(f32),
        sum_in[:, query_width : query_width + kv_width].astype(f32),
        sum_in[:, query_width + kv_width :].astype(f32),
        sum_out.astype(f32),
    ]
    moments_next = [decay * m + g for m, g in zip(moments, grads)]
    moment_gain_next = decay * moment_gain + grad_gain
    gain_next = gain - gain_rate / math.sqrt(total_tokens) * moment_gain_next
    own_in = jnp.concatenate([m.astype(b16) for m in moments_next[:3]], 1)
    own_out = moments_next[3].astype(b16)
    m_in = lax.dynamic_update_slice_in_dim(m_in, own_in, shard_index * own_in.shape[0], 0)
    m_out = lax.dynamic_update_slice_in_dim(m_out, own_out, shard_index * own_out.shape[0], 0)
    mix, mix_kv, scales = muon(m_in, m_out, kv_width)
    core = lax.rem(rep_index, 2)
    other = rep_index + 1 - 2 * core
    widths = [w.shape[1] // n_rep for w in weights]
    pairs = [(i, i ^ 1) for i in range(n_rep)]
    out_rows = w_outproj.shape[0]
    theirs = lax.ppermute(
        (
            rows_of(mix, other, widths[0]),
            rows_of(mix, shard_index, out_rows),
            rows_of(mix_kv, other, widths[1]),
            scales,
        ),
        "rep",
        pairs,
    )
    even = core == 0
    mix_query = jnp.where(even, rows_of(mix, rep_index, widths[0]), theirs[0])
    mix_out = jnp.where(even, theirs[1], rows_of(mix, shard_index, out_rows))
    kv_mine = rows_of(mix_kv, rep_index, widths[1])
    mix_key, mix_value = jnp.where(even, kv_mine, theirs[2]), jnp.where(even, theirs[2], kv_mine)
    first, second = jnp.where(even, scales, theirs[3]), jnp.where(even, theirs[3], scales)
    spans = (
        (0, query_width, mix_query, first[0, 0], first[1, 0]),
        (query_width, kv_width, mix_key, first[2, 0], first[3, 0]),
        (query_width + kv_width, kv_width, mix_value, second[2, 0], second[3, 0]),
    )
    updated = []
    for i, (at, width, mix_rows, straight, mixed) in enumerate(spans):
        whole = (weights[i].shape[0] * n_shard, width)
        ortho = straight * cols_of(moments_next[i], rep_index, widths[i]) + mixed * contract_cols(
            own_in[:, at : at + width], mix_rows
        )
        updated.append(cols_of(weights[i], rep_index, widths[i]) - muon_rate * math.sqrt(max(whole)) * ortho)
    whole = (out_rows * n_shard, w_outproj.shape[1])
    ortho = second[0, 0] * cols_of(moments_next[3], rep_index, widths[3]) + second[1, 0] * jnp.dot(
        mix_out, cols_of(m_out, rep_index, widths[3]), preferred_element_type=f32
    )
    updated.append(cols_of(w_outproj, rep_index, widths[3]) - muon_rate * math.sqrt(max(whole)) * ortho)
    return (
        result[None],
        grad_tokens[None],
        grad_gain,
        *grads,
        gain_next,
        *updated,
        moment_gain_next,
        *moments_next,
    )


def solution(mesh):
    in_specs = (
        P(("rep", "shard"), None, None),
        P(("rep", "shard"), None),
        P(("rep", "shard"), None, None),
        P("shard"),
        P("shard", None),
        P("shard", None),
        P("shard", None),
        P("shard", None),
        P("shard"),
        P("shard", None),
        P("shard", None),
        P("shard", None),
        P("shard", None),
    )
    out_specs = (
        P(("rep", "shard"), None, None),
        P(("rep", "shard"), None, None),
        P("shard"),
        P("shard", None),
        P("shard", None),
        P("shard", None),
        P("shard", None),
        P("shard"),
        P("shard", "rep"),
        P("shard", "rep"),
        P("shard", "rep"),
        P("shard", "rep"),
        P("shard"),
        P("shard", None),
        P("shard", None),
        P("shard", None),
        P("shard", None),
    )
    return jax.shard_map(on_device, mesh=mesh, in_specs=in_specs, out_specs=out_specs, check_vma=False)
```

```python
import functools
import math

import jax
import jax.numpy as jnp
from jax import lax
from jax.experimental import pallas as pl
from jax.experimental.pallas import tpu as pltpu
from jax.sharding import PartitionSpec as P

MESH = pl.DeviceIdType.MESH


class Links:
    def __init__(self, n_rep, n_shard):
        self.n_bits = n_rep.bit_length() - 1
        self.n_shard = n_shard
        self.rep = lax.axis_index("rep")
        self.shard = lax.axis_index("shard")
        self.bits = [lax.rem(lax.div(self.rep, 1 << b), 2) for b in range(self.n_bits)]
        far = list(range(1, self.n_bits))
        self.orders = (far, far[::-1])

    def flip(self, bit):
        return self.rep + (1 << bit) * (1 - 2 * self.bits[bit])

    def barrier(self, line):
        sem = pltpu.get_barrier_semaphore()
        count = self.n_bits
        for b in range(self.n_bits):
            pl.semaphore_signal(sem, 1, device_id=(self.flip(b), self.shard), device_id_type=MESH)
        if line:
            for step in (-1, 1):
                there = self.shard + step
                inside = jnp.logical_and(there >= 0, there < self.n_shard)

                @pl.when(inside)
                def _():
                    pl.semaphore_signal(sem, 1, device_id=(self.rep, there), device_id_type=MESH)

                count = count + inside.astype(jnp.int32)
        else:
            for k in range(1, self.n_shard):
                there = lax.rem(self.shard + k, self.n_shard)
                pl.semaphore_signal(sem, 1, device_id=(self.rep, there), device_id_type=MESH)
            count = count + self.n_shard - 1
        pl.semaphore_wait(sem, count)

    def where(self, fixed, free=()):
        return tuple(
            slice(None) if b in free else fixed.get(b, self.bits[b])
            for b in reversed(range(self.n_bits))
        )


def halves(ref):
    cols = ref.shape[-1]
    return (pl.ds(0, cols // 2), pl.ds(cols // 2, cols // 2))


def spread(links, full, q, half, step, send, recv):
    order = links.orders[half] + [0]
    bit, done = order[step], order[:step]
    view = full.at[(q, *links.where({}, done), slice(None), halves(full)[half])]
    return pltpu.make_async_remote_copy(
        view, view, send, recv, device_id=(links.flip(bit), links.shard), device_id_type=MESH
    )


def gather_kernel(n_rep, n_shard, n_arrays, *refs):
    local, row = refs[:n_arrays], refs[n_arrays]
    full, row_full = refs[n_arrays + 1 : 2 * n_arrays + 1], refs[2 * n_arrays + 1]
    keep_sem, line_send, line_recv, plane_send, plane_recv, row_send, row_recv = refs[2 * n_arrays + 2 :]
    links = Links(n_rep, n_shard)
    me = links.shard
    links.barrier(True)
    row_full[me] = row[...]

    def row_line(way, k):
        q, side = me - way * k, (way + 1) // 2
        return pltpu.make_async_remote_copy(
            row if k == 0 else row_full.at[q], row_full.at[q], row_send.at[side, k], row_recv.at[side, k],
            device_id=(links.rep, me + way), device_id_type=MESH,
        )

    def row_came(way, k):
        here, side = row_full.at[me - way * (k + 1)], (way + 1) // 2
        return pltpu.make_async_remote_copy(
            here, here, row_send.at[side, k], row_recv.at[side, k], device_id=(links.rep, me), device_id_type=MESH
        )
    keeps = [pltpu.make_async_copy(local[a], full[a].at[me], keep_sem.at[a]) for a in range(n_arrays)]

    def line(a, way, k):
        q = me - way * k
        here = links.where({})
        src = local[a].at[here] if k == 0 else full[a].at[(q, *here)]
        side = (way + 1) // 2
        return pltpu.make_async_remote_copy(
            src, full[a].at[(q, *here)], line_send.at[a, side, k], line_recv.at[a, side, k],
            device_id=(links.rep, me + way), device_id_type=MESH,
        )

    def came(a, way, k):
        q = me - way * (k + 1)
        here = full[a].at[(q, *links.where({}))]
        side = (way + 1) // 2
        return pltpu.make_async_remote_copy(
            here, here, line_send.at[a, side, k], line_recv.at[a, side, k],
            device_id=(links.rep, me), device_id_type=MESH,
        )

    def goes(way, k):
        q, there = me - way * k, me + way
        return (q >= 0) & (q < n_shard) & (there >= 0) & (there < n_shard)

    def comes(way, k):
        q = me - way * (k + 1)
        return (q >= 0) & (q < n_shard)

    ways = (1, -1)
    n_steps = links.n_bits
    for way in ways:
        @pl.when(goes(way, 0))
        def _():
            row_line(way, 0).start()
    for a in range(n_arrays):
        for way in ways:
            @pl.when(goes(way, 0))
            def _():
                line(a, way, 0).start()
    for keep in keeps:
        keep.start()

    def plane(a, way, k, half, step):
        q = me - way * (k + 1)
        side = (way + 1) // 2
        return spread(links, full[a], q, half, step,
                      plane_send.at[a, side, k, half, step], plane_recv.at[a, side, k, half, step])

    items = [(a, k) for a in range(n_arrays) for k in range(n_shard - 1)]
    for t in range(len(items) + n_steps):
        for i, (a, k) in enumerate(items):
            step = t - i
            if step < 0 or step > n_steps:
                continue
            for way in ways:
                @pl.when(comes(way, k))
                def _():
                    if step == 0 and a == 0:
                        row_came(way, k).wait_recv()
                        if k + 1 < n_shard - 1:
                            @pl.when(goes(way, k + 1))
                            def _():
                                row_line(way, k + 1).start()
                    if step == 0:
                        came(a, way, k).wait_recv()
                        if k + 1 < n_shard - 1:
                            @pl.when(goes(way, k + 1))
                            def _():
                                line(a, way, k + 1).start()
                    else:
                        for half in range(2):
                            plane(a, way, k, half, step - 1).wait_recv()
                    if step < n_steps:
                        for half in range(2):
                            plane(a, way, k, half, step).start()
    for keep in keeps:
        keep.wait()
    for way in ways:
        for k in range(n_shard - 1):
            @pl.when(goes(way, k))
            def _():
                row_line(way, k).wait_send()
    for a in range(n_arrays):
        for way in ways:
            for k in range(n_shard - 1):
                @pl.when(goes(way, k))
                def _():
                    line(a, way, k).wait_send()

                @pl.when(comes(way, k))
                def _():
                    for half in range(2):
                        for step in range(n_steps):
                            plane(a, way, k, half, step).wait_send()


def gather_all(blocks, row, n_rep, n_shard, collective_id):
    n_bits = n_rep.bit_length() - 1
    n = len(blocks)
    shaped = [b.reshape((2,) * n_bits + (b.shape[0] // n_rep, b.shape[1])) for b in blocks]
    steps = max(n_shard - 1, 1)
    out = pl.pallas_call(
        functools.partial(gather_kernel, n_rep, n_shard, n),
        out_shape=[jax.ShapeDtypeStruct((n_shard,) + s.shape, s.dtype) for s in shaped]
        + [jax.ShapeDtypeStruct((n_shard, 1) + row.shape, row.dtype)],
        in_specs=[pl.BlockSpec(memory_space=pltpu.VMEM)] * (n + 1),
        out_specs=[pl.BlockSpec(memory_space=pl.ANY)] * n + [pl.BlockSpec(memory_space=pltpu.VMEM)],
        scratch_shapes=[
            pltpu.SemaphoreType.DMA((n,)),
            pltpu.SemaphoreType.DMA((n, 2, steps)),
            pltpu.SemaphoreType.DMA((n, 2, steps)),
            pltpu.SemaphoreType.DMA((n, 2, steps, 2, n_bits)),
            pltpu.SemaphoreType.DMA((n, 2, steps, 2, n_bits)),
            pltpu.SemaphoreType.DMA((2, steps)),
            pltpu.SemaphoreType.DMA((2, steps)),
        ],
        compiler_params=pltpu.CompilerParams(collective_id=collective_id, has_side_effects=True),
        name="gather_all",
    )(*shaped, row[None])
    return [o.reshape(n_shard * b.shape[0], b.shape[1]) for o, b in zip(out, blocks)] + [out[n].reshape(-1)]


F32 = jnp.float32


class Sems:
    def __init__(self, send, recv):
        self.send, self.recv, self.names = send, recv, {}

    def pair(self, *name):
        i = self.names.setdefault(name, len(self.names))
        return self.send.at[i], self.recv.at[i]


def reduce_kernel(n_rep, n_shard, decay, n_sems, *refs):
    parts, gain, moments = refs[0:2], refs[2], refs[3:5]
    sums, wholes, gain_out = refs[5:7], refs[7:9], refs[9]
    rest = list(refs[10:])
    nb = n_rep.bit_length() - 1
    bufs = [[rest.pop(0) for _ in range(nb)] for _ in range(2)]
    zbuf = [rest.pop(0) for _ in range(2)]
    gpiece = [rest.pop(0) for _ in range(2)]
    mpiece = [rest.pop(0) for _ in range(2)]
    gacc, gcome, gz = rest.pop(0), rest.pop(0), rest.pop(0)
    keep_sem = rest.pop(0)
    sems = Sems(rest.pop(0), rest.pop(0))
    links = Links(n_rep, n_shard)
    me = links.shard
    links.barrier(False)

    def remote(src, dst, name, rep, shard):
        send, recv = sems.pair(*name)
        return pltpu.make_async_remote_copy(src, dst, send, recv, device_id=(rep, shard), device_id_type=MESH)

    def dest(k):
        return lax.rem(me + 1 + k, n_shard)

    def order(half):
        return [0] + links.orders[half]

    def pick(half, step, bit_value, fixed_lead):
        o = order(half)
        remaining = sorted(o[step:], reverse=True)
        return fixed_lead + tuple(bit_value if b == o[step] else slice(None) for b in remaining)

    def send_reduce(a, k, half, step):
        d, o = dest(k), order(half)
        bit = o[step]
        src = parts[a] if step == 0 else bufs[a][step - 1]
        cols = slice(None) if step == 0 else halves(parts[a])[half]
        view = src.at[pick(half, step, 1 - links.bits[bit], (d,)) + (slice(None), cols)]
        into = bufs[a][step].at[(d,) + (slice(None),) * (nb - step) + (cols,)]
        return remote(view, into, ("r", a, k, half, step), links.flip(bit), me)

    def add_reduce(a, k, half, step):
        d, o = dest(k), order(half)
        src = parts[a] if step == 0 else bufs[a][step - 1]
        n_left = nb - 1 - step
        cols = slice(None) if step == 0 else halves(parts[a])[half]
        mine = links.bits[o[step]]
        remaining = sorted(o[step:], reverse=True)

        def one(i, c):
            left = {}
            rest_bits = [b for b in remaining if b != o[step]]
            for pos, b in enumerate(rest_bits):
                left[b] = lax.rem(lax.div(i, 1 << (len(rest_bits) - 1 - pos)), 2)
            here = tuple(left[b] for b in rest_bits)
            there = tuple(mine if b == o[step] else left[b] for b in remaining)
            x = src[(d,) + there + (slice(None), cols)].astype(F32)
            y = bufs[a][step][(d,) + here + (slice(None), cols)].astype(F32)
            bufs[a][step][(d,) + here + (slice(None), cols)] = (x + y).astype(jnp.bfloat16)
            return c

        if n_left == 0:
            one(0, 0)
        else:
            lax.fori_loop(0, 1 << n_left, one, 0)

    def send_line(a, k):
        d = dest(k)
        return remote(bufs[a][nb - 1].at[d], zbuf[a].at[me], ("z", a, k), links.rep, d)

    def wait_line(a, k):
        q = lax.rem(me + n_shard - 1 - k, n_shard)
        return remote(zbuf[a].at[q], zbuf[a].at[q], ("z", a, k), links.rep, me)

    for a in (1, 0):
        for k in range(n_shard):
            send_reduce(a, k, 0, 0).start()

    def gain_send(b):
        return remote(gacc, gcome.at[b], ("gain", b), links.flip(b), me)

    def gain_line(k):
        d = dest(k)
        return remote(gacc.at[d], gz.at[me], ("gainz", k), links.rep, d)

    gacc[...] = gain[...]
    gain_send(0).start()

    def gain_step(b):
        gain_send(b).wait()
        gacc[...] = gacc[...] + gcome[b]
        if b + 1 < nb:
            gain_send(b + 1).start()
        else:
            for k in range(n_shard - 1):
                gain_line(k).start()

    def gain_end():
        acc = gacc[me]
        for k in range(n_shard - 1):
            gain_line(k).wait_send()
            q = lax.rem(me + n_shard - 1 - k, n_shard)
            remote(gz.at[q], gz.at[q], ("gainz", k), links.rep, me).wait_recv()
        for q in range(n_shard):
            acc = jnp.where(me == q, acc, acc + gz[q])
        gain_out[...] = acc

    here = links.where({})

    def g_step(a, half, step):
        o = links.orders[half] + [0]
        bit, done = o[step], o[:step]
        cols = halves(parts[a])[half]
        into = sums[a].at[links.where({}, done) + (slice(None), cols)]
        src = gpiece[a].at[:, cols] if step == 0 else into
        return remote(src, into, ("g", a, half, step), links.flip(bit), me)

    def keep(a, i):
        return pltpu.make_async_copy(gpiece[a], sums[a].at[here], keep_sem.at[a])

    def line(a, way, k):
        q = me - way * k
        at = wholes[a].at[(q,) + here]
        src = mpiece[a] if k == 0 else at
        return remote(src, at, ("l", a, way, k), links.rep, me + way)

    def came(a, way, k):
        at = wholes[a].at[(me - way * (k + 1),) + here]
        return remote(at, at, ("l", a, way, k), links.rep, me)

    def goes(way, k):
        q, there = me - way * k, me + way
        return (q >= 0) & (q < n_shard) & (there >= 0) & (there < n_shard)

    def comes(way, k):
        q = me - way * (k + 1)
        return (q >= 0) & (q < n_shard)

    def plane(a, way, k, half, step):
        o = links.orders[half] + [0]
        bit, done = o[step], o[:step]
        view = wholes[a].at[(me - way * (k + 1),) + links.where({}, done) + (slice(None), halves(parts[a])[half])]
        return remote(view, view, ("p", a, way, k, half, step), links.flip(bit), me)

    ways = (1, -1)

    def finish(a):
        for k in range(n_shard - 1):
            wait_line(a, k).wait_recv()
        acc = bufs[a][nb - 1][me].astype(F32)
        for k in range(n_shard - 1):
            acc = acc + zbuf[a][lax.rem(me + n_shard - 1 - k, n_shard)].astype(F32)
        g = acc.astype(jnp.bfloat16)
        gpiece[a][...] = g
        mpiece[a][...] = (decay * moments[a][...] + g.astype(F32)).astype(jnp.bfloat16)
        for way in ways:
            @pl.when(goes(way, 0))
            def _():
                line(a, way, 0).start()
        for half in range(2):
            g_step(a, half, 0).start()
        keep(a, 0).start()

    def gather_event(a, i, step):
        if i == 0:
            if step == 0:
                keep(a, 0).wait()
            if step < nb:
                for half in range(2):
                    g_step(a, half, step).wait_recv()
                    if step + 1 < nb:
                        g_step(a, half, step + 1).start()
            return
        k = i - 1
        for way in ways:
            @pl.when(comes(way, k))
            def _():
                if step == 0:
                    came(a, way, k).wait_recv()
                    if k + 1 < n_shard - 1:
                        @pl.when(goes(way, k + 1))
                        def _():
                            line(a, way, k + 1).start()
                else:
                    for half in range(2):
                        plane(a, way, k, half, step - 1).wait_recv()
                if step < nb:
                    for half in range(2):
                        plane(a, way, k, half, step).start()

    def reduce_event(a, k, step):
        for half in range(1 if step == 0 else 2):
            send_reduce(a, k, half, step).wait_recv()
            add_reduce(a, k, half, step)
            if step == 0 and nb > 1:
                send_reduce(a, k, 0, 1).start()
                send_reduce(a, k, 1, 1).start()
            elif step + 1 < nb:
                send_reduce(a, k, half, step + 1).start()
        if step == nb - 1 and k < n_shard - 1:
            send_line(a, k).start()

    events = []
    chunks = [(a, k) for a in (1, 0) for k in range(n_shard)]
    for t in range(len(chunks) + nb):
        if t < nb:
            events.append(functools.partial(gain_step, t))
        for step in reversed(range(nb)):
            i = t - step
            if 0 <= i < len(chunks):
                events.append(functools.partial(reduce_event, *chunks[i], step))
        if t == n_shard + nb:
            events.append(functools.partial(finish, 1))
            events.append(gain_end)
        i = t - n_shard - nb - 1
        if i >= 0:
            for j in range(n_shard):
                step = i - j
                if 0 <= step <= nb:
                    events.append(functools.partial(gather_event, 1, j, step))
    done_t = len(chunks) + nb - n_shard - nb - 1
    events.append(functools.partial(finish, 0))
    for t in range(n_shard + nb + 1):
        for a in (1, 0):
            i = t + (done_t if a == 1 else 0)
            for j in range(n_shard):
                step = i - j
                if 0 <= step <= nb:
                    events.append(functools.partial(gather_event, a, j, step))
    for event in events:
        event()

    for a in (1, 0):
        for k in range(n_shard):
            for step in range(nb):
                for half in range(1 if step == 0 else 2):
                    send_reduce(a, k, half, step).wait_send()
            if k < n_shard - 1:
                send_line(a, k).wait_send()
        for half in range(2):
            for step in range(nb):
                g_step(a, half, step).wait_send()
        for way in ways:
            for k in range(n_shard - 1):
                @pl.when(goes(way, k))
                def _():
                    line(a, way, k).wait_send()

                @pl.when(comes(way, k))
                def _():
                    for half in range(2):
                        for step in range(nb):
                            plane(a, way, k, half, step).wait_send()
    assert len(sems.names) <= n_sems, len(sems.names)


def reduce_and_gather(parts, gain_part, moment_pieces, decay, n_rep, n_shard, collective_id):
    nb = n_rep.bit_length() - 1
    bits = (2,) * nb
    b16 = jnp.bfloat16
    shaped = [p.reshape((n_shard,) + bits + (p.shape[0] // n_shard // n_rep, p.shape[1])) for p in parts]
    pieces = [s.shape[-2:] for s in shaped]
    own = gain_part.shape[0] // n_shard
    gain3 = gain_part.reshape(n_shard, 1, own)
    vmem, any_ = pl.BlockSpec(memory_space=pltpu.VMEM), pl.BlockSpec(memory_space=pl.ANY)
    scratch = []
    for p in pieces:
        for j in range(nb):
            scratch.append(pltpu.VMEM((n_shard,) + (2,) * (nb - 1 - j) + p, b16))
    scratch += [pltpu.VMEM((n_shard,) + p, b16) for p in pieces]
    scratch += [pltpu.VMEM(p, b16) for p in pieces] * 2
    scratch += [pltpu.VMEM(gain3.shape, F32), pltpu.VMEM((nb,) + gain3.shape, F32), pltpu.VMEM(gain3.shape, F32)]
    n_sems = 2 * (n_shard * (1 + 2 * (nb - 1)) + (n_shard - 1) + 2 * nb + 2 * (n_shard - 1) * (1 + 2 * nb)) + nb + n_shard
    scratch += [pltpu.SemaphoreType.DMA((2,)), pltpu.SemaphoreType.DMA((n_sems,)), pltpu.SemaphoreType.DMA((n_sems,))]
    out = pl.pallas_call(
        functools.partial(reduce_kernel, n_rep, n_shard, decay, n_sems),
        out_shape=[jax.ShapeDtypeStruct(bits + p, b16) for p in pieces]
        + [jax.ShapeDtypeStruct(s.shape, b16) for s in shaped]
        + [jax.ShapeDtypeStruct((1, own), F32)],
        in_specs=[vmem] * 5,
        out_specs=[any_] * 4 + [vmem],
        scratch_shapes=scratch,
        compiler_params=pltpu.CompilerParams(
            collective_id=collective_id, has_side_effects=True, vmem_limit_bytes=60 << 20
        ),
        name="reduce_and_gather",
    )(*shaped, gain3, *moment_pieces)
    g = [o.reshape(n_rep * p[0], p[1]) for o, p in zip(out[:2], pieces)]
    m = [o.reshape(q.shape) for o, q in zip(out[2:4], parts)]
    return g, m, out[4].reshape(own)


coef_a = 3.4445
coef_b = -4.775
coef_c = 2.0315
SWEEPS = 5


def nt(left, right):
    return lax.dot_general(left, right, (((1,), (1,)), ((), ())), preferred_element_type=jnp.float32)


def tn(left, right):
    return lax.dot_general(left, right, (((0,), (0,)), ((), ())), preferred_element_type=jnp.float32)


def mm(left, right):
    return jnp.dot(left, right, preferred_element_type=jnp.float32)


def eye(n):
    return lax.broadcasted_iota(jnp.int32, (n, n), 0) == lax.broadcasted_iota(jnp.int32, (n, n), 1)


def total(x):
    return jnp.sum(jnp.sum(x, axis=1, keepdims=True), axis=0, keepdims=True)


class Iterate:
    def __init__(self, e, ebf, k, kbf, h, hbf, fbf, tile, rows):
        self.e, self.ebf, self.k, self.kbf, self.h, self.hbf, self.fbf = e, ebf, k, kbf, h, hbf, fbf
        self.n = e.shape[0]
        self.tile = min(tile, self.n)
        self.rows = min(rows, self.n)

    def blocks(self, body):
        nr, nc = self.n // self.rows, self.n // self.tile

        def one(i, carry):
            j, r = lax.div(i, nr), lax.rem(i, nr)
            body(pl.ds(pl.multiple_of(r * self.rows, self.rows), self.rows),
                 pl.ds(pl.multiple_of(j * self.tile, self.tile), self.tile))
            return carry

        if nr * nc == 1:
            one(0, 0)
        else:
            lax.fori_loop(0, nr * nc, one, 0)

    def diagonals(self, body, init):
        def one(i, carry):
            d = pl.ds(pl.multiple_of(i * self.tile, self.tile), self.tile)
            return body(d, carry)

        if self.n == self.tile:
            return one(0, init)
        return lax.fori_loop(0, self.n // self.tile, one, init)

    def trace(self, ref):
        mask = eye(self.tile)
        zero = jnp.zeros((1, 1), jnp.float32)
        return self.diagonals(lambda d, c: c + total(jnp.where(mask, ref[d, d], 0.0)), zero)

    def centre(self, s):
        shift = self.trace(self.e) * (1.0 / self.n)
        mask = eye(self.tile)

        def one(d, c):
            moved = self.e[d, d] - jnp.where(mask, shift, 0.0)
            self.e[d, d] = moved
            self.ebf[d, d] = moved.astype(jnp.bfloat16)
            return c

        self.diagonals(one, 0)
        return s + shift

    def start(self, gram):
        def block(r, c):
            self.e[r, c] = gram(r, c)

        self.blocks(block)
        norm = jnp.sqrt(self.trace(self.e)) + 1e-06
        scale = 1.0 / (norm * norm)

        def scaled(r, c):
            x = self.e[r, c] * scale
            self.e[r, c] = x
            self.ebf[r, c] = x.astype(jnp.bfloat16)

        self.blocks(scaled)
        return self.centre(jnp.zeros((1, 1), jnp.float32)), 1.0 / norm

    def polynomial(self, s):
        p0 = coef_a + s * (coef_b + coef_c * s)
        p1 = coef_b + 2.0 * coef_c * s

        def block(r, c):
            f = p1 * self.e[r, c] + coef_c * mm(self.ebf[r, :], self.ebf[:, c])
            self.fbf[r, c] = f.astype(jnp.bfloat16)

        self.blocks(block)
        return p0

    def first(self):
        def block(r, c):
            f = self.fbf[r, c]
            self.h[r, c] = f.astype(jnp.float32)
            self.hbf[r, c] = f

        self.blocks(block)

    def grow(self, p0, q):
        def block(r, c):
            new = p0 * self.h[r, c] + q * self.fbf[r, c].astype(jnp.float32) + mm(self.fbf[r, :], self.hbf[:, c])
            self.k[r, c] = new

        self.blocks(block)

        def back(r, c):
            new = self.k[r, c]
            self.h[r, c] = new
            self.hbf[r, c] = new.astype(jnp.bfloat16)

        self.blocks(back)

    def advance(self, p0, s):
        def inner(r, c):
            new = p0 * self.e[r, c] + s * self.fbf[r, c].astype(jnp.float32) + mm(self.fbf[r, :], self.ebf[:, c])
            self.k[r, c] = new
            self.kbf[r, c] = new.astype(jnp.bfloat16)

        self.blocks(inner)
        beta = p0 * s

        def outer(r, c):
            new = p0 * self.k[r, c] + beta * self.fbf[r, c].astype(jnp.float32) + mm(self.fbf[r, :], self.kbf[:, c])
            self.e[r, c] = new
            self.ebf[r, c] = new.astype(jnp.bfloat16)

        self.blocks(outer)
        return self.centre(p0 * beta)


def muon_kernel(wide, m_in, m_out, h_out, hs_out, scal, x, *scratch):
    big = Iterate(*scratch[:7], tile=256, rows=512)
    small = Iterate(*scratch[7:], tile=256, rows=256)
    core = lax.rem(lax.axis_index("rep"), 2)
    n, ns = big.n, small.n

    @pl.when(core == 0)
    def _():
        def turn(i, c):
            r = pl.ds(pl.multiple_of(i * 256, 256), 256)
            x[:, r] = m_in[r, pl.ds(0, n)].T
            return c

        lax.fori_loop(0, wide // 256, turn, 0)

    @pl.when(core != 0)
    def _():
        def take(i, c):
            r = pl.ds(pl.multiple_of(i * 128, 128), 128)
            x[r, :] = m_out[r, :]
            return c

        lax.fori_loop(0, n // 128, take, 0)

    s, inv = big.start(lambda r, c: nt(x[r, :], x[c, :]))
    mine = m_in.at[:, pl.ds(pl.multiple_of(n + core * ns, 128), ns)]
    ss, sinv = small.start(lambda r, c: tn(mine[:, r], mine[:, c]))

    def sweep(it, carry):
        s, q, ss, sq = carry
        p0, sp0 = big.polynomial(s), small.polynomial(ss)

        @pl.when(it == 0)
        def _():
            big.first()
            small.first()

        @pl.when(it > 0)
        def _():
            big.grow(p0, q)
            small.grow(sp0, sq)

        q, sq = p0 * q, sp0 * sq
        s, ss = lax.cond(
            it < SWEEPS - 1,
            lambda: (big.advance(p0, s), small.advance(sp0, ss)),
            lambda: (s, ss),
        )
        return s, q, ss, sq

    one = jnp.ones((1, 1), jnp.float32)
    s, q, ss, sq = lax.fori_loop(0, SWEEPS, sweep, (s, one, ss, one))
    h_out[...] = big.hbf[...]
    hs_out[...] = small.hbf[...]
    row = lax.broadcasted_iota(jnp.int32, (8, 128), 0)
    scal[...] = jnp.where(row == 0, q * inv, jnp.where(row == 1, inv, jnp.where(row == 2, sq * sinv, sinv)))


def muon(m_in, m_out, kv):
    wide, n = m_in.shape[0], m_out.shape[0]
    sets = []
    for d in (n, kv):
        f32, b16 = pltpu.VMEM((d, d), jnp.float32), pltpu.VMEM((d, d), jnp.bfloat16)
        sets += [f32, b16, f32, b16, f32, b16, b16]
    vmem = pl.BlockSpec(memory_space=pltpu.VMEM)
    return pl.pallas_call(
        functools.partial(muon_kernel, wide),
        out_shape=[
            jax.ShapeDtypeStruct((n, n), jnp.bfloat16),
            jax.ShapeDtypeStruct((kv, kv), jnp.bfloat16),
            jax.ShapeDtypeStruct((8, 128), jnp.float32),
        ],
        in_specs=[vmem] * 2,
        out_specs=[vmem] * 3,
        scratch_shapes=[pltpu.VMEM((n, wide), jnp.bfloat16)] + sets,
        compiler_params=pltpu.CompilerParams(vmem_limit_bytes=60 << 20),
        name="muon",
    )(m_in, m_out)


HEAD_SIZE = 64
TILE = 256
norm_eps = 1e-05
rope_base = 500000.0


def tiles(count, body):
    def one(i, carry):
        body(i)
        return carry

    lax.fori_loop(0, count, one, 0)


def span(i, size):
    return pl.ds(pl.multiple_of(i * size, size), size)


def swap_halves(x):
    half, width = HEAD_SIZE // 2, x.shape[1]
    lane = lax.rem(lax.broadcasted_iota(jnp.int32, x.shape, 1), HEAD_SIZE)
    return jnp.where(lane < half, pltpu.roll(x, width - half, 1), pltpu.roll(x, half, 1))


def block_kernel(
    tok, cot, w_in, w_out, gain, cosine, sine, bias,
    out, grad_tok, part_in, part_out, part_gain,
    xn, xnt, inv_ref, q, dattn, attn_t, attn, dq_t, dqkv, dxn, row_acc, kx, vx, kxt, vxt, dk_acc, dv_acc,
):
    f32, b16 = jnp.float32, jnp.bfloat16
    seq, width = tok.shape
    q_width = w_out.shape[0]
    kv_width = (w_in.shape[1] - q_width) // 2
    kv_heads = kv_width // HEAD_SIZE
    pair = 2 * HEAD_SIZE
    pairs = q_width // pair
    n_q, n_tok = q_width // TILE, seq // TILE
    scale = 1.0 / math.sqrt(HEAD_SIZE)
    rows = 64

    def norm(i):
        r = span(i, rows)
        x = tok[r, :].astype(f32)
        inv = lax.rsqrt(jnp.mean(x * x, -1, keepdims=True) + norm_eps)
        inv_ref[r, :] = jnp.broadcast_to(inv, (rows, 128))
        xn[r, :] = (x * inv * gain[...]).astype(b16)

    tiles(seq // rows, norm)

    def tables():
        c, s = cosine[...], sine[...]
        return jnp.concatenate([c] * (TILE // c.shape[1]), 1), jnp.concatenate([s] * (TILE // s.shape[1]), 1)

    def query(i):
        x = mm(xn[...], w_in[:, span(i, TILE)])
        c, s = tables()
        q[:, span(i, TILE)] = (x * c + swap_halves(x) * s).astype(b16)

    tiles(n_q, query)
    lane = lax.broadcasted_iota(jnp.int32, (seq, pair), 1)
    low = lane < HEAD_SIZE

    def split(x, into, into_t):
        for g in range(kv_heads):
            two = x[:, (g // 2) * pair : (g // 2 + 1) * pair].astype(f32)
            other = pltpu.roll(two, HEAD_SIZE, 1)
            first, second = (two, other) if g % 2 == 0 else (other, two)
            lo, hi = jnp.where(low, first, 0.0).astype(b16), jnp.where(low, 0.0, second).astype(b16)
            into[g, 0], into[g, 1] = lo, hi
            into_t[g, 0], into_t[g, 1] = lo.T, hi.T

    for first, into, into_t, turned in ((q_width, kx, kxt, True), (q_width + kv_width, vx, vxt, False)):
        x = mm(xn[...], w_in[:, pl.ds(first, kv_width)])
        if turned:
            c, s = tables()
            x = x * c + swap_halves(x) * s
        split(x.astype(b16), into, into_t)

    def head_grad(i):
        dattn[:, span(i, TILE)] = nt(cot[...], w_out[span(i, TILE), :]).astype(b16)

    tiles(n_q, head_grad)

    per_group = pairs // kv_heads

    def heads(p):
        g = lax.div(p, per_group)
        lanes = span(p, pair)

        @pl.when(lax.rem(p, per_group) == 0)
        def _():
            dk_acc[...] = jnp.zeros_like(dk_acc)
            dv_acc[...] = jnp.zeros_like(dv_acc)

        for b in range(n_tok):
            qs = slice(b * TILE, (b + 1) * TILE)
            ks = slice(max(b - 1, 0) * TILE, (b + 1) * TILE)
            q_b, d_b = q[qs, lanes], dattn[qs, lanes]
            mask = bias[ks, qs]
            a_t, dq = None, None
            for side in range(2):
                score = nt(kx[g, side, ks, :], q_b) * scale + mask
                grown = jnp.exp(score)
                prob = grown * (1.0 / jnp.sum(grown, 0, keepdims=True))
                prob_b = prob.astype(b16)
                dp = nt(vx[g, side, ks, :], d_b)
                inner = jnp.sum(prob * dp, 0, keepdims=True)
                ds = (prob * (dp - inner) * scale).astype(b16)
                dv_acc[side, ks, :] += mm(prob_b, d_b)
                dk_acc[side, ks, :] += mm(ds, q_b)
                a_part = mm(vxt[g, side, :, ks], prob_b)
                q_part = mm(kxt[g, side, :, ks], ds)
                a_t = a_part if a_t is None else a_t + a_part
                dq = q_part if dq is None else dq + q_part
            attn_t[lanes, qs] = a_t.astype(b16)
            attn[qs, lanes] = a_t.T.astype(b16)
            turned_back = dq.T
            c, s = cosine[qs, :], sine[qs, :]
            dqkv[qs, lanes] = (turned_back * c - swap_halves(turned_back) * s).astype(b16)

        @pl.when(lax.rem(p, per_group) == per_group - 1)
        def _():
            def joined(acc):
                return acc[0] + pltpu.roll(acc[1], HEAD_SIZE, 1)

            dk, dv = joined(dk_acc), joined(dv_acc)
            dk = dk * cosine[...] - swap_halves(dk) * sine[...]
            for x, first in ((dk, q_width), (dv, q_width + kv_width)):
                at = span(lax.div(g, 2) + first // pair, pair)
                odd = lax.rem(g, 2)

                @pl.when(odd == 0)
                def _():
                    dqkv[:, at] = x.astype(b16)

                @pl.when(odd == 1)
                def _():
                    high = pltpu.roll(x, HEAD_SIZE, 1)
                    dqkv[:, at] = jnp.where(low, dqkv[:, at].astype(f32), high).astype(b16)

    tiles(pairs, heads)

    def project(i):
        c = span(i, TILE)
        out[:, c] = (tok[:, c].astype(f32) + mm(attn[...], w_out[:, c])).astype(b16)
        part_out[:, c] = mm(attn_t[...], cot[:, c]).astype(b16)

    tiles(width // TILE, project)

    row_acc[...] = jnp.zeros_like(row_acc)

    def input_grad(i):
        c = span(i, TILE)
        part_in[c, :] = tn(xn[:, c], dqkv[...]).astype(b16)
        d = nt(dqkv[...], w_in[c, :])
        normed = tok[:, c].astype(f32) * inv_ref[:, :1]
        both = d * normed
        part_gain[:, c] = jnp.sum(both, 0, keepdims=True)
        d = d * gain[:, c]
        dxn[:, c] = d
        row_acc[...] += jnp.broadcast_to(jnp.sum(d * normed, 1, keepdims=True), row_acc.shape)

    tiles(width // TILE, input_grad)

    def last(i):
        r = span(i, rows)
        inv = inv_ref[r, :1]
        normed = tok[r, :].astype(f32) * inv
        mean = row_acc[r, :1] * (1.0 / width)
        grad_tok[r, :] = (cot[r, :].astype(f32) + inv * (dxn[r, :] - normed * mean)).astype(b16)

    tiles(seq // rows, last)


def block(tok, cot, seg, w_in, w_out, gain):
    f32, b16 = jnp.float32, jnp.bfloat16
    seq, width = tok.shape
    q_width = w_out.shape[0]
    kv_width = (w_in.shape[1] - q_width) // 2
    kv_heads = kv_width // HEAD_SIZE
    pair = 2 * HEAD_SIZE
    index = jnp.arange(seq, dtype=jnp.int32)
    start = jnp.sum((seg[None, :] < seg[:, None]).astype(jnp.int32), 1)
    position = (index - start).astype(f32)
    half = HEAD_SIZE // 2
    frequency = rope_base ** (-2.0 * jnp.arange(half, dtype=f32) / HEAD_SIZE)
    angles = position[:, None] * frequency[None, :]
    c, s = jnp.cos(angles), jnp.sin(angles)
    cosine, sine = jnp.concatenate([c] * 4, 1), jnp.concatenate([-s, s] * 2, 1)
    allowed = (index[:, None] <= index[None, :]) & (seg[None, :] == seg[:, None])
    bias = jnp.where(allowed, 0.0, -1e30).astype(f32)
    vmem = pl.BlockSpec(memory_space=pltpu.VMEM)
    V = pltpu.VMEM
    return pl.pallas_call(
        block_kernel,
        out_shape=[
            jax.ShapeDtypeStruct((seq, width), b16),
            jax.ShapeDtypeStruct((seq, width), b16),
            jax.ShapeDtypeStruct(w_in.shape, b16),
            jax.ShapeDtypeStruct(w_out.shape, b16),
            jax.ShapeDtypeStruct((1, width), f32),
        ],
        in_specs=[vmem] * 8,
        out_specs=[vmem] * 5,
        scratch_shapes=[
            V((seq, width), b16),
            V((8, 128), b16),
            V((seq, 128), f32),
            V((seq, q_width), b16),
            V((seq, q_width), b16),
            V((q_width, seq), b16),
            V((seq, q_width), b16),
            V((8, 128), f32),
            V((seq, q_width + 2 * kv_width), b16),
            V((seq, width), f32),
            V((seq, 128), f32),
            V((kv_heads, 2, seq, pair), b16),
            V((kv_heads, 2, seq, pair), b16),
            V((kv_heads, 2, pair, seq), b16),
            V((kv_heads, 2, pair, seq), b16),
            V((2, seq, pair), f32),
            V((2, seq, pair), f32),
        ],
        compiler_params=pltpu.CompilerParams(vmem_limit_bytes=63 << 20),
        name="block",
    )(tok, cot, w_in, w_out, gain[None], cosine, sine, bias)


decay = 0.95
muon_rate = 0.02
gain_rate = 0.2


def rows_of(matrix, index, count):
    return lax.dynamic_slice_in_dim(matrix, index * count, count, 0)


def cols_of(matrix, index, count):
    return lax.dynamic_slice_in_dim(matrix, index * count, count, 1)


def on_device(
    tokens,
    segments,
    cotangent,
    gain,
    w_query,
    w_key,
    w_value,
    w_outproj,
    moment_gain,
    moment_query,
    moment_key,
    moment_value,
    moment_outproj,
):
    n_rep, n_shard = lax.axis_size("rep"), lax.axis_size("shard")
    total_tokens = tokens.shape[0] * tokens.shape[1] * n_rep * n_shard
    b16 = jnp.bfloat16
    w_in_bf = jnp.concatenate([w_query, w_key, w_value], 1).astype(b16)
    w_in_all, w_out_all, gain_all = gather_all(
        [w_in_bf, w_outproj.astype(b16)], lax.reduce_precision(gain, 8, 7), n_rep, n_shard, 0
    )
    result, grad_tokens, part_in, part_outproj, part_gain = block(
        tokens[0], cotangent[0], segments[0], w_in_all, w_out_all, gain_all
    )
    return finish(
        result, grad_tokens, part_in, part_outproj, part_gain[0], total_tokens, gain, (w_query, w_key, w_value, w_outproj),
        moment_gain, (moment_query, moment_key, moment_value, moment_outproj),
    )


def finish(result, grad_tokens, part_in, part_outproj, part_gain, total_tokens, gain, weights, moment_gain, moments):
    n_rep, n_shard = lax.axis_size("rep"), lax.axis_size("shard")
    rep_index, shard_index = lax.axis_index("rep"), lax.axis_index("shard")
    b16, f32 = jnp.bfloat16, jnp.float32
    w_query, w_key, w_value, w_outproj = weights
    query_width, kv_width = w_query.shape[1], w_key.shape[1]
    in_piece = jnp.concatenate([rows_of(m, rep_index, m.shape[0] // n_rep) for m in moments[:3]], 1)
    out_piece = rows_of(moments[3], rep_index, moments[3].shape[0] // n_rep)
    (sum_in, sum_out), (m_in, m_out), grad_gain = reduce_and_gather(
        [part_in, part_outproj], part_gain, [in_piece, out_piece], decay, n_rep, n_shard, 1
    )
    grads = [
        sum_in[:, :query_width].astype(f32),
        sum_in[:, query_width : query_width + kv_width].astype(f32),
        sum_in[:, query_width + kv_width :].astype(f32),
        sum_out.astype(f32),
    ]
    moments_next = [decay * m + g for m, g in zip(moments, grads)]
    moment_gain_next = decay * moment_gain + grad_gain
    gain_next = gain - gain_rate / math.sqrt(total_tokens) * moment_gain_next
    own_in = jnp.concatenate([m.astype(b16) for m in moments_next[:3]], 1)
    own_out = moments_next[3].astype(b16)
    m_in = lax.dynamic_update_slice_in_dim(m_in, own_in, shard_index * own_in.shape[0], 0)
    m_out = lax.dynamic_update_slice_in_dim(m_out, own_out, shard_index * own_out.shape[0], 0)
    mix, mix_kv, scales = muon(m_in, m_out, kv_width)
    core = lax.rem(rep_index, 2)
    other = rep_index + 1 - 2 * core
    widths = [w.shape[1] // n_rep for w in weights]
    pairs = [(i, i ^ 1) for i in range(n_rep)]
    out_rows = w_outproj.shape[0]
    theirs = lax.ppermute(
        (
            rows_of(mix, other, widths[0]),
            rows_of(mix, shard_index, out_rows),
            rows_of(mix_kv, other, widths[1]),
            scales,
        ),
        "rep",
        pairs,
    )
    even = core == 0
    mix_query = jnp.where(even, rows_of(mix, rep_index, widths[0]), theirs[0])
    mix_out = jnp.where(even, theirs[1], rows_of(mix, shard_index, out_rows))
    kv_mine = rows_of(mix_kv, rep_index, widths[1])
    mix_key, mix_value = jnp.where(even, kv_mine, theirs[2]), jnp.where(even, theirs[2], kv_mine)
    first, second = jnp.where(even, scales, theirs[3]), jnp.where(even, theirs[3], scales)
    spans = (
        (0, query_width, mix_query, first[0, 0], first[1, 0]),
        (query_width, kv_width, mix_key, first[2, 0], first[3, 0]),
        (query_width + kv_width, kv_width, mix_value, second[2, 0], second[3, 0]),
    )
    updated = []
    for i, (at, width, mix_rows, straight, mixed) in enumerate(spans):
        whole = (weights[i].shape[0] * n_shard, width)
        ortho = straight * cols_of(moments_next[i], rep_index, widths[i]) + mixed * nt(
            own_in[:, at : at + width], mix_rows
        )
        updated.append(cols_of(weights[i], rep_index, widths[i]) - muon_rate * math.sqrt(max(whole)) * ortho)
    whole = (out_rows * n_shard, w_outproj.shape[1])
    ortho = second[0, 0] * cols_of(moments_next[3], rep_index, widths[3]) + second[1, 0] * jnp.dot(
        mix_out, cols_of(m_out, rep_index, widths[3]), preferred_element_type=f32
    )
    updated.append(cols_of(w_outproj, rep_index, widths[3]) - muon_rate * math.sqrt(max(whole)) * ortho)
    return (
        result[None],
        grad_tokens[None],
        grad_gain,
        *grads,
        gain_next,
        *updated,
        moment_gain_next,
        *moments_next,
    )


def solution(mesh):
    in_specs = (
        P(("rep", "shard"), None, None),
        P(("rep", "shard"), None),
        P(("rep", "shard"), None, None),
        P("shard"),
        P("shard", None),
        P("shard", None),
        P("shard", None),
        P("shard", None),
        P("shard"),
        P("shard", None),
        P("shard", None),
        P("shard", None),
        P("shard", None),
    )
    out_specs = (
        P(("rep", "shard"), None, None),
        P(("rep", "shard"), None, None),
        P("shard"),
        P("shard", None),
        P("shard", None),
        P("shard", None),
        P("shard", None),
        P("shard"),
        P("shard", "rep"),
        P("shard", "rep"),
        P("shard", "rep"),
        P("shard", "rep"),
        P("shard"),
        P("shard", None),
        P("shard", None),
        P("shard", None),
        P("shard", None),
    )
    return jax.shard_map(on_device, mesh=mesh, in_specs=in_specs, out_specs=out_specs, check_vma=False)
```

```python
import functools
import math

import jax
import jax.numpy as jnp
from jax import lax
from jax.experimental import pallas as pl
from jax.experimental.pallas import tpu as pltpu
from jax.sharding import PartitionSpec as P

MESH = pl.DeviceIdType.MESH


class Links:
    def __init__(self, n_rep, n_shard):
        self.n_bits = n_rep.bit_length() - 1
        self.n_shard = n_shard
        self.rep = lax.axis_index("rep")
        self.shard = lax.axis_index("shard")
        self.bits = [lax.rem(lax.div(self.rep, 1 << b), 2) for b in range(self.n_bits)]
        far = list(range(1, self.n_bits))
        self.orders = (far, far[::-1])

    def flip(self, bit):
        return self.rep + (1 << bit) * (1 - 2 * self.bits[bit])

    def barrier(self, line):
        sem = pltpu.get_barrier_semaphore()
        count = self.n_bits
        for b in range(self.n_bits):
            pl.semaphore_signal(sem, 1, device_id=(self.flip(b), self.shard), device_id_type=MESH)
        if line:
            for step in (-1, 1):
                there = self.shard + step
                inside = jnp.logical_and(there >= 0, there < self.n_shard)

                @pl.when(inside)
                def _():
                    pl.semaphore_signal(sem, 1, device_id=(self.rep, there), device_id_type=MESH)

                count = count + inside.astype(jnp.int32)
        else:
            for k in range(1, self.n_shard):
                there = lax.rem(self.shard + k, self.n_shard)
                pl.semaphore_signal(sem, 1, device_id=(self.rep, there), device_id_type=MESH)
            count = count + self.n_shard - 1
        pl.semaphore_wait(sem, count)

    def where(self, fixed, free=()):
        return tuple(
            slice(None) if b in free else fixed.get(b, self.bits[b])
            for b in reversed(range(self.n_bits))
        )


def halves(ref):
    cols = ref.shape[-1]
    return (pl.ds(0, cols // 2), pl.ds(cols // 2, cols // 2))


def spread(links, full, q, half, step, send, recv):
    order = links.orders[half] + [0]
    bit, done = order[step], order[:step]
    view = full.at[(q, *links.where({}, done), slice(None), halves(full)[half])]
    return pltpu.make_async_remote_copy(
        view, view, send, recv, device_id=(links.flip(bit), links.shard), device_id_type=MESH
    )


def gather_kernel(n_rep, n_shard, n_arrays, *refs):
    local, row = refs[:n_arrays], refs[n_arrays]
    full, row_full = refs[n_arrays + 1 : 2 * n_arrays + 1], refs[2 * n_arrays + 1]
    keep_sem, line_send, line_recv, plane_send, plane_recv, row_send, row_recv = refs[2 * n_arrays + 2 :]
    links = Links(n_rep, n_shard)
    me = links.shard
    links.barrier(True)
    row_full[me] = row[...]

    def row_line(way, k):
        q, side = me - way * k, (way + 1) // 2
        return pltpu.make_async_remote_copy(
            row if k == 0 else row_full.at[q], row_full.at[q], row_send.at[side, k], row_recv.at[side, k],
            device_id=(links.rep, me + way), device_id_type=MESH,
        )

    def row_came(way, k):
        here, side = row_full.at[me - way * (k + 1)], (way + 1) // 2
        return pltpu.make_async_remote_copy(
            here, here, row_send.at[side, k], row_recv.at[side, k], device_id=(links.rep, me), device_id_type=MESH
        )
    keeps = [pltpu.make_async_copy(local[a], full[a].at[me], keep_sem.at[a]) for a in range(n_arrays)]

    def line(a, way, k):
        q = me - way * k
        here = links.where({})
        src = local[a].at[here] if k == 0 else full[a].at[(q, *here)]
        side = (way + 1) // 2
        return pltpu.make_async_remote_copy(
            src, full[a].at[(q, *here)], line_send.at[a, side, k], line_recv.at[a, side, k],
            device_id=(links.rep, me + way), device_id_type=MESH,
        )

    def came(a, way, k):
        q = me - way * (k + 1)
        here = full[a].at[(q, *links.where({}))]
        side = (way + 1) // 2
        return pltpu.make_async_remote_copy(
            here, here, line_send.at[a, side, k], line_recv.at[a, side, k],
            device_id=(links.rep, me), device_id_type=MESH,
        )

    def goes(way, k):
        q, there = me - way * k, me + way
        return (q >= 0) & (q < n_shard) & (there >= 0) & (there < n_shard)

    def comes(way, k):
        q = me - way * (k + 1)
        return (q >= 0) & (q < n_shard)

    ways = (1, -1)
    n_steps = links.n_bits
    for way in ways:
        @pl.when(goes(way, 0))
        def _():
            row_line(way, 0).start()
    for a in range(n_arrays):
        for way in ways:
            @pl.when(goes(way, 0))
            def _():
                line(a, way, 0).start()
    for keep in keeps:
        keep.start()

    def plane(a, way, k, half, step):
        q = me - way * (k + 1)
        side = (way + 1) // 2
        return spread(links, full[a], q, half, step,
                      plane_send.at[a, side, k, half, step], plane_recv.at[a, side, k, half, step])

    items = [(a, k) for a in range(n_arrays) for k in range(n_shard - 1)]
    for t in range(len(items) + n_steps):
        for i, (a, k) in enumerate(items):
            step = t - i
            if step < 0 or step > n_steps:
                continue
            for way in ways:
                @pl.when(comes(way, k))
                def _():
                    if step == 0 and a == 0:
                        row_came(way, k).wait_recv()
                        if k + 1 < n_shard - 1:
                            @pl.when(goes(way, k + 1))
                            def _():
                                row_line(way, k + 1).start()
                    if step == 0:
                        came(a, way, k).wait_recv()
                        if k + 1 < n_shard - 1:
                            @pl.when(goes(way, k + 1))
                            def _():
                                line(a, way, k + 1).start()
                    else:
                        for half in range(2):
                            plane(a, way, k, half, step - 1).wait_recv()
                    if step < n_steps:
                        for half in range(2):
                            plane(a, way, k, half, step).start()
    for keep in keeps:
        keep.wait()
    for way in ways:
        for k in range(n_shard - 1):
            @pl.when(goes(way, k))
            def _():
                row_line(way, k).wait_send()
    for a in range(n_arrays):
        for way in ways:
            for k in range(n_shard - 1):
                @pl.when(goes(way, k))
                def _():
                    line(a, way, k).wait_send()

                @pl.when(comes(way, k))
                def _():
                    for half in range(2):
                        for step in range(n_steps):
                            plane(a, way, k, half, step).wait_send()


def gather_all(blocks, row, n_rep, n_shard, collective_id):
    n_bits = n_rep.bit_length() - 1
    n = len(blocks)
    shaped = [b.reshape((2,) * n_bits + (b.shape[0] // n_rep, b.shape[1])) for b in blocks]
    steps = max(n_shard - 1, 1)
    out = pl.pallas_call(
        functools.partial(gather_kernel, n_rep, n_shard, n),
        out_shape=[jax.ShapeDtypeStruct((n_shard,) + s.shape, s.dtype) for s in shaped]
        + [jax.ShapeDtypeStruct((n_shard, 1) + row.shape, row.dtype)],
        in_specs=[pl.BlockSpec(memory_space=pltpu.VMEM)] * (n + 1),
        out_specs=[pl.BlockSpec(memory_space=pl.ANY)] * n + [pl.BlockSpec(memory_space=pltpu.VMEM)],
        scratch_shapes=[
            pltpu.SemaphoreType.DMA((n,)),
            pltpu.SemaphoreType.DMA((n, 2, steps)),
            pltpu.SemaphoreType.DMA((n, 2, steps)),
            pltpu.SemaphoreType.DMA((n, 2, steps, 2, n_bits)),
            pltpu.SemaphoreType.DMA((n, 2, steps, 2, n_bits)),
            pltpu.SemaphoreType.DMA((2, steps)),
            pltpu.SemaphoreType.DMA((2, steps)),
        ],
        compiler_params=pltpu.CompilerParams(collective_id=collective_id, has_side_effects=True),
        name="gather_all",
    )(*shaped, row[None])
    return [o.reshape(n_shard * b.shape[0], b.shape[1]) for o, b in zip(out, blocks)] + [out[n].reshape(-1)]


F32 = jnp.float32


class Sems:
    def __init__(self, send, recv):
        self.send, self.recv, self.names = send, recv, {}

    def pair(self, *name):
        i = self.names.setdefault(name, len(self.names))
        return self.send.at[i], self.recv.at[i]


def reduce_kernel(n_rep, n_shard, decay, n_sems, *refs):
    parts, gain, moments = refs[0:2], refs[2], refs[3:5]
    sums, wholes, gain_out = refs[5:7], refs[7:9], refs[9]
    rest = list(refs[10:])
    nb = n_rep.bit_length() - 1
    bufs = [[rest.pop(0) for _ in range(nb)] for _ in range(2)]
    zbuf = [rest.pop(0) for _ in range(2)]
    gpiece = [rest.pop(0) for _ in range(2)]
    mpiece = [rest.pop(0) for _ in range(2)]
    gacc, gcome, gz = rest.pop(0), rest.pop(0), rest.pop(0)
    keep_sem = rest.pop(0)
    sems = Sems(rest.pop(0), rest.pop(0))
    links = Links(n_rep, n_shard)
    me = links.shard
    links.barrier(False)

    def remote(src, dst, name, rep, shard):
        send, recv = sems.pair(*name)
        return pltpu.make_async_remote_copy(src, dst, send, recv, device_id=(rep, shard), device_id_type=MESH)

    def dest(k):
        return lax.rem(me + 1 + k, n_shard)

    def order(half):
        return [0] + links.orders[half]

    def pick(half, step, bit_value, fixed_lead):
        o = order(half)
        remaining = sorted(o[step:], reverse=True)
        return fixed_lead + tuple(bit_value if b == o[step] else slice(None) for b in remaining)

    def send_reduce(a, k, half, step):
        d, o = dest(k), order(half)
        bit = o[step]
        src = parts[a] if step == 0 else bufs[a][step - 1]
        cols = slice(None) if step == 0 else halves(parts[a])[half]
        view = src.at[pick(half, step, 1 - links.bits[bit], (d,)) + (slice(None), cols)]
        into = bufs[a][step].at[(d,) + (slice(None),) * (nb - step) + (cols,)]
        return remote(view, into, ("r", a, k, half, step), links.flip(bit), me)

    def add_reduce(a, k, half, step):
        d, o = dest(k), order(half)
        src = parts[a] if step == 0 else bufs[a][step - 1]
        n_left = nb - 1 - step
        cols = slice(None) if step == 0 else halves(parts[a])[half]
        mine = links.bits[o[step]]
        remaining = sorted(o[step:], reverse=True)

        def one(i, c):
            left = {}
            rest_bits = [b for b in remaining if b != o[step]]
            for pos, b in enumerate(rest_bits):
                left[b] = lax.rem(lax.div(i, 1 << (len(rest_bits) - 1 - pos)), 2)
            here = tuple(left[b] for b in rest_bits)
            there = tuple(mine if b == o[step] else left[b] for b in remaining)
            x = src[(d,) + there + (slice(None), cols)].astype(F32)
            y = bufs[a][step][(d,) + here + (slice(None), cols)].astype(F32)
            bufs[a][step][(d,) + here + (slice(None), cols)] = (x + y).astype(jnp.bfloat16)
            return c

        if n_left == 0:
            one(0, 0)
        else:
            lax.fori_loop(0, 1 << n_left, one, 0)

    def send_line(a, k):
        d = dest(k)
        return remote(bufs[a][nb - 1].at[d], zbuf[a].at[me], ("z", a, k), links.rep, d)

    def wait_line(a, k):
        q = lax.rem(me + n_shard - 1 - k, n_shard)
        return remote(zbuf[a].at[q], zbuf[a].at[q], ("z", a, k), links.rep, me)

    for a in (1, 0):
        for k in range(n_shard):
            send_reduce(a, k, 0, 0).start()

    def gain_send(b):
        return remote(gacc, gcome.at[b], ("gain", b), links.flip(b), me)

    def gain_line(k):
        d = dest(k)
        return remote(gacc.at[d], gz.at[me], ("gainz", k), links.rep, d)

    gacc[...] = gain[...]
    gain_send(0).start()

    def gain_step(b):
        gain_send(b).wait()
        gacc[...] = gacc[...] + gcome[b]
        if b + 1 < nb:
            gain_send(b + 1).start()
        else:
            for k in range(n_shard - 1):
                gain_line(k).start()

    def gain_end():
        acc = gacc[me]
        for k in range(n_shard - 1):
            gain_line(k).wait_send()
            q = lax.rem(me + n_shard - 1 - k, n_shard)
            remote(gz.at[q], gz.at[q], ("gainz", k), links.rep, me).wait_recv()
        for q in range(n_shard):
            acc = jnp.where(me == q, acc, acc + gz[q])
        gain_out[...] = acc

    here = links.where({})

    def g_step(a, half, step):
        o = links.orders[half] + [0]
        bit, done = o[step], o[:step]
        cols = halves(parts[a])[half]
        into = sums[a].at[links.where({}, done) + (slice(None), cols)]
        src = gpiece[a].at[:, cols] if step == 0 else into
        return remote(src, into, ("g", a, half, step), links.flip(bit), me)

    def keep(a, i):
        return pltpu.make_async_copy(gpiece[a], sums[a].at[here], keep_sem.at[a])

    def line(a, way, k):
        q = me - way * k
        at = wholes[a].at[(q,) + here]
        src = mpiece[a] if k == 0 else at
        return remote(src, at, ("l", a, way, k), links.rep, me + way)

    def came(a, way, k):
        at = wholes[a].at[(me - way * (k + 1),) + here]
        return remote(at, at, ("l", a, way, k), links.rep, me)

    def goes(way, k):
        q, there = me - way * k, me + way
        return (q >= 0) & (q < n_shard) & (there >= 0) & (there < n_shard)

    def comes(way, k):
        q = me - way * (k + 1)
        return (q >= 0) & (q < n_shard)

    def plane(a, way, k, half, step):
        o = links.orders[half] + [0]
        bit, done = o[step], o[:step]
        view = wholes[a].at[(me - way * (k + 1),) + links.where({}, done) + (slice(None), halves(parts[a])[half])]
        return remote(view, view, ("p", a, way, k, half, step), links.flip(bit), me)

    ways = (1, -1)

    def finish(a):
        for k in range(n_shard - 1):
            wait_line(a, k).wait_recv()
        acc = bufs[a][nb - 1][me].astype(F32)
        for k in range(n_shard - 1):
            acc = acc + zbuf[a][lax.rem(me + n_shard - 1 - k, n_shard)].astype(F32)
        g = acc.astype(jnp.bfloat16)
        gpiece[a][...] = g
        mpiece[a][...] = (decay * moments[a][...] + g.astype(F32)).astype(jnp.bfloat16)
        for way in ways:
            @pl.when(goes(way, 0))
            def _():
                line(a, way, 0).start()
        for half in range(2):
            g_step(a, half, 0).start()
        keep(a, 0).start()

    def gather_event(a, i, step):
        if i == 0:
            if step == 0:
                keep(a, 0).wait()
            if step < nb:
                for half in range(2):
                    g_step(a, half, step).wait_recv()
                    if step + 1 < nb:
                        g_step(a, half, step + 1).start()
            return
        k = i - 1
        for way in ways:
            @pl.when(comes(way, k))
            def _():
                if step == 0:
                    came(a, way, k).wait_recv()
                    if k + 1 < n_shard - 1:
                        @pl.when(goes(way, k + 1))
                        def _():
                            line(a, way, k + 1).start()
                else:
                    for half in range(2):
                        plane(a, way, k, half, step - 1).wait_recv()
                if step < nb:
                    for half in range(2):
                        plane(a, way, k, half, step).start()

    def reduce_event(a, k, step):
        for half in range(1 if step == 0 else 2):
            send_reduce(a, k, half, step).wait_recv()
            add_reduce(a, k, half, step)
            if step == 0 and nb > 1:
                send_reduce(a, k, 0, 1).start()
                send_reduce(a, k, 1, 1).start()
            elif step + 1 < nb:
                send_reduce(a, k, half, step + 1).start()
        if step == nb - 1 and k < n_shard - 1:
            send_line(a, k).start()

    events = []
    chunks = [(a, k) for a in (1, 0) for k in range(n_shard)]
    for t in range(len(chunks) + nb):
        if t < nb:
            events.append(functools.partial(gain_step, t))
        for step in reversed(range(nb)):
            i = t - step
            if 0 <= i < len(chunks):
                events.append(functools.partial(reduce_event, *chunks[i], step))
        if t == n_shard + nb:
            events.append(functools.partial(finish, 1))
            events.append(gain_end)
        i = t - n_shard - nb - 1
        if i >= 0:
            for j in range(n_shard):
                step = i - j
                if 0 <= step <= nb:
                    events.append(functools.partial(gather_event, 1, j, step))
    done_t = len(chunks) + nb - n_shard - nb - 1
    events.append(functools.partial(finish, 0))
    for t in range(n_shard + nb + 1):
        for a in (1, 0):
            i = t + (done_t if a == 1 else 0)
            for j in range(n_shard):
                step = i - j
                if 0 <= step <= nb:
                    events.append(functools.partial(gather_event, a, j, step))
    for event in events:
        event()

    for a in (1, 0):
        for k in range(n_shard):
            for step in range(nb):
                for half in range(1 if step == 0 else 2):
                    send_reduce(a, k, half, step).wait_send()
            if k < n_shard - 1:
                send_line(a, k).wait_send()
        for half in range(2):
            for step in range(nb):
                g_step(a, half, step).wait_send()
        for way in ways:
            for k in range(n_shard - 1):
                @pl.when(goes(way, k))
                def _():
                    line(a, way, k).wait_send()

                @pl.when(comes(way, k))
                def _():
                    for half in range(2):
                        for step in range(nb):
                            plane(a, way, k, half, step).wait_send()
    assert len(sems.names) <= n_sems, len(sems.names)


def reduce_and_gather(parts, gain_part, moment_pieces, decay, n_rep, n_shard, collective_id):
    nb = n_rep.bit_length() - 1
    bits = (2,) * nb
    b16 = jnp.bfloat16
    shaped = [p.reshape((n_shard,) + bits + (p.shape[0] // n_shard // n_rep, p.shape[1])) for p in parts]
    pieces = [s.shape[-2:] for s in shaped]
    own = gain_part.shape[0] // n_shard
    gain3 = gain_part.reshape(n_shard, 1, own)
    vmem, any_ = pl.BlockSpec(memory_space=pltpu.VMEM), pl.BlockSpec(memory_space=pl.ANY)
    scratch = []
    for p in pieces:
        for j in range(nb):
            scratch.append(pltpu.VMEM((n_shard,) + (2,) * (nb - 1 - j) + p, b16))
    scratch += [pltpu.VMEM((n_shard,) + p, b16) for p in pieces]
    scratch += [pltpu.VMEM(p, b16) for p in pieces] * 2
    scratch += [pltpu.VMEM(gain3.shape, F32), pltpu.VMEM((nb,) + gain3.shape, F32), pltpu.VMEM(gain3.shape, F32)]
    n_sems = 2 * (n_shard * (1 + 2 * (nb - 1)) + (n_shard - 1) + 2 * nb + 2 * (n_shard - 1) * (1 + 2 * nb)) + nb + n_shard
    scratch += [pltpu.SemaphoreType.DMA((2,)), pltpu.SemaphoreType.DMA((n_sems,)), pltpu.SemaphoreType.DMA((n_sems,))]
    out = pl.pallas_call(
        functools.partial(reduce_kernel, n_rep, n_shard, decay, n_sems),
        out_shape=[jax.ShapeDtypeStruct(bits + p, b16) for p in pieces]
        + [jax.ShapeDtypeStruct(s.shape, b16) for s in shaped]
        + [jax.ShapeDtypeStruct((1, own), F32)],
        in_specs=[vmem] * 5,
        out_specs=[any_] * 4 + [vmem],
        scratch_shapes=scratch,
        compiler_params=pltpu.CompilerParams(
            collective_id=collective_id, has_side_effects=True, vmem_limit_bytes=60 << 20
        ),
        name="reduce_and_gather",
    )(*shaped, gain3, *moment_pieces)
    g = [o.reshape(n_rep * p[0], p[1]) for o, p in zip(out[:2], pieces)]
    m = [o.reshape(q.shape) for o, q in zip(out[2:4], parts)]
    return g, m, out[4].reshape(own)


coef_a = 3.4445
coef_b = -4.775
coef_c = 2.0315
SWEEPS = 5
decay = 0.95
muon_rate = 0.02


def nt(left, right):
    return lax.dot_general(left, right, (((1,), (1,)), ((), ())), preferred_element_type=jnp.float32)


def tn(left, right):
    return lax.dot_general(left, right, (((0,), (0,)), ((), ())), preferred_element_type=jnp.float32)


def mm(left, right):
    return jnp.dot(left, right, preferred_element_type=jnp.float32)


def tiles(count, body):
    def one(i, carry):
        body(i)
        return carry

    lax.fori_loop(0, count, one, 0)


def span(i, size):
    return pl.ds(pl.multiple_of(i * size, size), size)


def total(x):
    return jnp.sum(jnp.sum(x, axis=1, keepdims=True), axis=0, keepdims=True)


class Iterate:
    def __init__(self, e, ebf, k, kbf, h, hbf, fbf):
        self.e, self.ebf, self.k, self.kbf, self.h, self.hbf, self.fbf = e, ebf, k, kbf, h, hbf, fbf
        self.n = e.shape[0]
        self.wide = min(512, self.n)
        self.diag = min(256, self.n)
        self.columns = [slice(c, c + self.wide) for c in range(0, self.n, self.wide)]
        self.squares = [slice(d, d + self.diag) for d in range(0, self.n, self.diag)]

    def eye(self):
        shape = (self.diag, self.diag)
        return lax.broadcasted_iota(jnp.int32, shape, 0) == lax.broadcasted_iota(jnp.int32, shape, 1)

    def trace(self, ref):
        mask = self.eye()
        return sum(total(jnp.where(mask, ref[d, d], 0.0)) for d in self.squares)

    def centre(self, s):
        shift = self.trace(self.e) * (1.0 / self.n)
        mask = self.eye()
        for d in self.squares:
            moved = self.e[d, d] - jnp.where(mask, shift, 0.0)
            self.e[d, d] = moved
            self.ebf[d, d] = moved.astype(jnp.bfloat16)
        return s + shift

    def start(self):
        norm = jnp.sqrt(self.trace(self.e)) + 1e-06
        scale = 1.0 / (norm * norm)
        for c in self.columns:
            x = self.e[:, c] * scale
            self.e[:, c] = x
            self.ebf[:, c] = x.astype(jnp.bfloat16)
        return self.centre(jnp.zeros((1, 1), jnp.float32)), 1.0 / norm

    def polynomial(self, s, c):
        p1 = coef_b + 2.0 * coef_c * s
        f = p1 * self.e[:, c] + coef_c * mm(self.ebf[...], self.ebf[:, c])
        self.fbf[:, c] = f.astype(jnp.bfloat16)

    def first(self):
        for c in self.columns:
            f = self.fbf[:, c]
            self.h[:, c] = f.astype(jnp.float32)
            self.hbf[0, :, c] = f

    def grow(self, p0, q, c, now, later):
        new = p0 * self.h[:, c] + q * self.fbf[:, c].astype(jnp.float32) + mm(self.fbf[...], self.hbf[now, :, c])
        self.h[:, c] = new
        self.hbf[later, :, c] = new.astype(jnp.bfloat16)

    def inner(self, p0, s, c):
        new = p0 * self.e[:, c] + s * self.fbf[:, c].astype(jnp.float32) + mm(self.fbf[...], self.ebf[:, c])
        self.k[:, c] = new
        self.kbf[:, c] = new.astype(jnp.bfloat16)

    def outer(self, p0, beta, c):
        new = p0 * self.k[:, c] + beta * self.fbf[:, c].astype(jnp.float32) + mm(self.fbf[...], self.kbf[:, c])
        self.e[:, c] = new
        self.ebf[:, c] = new.astype(jnp.bfloat16)


def muon_kernel(*refs):
    m_in, m_out = refs[:2]
    g_in, g_out, moments = refs[2], refs[3], refs[4:8]
    grads_out, moments_out = refs[8:12], refs[12:16]
    h_out, hs_out, scal = refs[16:19]
    grads, news = refs[19:23], refs[23:27]
    tall, x, small_m, in_sem, out_sem = refs[27:32]
    big, small = Iterate(*refs[32:39]), Iterate(*refs[39:46])
    f32, b16 = jnp.float32, jnp.bfloat16
    core = lax.rem(lax.axis_index("rep"), 2)
    shard = lax.axis_index("shard")
    n, ns = big.n, small.n
    own_in, own_out = g_in.shape[0], g_out.shape[0]
    columns = [(0, n), (n, ns), (n + ns, ns)]

    wide = pltpu.make_async_copy(m_in.at[:, pl.ds(0, n)], tall, in_sem.at[0])
    flat = pltpu.make_async_copy(m_out, x, in_sem.at[0])
    kv = pltpu.make_async_copy(m_in.at[:, pl.ds(pl.multiple_of(n + core * ns, 128), ns)], small_m, in_sem.at[1])

    @pl.when(core == 0)
    def _():
        wide.start()

    @pl.when(core != 0)
    def _():
        flat.start()

    kv.start()

    rows = 64
    copies = []
    for i in range(4):
        g, (at, width) = (g_in, columns[i]) if i < 3 else (g_out, (0, g_out.shape[1]))

        def update(j, i=i, g=g, at=at, width=width):
            r = span(j, rows)
            grad = g[r, at : at + width].astype(f32)
            grads[i][r, :] = grad
            news[i][r, :] = decay * moments[i][r, :] + grad

        tiles(g.shape[0] // rows, update)
        copies.append(pltpu.make_async_copy(grads[i], grads_out[i], out_sem.at[2 * i]))
        copies.append(pltpu.make_async_copy(news[i], moments_out[i], out_sem.at[2 * i + 1]))
        copies[-2].start()
        copies[-1].start()
    kv.wait()
    mine = span(shard, own_in)

    @pl.when(core == 0)
    def _():
        wide.wait()
        tall[mine, :] = news[0][...].astype(b16)
        small_m[mine, :] = news[1][...].astype(b16)
        tiles(tall.shape[0] // 256, lambda i: x.__setitem__((slice(None), span(i, 256)), tall[span(i, 256), :].T))

    @pl.when(core != 0)
    def _():
        flat.wait()
        x[span(shard, own_out), :] = news[3][...].astype(b16)
        small_m[mine, :] = news[2][...].astype(b16)

    tiles(n // big.wide, lambda j: big.e.__setitem__((slice(None), span(j, big.wide)), nt(x[...], x[span(j, big.wide), :])))
    small.e[...] = tn(small_m[...], small_m[...])
    s, inv = big.start()
    ss, sinv = small.start()

    def sweep(it, carry):
        s, q, ss, sq = carry
        now, later = lax.rem(it + 1, 2), lax.rem(it, 2)
        p0 = coef_a + s * (coef_b + coef_c * s)
        sp0 = coef_a + ss * (coef_b + coef_c * ss)

        def each(method, *args):
            for i, c in enumerate(big.columns):
                getattr(big, method)(*[a[0] for a in args], c, *extra)
                if i == 0:
                    for d in small.columns:
                        getattr(small, method)(*[a[1] for a in args], d, *extra)

        extra = ()
        each("polynomial", (s, ss))

        @pl.when(it == 0)
        def _():
            big.first()
            small.first()

        extra = (now, later)

        @pl.when(it > 0)
        def _():
            each("grow", (p0, sp0), (q, sq))

        extra = ()
        q, sq = p0 * q, sp0 * sq

        def advance():
            each("inner", (p0, sp0), (s, ss))
            beta, sbeta = p0 * s, sp0 * ss
            each("outer", (p0, sp0), (beta, sbeta))
            return big.centre(p0 * beta), small.centre(sp0 * sbeta)

        s, ss = lax.cond(it < SWEEPS - 1, advance, lambda: (s, ss))
        return s, q, ss, sq

    one = jnp.ones((1, 1), f32)
    s, q, ss, sq = lax.fori_loop(0, SWEEPS, sweep, (s, one, ss, one))
    last = (SWEEPS - 1) % 2
    h_out[...] = big.hbf[last]
    hs_out[...] = small.hbf[last]
    row = lax.broadcasted_iota(jnp.int32, (8, 128), 0)
    scal[...] = jnp.where(row == 0, q * inv, jnp.where(row == 1, inv, jnp.where(row == 2, sq * sinv, sinv)))
    for copy in copies:
        copy.wait()


def muon(m_in, m_out, g_in, g_out, moments):
    f32, b16 = jnp.float32, jnp.bfloat16
    tall, n, kv = m_in.shape[0], m_out.shape[0], moments[1].shape[1]
    V = pltpu.VMEM
    sets = []
    for d in (n, kv):
        sets += [V((d, d), f32), V((d, d), b16), V((d, d), f32), V((d, d), b16), V((d, d), f32), V((2, d, d), b16), V((d, d), b16)]
    vmem, any_ = pl.BlockSpec(memory_space=pltpu.VMEM), pl.BlockSpec(memory_space=pl.ANY)
    own = [jax.ShapeDtypeStruct(m.shape, f32) for m in moments]
    out = pl.pallas_call(
        muon_kernel,
        out_shape=own
        + own
        + [
            jax.ShapeDtypeStruct((n, n), b16),
            jax.ShapeDtypeStruct((kv, kv), b16),
            jax.ShapeDtypeStruct((8, 128), f32),
        ],
        in_specs=[any_] * 2 + [vmem] * 6,
        out_specs=[any_] * 8 + [vmem] * 3,
        scratch_shapes=[V(m.shape, f32) for m in moments] * 2
        + [
            V((tall, n), b16),
            V(m_out.shape, b16),
            V((tall, kv), b16),
            pltpu.SemaphoreType.DMA((2,)),
            pltpu.SemaphoreType.DMA((8,)),
        ]
        + sets,
        compiler_params=pltpu.CompilerParams(vmem_limit_bytes=63 << 20),
        name="muon",
    )(m_in, m_out, g_in, g_out, *moments)
    return out[:4], out[4:8], out[8:]


def swap_kernel(n_rep, h, hs, scal, h_pair, hs_come, scal_come, send, recv):
    rep, shard = lax.axis_index("rep"), lax.axis_index("shard")
    core = lax.rem(rep, 2)
    other = rep + 1 - 2 * core
    sem = pltpu.get_barrier_semaphore()
    pl.semaphore_signal(sem, 1, device_id=(other, shard), device_id_type=pl.DeviceIdType.MESH)
    pl.semaphore_wait(sem, 1)

    def remote(src, dst, i):
        return pltpu.make_async_remote_copy(
            src, dst, send.at[i], recv.at[i], device_id=(other, shard), device_id_type=pl.DeviceIdType.MESH
        )

    count = h_pair.shape[0]
    at = jnp.where(core == 0, lax.div(rep, 2), shard)
    copies = [remote(h.at[span(at, count), :], h_pair, 0), remote(hs, hs_come, 1), remote(scal, scal_come, 2)]
    for c in copies:
        c.start()
    for c in copies:
        c.wait()


def swap(h, hs, scal, count, n_rep, collective_id):
    any_ = pl.BlockSpec(memory_space=pl.ANY)
    return pl.pallas_call(
        functools.partial(swap_kernel, n_rep),
        out_shape=[
            jax.ShapeDtypeStruct((count, h.shape[1]), h.dtype),
            jax.ShapeDtypeStruct(hs.shape, hs.dtype),
            jax.ShapeDtypeStruct(scal.shape, scal.dtype),
        ],
        in_specs=[any_] * 3,
        out_specs=[any_] * 3,
        scratch_shapes=[pltpu.SemaphoreType.DMA((3,)), pltpu.SemaphoreType.DMA((3,))],
        compiler_params=pltpu.CompilerParams(collective_id=collective_id, has_side_effects=True),
        name="swap",
    )(h, hs, scal)


def window(index, width):
    size = max(width, 128)
    start = lax.div(index * width, size) * size
    return pl.ds(pl.multiple_of(start, 128), size), size, index * width - start


def cut(x, size, offset, width):
    return x if size == width else pltpu.roll(x, lax.rem(size - offset, size), 1)[:, :width]


def update_kernel(h, h_pair, hs, hs_come, scal, scal_come, m_out, mq, mk, mv, mo, wq, wk, wv, wo, *refs):
    nexts, (hq, ho, flat, mo_win), weight_wins, (h_sem, sem) = refs[:4], refs[4:8], refs[8:12], refs[12:]
    f32, b16 = jnp.float32, jnp.bfloat16
    rep, shard = lax.axis_index("rep"), lax.axis_index("shard")
    even = lax.rem(rep, 2) == 0
    widths = [o.shape[1] for o in nexts]
    wins = [window(rep, w) for w in widths]
    own_out = ho.shape[0]
    copies = [
        pltpu.make_async_copy(m_out.at[:, wins[3][0]], flat, sem.at[4]),
        pltpu.make_async_copy(mo.at[:, wins[3][0]], mo_win, sem.at[5]),
    ] + [pltpu.make_async_copy(w.at[:, wins[i][0]], weight_wins[i], sem.at[i]) for i, w in enumerate((wq, wk, wv, wo))]
    for copy in copies:
        copy.start()
    rows_q = h.at[span(rep, widths[0]), :], h_pair.at[pl.ds(h_pair.shape[0] - widths[0], widths[0]), :]
    rows_o = h_pair, h.at[span(shard, own_out), :]
    mixes = [[pltpu.make_async_copy(a, b, h_sem.at[i]) for i, (a, b) in enumerate(((q, hq), (o, ho)))] for q, o in zip(rows_q, rows_o)]
    for side, here in ((0, even), (1, jnp.logical_not(even))):
        @pl.when(here)
        def _():
            for copy in mixes[side]:
                copy.start()
            for copy in mixes[side]:
                copy.wait()
    for copy in copies:
        copy.wait()
    first = jnp.where(even, scal[...], scal_come[...])
    second = jnp.where(even, scal_come[...], scal[...])
    flat[span(shard, own_out), :] = mo_win[...].astype(b16)

    def rows_of(i):
        at = span(rep, widths[i])
        mine, theirs = hs[at, :].astype(f32), hs_come[at, :].astype(f32)
        return jnp.where(even == (i == 1), mine, theirs).astype(b16)

    parts = (
        (mq, lambda: nt(mq[...].astype(b16), hq[...]), first[0:1, 0:1], first[1:2, 0:1]),
        (mk, lambda: nt(mk[...].astype(b16), rows_of(1)), first[2:3, 0:1], first[3:4, 0:1]),
        (mv, lambda: nt(mv[...].astype(b16), rows_of(2)), second[2:3, 0:1], second[3:4, 0:1]),
        (None, lambda: mm(ho[...], flat[...]), second[0:1, 0:1], second[1:2, 0:1]),
    )
    n_shard = lax.axis_size("shard")
    for i, (moment, product, straight, mixed) in enumerate(parts):
        at, size, offset = wins[i]
        here = mo_win[...] if moment is None else cut(moment[:, at], size, offset, widths[i])
        ortho = straight * here + mixed * product()
        whole = (weight_wins[i].shape[0] * n_shard, (wq, wk, wv, wo)[i].shape[1])
        weight = cut(weight_wins[i][...], size, offset, widths[i])
        nexts[i][...] = weight - muon_rate * math.sqrt(max(whole)) * ortho


def update(h, hs, scal, m_out, moments, weights, n_rep, collective_id):
    f32, b16 = jnp.float32, jnp.bfloat16
    widths = [w.shape[1] // n_rep for w in weights]
    own_out = weights[3].shape[0]
    assert 2 * widths[0] == own_out
    h_pair, hs_come, scal_come = swap(h, hs, scal, own_out, n_rep, collective_id)
    vmem, any_ = pl.BlockSpec(memory_space=pltpu.VMEM), pl.BlockSpec(memory_space=pl.ANY)
    V = pltpu.VMEM
    sizes = [max(w, 128) for w in widths]
    return pl.pallas_call(
        update_kernel,
        out_shape=[jax.ShapeDtypeStruct((w.shape[0], width), f32) for w, width in zip(weights, widths)],
        in_specs=[any_] * 2 + [vmem] * 4 + [any_] + [vmem] * 3 + [any_] * 5,
        out_specs=[vmem] * 4,
        scratch_shapes=[
            V((widths[0], h.shape[1]), b16),
            V((own_out, h.shape[1]), b16),
            V((m_out.shape[0], sizes[3]), b16),
            V((own_out, sizes[3]), f32),
        ]
        + [V((w.shape[0], size), f32) for w, size in zip(weights, sizes)]
        + [pltpu.SemaphoreType.DMA((2,)), pltpu.SemaphoreType.DMA((6,))],
        name="update",
    )(h, h_pair, hs, hs_come, scal, scal_come, m_out, *moments, *weights)


HEAD_SIZE = 64
TILE = 256
norm_eps = 1e-05
rope_base = 500000.0


def swap_halves(x):
    half, width = HEAD_SIZE // 2, x.shape[1]
    lane = lax.rem(lax.broadcasted_iota(jnp.int32, x.shape, 1), HEAD_SIZE)
    return jnp.where(lane < half, pltpu.roll(x, width - half, 1), pltpu.roll(x, half, 1))


def block_kernel(
    tok, cot, w_in, w_out, gain, cosine, sine, bias,
    out, grad_tok, part_in, part_out, part_gain,
    xn, xnt, inv_ref, q, dattn, attn_t, attn, dq_t, dqkv, dxn, row_acc, kx, vx, kxt, vxt, dk_acc, dv_acc,
):
    f32, b16 = jnp.float32, jnp.bfloat16
    seq, width = tok.shape
    q_width = w_out.shape[0]
    kv_width = (w_in.shape[1] - q_width) // 2
    kv_heads = kv_width // HEAD_SIZE
    pair = 2 * HEAD_SIZE
    pairs = q_width // pair
    n_q, n_tok = q_width // TILE, seq // TILE
    scale = 1.0 / math.sqrt(HEAD_SIZE)
    rows = 64

    def norm(i):
        r = span(i, rows)
        x = tok[r, :].astype(f32)
        inv = lax.rsqrt(jnp.mean(x * x, -1, keepdims=True) + norm_eps)
        inv_ref[r, :] = jnp.broadcast_to(inv, (rows, 128))
        xn[r, :] = (x * inv * gain[...]).astype(b16)

    tiles(seq // rows, norm)

    def tables():
        c, s = cosine[...], sine[...]
        return jnp.concatenate([c] * (TILE // c.shape[1]), 1), jnp.concatenate([s] * (TILE // s.shape[1]), 1)

    def query(i):
        x = mm(xn[...], w_in[:, span(i, TILE)])
        c, s = tables()
        q[:, span(i, TILE)] = (x * c + swap_halves(x) * s).astype(b16)

    tiles(n_q, query)
    lane = lax.broadcasted_iota(jnp.int32, (seq, pair), 1)
    low = lane < HEAD_SIZE

    def split(x, into, into_t):
        for g in range(kv_heads):
            two = x[:, (g // 2) * pair : (g // 2 + 1) * pair].astype(f32)
            other = pltpu.roll(two, HEAD_SIZE, 1)
            first, second = (two, other) if g % 2 == 0 else (other, two)
            lo, hi = jnp.where(low, first, 0.0).astype(b16), jnp.where(low, 0.0, second).astype(b16)
            into[g, 0], into[g, 1] = lo, hi
            into_t[g, 0], into_t[g, 1] = lo.T, hi.T

    for first, into, into_t, turned in ((q_width, kx, kxt, True), (q_width + kv_width, vx, vxt, False)):
        x = mm(xn[...], w_in[:, pl.ds(first, kv_width)])
        if turned:
            c, s = tables()
            x = x * c + swap_halves(x) * s
        split(x.astype(b16), into, into_t)

    def head_grad(i):
        dattn[:, span(i, TILE)] = nt(cot[...], w_out[span(i, TILE), :]).astype(b16)

    tiles(n_q, head_grad)

    per_group = pairs // kv_heads

    def heads(p):
        g = lax.div(p, per_group)
        lanes = span(p, pair)

        @pl.when(lax.rem(p, per_group) == 0)
        def _():
            dk_acc[...] = jnp.zeros_like(dk_acc)
            dv_acc[...] = jnp.zeros_like(dv_acc)

        for b in range(n_tok):
            qs = slice(b * TILE, (b + 1) * TILE)
            ks = slice(max(b - 1, 0) * TILE, (b + 1) * TILE)
            q_b, d_b = q[qs, lanes], dattn[qs, lanes]
            mask = bias[ks, qs]
            a_t, dq = None, None
            for side in range(2):
                score = nt(kx[g, side, ks, :], q_b) * scale + mask
                grown = jnp.exp(score)
                prob = grown * (1.0 / jnp.sum(grown, 0, keepdims=True))
                prob_b = prob.astype(b16)
                dp = nt(vx[g, side, ks, :], d_b)
                inner = jnp.sum(prob * dp, 0, keepdims=True)
                ds = (prob * (dp - inner) * scale).astype(b16)
                dv_acc[side, ks, :] += mm(prob_b, d_b)
                dk_acc[side, ks, :] += mm(ds, q_b)
                a_part = mm(vxt[g, side, :, ks], prob_b)
                q_part = mm(kxt[g, side, :, ks], ds)
                a_t = a_part if a_t is None else a_t + a_part
                dq = q_part if dq is None else dq + q_part
            attn_t[lanes, qs] = a_t.astype(b16)
            attn[qs, lanes] = a_t.T.astype(b16)
            turned_back = dq.T
            c, s = cosine[qs, :], sine[qs, :]
            dqkv[qs, lanes] = (turned_back * c - swap_halves(turned_back) * s).astype(b16)

        @pl.when(lax.rem(p, per_group) == per_group - 1)
        def _():
            def joined(acc):
                return acc[0] + pltpu.roll(acc[1], HEAD_SIZE, 1)

            dk, dv = joined(dk_acc), joined(dv_acc)
            dk = dk * cosine[...] - swap_halves(dk) * sine[...]
            for x, first in ((dk, q_width), (dv, q_width + kv_width)):
                at = span(lax.div(g, 2) + first // pair, pair)
                odd = lax.rem(g, 2)

                @pl.when(odd == 0)
                def _():
                    dqkv[:, at] = x.astype(b16)

                @pl.when(odd == 1)
                def _():
                    high = pltpu.roll(x, HEAD_SIZE, 1)
                    dqkv[:, at] = jnp.where(low, dqkv[:, at].astype(f32), high).astype(b16)

    tiles(pairs, heads)

    def project(i):
        c = span(i, TILE)
        out[:, c] = (tok[:, c].astype(f32) + mm(attn[...], w_out[:, c])).astype(b16)
        part_out[:, c] = mm(attn_t[...], cot[:, c]).astype(b16)

    tiles(width // TILE, project)

    row_acc[...] = jnp.zeros_like(row_acc)

    def input_grad(i):
        c = span(i, TILE)
        part_in[c, :] = tn(xn[:, c], dqkv[...]).astype(b16)
        d = nt(dqkv[...], w_in[c, :])
        normed = tok[:, c].astype(f32) * inv_ref[:, :1]
        both = d * normed
        part_gain[:, c] = jnp.sum(both, 0, keepdims=True)
        d = d * gain[:, c]
        dxn[:, c] = d
        row_acc[...] += jnp.broadcast_to(jnp.sum(d * normed, 1, keepdims=True), row_acc.shape)

    tiles(width // TILE, input_grad)

    def last(i):
        r = span(i, rows)
        inv = inv_ref[r, :1]
        normed = tok[r, :].astype(f32) * inv
        mean = row_acc[r, :1] * (1.0 / width)
        grad_tok[r, :] = (cot[r, :].astype(f32) + inv * (dxn[r, :] - normed * mean)).astype(b16)

    tiles(seq // rows, last)


def block(tok, cot, seg, w_in, w_out, gain):
    f32, b16 = jnp.float32, jnp.bfloat16
    seq, width = tok.shape
    q_width = w_out.shape[0]
    kv_width = (w_in.shape[1] - q_width) // 2
    kv_heads = kv_width // HEAD_SIZE
    pair = 2 * HEAD_SIZE
    index = jnp.arange(seq, dtype=jnp.int32)
    start = jnp.sum((seg[None, :] < seg[:, None]).astype(jnp.int32), 1)
    position = (index - start).astype(f32)
    half = HEAD_SIZE // 2
    frequency = rope_base ** (-2.0 * jnp.arange(half, dtype=f32) / HEAD_SIZE)
    angles = position[:, None] * frequency[None, :]
    c, s = jnp.cos(angles), jnp.sin(angles)
    cosine, sine = jnp.concatenate([c] * 4, 1), jnp.concatenate([-s, s] * 2, 1)
    allowed = (index[:, None] <= index[None, :]) & (seg[None, :] == seg[:, None])
    bias = jnp.where(allowed, 0.0, -1e30).astype(f32)
    vmem = pl.BlockSpec(memory_space=pltpu.VMEM)
    V = pltpu.VMEM
    return pl.pallas_call(
        block_kernel,
        out_shape=[
            jax.ShapeDtypeStruct((seq, width), b16),
            jax.ShapeDtypeStruct((seq, width), b16),
            jax.ShapeDtypeStruct(w_in.shape, b16),
            jax.ShapeDtypeStruct(w_out.shape, b16),
            jax.ShapeDtypeStruct((1, width), f32),
        ],
        in_specs=[vmem] * 8,
        out_specs=[vmem] * 5,
        scratch_shapes=[
            V((seq, width), b16),
            V((8, 128), b16),
            V((seq, 128), f32),
            V((seq, q_width), b16),
            V((seq, q_width), b16),
            V((q_width, seq), b16),
            V((seq, q_width), b16),
            V((8, 128), f32),
            V((seq, q_width + 2 * kv_width), b16),
            V((seq, width), f32),
            V((seq, 128), f32),
            V((kv_heads, 2, seq, pair), b16),
            V((kv_heads, 2, seq, pair), b16),
            V((kv_heads, 2, pair, seq), b16),
            V((kv_heads, 2, pair, seq), b16),
            V((2, seq, pair), f32),
            V((2, seq, pair), f32),
        ],
        compiler_params=pltpu.CompilerParams(vmem_limit_bytes=63 << 20),
        name="block",
    )(tok, cot, w_in, w_out, gain[None], cosine, sine, bias)


gain_rate = 0.2


def rows_of(matrix, index, count):
    return lax.dynamic_slice_in_dim(matrix, index * count, count, 0)


def cols_of(matrix, index, count):
    return lax.dynamic_slice_in_dim(matrix, index * count, count, 1)


def on_device(
    tokens,
    segments,
    cotangent,
    gain,
    w_query,
    w_key,
    w_value,
    w_outproj,
    moment_gain,
    moment_query,
    moment_key,
    moment_value,
    moment_outproj,
):
    n_rep, n_shard = lax.axis_size("rep"), lax.axis_size("shard")
    total_tokens = tokens.shape[0] * tokens.shape[1] * n_rep * n_shard
    b16 = jnp.bfloat16
    w_in_bf = jnp.concatenate([w_query, w_key, w_value], 1).astype(b16)
    w_in_all, w_out_all, gain_all = gather_all(
        [w_in_bf, w_outproj.astype(b16)], lax.reduce_precision(gain, 8, 7), n_rep, n_shard, 0
    )
    result, grad_tokens, part_in, part_outproj, part_gain = block(
        tokens[0], cotangent[0], segments[0], w_in_all, w_out_all, gain_all
    )
    return finish(
        result, grad_tokens, part_in, part_outproj, part_gain[0], total_tokens, gain, (w_query, w_key, w_value, w_outproj),
        moment_gain, (moment_query, moment_key, moment_value, moment_outproj),
    )


def finish(result, grad_tokens, part_in, part_outproj, part_gain, total_tokens, gain, weights, moment_gain, moments):
    n_rep, n_shard = lax.axis_size("rep"), lax.axis_size("shard")
    rep_index = lax.axis_index("rep")
    in_piece = jnp.concatenate([rows_of(m, rep_index, m.shape[0] // n_rep) for m in moments[:3]], 1)
    out_piece = rows_of(moments[3], rep_index, moments[3].shape[0] // n_rep)
    (sum_in, sum_out), (m_in, m_out), grad_gain = reduce_and_gather(
        [part_in, part_outproj], part_gain, [in_piece, out_piece], decay, n_rep, n_shard, 1
    )
    moment_gain_next = decay * moment_gain + grad_gain
    gain_next = gain - gain_rate / math.sqrt(total_tokens) * moment_gain_next
    grads, moments_next, (mix, mix_kv, scales) = muon(m_in, m_out, sum_in, sum_out, moments)
    updated = update(mix, mix_kv, scales, m_out, moments_next, weights, n_rep, 2)
    return (
        result[None],
        grad_tokens[None],
        grad_gain,
        *grads,
        gain_next,
        *updated,
        moment_gain_next,
        *moments_next,
    )


def solution(mesh):
    in_specs = (
        P(("rep", "shard"), None, None),
        P(("rep", "shard"), None),
        P(("rep", "shard"), None, None),
        P("shard"),
        P("shard", None),
        P("shard", None),
        P("shard", None),
        P("shard", None),
        P("shard"),
        P("shard", None),
        P("shard", None),
        P("shard", None),
        P("shard", None),
    )
    out_specs = (
        P(("rep", "shard"), None, None),
        P(("rep", "shard"), None, None),
        P("shard"),
        P("shard", None),
        P("shard", None),
        P("shard", None),
        P("shard", None),
        P("shard"),
        P("shard", "rep"),
        P("shard", "rep"),
        P("shard", "rep"),
        P("shard", "rep"),
        P("shard"),
        P("shard", None),
        P("shard", None),
        P("shard", None),
        P("shard", None),
    )
    return jax.shard_map(on_device, mesh=mesh, in_specs=in_specs, out_specs=out_specs, check_vma=False)
```

```python
import functools
import math

import jax
import jax.numpy as jnp
from jax import lax
from jax.experimental import pallas as pl
from jax.experimental.pallas import tpu as pltpu
from jax.sharding import PartitionSpec as P

coef_a = 3.4445
coef_b = -4.775
coef_c = 2.0315
SWEEPS = 5
decay = 0.95
muon_rate = 0.02


def nt(left, right):
    return lax.dot_general(left, right, (((1,), (1,)), ((), ())), preferred_element_type=jnp.float32)


def tn(left, right):
    return lax.dot_general(left, right, (((0,), (0,)), ((), ())), preferred_element_type=jnp.float32)


def mm(left, right):
    return jnp.dot(left, right, preferred_element_type=jnp.float32)


def tiles(count, body):
    def one(i, carry):
        body(i)
        return carry

    lax.fori_loop(0, count, one, 0)


def span(i, size):
    return pl.ds(pl.multiple_of(i * size, size), size)


def total(x):
    return jnp.sum(jnp.sum(x, axis=1, keepdims=True), axis=0, keepdims=True)


class Iterate:
    def __init__(self, e, ebf, k, kbf, h, hbf, fbf):
        self.e, self.ebf, self.k, self.kbf, self.h, self.hbf, self.fbf = e, ebf, k, kbf, h, hbf, fbf
        self.n = e.shape[0]
        self.wide = min(512, self.n)
        self.diag = min(256, self.n)
        self.columns = [slice(c, c + self.wide) for c in range(0, self.n, self.wide)]
        self.squares = [slice(d, d + self.diag) for d in range(0, self.n, self.diag)]

    def eye(self):
        shape = (self.diag, self.diag)
        return lax.broadcasted_iota(jnp.int32, shape, 0) == lax.broadcasted_iota(jnp.int32, shape, 1)

    def trace(self, ref):
        mask = self.eye()
        return sum(total(jnp.where(mask, ref[d, d], 0.0)) for d in self.squares)

    def centre(self, s):
        shift = self.trace(self.e) * (1.0 / self.n)
        mask = self.eye()
        for d in self.squares:
            moved = self.e[d, d] - jnp.where(mask, shift, 0.0)
            self.e[d, d] = moved
            self.ebf[d, d] = moved.astype(jnp.bfloat16)
        return s + shift

    def start(self):
        norm = jnp.sqrt(self.trace(self.e)) + 1e-06
        scale = 1.0 / (norm * norm)
        for c in self.columns:
            x = self.e[:, c] * scale
            self.e[:, c] = x
            self.ebf[:, c] = x.astype(jnp.bfloat16)
        return self.centre(jnp.zeros((1, 1), jnp.float32)), 1.0 / norm

    def polynomial(self, s, c):
        p1 = coef_b + 2.0 * coef_c * s
        f = p1 * self.e[:, c] + coef_c * mm(self.ebf[...], self.ebf[:, c])
        self.fbf[:, c] = f.astype(jnp.bfloat16)

    def first(self):
        for c in self.columns:
            f = self.fbf[:, c]
            self.h[:, c] = f.astype(jnp.float32)
            self.hbf[0, :, c] = f

    def grow(self, p0, q, c, now, later):
        new = p0 * self.h[:, c] + q * self.fbf[:, c].astype(jnp.float32) + mm(self.fbf[...], self.hbf[now, :, c])
        self.h[:, c] = new
        self.hbf[later, :, c] = new.astype(jnp.bfloat16)

    def inner(self, p0, s, c):
        new = p0 * self.e[:, c] + s * self.fbf[:, c].astype(jnp.float32) + mm(self.fbf[...], self.ebf[:, c])
        self.k[:, c] = new
        self.kbf[:, c] = new.astype(jnp.bfloat16)

    def outer(self, p0, beta, c):
        new = p0 * self.k[:, c] + beta * self.fbf[:, c].astype(jnp.float32) + mm(self.fbf[...], self.kbf[:, c])
        self.e[:, c] = new
        self.ebf[:, c] = new.astype(jnp.bfloat16)


def muon_kernel(*refs):
    m_in, m_out = refs[:2]
    g_in, g_out, moments = refs[2], refs[3], refs[4:8]
    grads_out, moments_out = refs[8:12], refs[12:16]
    h_out, hs_out, scal = refs[16:19]
    grads, news = refs[19:23], refs[23:27]
    tall, lump, x, small_m, in_sem, out_sem = refs[27:33]
    big, small = Iterate(*refs[33:40]), Iterate(*refs[40:47])
    f32, b16 = jnp.float32, jnp.bfloat16
    core = lax.rem(lax.axis_index("rep"), 2)
    shard = lax.axis_index("shard")
    n, ns = big.n, small.n
    own_in = g_in.shape[0]
    n_rep, own_out, cols_out = g_out.shape
    columns = [(0, n), (n, ns), (n + ns, ns)]

    wide = pltpu.make_async_copy(m_in.at[:, pl.ds(0, n)], tall, in_sem.at[0])
    flat = pltpu.make_async_copy(m_out, lump, in_sem.at[0])
    kv = pltpu.make_async_copy(m_in.at[:, pl.ds(pl.multiple_of(n + core * ns, 128), ns)], small_m, in_sem.at[1])

    @pl.when(core == 0)
    def _():
        wide.start()

    @pl.when(core != 0)
    def _():
        flat.start()

    kv.start()

    rows = 64
    copies = []
    for i in range(4):
        if i < 3:
            def update(j, i=i, at=columns[i][0], width=columns[i][1]):
                r = span(j, rows)
                grad = g_in[r, at : at + width].astype(f32)
                grads[i][r, :] = grad
                news[i][r, :] = decay * moments[i][r, :] + grad

            tiles(own_in // rows, update)
        else:
            def update(r, i=i):
                at = span(r, cols_out)
                grad = g_out[r].astype(f32)
                grads[i][:, at] = grad
                news[i][:, at] = decay * moments[i][:, at] + grad

            tiles(n_rep, update)
        copies.append(pltpu.make_async_copy(grads[i], grads_out[i], out_sem.at[2 * i]))
        copies.append(pltpu.make_async_copy(news[i], moments_out[i], out_sem.at[2 * i + 1]))
        copies[-2].start()
        copies[-1].start()
    kv.wait()
    mine = span(shard, own_in)

    @pl.when(core == 0)
    def _():
        wide.wait()
        tall[mine, :] = news[0][...].astype(b16)
        small_m[mine, :] = news[1][...].astype(b16)
        tiles(tall.shape[0] // 256, lambda i: x.__setitem__((slice(None), span(i, 256)), tall[span(i, 256), :].T))

    @pl.when(core != 0)
    def _():
        flat.wait()
        for s in range(lump.shape[0]):
            tiles(n_rep, lambda r, s=s: x.__setitem__((slice(s * own_out, (s + 1) * own_out), span(r, cols_out)), lump[s, r]))
        x[span(shard, own_out), :] = news[3][...].astype(b16)
        small_m[mine, :] = news[2][...].astype(b16)

    tiles(n // big.wide, lambda j: big.e.__setitem__((slice(None), span(j, big.wide)), nt(x[...], x[span(j, big.wide), :])))
    small.e[...] = tn(small_m[...], small_m[...])
    s, inv = big.start()
    ss, sinv = small.start()

    def sweep(it, carry):
        s, q, ss, sq = carry
        now, later = lax.rem(it + 1, 2), lax.rem(it, 2)
        p0 = coef_a + s * (coef_b + coef_c * s)
        sp0 = coef_a + ss * (coef_b + coef_c * ss)

        def each(method, *args):
            for i, c in enumerate(big.columns):
                getattr(big, method)(*[a[0] for a in args], c, *extra)
                if i == 0:
                    for d in small.columns:
                        getattr(small, method)(*[a[1] for a in args], d, *extra)

        extra = ()
        each("polynomial", (s, ss))

        @pl.when(it == 0)
        def _():
            big.first()
            small.first()

        extra = (now, later)

        @pl.when(it > 0)
        def _():
            each("grow", (p0, sp0), (q, sq))

        extra = ()
        q, sq = p0 * q, sp0 * sq

        def advance():
            each("inner", (p0, sp0), (s, ss))
            beta, sbeta = p0 * s, sp0 * ss
            each("outer", (p0, sp0), (beta, sbeta))
            return big.centre(p0 * beta), small.centre(sp0 * sbeta)

        s, ss = lax.cond(it < SWEEPS - 1, advance, lambda: (s, ss))
        return s, q, ss, sq

    one = jnp.ones((1, 1), f32)
    s, q, ss, sq = lax.fori_loop(0, SWEEPS, sweep, (s, one, ss, one))
    last = (SWEEPS - 1) % 2
    h_out[...] = big.hbf[last]
    hs_out[...] = small.hbf[last]
    row = lax.broadcasted_iota(jnp.int32, (8, 128), 0)
    scal[...] = jnp.where(row == 0, q * inv, jnp.where(row == 1, inv, jnp.where(row == 2, sq * sinv, sinv)))
    for copy in copies:
        copy.wait()


def muon(m_in, m_out, g_in, g_out, moments):
    f32, b16 = jnp.float32, jnp.bfloat16
    tall, n, kv = m_in.shape[0], m_out.shape[0] * m_out.shape[2], moments[1].shape[1]
    V = pltpu.VMEM
    sets = []
    for d in (n, kv):
        sets += [V((d, d), f32), V((d, d), b16), V((d, d), f32), V((d, d), b16), V((d, d), f32), V((2, d, d), b16), V((d, d), b16)]
    vmem, any_ = pl.BlockSpec(memory_space=pltpu.VMEM), pl.BlockSpec(memory_space=pl.ANY)
    own = [jax.ShapeDtypeStruct(m.shape, f32) for m in moments]
    out = pl.pallas_call(
        muon_kernel,
        out_shape=own
        + own
        + [
            jax.ShapeDtypeStruct((n, n), b16),
            jax.ShapeDtypeStruct((kv, kv), b16),
            jax.ShapeDtypeStruct((8, 128), f32),
        ],
        in_specs=[any_] * 2 + [vmem] * 6,
        out_specs=[any_] * 8 + [vmem] * 3,
        scratch_shapes=[V(m.shape, f32) for m in moments] * 2
        + [
            V((tall, n), b16),
            V(m_out.shape, b16),
            V((n, m_out.shape[1] * m_out.shape[3]), b16),
            V((tall, kv), b16),
            pltpu.SemaphoreType.DMA((2,)),
            pltpu.SemaphoreType.DMA((8,)),
        ]
        + sets,
        compiler_params=pltpu.CompilerParams(vmem_limit_bytes=63 << 20),
        name="muon",
    )(m_in, m_out, g_in, g_out, *moments)
    return out[:4], out[4:8], out[8:]


def swap_kernel(n_rep, h, hs, scal, h_pair, hs_come, scal_come, send, recv):
    rep, shard = lax.axis_index("rep"), lax.axis_index("shard")
    core = lax.rem(rep, 2)
    other = rep + 1 - 2 * core
    sem = pltpu.get_barrier_semaphore()
    pl.semaphore_signal(sem, 1, device_id=(other, shard), device_id_type=pl.DeviceIdType.MESH)
    pl.semaphore_wait(sem, 1)

    def remote(src, dst, i):
        return pltpu.make_async_remote_copy(
            src, dst, send.at[i], recv.at[i], device_id=(other, shard), device_id_type=pl.DeviceIdType.MESH
        )

    count = h_pair.shape[0]
    at = jnp.where(core == 0, lax.div(rep, 2), shard)
    copies = [remote(h.at[span(at, count), :], h_pair, 0), remote(hs, hs_come, 1), remote(scal, scal_come, 2)]
    for c in copies:
        c.start()
    for c in copies:
        c.wait()


def swap(h, hs, scal, count, n_rep, collective_id):
    any_ = pl.BlockSpec(memory_space=pl.ANY)
    return pl.pallas_call(
        functools.partial(swap_kernel, n_rep),
        out_shape=[
            jax.ShapeDtypeStruct((count, h.shape[1]), h.dtype),
            jax.ShapeDtypeStruct(hs.shape, hs.dtype),
            jax.ShapeDtypeStruct(scal.shape, scal.dtype),
        ],
        in_specs=[any_] * 3,
        out_specs=[any_] * 3,
        scratch_shapes=[pltpu.SemaphoreType.DMA((3,)), pltpu.SemaphoreType.DMA((3,))],
        compiler_params=pltpu.CompilerParams(collective_id=collective_id, has_side_effects=True),
        name="swap",
    )(h, hs, scal)


def window(index, width):
    size = max(width, 128)
    start = lax.div(index * width, size) * size
    return pl.ds(pl.multiple_of(start, 128), size), size, index * width - start


def cut(x, size, offset, width):
    return x if size == width else pltpu.roll(x, lax.rem(size - offset, size), 1)[:, :width]


def update_kernel(h, h_pair, hs, hs_come, scal, scal_come, m_out, mq, mk, mv, mo, wq, wk, wv, wo, *refs):
    nexts, (hq, ho, flat, mo_win), weight_wins, (h_sem, sem) = refs[:4], refs[4:8], refs[8:12], refs[12:]
    f32, b16 = jnp.float32, jnp.bfloat16
    rep, shard = lax.axis_index("rep"), lax.axis_index("shard")
    even = lax.rem(rep, 2) == 0
    widths = [o.shape[1] for o in nexts]
    wins = [window(rep, w) for w in widths]
    own_out = ho.shape[0]
    copies = [
        pltpu.make_async_copy(m_out.at[:, rep], flat, sem.at[4]),
        pltpu.make_async_copy(mo.at[:, wins[3][0]], mo_win, sem.at[5]),
    ] + [pltpu.make_async_copy(w.at[:, wins[i][0]], weight_wins[i], sem.at[i]) for i, w in enumerate((wq, wk, wv, wo))]
    for copy in copies:
        copy.start()
    rows_q = h.at[span(rep, widths[0]), :], h_pair.at[pl.ds(h_pair.shape[0] - widths[0], widths[0]), :]
    rows_o = h_pair, h.at[span(shard, own_out), :]
    mixes = [[pltpu.make_async_copy(a, b, h_sem.at[i]) for i, (a, b) in enumerate(((q, hq), (o, ho)))] for q, o in zip(rows_q, rows_o)]
    for side, here in ((0, even), (1, jnp.logical_not(even))):
        @pl.when(here)
        def _():
            for copy in mixes[side]:
                copy.start()
            for copy in mixes[side]:
                copy.wait()
    for copy in copies:
        copy.wait()
    first = jnp.where(even, scal[...], scal_come[...])
    second = jnp.where(even, scal_come[...], scal[...])
    flat[shard] = mo_win[...].astype(b16)

    def rows_of(i):
        at = span(rep, widths[i])
        mine, theirs = hs[at, :].astype(f32), hs_come[at, :].astype(f32)
        return jnp.where(even == (i == 1), mine, theirs).astype(b16)

    parts = (
        (mq, lambda: nt(mq[...].astype(b16), hq[...]), first[0:1, 0:1], first[1:2, 0:1]),
        (mk, lambda: nt(mk[...].astype(b16), rows_of(1)), first[2:3, 0:1], first[3:4, 0:1]),
        (mv, lambda: nt(mv[...].astype(b16), rows_of(2)), second[2:3, 0:1], second[3:4, 0:1]),
        (None, lambda: mm(ho[...], flat[...].reshape(-1, flat.shape[2])), second[0:1, 0:1], second[1:2, 0:1]),
    )
    n_shard = lax.axis_size("shard")
    for i, (moment, product, straight, mixed) in enumerate(parts):
        at, size, offset = wins[i]
        here = mo_win[...] if moment is None else cut(moment[:, at], size, offset, widths[i])
        ortho = straight * here + mixed * product()
        whole = (weight_wins[i].shape[0] * n_shard, (wq, wk, wv, wo)[i].shape[1])
        weight = cut(weight_wins[i][...], size, offset, widths[i])
        nexts[i][...] = weight - muon_rate * math.sqrt(max(whole)) * ortho


def update(h, hs, scal, m_out, moments, weights, n_rep, collective_id):
    f32, b16 = jnp.float32, jnp.bfloat16
    widths = [w.shape[1] // n_rep for w in weights]
    own_out = weights[3].shape[0]
    assert 2 * widths[0] == own_out and m_out.shape[3] == widths[3]
    h_pair, hs_come, scal_come = swap(h, hs, scal, own_out, n_rep, collective_id)
    vmem, any_ = pl.BlockSpec(memory_space=pltpu.VMEM), pl.BlockSpec(memory_space=pl.ANY)
    V = pltpu.VMEM
    sizes = [max(w, 128) for w in widths]
    return pl.pallas_call(
        update_kernel,
        out_shape=[jax.ShapeDtypeStruct((w.shape[0], width), f32) for w, width in zip(weights, widths)],
        in_specs=[any_] * 2 + [vmem] * 4 + [any_] + [vmem] * 3 + [any_] * 5,
        out_specs=[vmem] * 4,
        scratch_shapes=[
            V((widths[0], h.shape[1]), b16),
            V((own_out, h.shape[1]), b16),
            V((m_out.shape[0],) + m_out.shape[2:], b16),
            V((own_out, sizes[3]), f32),
        ]
        + [V((w.shape[0], size), f32) for w, size in zip(weights, sizes)]
        + [pltpu.SemaphoreType.DMA((2,)), pltpu.SemaphoreType.DMA((6,))],
        name="update",
    )(h, h_pair, hs, hs_come, scal, scal_come, m_out, *moments, *weights)


HEAD_SIZE = 64
TILE = 256
norm_eps = 1e-05
rope_base = 500000.0
F32, B16 = jnp.float32, jnp.bfloat16
MESH = pl.DeviceIdType.MESH
WAYS = (1, -1)


class Links:
    def __init__(self, n_rep, n_shard, send, recv):
        self.n_bits, self.n_shard = n_rep.bit_length() - 1, n_shard
        self.rep, self.shard = lax.axis_index("rep"), lax.axis_index("shard")
        self.bits = [lax.rem(lax.div(self.rep, 1 << b), 2) for b in range(self.n_bits)]
        far = list(range(1, self.n_bits))
        self.orders = (far, far[::-1])
        self.send, self.recv, self.names = send, recv, {}

    def flip(self, bit):
        return self.rep + (1 << bit) * (1 - 2 * self.bits[bit])

    def barrier(self):
        sem = pltpu.get_barrier_semaphore()
        for b in range(self.n_bits):
            pl.semaphore_signal(sem, 1, device_id=(self.flip(b), self.shard), device_id_type=MESH)
        for k in range(1, self.n_shard):
            there = lax.rem(self.shard + k, self.n_shard)
            pl.semaphore_signal(sem, 1, device_id=(self.rep, there), device_id_type=MESH)
        pl.semaphore_wait(sem, self.n_bits + self.n_shard - 1)

    def where(self, free=()):
        return tuple(slice(None) if b in free else self.bits[b] for b in reversed(range(self.n_bits)))

    def remote(self, src, dst, name, rep, shard):
        i = self.names.setdefault(name, len(self.names))
        return pltpu.make_async_remote_copy(
            src, dst, self.send.at[i], self.recv.at[i], device_id=(rep, shard), device_id_type=MESH
        )

    def goes(self, way, k):
        q, there = self.shard - way * k, self.shard + way
        return (q >= 0) & (q < self.n_shard) & (there >= 0) & (there < self.n_shard)

    def comes(self, way, k):
        q = self.shard - way * (k + 1)
        return (q >= 0) & (q < self.n_shard)


class Gather:
    def __init__(self, links, name, full, half, first=None):
        self.links, self.name, self.full, self.half, self.first = links, name, full, half, first

    def line(self, way, k):
        at = self.full.at[(self.links.shard - way * k,) + self.links.where()]
        src = self.first if k == 0 and self.first is not None else at
        return self.links.remote(src, at, (self.name, "l", way, k), self.links.rep, self.links.shard + way)

    def came(self, way, k):
        at = self.full.at[(self.links.shard - way * (k + 1),) + self.links.where()]
        return self.links.remote(at, at, (self.name, "l", way, k), self.links.rep, self.links.shard)

    def plane(self, way, k, h, step):
        links = self.links
        order = links.orders[h] + [0]
        view = self.full.at[(links.shard - way * (k + 1),) + links.where(order[:step]) + self.half[h]]
        return links.remote(view, view, (self.name, "p", way, k, h, step), links.flip(order[step]), links.shard)

    def start(self):
        for way in WAYS:
            @pl.when(self.links.goes(way, 0))
            def _():
                self.line(way, 0).start()

    def event(self, k, step, then=None):
        links = self.links
        for way in WAYS:
            @pl.when(links.comes(way, k))
            def _():
                if step == 0:
                    self.came(way, k).wait_recv()
                    if k + 1 < links.n_shard - 1:
                        @pl.when(links.goes(way, k + 1))
                        def _():
                            self.line(way, k + 1).start()
                else:
                    for h in range(2):
                        self.plane(way, k, h, step - 1).wait_recv()
                if step < links.n_bits:
                    for h in range(2):
                        self.plane(way, k, h, step).start()
                elif then is not None:
                    then(links.shard - way * (k + 1))

    def drain(self):
        links = self.links
        for way in WAYS:
            for k in range(links.n_shard - 1):
                @pl.when(links.goes(way, k))
                def _():
                    self.line(way, k).wait_send()

                @pl.when(links.comes(way, k))
                def _():
                    for h in range(2):
                        for step in range(links.n_bits):
                            self.plane(way, k, h, step).wait_send()


class Reduce:
    def __init__(self, links, name, part, bufs, zbuf, gpiece, mpiece, moment, sums, wholes, half, keep_sem):
        self.links, self.name, self.part, self.bufs, self.zbuf = links, name, part, bufs, zbuf
        self.gpiece, self.mpiece, self.moment, self.sums, self.half = gpiece, mpiece, moment, sums, half
        self.whole = Gather(links, name + "m", wholes, half, mpiece)
        self.keep = lambda: pltpu.make_async_copy(gpiece, sums.at[links.where()], keep_sem)

    def dest(self, k):
        return lax.rem(self.links.shard + 1 + k, self.links.n_shard)

    def origin(self, k):
        return lax.rem(self.links.shard + self.links.n_shard - 1 - k, self.links.n_shard)

    def order(self, h):
        return [0] + self.links.orders[h]

    def cut(self, h, step):
        return (slice(None), slice(None)) if step == 0 else self.half[h]

    def send(self, k, h, step):
        links, o = self.links, self.order(h)
        bit = o[step]
        src = self.part if step == 0 else self.bufs[step - 1]
        left = sorted(o[step:], reverse=True)
        pick = tuple(1 - links.bits[bit] if b == bit else slice(None) for b in left)
        d, cut = self.dest(k), self.cut(h, step)
        into = self.bufs[step].at[(d,) + (slice(None),) * (links.n_bits - 1 - step) + cut]
        return links.remote(src.at[(d,) + pick + cut], into, (self.name, "r", k, h, step), links.flip(bit), links.shard)

    def add(self, k, h, step):
        links, o = self.links, self.order(h)
        src = self.part if step == 0 else self.bufs[step - 1]
        left = sorted(o[step:], reverse=True)
        others = [b for b in left if b != o[step]]
        d, cut = self.dest(k), self.cut(h, step)

        def one(i):
            at = {b: lax.rem(lax.div(i, 1 << (len(others) - 1 - n)), 2) for n, b in enumerate(others)}
            here = (d,) + tuple(at[b] for b in others) + cut
            there = (d,) + tuple(links.bits[b] if b == o[step] else at[b] for b in left) + cut
            both = src[there].astype(F32) + self.bufs[step][here].astype(F32)
            self.bufs[step][here] = both.astype(B16)

        if others:
            tiles(1 << len(others), one)
        else:
            one(0)

    def send_line(self, k):
        links, d = self.links, self.dest(k)
        return links.remote(self.bufs[-1].at[d], self.zbuf.at[links.shard], (self.name, "z", k), links.rep, d)

    def come_line(self, k):
        links, at = self.links, self.zbuf.at[self.origin(k)]
        return links.remote(at, at, (self.name, "z", k), links.rep, links.shard)

    def start(self, k):
        self.send(k, 0, 0).start()

    def event(self, k, step):
        last = self.links.n_bits - 1
        for h in range(1 if step == 0 else 2):
            self.send(k, h, step).wait_recv()
            self.add(k, h, step)
            if step == 0 and last > 0:
                self.send(k, 0, 1).start()
                self.send(k, 1, 1).start()
            elif step < last:
                self.send(k, h, step + 1).start()
        if step == last and k < self.links.n_shard - 1:
            self.send_line(k).start()

    def gather_sum(self, h, step):
        links = self.links
        order = links.orders[h] + [0]
        into = self.sums.at[links.where(order[:step]) + self.half[h]]
        src = self.gpiece.at[self.half[h]] if step == 0 else into
        return links.remote(src, into, (self.name, "g", h, step), links.flip(order[step]), links.shard)

    def finish(self, decay):
        links = self.links
        for k in range(links.n_shard - 1):
            self.come_line(k).wait_recv()
        acc = self.bufs[-1][links.shard].astype(F32)
        for k in range(links.n_shard - 1):
            acc = acc + self.zbuf[self.origin(k)].astype(F32)
        g = acc.astype(B16)
        self.gpiece[...] = g
        self.mpiece[...] = (decay * self.moment[...] + g.astype(F32)).astype(B16)
        self.whole.start()
        for h in range(2):
            self.gather_sum(h, 0).start()
        self.keep().start()

    def gather_event(self, i, step):
        if i > 0:
            self.whole.event(i - 1, step)
            return
        if step == 0:
            self.keep().wait()
        if step < self.links.n_bits:
            for h in range(2):
                self.gather_sum(h, step).wait_recv()
                if step + 1 < self.links.n_bits:
                    self.gather_sum(h, step + 1).start()

    def drain(self):
        links = self.links
        for k in range(links.n_shard):
            for step in range(links.n_bits):
                for h in range(1 if step == 0 else 2):
                    self.send(k, h, step).wait_send()
            if k < links.n_shard - 1:
                self.send_line(k).wait_send()
        for h in range(2):
            for step in range(links.n_bits):
                self.gather_sum(h, step).wait_send()
        self.whole.drain()


class GainSum:
    def __init__(self, links, acc, come, line):
        self.links, self.acc, self.come, self.line = links, acc, come, line

    def send(self, b):
        return self.links.remote(self.acc, self.come.at[b], ("gain", b), self.links.flip(b), self.links.shard)

    def send_line(self, k):
        links = self.links
        d = lax.rem(links.shard + 1 + k, links.n_shard)
        return links.remote(self.acc.at[d], self.line.at[links.shard], ("gainz", k), links.rep, d)

    def event(self, b):
        links = self.links
        self.send(b).wait()
        self.acc[...] = self.acc[...] + self.come[b]
        if b + 1 < links.n_bits:
            self.send(b + 1).start()
        else:
            for k in range(links.n_shard - 1):
                self.send_line(k).start()

    def end(self):
        links = self.links
        for k in range(links.n_shard - 1):
            self.send_line(k).wait_send()
            at = self.line.at[lax.rem(links.shard + links.n_shard - 1 - k, links.n_shard)]
            links.remote(at, at, ("gainz", k), links.rep, links.shard).wait_recv()
        acc = self.acc[links.shard]
        for q in range(links.n_shard):
            acc = jnp.where(links.shard == q, acc, acc + self.line[q])
        return acc


def swap_halves(x):
    half, width = HEAD_SIZE // 2, x.shape[1]
    lane = lax.rem(lax.broadcasted_iota(jnp.int32, x.shape, 1), HEAD_SIZE)
    return jnp.where(lane < half, pltpu.roll(x, width - half, 1), pltpu.roll(x, half, 1))


def flat(x):
    return x.reshape(-1, x.shape[-1])


def bits_of(r, n_bits):
    return tuple((r >> b) & 1 for b in reversed(range(n_bits)))


def layer_kernel(
    n_rep, n_shard, decay,
    tok, cot, seg_col, seg_row, frequency, gain, w_query, w_key, w_value, w_outproj, m_query, m_key, m_value, m_outproj,
    out, grad_tok, sums_in, sums_out, wholes_in, wholes_out, gain_out,
    w_in, w_out, gain_full, xn, inv_ref, q, dattn, attn_t, attn, dqkv, dxn, row_acc, kx, vx, kxt, vxt, dk_acc, dv_acc,
    bias, cosine, sine, inv_l, part_in, part_out, gain_acc, gain_come, gain_line, moment_in, moment_out,
    zbuf_in, gp_in, mp_in, zbuf_out, gp_out, mp_out, load_sem, keep_sem, send, recv, *bufs,
):
    seq, width = tok.shape
    q_width, kv_width = w_query.shape[1], w_key.shape[1]
    kv_heads = kv_width // HEAD_SIZE
    pair = 2 * HEAD_SIZE
    pairs = q_width // pair
    per_group = pairs // kv_heads
    n_tok = seq // TILE
    scale = 1.0 / math.sqrt(HEAD_SIZE)
    rows = 64
    nb = n_rep.bit_length() - 1
    own_in, own_out = width // n_shard, q_width // n_shard
    rows_in, cols_out = own_in // n_rep, width // n_rep
    spans_in = ((0, q_width), (q_width, kv_width), (q_width + kv_width, kv_width))

    links = Links(n_rep, n_shard, send, recv)
    me, rep = links.shard, links.rep
    all_in = w_in.shape[-1]
    half_in = [(slice(None), pl.ds(h * (all_in // 2), all_in // 2)) for h in range(2)]
    half_out = [(pl.ds(h * (own_out // 2), own_out // 2), slice(None)) for h in range(2)]
    get_in, get_out = Gather(links, "wi", w_in, half_in), Gather(links, "wo", w_out, half_out)
    sum_in = Reduce(links, "i", part_in, bufs[:nb], zbuf_in, gp_in, mp_in, moment_in, sums_in, wholes_in, half_in, keep_sem.at[0])
    sum_out = Reduce(links, "o", part_out, bufs[nb:], zbuf_out, gp_out, mp_out, moment_out, sums_out, wholes_out, half_out, keep_sem.at[1])
    sum_gain = GainSum(links, gain_acc, gain_come, gain_line)

    loads = [
        pltpu.make_async_copy(w, dxn.at[pl.ds(0, own_in), pl.ds(at, size)], load_sem.at[i])
        for i, ((at, size), w) in enumerate(zip(spans_in, (w_query, w_key, w_value)))
    ]
    for load in loads:
        load.start()
    links.barrier()
    for load in loads:
        load.wait()
    for r in range(n_rep):
        w_in[(me,) + bits_of(r, nb)] = dxn[r * rows_in : (r + 1) * rows_in, :all_in].astype(B16)
    get_in.start()
    load_out = pltpu.make_async_copy(w_outproj, dxn.at[pl.ds(0, own_out), :], load_sem.at[3])
    load_out.start()

    def gain_line_copy(way, k):
        at = gain_full.at[me - way * k]
        return links.remote(at, at, ("gf", way, k), rep, me + way)

    def gain_came(way, k):
        at = gain_full.at[me - way * (k + 1)]
        return links.remote(at, at, ("gf", way, k), rep, me)

    gain_full[me] = gain[...].astype(B16).astype(F32)
    load_out.wait()
    for r in range(n_rep):
        w_out[(me,) + bits_of(r, nb)] = dxn[:own_out, r * cols_out : (r + 1) * cols_out].astype(B16)
    for way in WAYS:
        @pl.when(links.goes(way, 0))
        def _():
            gain_line_copy(way, 0).start()
    get_out.start()
    loads = [
        pltpu.make_async_copy(m.at[span(rep, rows_in), :], moment_in.at[:, pl.ds(at, size)], load_sem.at[i])
        for i, ((at, size), m) in enumerate(zip(spans_in, (m_query, m_key, m_value)))
    ] + [pltpu.make_async_copy(m_outproj.at[:, span(rep, cols_out)], moment_out, load_sem.at[3])]
    for load in loads:
        load.start()

    def masks(i):
        r = span(i, rows)
        key = lax.broadcasted_iota(jnp.int32, (rows, seq), 0) + i * rows
        query = lax.broadcasted_iota(jnp.int32, (rows, seq), 1)
        seen = (key <= query) & (seg_col[r, :] == seg_row[...])
        bias[r, :] = jnp.where(seen, 0.0, -1e30)
        start = jnp.sum((seg_row[...] < seg_col[r, :]).astype(F32), 1, keepdims=True)
        at = lax.broadcasted_iota(jnp.int32, (rows, 1), 0) + i * rows
        angle = (at.astype(F32) - start) * frequency[...]
        lane = lax.rem(lax.broadcasted_iota(jnp.int32, (rows, pair), 1), HEAD_SIZE)
        cosine[r, :] = jnp.cos(angle)
        s = jnp.sin(angle)
        sine[r, :] = jnp.where(lane < HEAD_SIZE // 2, -s, s)
        x = tok[r, :].astype(F32)
        inv = lax.rsqrt(jnp.mean(x * x, -1, keepdims=True) + norm_eps)
        inv_ref[r, :] = jnp.broadcast_to(inv, (rows, 128))

    tiles(seq // rows, masks)

    for k in range(n_shard - 1):
        for way in WAYS:
            @pl.when(links.comes(way, k))
            def _():
                gain_came(way, k).wait_recv()
                if k + 1 < n_shard - 1:
                    @pl.when(links.goes(way, k + 1))
                    def _():
                        gain_line_copy(way, k + 1).start()

    def gains():
        return jnp.concatenate([gain_full[s] for s in range(n_shard)], 1)

    def norm(i):
        r = span(i, rows)
        xn[r, :] = (tok[r, :].astype(F32) * inv_ref[r, :1] * gains()).astype(B16)

    tiles(seq // rows, norm)

    def project(s, fresh=False):
        x = xn[:, span(s, own_in)]

        def columns(c):
            part = mm(x, flat(w_in[(s,) + (slice(None),) * (nb + 1) + (span(c, TILE),)]))
            at = span(c, TILE)
            dxn[:, at] = part if fresh else dxn[:, at] + part

        tiles(all_in // TILE, columns)

    project(me, True)
    items = [(get_in, k) for k in range(n_shard - 1)] + [(get_out, k) for k in range(n_shard - 1)]

    def gather_time(t):
        for i, (gather, k) in enumerate(items):
            if 0 <= t - i <= nb:
                gather.event(k, t - i, project if gather is get_in else None)

    first_phase = n_shard - 1 + nb
    for t in range(first_phase):
        gather_time(t)
    later = list(range(first_phase, len(items) + nb))

    def tables():
        c, s = cosine[...], sine[...]
        return jnp.concatenate([c] * (TILE // pair), 1), jnp.concatenate([s] * (TILE // pair), 1)

    def query_tile(i):
        at = span(i, TILE)
        x = dxn[:, at]
        c, s = tables()
        q[:, at] = (x * c + swap_halves(x) * s).astype(B16)

    tiles(q_width // TILE, query_tile)
    low = lax.broadcasted_iota(jnp.int32, (seq, pair), 1) < HEAD_SIZE

    def split(x, into, into_t):
        for g in range(kv_heads):
            two = x[:, (g // 2) * pair : (g // 2 + 1) * pair].astype(B16).astype(F32)
            other = pltpu.roll(two, HEAD_SIZE, 1)
            first, second = (two, other) if g % 2 == 0 else (other, two)
            lo, hi = jnp.where(low, first, 0.0).astype(B16), jnp.where(low, 0.0, second).astype(B16)
            into[g, 0], into[g, 1] = lo, hi
            into_t[g, 0], into_t[g, 1] = lo.T, hi.T

    for first, into, into_t, turned in ((q_width, kx, kxt, True), (q_width + kv_width, vx, vxt, False)):
        x = dxn[:, first : first + kv_width]
        if turned:
            c, s = tables()
            x = x * c + swap_halves(x) * s
        split(x, into, into_t)

    def blocks():
        for b in range(n_tok):
            yield slice(b * TILE, (b + 1) * TILE), slice(max(b - 1, 0) * TILE, (b + 1) * TILE)

    def forward(p):
        for i, t in enumerate(later):
            @pl.when(p == min(1 + (i * pairs) // (2 * len(later)) * 2, pairs - 1))
            def _():
                gather_time(t)

        g = lax.div(p, per_group)
        lanes = span(p, pair)
        for qs, ks in blocks():
            q_b, mask, a_t = q[qs, lanes], bias[ks, qs], None
            for side in range(2):
                grown = jnp.exp(nt(kx[g, side, ks, :], q_b) * scale + mask)
                inv = 1.0 / jnp.sum(grown, 0, keepdims=True)
                inv_l[p, side, :, qs] = inv
                part = mm(vxt[g, side, :, ks], (grown * inv).astype(B16))
                a_t = part if a_t is None else a_t + part
            attn_t[lanes, qs] = a_t.astype(B16)
            attn[qs, lanes] = a_t.T.astype(B16)

    tiles(pairs, forward)

    for r in range(n_rep):
        c = slice(r * cols_out, (r + 1) * cols_out)
        x = mm(attn_t[...], cot[:, c]).astype(B16)
        part_out[(slice(None),) + bits_of(r, nb)] = x.reshape(n_shard, own_out, cols_out)
    for k in range(n_shard):
        sum_out.start(k)

    def head_grad(s):
        x = None
        for r in range(n_rep):
            part = nt(cot[:, r * cols_out : (r + 1) * cols_out], w_out[(s,) + bits_of(r, nb)])
            x = part if x is None else x + part
        dattn[:, span(s, own_out)] = x.astype(B16)

    tiles(n_shard, head_grad)

    def reduce_time(who, t):
        for step in reversed(range(nb)):
            if 0 <= t - step < n_shard:
                who.event(t - step, step)

    out_times = list(range(n_shard + nb - 1))

    def backward(p):
        for t in out_times:
            @pl.when(p == min(2 + t, pairs - 1))
            def _():
                reduce_time(sum_out, t)

        g = lax.div(p, per_group)
        lanes = span(p, pair)

        @pl.when(lax.rem(p, per_group) == 0)
        def _():
            dk_acc[...] = jnp.zeros_like(dk_acc)
            dv_acc[...] = jnp.zeros_like(dv_acc)

        for qs, ks in blocks():
            q_b, d_b, mask, dq = q[qs, lanes], dattn[qs, lanes], bias[ks, qs], None
            for side in range(2):
                grown = jnp.exp(nt(kx[g, side, ks, :], q_b) * scale + mask)
                prob = grown * inv_l[p, side, :, qs]
                dp = nt(vx[g, side, ks, :], d_b)
                inner = jnp.sum(prob * dp, 0, keepdims=True)
                ds = (prob * (dp - inner) * scale).astype(B16)
                dv_acc[side, ks, :] += mm(prob.astype(B16), d_b)
                dk_acc[side, ks, :] += mm(ds, q_b)
                part = mm(kxt[g, side, :, ks], ds)
                dq = part if dq is None else dq + part
            x = dq.T
            dqkv[qs, lanes] = (x * cosine[qs, :] - swap_halves(x) * sine[qs, :]).astype(B16)

        @pl.when(lax.rem(p, per_group) == per_group - 1)
        def _():
            def joined(acc):
                return acc[0] + pltpu.roll(acc[1], HEAD_SIZE, 1)

            dk, dv = joined(dk_acc), joined(dv_acc)
            dk = dk * cosine[...] - swap_halves(dk) * sine[...]
            for x, first in ((dk, q_width), (dv, q_width + kv_width)):
                at = span(lax.div(g, 2) + first // pair, pair)
                odd = lax.rem(g, 2)

                @pl.when(odd == 0)
                def _():
                    dqkv[:, at] = x.astype(B16)

                @pl.when(odd == 1)
                def _():
                    high = pltpu.roll(x, HEAD_SIZE, 1)
                    dqkv[:, at] = jnp.where(low, dqkv[:, at].astype(F32), high).astype(B16)

    tiles(pairs, backward)

    def weight_grad(k):
        s = sum_in.dest(k)
        x = tn(xn[:, span(s, own_in)], dqkv[...]).astype(B16)
        part_in[s] = x.reshape((2,) * nb + (rows_in, all_in))
        sum_in.start(k)

    for k in range(n_shard):
        weight_grad(k)

    row_acc[...] = jnp.zeros_like(row_acc)

    def input_grad(s):
        c = slice(s * own_in, (s + 1) * own_in)
        d = nt(dqkv[...], flat(w_in[s]))
        normed = tok[:, c].astype(F32) * inv_ref[:, :1]
        gain_acc[s] = jnp.sum(d * normed, 0, keepdims=True)
        d = d * gain_full[s]
        dxn[:, c] = d
        row_acc[...] += jnp.broadcast_to(jnp.sum(d * normed, 1, keepdims=True), row_acc.shape)

    def token_grad(i):
        r = span(i, rows)
        inv = inv_ref[r, :1]
        normed = tok[r, :].astype(F32) * inv
        mean = row_acc[r, :1] * (1.0 / width)
        grad_tok[r, :] = (cot[r, :].astype(F32) + inv * (dxn[r, :] - normed * mean)).astype(B16)

    def output(r):
        c = slice(r * cols_out, (r + 1) * cols_out)
        x = mm(attn[...], flat(w_out[(slice(None),) + bits_of(r, nb)]))
        out[:, c] = (tok[:, c].astype(F32) + x).astype(B16)

    for load in loads:
        load.wait()
    input_grad(0)
    sum_out.finish(decay)
    for s in range(1, n_shard):
        input_grad(s)
        if s == n_shard // 2:
            reduce_time(sum_in, 0)
    sum_gain.send(0).start()
    reduce_time(sum_in, 1)
    tiles(seq // rows, token_grad)

    def gather_sums_time(who, t):
        for i in range(n_shard):
            if 0 <= t - i <= nb:
                who.gather_event(i, t - i)

    n_times = n_shard + nb
    for r in range(n_rep):
        output(r)
        if r == n_rep // 2:
            reduce_time(sum_in, 2)
            gather_sums_time(sum_out, 0)
    sum_gain.event(0)
    done = 1
    for t in range(3, n_shard + nb - 1):
        reduce_time(sum_in, t)
        if done < n_times:
            gather_sums_time(sum_out, done)
            done += 1
        if t - 2 < nb:
            sum_gain.event(t - 2)
    for b in range(max(n_shard + nb - 3, 1), nb):
        sum_gain.event(b)
    sum_in.finish(decay)
    gain_out[...] = sum_gain.end()
    for t in range(n_times):
        if done < n_times:
            gather_sums_time(sum_out, done)
            done += 1
        gather_sums_time(sum_in, t)

    for who in (get_in, get_out, sum_out, sum_in):
        who.drain()
    for way in WAYS:
        for k in range(n_shard - 1):
            @pl.when(links.goes(way, k))
            def _():
                gain_line_copy(way, k).wait_send()
    assert len(links.names) <= send.shape[0]


def layer(tok, cot, seg, gain, weights, moments, decay, n_rep, n_shard, collective_id):
    seq, width = tok.shape
    w_query, w_key, _, w_outproj = weights
    q_width, kv_width = w_query.shape[1], w_key.shape[1]
    all_in = q_width + 2 * kv_width
    kv_heads, pair = kv_width // HEAD_SIZE, 2 * HEAD_SIZE
    nb = n_rep.bit_length() - 1
    bits = (2,) * nb
    own_in, own_out = width // n_shard, q_width // n_shard
    piece_in, piece_out = (own_in // n_rep, all_in), (own_out, width // n_rep)
    half = HEAD_SIZE // 2
    frequency = rope_base ** (-2.0 * jnp.arange(half, dtype=F32) / HEAD_SIZE)
    frequency = jnp.concatenate([frequency] * (pair // half))[None]
    vmem, any_ = pl.BlockSpec(memory_space=pltpu.VMEM), pl.BlockSpec(memory_space=pl.ANY)
    V, D = pltpu.VMEM, pltpu.SemaphoreType.DMA
    n_sems = (
        2 * 2 * 2 * (n_shard - 1) * (1 + 2 * nb) + 2 * (n_shard * (1 + 2 * (nb - 1)) + n_shard - 1 + 2 * nb) + nb + 3 * n_shard
    )
    bufs = [V((n_shard,) + (2,) * (nb - 1 - j) + piece, B16) for piece in (piece_in, piece_out) for j in range(nb)]
    shape = jax.ShapeDtypeStruct
    return pl.pallas_call(
        functools.partial(layer_kernel, n_rep, n_shard, decay),
        out_shape=[
            shape((seq, width), B16),
            shape((seq, width), B16),
            shape(bits + piece_in, B16),
            shape(bits + piece_out, B16),
            shape((n_shard,) + bits + piece_in, B16),
            shape((n_shard,) + bits + piece_out, B16),
            shape((1, own_in), F32),
        ],
        in_specs=[vmem] * 6 + [any_] * 8,
        out_specs=[vmem] * 2 + [any_] * 4 + [vmem],
        scratch_shapes=[
            V((n_shard,) + bits + piece_in, B16),
            V((n_shard,) + bits + piece_out, B16),
            V((n_shard, 1, own_in), F32),
            V((seq, width), B16),
            V((seq, 128), F32),
            V((seq, q_width), B16),
            V((seq, q_width), B16),
            V((q_width, seq), B16),
            V((seq, q_width), B16),
            V((seq, all_in), B16),
            V((seq, width), F32),
            V((seq, 128), F32),
            V((kv_heads, 2, seq, pair), B16),
            V((kv_heads, 2, seq, pair), B16),
            V((kv_heads, 2, pair, seq), B16),
            V((kv_heads, 2, pair, seq), B16),
            V((2, seq, pair), F32),
            V((2, seq, pair), F32),
            V((seq, seq), F32),
            V((seq, pair), F32),
            V((seq, pair), F32),
            V((q_width // pair, 2, 1, seq), F32),
            V((n_shard,) + bits + piece_in, B16),
            V((n_shard,) + bits + piece_out, B16),
            V((n_shard, 1, own_in), F32),
            V((nb, n_shard, 1, own_in), F32),
            V((n_shard, 1, own_in), F32),
            V(piece_in, F32),
            V(piece_out, F32),
            V((n_shard,) + piece_in, B16),
            V(piece_in, B16),
            V(piece_in, B16),
            V((n_shard,) + piece_out, B16),
            V(piece_out, B16),
            V(piece_out, B16),
            D((4,)),
            D((2,)),
            D((n_sems,)),
            D((n_sems,)),
        ]
        + bufs,
        compiler_params=pltpu.CompilerParams(
            collective_id=collective_id, has_side_effects=True, vmem_limit_bytes=67_043_328
        ),
        name="layer",
    )(tok, cot, seg[:, None], seg[None], frequency, gain[None], *weights, *moments)


gain_rate = 0.2


def on_device(
    tokens,
    segments,
    cotangent,
    gain,
    w_query,
    w_key,
    w_value,
    w_outproj,
    moment_gain,
    moment_query,
    moment_key,
    moment_value,
    moment_outproj,
):
    n_rep, n_shard = lax.axis_size("rep"), lax.axis_size("shard")
    total_tokens = tokens.shape[0] * tokens.shape[1] * n_rep * n_shard
    weights = (w_query, w_key, w_value, w_outproj)
    moments = (moment_query, moment_key, moment_value, moment_outproj)
    result, grad_tokens, sum_in, sum_out, m_in, m_out, grad_gain = layer(
        tokens[0], cotangent[0], segments[0], gain, weights, moments, decay, n_rep, n_shard, 0
    )
    grad_gain = grad_gain[0]
    moment_gain_next = decay * moment_gain + grad_gain
    gain_next = gain - gain_rate / math.sqrt(total_tokens) * moment_gain_next
    own_out, cols_out = sum_out.shape[-2:]
    m_out = m_out.reshape(n_shard, n_rep, own_out, cols_out)
    all_in = sum_in.shape[-1]
    grads, moments_next, (mix, mix_kv, scales) = muon(
        m_in.reshape(-1, all_in), m_out, sum_in.reshape(-1, all_in), sum_out.reshape(n_rep, own_out, cols_out), moments
    )
    updated = update(mix, mix_kv, scales, m_out, moments_next, weights, n_rep, 1)
    return (
        result[None],
        grad_tokens[None],
        grad_gain,
        *grads,
        gain_next,
        *updated,
        moment_gain_next,
        *moments_next,
    )


def solution(mesh):
    in_specs = (
        P(("rep", "shard"), None, None),
        P(("rep", "shard"), None),
        P(("rep", "shard"), None, None),
        P("shard"),
        P("shard", None),
        P("shard", None),
        P("shard", None),
        P("shard", None),
        P("shard"),
        P("shard", None),
        P("shard", None),
        P("shard", None),
        P("shard", None),
    )
    out_specs = (
        P(("rep", "shard"), None, None),
        P(("rep", "shard"), None, None),
        P("shard"),
        P("shard", None),
        P("shard", None),
        P("shard", None),
        P("shard", None),
        P("shard"),
        P("shard", "rep"),
        P("shard", "rep"),
        P("shard", "rep"),
        P("shard", "rep"),
        P("shard"),
        P("shard", None),
        P("shard", None),
        P("shard", None),
        P("shard", None),
    )
    return jax.shard_map(on_device, mesh=mesh, in_specs=in_specs, out_specs=out_specs, check_vma=False)
```

```python
import functools
import math

import jax
import jax.numpy as jnp
import numpy as np
from jax import lax
from jax.experimental import pallas as pl
from jax.experimental.pallas import tpu as pltpu
from jax.sharding import PartitionSpec as P

coef_a = 3.4445
coef_b = -4.775
coef_c = 2.0315
SWEEPS = 5
decay = 0.95
muon_rate = 0.02


def nt(left, right):
    return lax.dot_general(left, right, (((1,), (1,)), ((), ())), preferred_element_type=jnp.float32)


def tn(left, right):
    return lax.dot_general(left, right, (((0,), (0,)), ((), ())), preferred_element_type=jnp.float32)


def mm(left, right):
    return jnp.dot(left, right, preferred_element_type=jnp.float32)


def tiles(count, body):
    def one(i, carry):
        body(i)
        return carry

    lax.fori_loop(0, count, one, 0)


def span(i, size):
    return pl.ds(pl.multiple_of(i * size, size), size)


def total(x):
    return jnp.sum(jnp.sum(x, axis=1, keepdims=True), axis=0, keepdims=True)


class Iterate:
    def __init__(self, e, ebf, k, kbf, h, hbf, fbf):
        self.e, self.ebf, self.k, self.kbf, self.h, self.hbf, self.fbf = e, ebf, k, kbf, h, hbf, fbf
        self.n = e.shape[0]
        self.wide = min(512, self.n)
        self.diag = min(256, self.n)
        self.columns = [slice(c, c + self.wide) for c in range(0, self.n, self.wide)]
        self.squares = [slice(d, d + self.diag) for d in range(0, self.n, self.diag)]

    def eye(self):
        shape = (self.diag, self.diag)
        return lax.broadcasted_iota(jnp.int32, shape, 0) == lax.broadcasted_iota(jnp.int32, shape, 1)

    def trace(self, ref):
        mask = self.eye()
        return sum(total(jnp.where(mask, ref[d, d], 0.0)) for d in self.squares)

    def centre(self, s):
        shift = self.trace(self.e) * (1.0 / self.n)
        mask = self.eye()
        for d in self.squares:
            moved = self.e[d, d] - jnp.where(mask, shift, 0.0)
            self.e[d, d] = moved
            self.ebf[d, d] = moved.astype(jnp.bfloat16)
        return s + shift

    def start(self):
        norm = jnp.sqrt(self.trace(self.e)) + 1e-06
        scale = 1.0 / (norm * norm)
        for c in self.columns:
            x = self.e[:, c] * scale
            self.e[:, c] = x
            self.ebf[:, c] = x.astype(jnp.bfloat16)
        return self.centre(jnp.zeros((1, 1), jnp.float32)), 1.0 / norm

    def polynomial(self, s, c):
        p1 = coef_b + 2.0 * coef_c * s
        f = p1 * self.e[:, c] + coef_c * mm(self.ebf[...], self.ebf[:, c])
        self.fbf[:, c] = f.astype(jnp.bfloat16)

    def first(self):
        for c in self.columns:
            f = self.fbf[:, c]
            self.h[:, c] = f.astype(jnp.float32)
            self.hbf[0, :, c] = f

    def grow(self, p0, q, c, now, later):
        new = p0 * self.h[:, c] + q * self.fbf[:, c].astype(jnp.float32) + mm(self.fbf[...], self.hbf[now, :, c])
        self.h[:, c] = new
        self.hbf[later, :, c] = new.astype(jnp.bfloat16)

    def inner(self, p0, s, c):
        new = p0 * self.e[:, c] + s * self.fbf[:, c].astype(jnp.float32) + mm(self.fbf[...], self.ebf[:, c])
        self.k[:, c] = new
        self.kbf[:, c] = new.astype(jnp.bfloat16)

    def outer(self, p0, beta, c):
        new = p0 * self.k[:, c] + beta * self.fbf[:, c].astype(jnp.float32) + mm(self.fbf[...], self.kbf[:, c])
        self.e[:, c] = new
        self.ebf[:, c] = new.astype(jnp.bfloat16)


def muon_kernel(*refs):
    refs = list(refs)

    def take(count):
        return [refs.pop(0) for _ in range(count)]

    m_in, m_out, *passed = take(4)
    g_in, g_out, *moments = take(6)
    grads_out, moments_out, passed_out = take(4), take(4), take(2)
    h_out, hs_out, scal = take(3)
    grads, news, held = take(4), take(4), take(2)
    sums_in, sums_out, tall, lump, x, small_m = take(6)
    in_sem, own_sem, out_sem, pass_sem = take(4)
    big, small = Iterate(*take(7)), Iterate(*take(7))
    f32, b16 = jnp.float32, jnp.bfloat16
    core = lax.rem(lax.axis_index("rep"), 2)
    shard = lax.axis_index("shard")
    n, ns = big.n, small.n
    own_in = g_in.shape[0]
    n_rep, own_out, cols_out = g_out.shape
    chunk, q_part, kv_part = (n + 2 * ns) // 2, n // 2, ns // 2
    firsts = [(0, q_part), (q_part, kv_part), (q_part + kv_part, kv_part)]

    wide = [
        pltpu.make_async_copy(m_in.at[:, pl.ds(c * chunk, q_part)], tall.at[:, pl.ds(c * q_part, q_part)], in_sem.at[c])
        for c in range(2)
    ]
    flat = pltpu.make_async_copy(m_out, lump, in_sem.at[0])
    kv = [
        pltpu.make_async_copy(
            m_in.at[:, pl.ds(pl.multiple_of(c * chunk + q_part + core * kv_part, 128), kv_part)],
            small_m.at[:, pl.ds(c * kv_part, kv_part)],
            in_sem.at[2 + c],
        )
        for c in range(2)
    ]
    own = [pltpu.make_async_copy(a, b, own_sem.at[i]) for i, (a, b) in enumerate(zip(moments, news))]
    own_sums = [pltpu.make_async_copy(g_in, sums_in, own_sem.at[4]), pltpu.make_async_copy(g_out, sums_out, own_sem.at[5])]
    passing = [pltpu.make_async_copy(a, b, pass_sem.at[i]) for i, (a, b) in enumerate(zip(passed, held))]
    leaving = [pltpu.make_async_copy(a, b, pass_sem.at[i]) for i, (a, b) in enumerate(zip(held, passed_out))]

    @pl.when(core == 0)
    def _():
        for copy in wide:
            copy.start()

    @pl.when(core != 0)
    def _():
        flat.start()

    for copy in kv + own_sums + own + passing:
        copy.start()

    mine = span(shard, own_in)
    rows = 64

    @pl.when(core == 0)
    def _():
        for copy in wide:
            copy.wait()
        tiles(tall.shape[0] // 256, lambda i: x.__setitem__((slice(None), span(i, 256)), tall[span(i, 256), :].T))

    @pl.when(core != 0)
    def _():
        flat.wait()
        for s in range(lump.shape[0]):
            tiles(n_rep, lambda r, s=s: x.__setitem__((slice(s * own_out, (s + 1) * own_out), span(r, cols_out)), lump[s, r]))

    for copy in kv + own_sums + own:
        copy.wait()
    for i in range(4):
        if i < 3:
            def update(j, i=i, first=firsts[i][0], width=firsts[i][1]):
                r = span(j, rows)
                for c in range(2):
                    at, to = c * chunk + first, slice(c * width, (c + 1) * width)
                    grad = sums_in[r, at : at + width].astype(f32)
                    grads[i][r, to] = grad
                    news[i][r, to] = decay * news[i][r, to] + grad

            tiles(own_in // rows, update)
        else:
            def update(r, i=i):
                at = span(r, cols_out)
                grad = sums_out[r].astype(f32)
                grads[i][:, at] = grad
                news[i][:, at] = decay * news[i][:, at] + grad

            tiles(n_rep, update)

    @pl.when(core == 0)
    def _():
        x[:, mine] = news[0][...].astype(b16).T
        small_m[mine, :] = news[1][...].astype(b16)

    @pl.when(core != 0)
    def _():
        x[span(shard, own_out), :] = news[3][...].astype(b16)
        small_m[mine, :] = news[2][...].astype(b16)

    copies = [
        pltpu.make_async_copy(a, b, out_sem.at[i])
        for i, (a, b) in enumerate(zip(grads + news, grads_out + moments_out))
    ]
    for copy in copies:
        copy.start()
    for a, b in zip(passing, leaving):
        a.wait()
        b.start()
    tiles(n // big.wide, lambda j: big.e.__setitem__((slice(None), span(j, big.wide)), nt(x[...], x[span(j, big.wide), :])))
    small.e[...] = tn(small_m[...], small_m[...])
    s, inv = big.start()
    ss, sinv = small.start()

    def sweep(it, carry):
        s, q, ss, sq = carry
        now, later = lax.rem(it + 1, 2), lax.rem(it, 2)
        p0 = coef_a + s * (coef_b + coef_c * s)
        sp0 = coef_a + ss * (coef_b + coef_c * ss)

        def each(method, *args):
            for i, c in enumerate(big.columns):
                getattr(big, method)(*[a[0] for a in args], c, *extra)
                if i == 0:
                    for d in small.columns:
                        getattr(small, method)(*[a[1] for a in args], d, *extra)

        extra = ()
        each("polynomial", (s, ss))

        @pl.when(it == 0)
        def _():
            big.first()
            small.first()

        extra = (now, later)

        @pl.when(it > 0)
        def _():
            each("grow", (p0, sp0), (q, sq))

        extra = ()
        q, sq = p0 * q, sp0 * sq

        def advance():
            each("inner", (p0, sp0), (s, ss))
            beta, sbeta = p0 * s, sp0 * ss
            each("outer", (p0, sp0), (beta, sbeta))
            return big.centre(p0 * beta), small.centre(sp0 * sbeta)

        s, ss = lax.cond(it < SWEEPS - 1, advance, lambda: (s, ss))
        return s, q, ss, sq

    one = jnp.ones((1, 1), f32)
    s, q, ss, sq = lax.fori_loop(0, SWEEPS, sweep, (s, one, ss, one))
    last = (SWEEPS - 1) % 2
    h_out[...] = big.hbf[last]
    hs_out[...] = small.hbf[last]
    row = lax.broadcasted_iota(jnp.int32, (8, 128), 0)
    scal[...] = jnp.where(row == 0, q * inv, jnp.where(row == 1, inv, jnp.where(row == 2, sq * sinv, sinv)))
    for copy in copies + leaving:
        copy.wait()


def muon(m_in, m_out, g_in, g_out, moments, passed):
    f32, b16 = jnp.float32, jnp.bfloat16
    tall, n, kv = m_in.shape[0], m_out.shape[0] * m_out.shape[2], moments[1].shape[1]
    V = pltpu.VMEM
    sets = []
    for d in (n, kv):
        sets += [V((d, d), f32), V((d, d), b16), V((d, d), f32), V((d, d), b16), V((d, d), f32), V((2, d, d), b16), V((d, d), b16)]
    vmem, any_ = pl.BlockSpec(memory_space=pltpu.VMEM), pl.BlockSpec(memory_space=pl.ANY)
    own = [jax.ShapeDtypeStruct(m.shape, f32) for m in moments]
    out = pl.pallas_call(
        muon_kernel,
        out_shape=own
        + own
        + [jax.ShapeDtypeStruct(p.shape, p.dtype) for p in passed]
        + [
            jax.ShapeDtypeStruct((n, n), b16),
            jax.ShapeDtypeStruct((kv, kv), b16),
            jax.ShapeDtypeStruct((8, 128), f32),
        ],
        in_specs=[any_] * 10,
        out_specs=[any_] * 10 + [vmem] * 3,
        scratch_shapes=[V(m.shape, f32) for m in moments] * 2
        + [V(p.shape, p.dtype) for p in passed]
        + [
            V(g_in.shape, b16),
            V(g_out.shape, b16),
            V((tall, n), b16),
            V(m_out.shape, b16),
            V((n, m_out.shape[1] * m_out.shape[3]), b16),
            V((tall, kv), b16),
            pltpu.SemaphoreType.DMA((4,)),
            pltpu.SemaphoreType.DMA((6,)),
            pltpu.SemaphoreType.DMA((8,)),
            pltpu.SemaphoreType.DMA((2,)),
        ]
        + sets,
        compiler_params=pltpu.CompilerParams(vmem_limit_bytes=63 << 20),
        name="muon",
    )(m_in, m_out, *passed, g_in, g_out, *moments)
    return out[:4], out[4:8], out[8:10], out[10:]


def swap_kernel(n_rep, h, hs, scal, h_pair, hs_come, scal_come, send, recv):
    rep, shard = lax.axis_index("rep"), lax.axis_index("shard")
    core = lax.rem(rep, 2)
    other = rep + 1 - 2 * core
    sem = pltpu.get_barrier_semaphore()
    pl.semaphore_signal(sem, 1, device_id=(other, shard), device_id_type=pl.DeviceIdType.MESH)
    pl.semaphore_wait(sem, 1)

    def remote(src, dst, i):
        return pltpu.make_async_remote_copy(
            src, dst, send.at[i], recv.at[i], device_id=(other, shard), device_id_type=pl.DeviceIdType.MESH
        )

    count = h_pair.shape[0]
    at = jnp.where(core == 0, lax.div(rep, 2), shard)
    copies = [remote(h.at[span(at, count), :], h_pair, 0), remote(hs, hs_come, 1), remote(scal, scal_come, 2)]
    for c in copies:
        c.start()
    for c in copies:
        c.wait()


def swap(h, hs, scal, count, n_rep, collective_id):
    any_ = pl.BlockSpec(memory_space=pl.ANY)
    return pl.pallas_call(
        functools.partial(swap_kernel, n_rep),
        out_shape=[
            jax.ShapeDtypeStruct((count, h.shape[1]), h.dtype),
            jax.ShapeDtypeStruct(hs.shape, hs.dtype),
            jax.ShapeDtypeStruct(scal.shape, scal.dtype),
        ],
        in_specs=[any_] * 3,
        out_specs=[any_] * 3,
        scratch_shapes=[pltpu.SemaphoreType.DMA((3,)), pltpu.SemaphoreType.DMA((3,))],
        compiler_params=pltpu.CompilerParams(collective_id=collective_id, has_side_effects=True),
        name="swap",
    )(h, hs, scal)


def window(index, width):
    size = max(width, 128)
    start = lax.div(index * width, size) * size
    return pl.ds(pl.multiple_of(start, 128), size), size, index * width - start


def cut(x, size, offset, width):
    return x if size == width else pltpu.roll(x, lax.rem(size - offset, size), 1)[:, :width]


def update_kernel(h, h_pair, hs, hs_come, scal, scal_come, m_out, mq, mk, mv, mo, wq, wk, wv, wo, *refs):
    nexts, (hq, ho, flat, mo_win), weight_wins, (h_sem, sem) = refs[:4], refs[4:8], refs[8:12], refs[12:]
    f32, b16 = jnp.float32, jnp.bfloat16
    rep, shard = lax.axis_index("rep"), lax.axis_index("shard")
    even = lax.rem(rep, 2) == 0
    widths = [nexts[0].shape[1], nexts[1].shape[0], nexts[2].shape[0], nexts[3].shape[1]]
    wins = [window(rep, w) for w in widths]
    own_out = ho.shape[0]
    copies = [
        pltpu.make_async_copy(m_out.at[:, rep], flat, sem.at[4]),
        pltpu.make_async_copy(mo.at[:, wins[3][0]], mo_win, sem.at[5]),
    ] + [pltpu.make_async_copy(w.at[:, wins[i][0]], weight_wins[i], sem.at[i]) for i, w in enumerate((wq, wk, wv, wo))]
    for copy in copies:
        copy.start()
    rows_q = h.at[span(rep, widths[0]), :], h_pair.at[pl.ds(h_pair.shape[0] - widths[0], widths[0]), :]
    rows_o = h_pair, h.at[span(shard, own_out), :]
    mixes = [[pltpu.make_async_copy(a, b, h_sem.at[i]) for i, (a, b) in enumerate(((q, hq), (o, ho)))] for q, o in zip(rows_q, rows_o)]
    for side, here in ((0, even), (1, jnp.logical_not(even))):
        @pl.when(here)
        def _():
            for copy in mixes[side]:
                copy.start()
            for copy in mixes[side]:
                copy.wait()
    for copy in copies:
        copy.wait()
    first = jnp.where(even, scal[...], scal_come[...])
    second = jnp.where(even, scal_come[...], scal[...])
    flat[shard] = mo_win[...].astype(b16)

    def rows_of(i):
        at = span(rep, widths[i])
        mine, theirs = hs[at, :].astype(f32), hs_come[at, :].astype(f32)
        return jnp.where(even == (i == 1), mine, theirs).astype(b16)

    parts = (
        (mq, lambda: nt(mq[...].astype(b16), hq[...]), first[0:1, 0:1], first[1:2, 0:1]),
        (mk, lambda: nt(rows_of(1), mk[...].astype(b16)), first[2:3, 0:1], first[3:4, 0:1]),
        (mv, lambda: nt(rows_of(2), mv[...].astype(b16)), second[2:3, 0:1], second[3:4, 0:1]),
        (None, lambda: mm(ho[...], flat[...].reshape(-1, flat.shape[2])), second[0:1, 0:1], second[1:2, 0:1]),
    )
    n_shard = lax.axis_size("shard")
    for i, (moment, product, straight, mixed) in enumerate(parts):
        at, size, offset = wins[i]

        def mine(x):
            x = cut(x, size, offset, widths[i])
            return x.T if i in (1, 2) else x

        here = mine(mo_win[...] if moment is None else moment[:, at])
        ortho = straight * here + mixed * product()
        whole = (weight_wins[i].shape[0] * n_shard, (wq, wk, wv, wo)[i].shape[1])
        nexts[i][...] = mine(weight_wins[i][...]) - muon_rate * math.sqrt(max(whole)) * ortho


def update(h, hs, scal, m_out, moments, weights, n_rep, collective_id):
    f32, b16 = jnp.float32, jnp.bfloat16
    widths = [w.shape[1] // n_rep for w in weights]
    own_out = weights[3].shape[0]
    assert 2 * widths[0] == own_out and m_out.shape[3] == widths[3]
    h_pair, hs_come, scal_come = swap(h, hs, scal, own_out, n_rep, collective_id)
    vmem, any_ = pl.BlockSpec(memory_space=pltpu.VMEM), pl.BlockSpec(memory_space=pl.ANY)
    V = pltpu.VMEM
    sizes = [max(w, 128) for w in widths]
    shapes = [(w.shape[0], width) for w, width in zip(weights, widths)]
    out = pl.pallas_call(
        update_kernel,
        out_shape=[jax.ShapeDtypeStruct(s[::-1] if i in (1, 2) else s, f32) for i, s in enumerate(shapes)],
        in_specs=[any_] * 2 + [vmem] * 4 + [any_] + [vmem] * 3 + [any_] * 5,
        out_specs=[vmem] * 4,
        scratch_shapes=[
            V((widths[0], h.shape[1]), b16),
            V((own_out, h.shape[1]), b16),
            V((m_out.shape[0],) + m_out.shape[2:], b16),
            V((own_out, sizes[3]), f32),
        ]
        + [V((w.shape[0], size), f32) for w, size in zip(weights, sizes)]
        + [pltpu.SemaphoreType.DMA((2,)), pltpu.SemaphoreType.DMA((6,))],
        name="update",
    )(h, h_pair, hs, hs_come, scal, scal_come, m_out, *moments, *weights)
    return out[0], out[1].T, out[2].T, out[3]


HEAD_SIZE = 64
TILE = 256
norm_eps = 1e-05
rope_base = 500000.0
F32, B16 = jnp.float32, jnp.bfloat16
MESH = pl.DeviceIdType.MESH
WAYS = (1, -1)


class Links:
    def __init__(self, n_rep, n_shard, send, recv):
        self.n_bits, self.n_shard = n_rep.bit_length() - 1, n_shard
        self.rep, self.shard = lax.axis_index("rep"), lax.axis_index("shard")
        self.bits = [lax.rem(lax.div(self.rep, 1 << b), 2) for b in range(self.n_bits)]
        far = list(range(1, self.n_bits))
        self.orders = (far, far[::-1])
        self.send, self.recv, self.names = send, recv, {}

    def flip(self, bit):
        return self.rep + (1 << bit) * (1 - 2 * self.bits[bit])

    def barrier(self):
        sem = pltpu.get_barrier_semaphore()
        for b in range(self.n_bits):
            pl.semaphore_signal(sem, 1, device_id=(self.flip(b), self.shard), device_id_type=MESH)
        for k in range(1, self.n_shard):
            there = lax.rem(self.shard + k, self.n_shard)
            pl.semaphore_signal(sem, 1, device_id=(self.rep, there), device_id_type=MESH)
        pl.semaphore_wait(sem, self.n_bits + self.n_shard - 1)

    def where(self, free=()):
        return tuple(slice(None) if b in free else self.bits[b] for b in reversed(range(self.n_bits)))

    def remote(self, src, dst, name, rep, shard):
        i = self.names.setdefault(name, len(self.names))
        return pltpu.make_async_remote_copy(
            src, dst, self.send.at[i], self.recv.at[i], device_id=(rep, shard), device_id_type=MESH
        )

    def goes(self, way, k):
        q, there = self.shard - way * k, self.shard + way
        return (q >= 0) & (q < self.n_shard) & (there >= 0) & (there < self.n_shard)

    def comes(self, way, k):
        q = self.shard - way * (k + 1)
        return (q >= 0) & (q < self.n_shard)


class Gather:
    def __init__(self, links, name, full, part, half, first=None):
        self.links, self.name, self.full, self.part, self.half, self.first = links, name, full, part, half, first

    def line(self, way, k):
        at = self.full.at[(self.links.shard - way * k,) + self.links.where() + self.part]
        src = self.first if k == 0 and self.first is not None else at
        return self.links.remote(src, at, (self.name, "l", way, k), self.links.rep, self.links.shard + way)

    def came(self, way, k):
        at = self.full.at[(self.links.shard - way * (k + 1),) + self.links.where() + self.part]
        return self.links.remote(at, at, (self.name, "l", way, k), self.links.rep, self.links.shard)

    def plane(self, way, k, h, step):
        links = self.links
        order = links.orders[h] + [0]
        view = self.full.at[(links.shard - way * (k + 1),) + links.where(order[:step]) + self.half[h]]
        return links.remote(view, view, (self.name, "p", way, k, h, step), links.flip(order[step]), links.shard)

    def start(self):
        for way in WAYS:
            @pl.when(self.links.goes(way, 0))
            def _():
                self.line(way, 0).start()

    def event(self, k, step, then=None):
        links = self.links
        for way in WAYS:
            @pl.when(links.comes(way, k))
            def _():
                if step == 0:
                    self.came(way, k).wait_recv()
                    if k + 1 < links.n_shard - 1:
                        @pl.when(links.goes(way, k + 1))
                        def _():
                            self.line(way, k + 1).start()
                for h in range(2):
                    if step > 0:
                        self.plane(way, k, h, step - 1).wait_recv()
                    if step < links.n_bits:
                        self.plane(way, k, h, step).start()
                if step == links.n_bits and then is not None:
                    then(links.shard - way * (k + 1))

    def drain(self):
        links = self.links
        for way in WAYS:
            for k in range(links.n_shard - 1):
                @pl.when(links.goes(way, k))
                def _():
                    self.line(way, k).wait_send()

                @pl.when(links.comes(way, k))
                def _():
                    for h in range(2):
                        for step in range(links.n_bits):
                            self.plane(way, k, h, step).wait_send()


class Reduce:
    def __init__(self, links, name, refs, region, half, keep_sem):
        self.links, self.name, self.region, self.half = links, name, region, half
        self.part, self.bufs, self.zbuf, self.gpiece, self.mpiece, self.moment, self.sums, wholes = refs
        self.whole = Gather(links, name + "m", wholes, region, half, self.mpiece.at[region])
        self.keep = lambda: pltpu.make_async_copy(
            self.gpiece.at[region], self.sums.at[links.where() + region], keep_sem
        )

    def dest(self, k):
        return lax.rem(self.links.shard + 1 + k, self.links.n_shard)

    def origin(self, k):
        return lax.rem(self.links.shard + self.links.n_shard - 1 - k, self.links.n_shard)

    def order(self, h):
        return [0] + self.links.orders[h]

    def cut(self, h, step):
        return self.region if step == 0 else self.half[h]

    def send(self, k, h, step):
        links, o = self.links, self.order(h)
        bit = o[step]
        src = self.part if step == 0 else self.bufs[step - 1]
        left = sorted(o[step:], reverse=True)
        pick = tuple(1 - links.bits[bit] if b == bit else slice(None) for b in left)
        d, cut = self.dest(k), self.cut(h, step)
        into = self.bufs[step].at[(d,) + (slice(None),) * (links.n_bits - 1 - step) + cut]
        return links.remote(src.at[(d,) + pick + cut], into, (self.name, "r", k, h, step), links.flip(bit), links.shard)

    def add(self, k, h, step):
        links, o = self.links, self.order(h)
        src = self.part if step == 0 else self.bufs[step - 1]
        left = sorted(o[step:], reverse=True)
        others = [b for b in left if b != o[step]]
        d, cut = self.dest(k), self.cut(h, step)

        def one(i):
            at = {b: lax.rem(lax.div(i, 1 << (len(others) - 1 - n)), 2) for n, b in enumerate(others)}
            here = (d,) + tuple(at[b] for b in others) + cut
            there = (d,) + tuple(links.bits[b] if b == o[step] else at[b] for b in left) + cut
            both = src[there].astype(F32) + self.bufs[step][here].astype(F32)
            self.bufs[step][here] = both.astype(B16)

        if others:
            tiles(1 << len(others), one)
        else:
            one(0)

    def send_line(self, k):
        links, d = self.links, self.dest(k)
        src, into = self.bufs[-1].at[(d,) + self.region], self.zbuf.at[(links.shard,) + self.region]
        return links.remote(src, into, (self.name, "z", k), links.rep, d)

    def come_line(self, k):
        links, at = self.links, self.zbuf.at[(self.origin(k),) + self.region]
        return links.remote(at, at, (self.name, "z", k), links.rep, links.shard)

    def start(self, k):
        self.send(k, 0, 0).start()

    def event(self, k, step):
        last = self.links.n_bits - 1
        for h in range(1 if step == 0 else 2):
            self.send(k, h, step).wait_recv()
            self.add(k, h, step)
            if step == 0 and last > 0:
                self.send(k, 0, 1).start()
                self.send(k, 1, 1).start()
            elif step < last:
                self.send(k, h, step + 1).start()
        if step == last and k < self.links.n_shard - 1:
            self.send_line(k).start()

    def gather_sum(self, h, step):
        links = self.links
        order = links.orders[h] + [0]
        into = self.sums.at[links.where(order[:step]) + self.half[h]]
        src = self.gpiece.at[self.half[h]] if step == 0 else into
        return links.remote(src, into, (self.name, "g", h, step), links.flip(order[step]), links.shard)

    def finish(self, decay):
        links = self.links
        for k in range(links.n_shard - 1):
            self.come_line(k).wait_recv()
        acc = self.bufs[-1][(links.shard,) + self.region].astype(F32)
        for k in range(links.n_shard - 1):
            acc = acc + self.zbuf[(self.origin(k),) + self.region].astype(F32)
        g = acc.astype(B16)
        self.gpiece[self.region] = g
        self.mpiece[self.region] = (decay * self.moment[self.region] + g.astype(F32)).astype(B16)
        self.whole.start()
        for h in range(2):
            self.gather_sum(h, 0).start()
        self.keep().start()

    def gather_event(self, i, step):
        if i > 0:
            self.whole.event(i - 1, step)
            return
        if step == 0:
            self.keep().wait()
        if step < self.links.n_bits:
            for h in range(2):
                self.gather_sum(h, step).wait_recv()
                if step + 1 < self.links.n_bits:
                    self.gather_sum(h, step + 1).start()

    def drain(self):
        links = self.links
        for k in range(links.n_shard):
            for step in range(links.n_bits):
                for h in range(1 if step == 0 else 2):
                    self.send(k, h, step).wait_send()
            if k < links.n_shard - 1:
                self.send_line(k).wait_send()
        for h in range(2):
            for step in range(links.n_bits):
                self.gather_sum(h, step).wait_send()
        self.whole.drain()


class GainSum:
    def __init__(self, links, acc, come, line):
        self.links, self.acc, self.come, self.line = links, acc, come, line

    def send(self, b):
        return self.links.remote(self.acc, self.come.at[b], ("gain", b), self.links.flip(b), self.links.shard)

    def send_line(self, k):
        links = self.links
        d = lax.rem(links.shard + 1 + k, links.n_shard)
        return links.remote(self.acc.at[d], self.line.at[links.shard], ("gainz", k), links.rep, d)

    def event(self, b):
        links = self.links
        self.send(b).wait()
        self.acc[...] = self.acc[...] + self.come[b]
        if b + 1 < links.n_bits:
            self.send(b + 1).start()
        else:
            for k in range(links.n_shard - 1):
                self.send_line(k).start()

    def end(self):
        links = self.links
        for k in range(links.n_shard - 1):
            self.send_line(k).wait_send()
            at = self.line.at[lax.rem(links.shard + links.n_shard - 1 - k, links.n_shard)]
            links.remote(at, at, ("gainz", k), links.rep, links.shard).wait_recv()
        acc = self.acc[links.shard]
        for q in range(links.n_shard):
            acc = jnp.where(links.shard == q, acc, acc + self.line[q])
        return acc


def swap_halves(x):
    half, width = HEAD_SIZE // 2, x.shape[1]
    lane = lax.rem(lax.broadcasted_iota(jnp.int32, x.shape, 1), HEAD_SIZE)
    return jnp.where(lane < half, pltpu.roll(x, width - half, 1), pltpu.roll(x, half, 1))


def flat(x):
    return x.reshape(-1, x.shape[-1])


def bits_of(r, n_bits):
    return tuple(lax.rem(lax.div(r, 1 << b), 2) if isinstance(r, jax.Array) else (r >> b) & 1 for b in reversed(range(n_bits)))


def layer_kernel(
    n_rep, n_shard, decay,
    tok_hbm, cot_hbm, seg_row, frequency, gain, w_query, w_key, w_value, w_outproj, m_query, m_key, m_value, m_outproj,
    out, grad_tok, sums_in, sums_out, wholes_in, wholes_out, gain_out,
    tok, cot, w_in, w_out, gain_full, xn, inv_ref, q, dattn, attn_t, attn, dqkv, dxn, row_acc, kx, vx, kxt, vxt, dk_acc, dv_acc,
    bias, cosine, sine, inv_l, part_in, part_out, gain_acc, gain_come, gain_line, moment_in, moment_out,
    zbuf_in, gp_in, mp_in, zbuf_out, gp_out, mp_out, load_sem, keep_sem, send, recv, *bufs,
):
    seq, width = tok.shape
    q_width, kv_width = w_query.shape[1], w_key.shape[1]
    kv_heads = kv_width // HEAD_SIZE
    pair = 2 * HEAD_SIZE
    pairs = q_width // pair
    per_group = pairs // kv_heads
    n_tok = seq // TILE
    scale = 1.0 / math.sqrt(HEAD_SIZE)
    rows = 64
    nb = n_rep.bit_length() - 1
    own_in, own_out = width // n_shard, q_width // n_shard
    rows_in, cols_out = own_in // n_rep, width // n_rep
    all_in = w_in.shape[-1]
    chunk, q_part, kv_part = all_in // 2, q_width // 2, kv_width // 2
    places = [
        (i, c * size, c * chunk + first, size)
        for c in range(2)
        for i, (first, size) in enumerate(((0, q_part), (q_part, kv_part), (q_part + kv_part, kv_part)))
    ]

    links = Links(n_rep, n_shard, send, recv)
    me, rep = links.shard, links.rep
    both = slice(None)
    part_cols = [(both, pl.ds(c * chunk, chunk)) for c in range(2)]
    half_cols = [[(both, pl.ds(c * chunk + h * (chunk // 2), chunk // 2)) for h in range(2)] for c in range(2)]
    half_in = [(both, pl.ds(h * chunk, chunk)) for h in range(2)]
    half_out = [(pl.ds(h * (own_out // 2), own_out // 2), both) for h in range(2)]
    get_in, get_out = Gather(links, "wi", w_in, (both, both), half_in), Gather(links, "wo", w_out, (both, both), half_out)
    refs_in = (part_in, bufs[:nb], zbuf_in, gp_in, mp_in, moment_in, sums_in, wholes_in)
    refs_out = (part_out, bufs[nb:], zbuf_out, gp_out, mp_out, moment_out, sums_out, wholes_out)
    sum_in = [Reduce(links, f"i{c}", refs_in, part_cols[c], half_cols[c], keep_sem.at[c]) for c in range(2)]
    sum_out = Reduce(links, "o", refs_out, (both, both), half_out, keep_sem.at[2])
    sum_gain = GainSum(links, gain_acc, gain_come, gain_line)

    ws, ms = (w_query, w_key, w_value), (m_query, m_key, m_value)
    loads = [
        pltpu.make_async_copy(ws[i].at[:, pl.ds(at, size)], dxn.at[pl.ds(0, own_in), pl.ds(to, size)], load_sem.at[n])
        for n, (i, at, to, size) in enumerate(places)
    ]
    early = [pltpu.make_async_copy(a, b, load_sem.at[7 + i]) for i, (a, b) in enumerate(((tok_hbm, tok), (cot_hbm, cot)))]
    for load in loads + early:
        load.start()
    links.barrier()

    def gain_line_copy(way, k):
        at = gain_full.at[me - way * k]
        return links.remote(gain if k == 0 else at, at, ("gf", way, k), rep, me + way)

    def gain_came(way, k):
        at = gain_full.at[me - way * (k + 1)]
        return links.remote(at, at, ("gf", way, k), rep, me)

    gain_full[me] = gain[...]
    for way in WAYS:
        @pl.when(links.goes(way, 0))
        def _():
            gain_line_copy(way, 0).start()
    for load in loads:
        load.wait()
    for r in range(n_rep):
        w_in[(me,) + bits_of(r, nb)] = dxn[r * rows_in : (r + 1) * rows_in, :all_in].astype(B16)
    get_in.start()
    load_out = pltpu.make_async_copy(w_outproj, dxn.at[pl.ds(0, own_out), :], load_sem.at[6])
    load_out.start()
    load_out.wait()
    for r in range(n_rep):
        w_out[(me,) + bits_of(r, nb)] = dxn[:own_out, r * cols_out : (r + 1) * cols_out].astype(B16)
    loads = [
        pltpu.make_async_copy(ms[i].at[span(rep, rows_in), pl.ds(at, size)], moment_in.at[:, pl.ds(to, size)], load_sem.at[n])
        for n, (i, at, to, size) in enumerate(places)
    ] + [pltpu.make_async_copy(m_outproj.at[:, span(rep, cols_out)], moment_out, load_sem.at[6])]
    for load in loads:
        load.start()

    row_acc[...] = jnp.broadcast_to(seg_row[...].astype(F32), (row_acc.shape[1], seq)).T
    own_seg = seg_row[...].astype(F32)

    def masks(i):
        r = span(i, rows)
        seg_col = row_acc[r, :1]
        key = lax.broadcasted_iota(jnp.int32, (rows, seq), 0) + i * rows
        query = lax.broadcasted_iota(jnp.int32, (rows, seq), 1)
        seen = (key <= query) & (seg_col == own_seg)
        bias[r, :] = jnp.where(seen, 0.0, -1e30)
        start = jnp.sum(jnp.where(own_seg < seg_col, 1.0, 0.0), 1, keepdims=True)
        at = lax.broadcasted_iota(jnp.int32, (rows, 1), 0) + i * rows
        angle = (at.astype(F32) - start) * frequency[...]
        lane = lax.rem(lax.broadcasted_iota(jnp.int32, (rows, pair), 1), HEAD_SIZE)
        cosine[r, :] = jnp.cos(angle)
        s = jnp.sin(angle)
        sine[r, :] = jnp.where(lane < HEAD_SIZE // 2, -s, s)
        x = tok[r, :].astype(F32)
        inv = lax.rsqrt(jnp.mean(x * x, -1, keepdims=True) + norm_eps)
        inv_ref[r, :] = jnp.broadcast_to(inv, (rows, 128))

    early[0].wait()
    tiles(seq // rows, masks)
    early[1].wait()

    for k in range(n_shard - 1):
        for way in WAYS:
            @pl.when(links.comes(way, k))
            def _():
                gain_came(way, k).wait_recv()
                if k + 1 < n_shard - 1:
                    @pl.when(links.goes(way, k + 1))
                    def _():
                        gain_line_copy(way, k + 1).start()

    def gains():
        return jnp.concatenate([gain_full[s] for s in range(n_shard)], 1)

    def norm(i):
        r = span(i, rows)
        xn[r, :] = (tok[r, :].astype(F32) * inv_ref[r, :1] * gains()).astype(B16)

    tiles(seq // rows, norm)

    def project(s, fresh=False):
        x = xn[:, span(s, own_in)]

        def columns(c):
            part = mm(x, flat(w_in[(s,) + (slice(None),) * (nb + 1) + (span(c, TILE),)]))
            at = span(c, TILE)
            dxn[:, at] = part if fresh else dxn[:, at] + part

        tiles(all_in // TILE, columns)

    project(me, True)
    items = [(get_in, k, k) for k in range(n_shard - 1)] + [(get_out, k, n_shard + k) for k in range(n_shard - 1)]

    def gather_time(t):
        for gather, k, at in items:
            if 0 <= t - at <= nb:
                gather.event(k, t - at, project if gather is get_in else None)

    first_phase = n_shard - 1 + nb
    for t in range(first_phase):
        gather_time(t)
        if t == 1:
            get_out.start()
    later = list(range(first_phase, items[-1][2] + nb + 1))

    def tables():
        c, s = cosine[...], sine[...]
        return jnp.concatenate([c] * (TILE // pair), 1), jnp.concatenate([s] * (TILE // pair), 1)

    def query_tile(i):
        per = q_part // TILE
        x = dxn[:, pl.ds(pl.multiple_of(lax.div(i, per) * chunk + lax.rem(i, per) * TILE, TILE), TILE)]
        c, s = tables()
        q[:, span(i, TILE)] = (x * c + swap_halves(x) * s).astype(B16) * B16(scale)

    tiles(q_width // TILE, query_tile)
    low = lax.broadcasted_iota(jnp.int32, (seq, pair), 1) < HEAD_SIZE

    def split(x, into, into_t, shrink):
        for g in range(kv_heads):
            two = x[:, (g // 2) * pair : (g // 2 + 1) * pair].astype(B16).astype(F32)
            other = pltpu.roll(two, HEAD_SIZE, 1)
            first, second = (two, other) if g % 2 == 0 else (other, two)
            sides = jnp.where(low, first, 0.0).astype(B16), jnp.where(low, 0.0, second).astype(B16)
            for b in range(n_tok):
                for side in range(2):
                    at = slice((2 * b + side) * TILE, (2 * b + side + 1) * TILE)
                    part = sides[side][b * TILE : (b + 1) * TILE]
                    into[g, at, :] = part
                    into_t[g, :, at] = part.T * B16(shrink)

    for first, into, into_t, turned in ((q_part, kx, kxt, True), (q_part + kv_part, vx, vxt, False)):
        x = jnp.concatenate([dxn[:, c * chunk + first : c * chunk + first + kv_part] for c in range(2)], 1)
        if turned:
            c, s = tables()
            x = x * c + swap_halves(x) * s
        split(x, into, into_t, scale if turned else 1.0)

    def blocks():
        for b in range(n_tok):
            first = max(b - 1, 0)
            yield b, slice(b * TILE, (b + 1) * TILE), slice(2 * first * TILE, 2 * (b + 1) * TILE), range(first, b + 1)

    def tile_of(x, j):
        return x[j * TILE : (j + 1) * TILE]

    together = 2

    def forward(i):
        for n, t in enumerate(later):
            @pl.when(i == min(1 + n, pairs // together))
            def _():
                gather_time(t)

        here = [(i * together + u, *block) for u in range(together) for block in blocks()]
        scores = [nt(kx[lax.div(p, per_group), rs, :], q[qs, span(p, pair)]) for p, b, qs, rs, keys in here]
        probs = []
        for (p, b, qs, rs, keys), score in zip(here, scores):
            grown = [
                jnp.exp(tile_of(score, 2 * j + side) + bias[key * TILE : (key + 1) * TILE, qs])
                for j, key in enumerate(keys)
                for side in range(2)
            ]
            inv = []
            for side in range(2):
                inv.append(1.0 / sum(jnp.sum(x, 0, keepdims=True) for x in grown[side::2]))
                inv_l[p, side, :, qs] = inv[side]
            probs.append(jnp.concatenate([(x * inv[j % 2]).astype(B16) for j, x in enumerate(grown)], 0))
        for (p, b, qs, rs, keys), prob in zip(here, probs):
            a_t = mm(vxt[lax.div(p, per_group), :, rs], prob)
            attn_t[span(p, pair), qs] = a_t.astype(B16)
            attn[qs, span(p, pair)] = a_t.T.astype(B16)

    tiles(pairs // together, forward)

    def out_grad(r):
        x = mm(attn_t[...], cot[:, span(r, cols_out)]).astype(B16)
        part_out[(slice(None),) + bits_of(r, nb)] = x.reshape(n_shard, own_out, cols_out)

    tiles(n_rep, out_grad)
    for k in range(n_shard):
        sum_out.start(k)
    for t in later[max(pairs // together - 1, 0) :]:
        gather_time(t)

    def head_grad(s):
        x = None
        for r in range(n_rep):
            part = nt(cot[:, r * cols_out : (r + 1) * cols_out], w_out[(s,) + bits_of(r, nb)])
            x = part if x is None else x + part
        dattn[:, span(s, own_out)] = x.astype(B16)

    tiles(n_shard, head_grad)

    def reduce_time(who, t):
        for step in reversed(range(nb)):
            if 0 <= t - step < n_shard:
                who.event(t - step, step)

    def weight_grad(c):
        cols = dqkv[:, c * chunk : (c + 1) * chunk]

        def one(k):
            s = sum_in[c].dest(k)
            x = tn(xn[:, span(s, own_in)], cols).astype(B16)
            part_in[(s,) + (both,) * nb + part_cols[c]] = x.reshape((2,) * nb + (rows_in, chunk))

        tiles(n_shard, one)
        for k in range(n_shard):
            sum_in[c].start(k)

    n_reduce, n_gather = n_shard + nb - 1, n_shard + nb

    in_loop = (2 * n_reduce) // 3

    def backward(p):
        for t in range(in_loop):
            @pl.when(p == 1 + (t * (pairs - 1)) // in_loop)
            def _():
                reduce_time(sum_out, t)

        @pl.when(p == pairs // 2)
        def _():
            weight_grad(0)

        g = lax.div(p, per_group)
        lanes = span(p, pair)

        @pl.when(lax.rem(p, per_group) == 0)
        def _():
            dk_acc[...] = jnp.zeros_like(dk_acc)
            dv_acc[...] = jnp.zeros_like(dv_acc)

        scores = [(nt(kx[g, rs, :], q[qs, lanes]), nt(vx[g, rs, :], dattn[qs, lanes])) for b, qs, rs, keys in blocks()]
        grads = []
        for (b, qs, rs, keys), (score, dp) in zip(blocks(), scores):
            prob = [
                jnp.exp(tile_of(score, 2 * j + side) + bias[key * TILE : (key + 1) * TILE, qs]) * inv_l[p, side, :, qs]
                for j, key in enumerate(keys)
                for side in range(2)
            ]
            inner = [
                sum(jnp.sum(x * tile_of(dp, 2 * j + side), 0, keepdims=True) for j, x in enumerate(prob[side::2]))
                for side in range(2)
            ]
            ds = [(x * (tile_of(dp, j) - inner[j % 2])).astype(B16) for j, x in enumerate(prob)]
            grads.append((jnp.concatenate([x.astype(B16) for x in prob], 0), jnp.concatenate(ds, 0)))
        for (b, qs, rs, keys), (prob, ds) in zip(blocks(), grads):
            dv_acc[rs, :] += mm(prob, dattn[qs, lanes])
            dk_acc[rs, :] += mm(ds, q[qs, lanes])
            x = mm(kxt[g, :, rs], ds).T
            half_pairs = pairs // 2
            to = lax.div(p, half_pairs) * chunk + lax.rem(p, half_pairs) * pair
            dqkv[qs, pl.ds(pl.multiple_of(to, pair), pair)] = (x * cosine[qs, :] - swap_halves(x) * sine[qs, :]).astype(B16)

        @pl.when(lax.rem(p, per_group) == per_group - 1)
        def _():
            def joined(acc):
                both = [acc[j * TILE : (j + 1) * TILE, :] for j in range(2 * n_tok)]
                return jnp.concatenate([both[2 * b] + pltpu.roll(both[2 * b + 1], HEAD_SIZE, 1) for b in range(n_tok)], 0)

            dk, dv = joined(dk_acc), joined(dv_acc)
            dk = dk * cosine[...] - swap_halves(dk) * sine[...]
            for x, first in ((dk, q_part), (dv, q_part + kv_part)):
                half_groups = kv_heads // 2
                to = lax.div(g, half_groups) * chunk + first + lax.div(lax.rem(g, half_groups), 2) * pair
                at = pl.ds(pl.multiple_of(to, pair), pair)
                odd = lax.rem(g, 2)

                @pl.when(odd == 0)
                def _():
                    dqkv[:, at] = x.astype(B16)

                @pl.when(odd == 1)
                def _():
                    high = pltpu.roll(x, HEAD_SIZE, 1)
                    dqkv[:, at] = jnp.where(low, dqkv[:, at].astype(F32), high).astype(B16)

    tiles(pairs, backward)

    weight_grad(1)
    for load in loads:
        load.wait()

    row_acc[...] = jnp.zeros_like(row_acc)

    def input_grad(s):
        c = slice(s * own_in, (s + 1) * own_in)
        d = nt(dqkv[...], flat(w_in[s]))
        normed = tok[:, c].astype(F32) * inv_ref[:, :1]
        gain_acc[s] = jnp.sum(d * normed, 0, keepdims=True)
        d = d * gain_full[s]
        dxn[:, c] = d
        row_acc[...] += jnp.broadcast_to(jnp.sum(d * normed, 1, keepdims=True), row_acc.shape)

    def token_grad(i):
        r = span(i, rows)
        inv = inv_ref[r, :1]
        normed = tok[r, :].astype(F32) * inv
        mean = row_acc[r, :1] * (1.0 / width)
        grad_tok[r, :] = (cot[r, :].astype(F32) + inv * (dxn[r, :] - normed * mean)).astype(B16)

    def output(r):
        c = span(r, cols_out)
        x = mm(attn[...], flat(w_out[(slice(None),) + bits_of(r, nb)]))
        out[:, c] = (tok[:, c].astype(F32) + x).astype(B16)

    def gather_sums_time(who, t):
        for i in range(n_shard):
            if 0 <= t - i <= nb:
                who.gather_event(i, t - i)

    todo = []

    def then(method, *args):
        todo.append(functools.partial(method, *args))

    def gain_end():
        gain_out[...] = sum_gain.end()

    out_end = n_reduce - in_loop
    for u in range(3 * n_gather + n_reduce):
        if u < out_end:
            then(reduce_time, sum_out, in_loop + u)
        if u < n_reduce:
            then(reduce_time, sum_in[0], u)
        if 0 <= u - 2 < n_reduce:
            then(reduce_time, sum_in[1], u - 2)
        if u == out_end + 1:
            then(sum_out.finish, decay)
        if u == n_reduce + 1:
            then(sum_in[0].finish, decay)
        if u == n_reduce + 3:
            then(sum_in[1].finish, decay)
        for who, lag in ((sum_in[0], n_reduce + 2), (sum_in[1], n_reduce + 4), (sum_out, out_end + 2)):
            if 0 <= u - lag < n_gather:
                then(gather_sums_time, who, u - lag)
        if 0 <= u - n_reduce - 3 < nb:
            then(sum_gain.event, u - n_reduce - 3)
        if u == n_reduce + nb + 4:
            then(gain_end)

    def advance():
        todo.pop(0)()

    for s in range(n_shard):
        advance()
        input_grad(s)
    sum_gain.send(0).start()
    advance()
    tiles(seq // rows, token_grad)
    advance()
    tiles(n_rep // 2, output)
    advance()
    tiles(n_rep // 2, lambda r: output(r + n_rep // 2))
    while todo:
        advance()

    for who in (get_in, get_out, sum_out, *sum_in):
        who.drain()
    for way in WAYS:
        for k in range(n_shard - 1):
            @pl.when(links.goes(way, k))
            def _():
                gain_line_copy(way, k).wait_send()
    assert len(links.names) <= send.shape[0]


def layer(tok, cot, seg, gain, weights, moments, decay, n_rep, n_shard, collective_id):
    seq, width = tok.shape
    w_query, w_key, _, w_outproj = weights
    q_width, kv_width = w_query.shape[1], w_key.shape[1]
    all_in = q_width + 2 * kv_width
    kv_heads, pair = kv_width // HEAD_SIZE, 2 * HEAD_SIZE
    nb = n_rep.bit_length() - 1
    bits = (2,) * nb
    own_in, own_out = width // n_shard, q_width // n_shard
    piece_in, piece_out = (own_in // n_rep, all_in), (own_out, width // n_rep)
    half = HEAD_SIZE // 2
    frequency = np.tile((rope_base ** (-2.0 * np.arange(half) / HEAD_SIZE)).astype(np.float32), pair // half)[None]
    vmem, any_ = pl.BlockSpec(memory_space=pltpu.VMEM), pl.BlockSpec(memory_space=pl.ANY)
    V, D = pltpu.VMEM, pltpu.SemaphoreType.DMA
    n_sems = (
        5 * 2 * (n_shard - 1) * (1 + 2 * nb) + 3 * (n_shard * (1 + 2 * (nb - 1)) + n_shard - 1 + 2 * nb) + nb + 3 * n_shard
    )
    bufs = [V((n_shard,) + (2,) * (nb - 1 - j) + piece, B16) for piece in (piece_in, piece_out) for j in range(nb)]
    shape = jax.ShapeDtypeStruct
    return pl.pallas_call(
        functools.partial(layer_kernel, n_rep, n_shard, decay),
        out_shape=[
            shape((seq, width), B16),
            shape((seq, width), B16),
            shape(bits + piece_in, B16),
            shape(bits + piece_out, B16),
            shape((n_shard,) + bits + piece_in, B16),
            shape((n_shard,) + bits + piece_out, B16),
            shape((1, own_in), F32),
        ],
        in_specs=[any_] * 2 + [vmem] * 3 + [any_] * 8,
        out_specs=[vmem] * 2 + [any_] * 4 + [vmem],
        scratch_shapes=[
            V((seq, width), B16),
            V((seq, width), B16),
            V((n_shard,) + bits + piece_in, B16),
            V((n_shard,) + bits + piece_out, B16),
            V((n_shard, 1, own_in), F32),
            V((seq, width), B16),
            V((seq, 128), F32),
            V((seq, q_width), B16),
            V((seq, q_width), B16),
            V((q_width, seq), B16),
            V((seq, q_width), B16),
            V((seq, all_in), B16),
            V((seq, width), F32),
            V((seq, 128), F32),
            V((kv_heads, 2 * seq, pair), B16),
            V((kv_heads, 2 * seq, pair), B16),
            V((kv_heads, pair, 2 * seq), B16),
            V((kv_heads, pair, 2 * seq), B16),
            V((2 * seq, pair), F32),
            V((2 * seq, pair), F32),
            V((seq, seq), F32),
            V((seq, pair), F32),
            V((seq, pair), F32),
            V((q_width // pair, 2, 1, seq), F32),
            V((n_shard,) + bits + piece_in, B16),
            V((n_shard,) + bits + piece_out, B16),
            V((n_shard, 1, own_in), F32),
            V((nb, n_shard, 1, own_in), F32),
            V((n_shard, 1, own_in), F32),
            V(piece_in, F32),
            V(piece_out, F32),
            V((n_shard,) + piece_in, B16),
            V(piece_in, B16),
            V(piece_in, B16),
            V((n_shard,) + piece_out, B16),
            V(piece_out, B16),
            V(piece_out, B16),
            D((9,)),
            D((3,)),
            D((n_sems,)),
            D((n_sems,)),
        ]
        + bufs,
        compiler_params=pltpu.CompilerParams(
            collective_id=collective_id, has_side_effects=True, vmem_limit_bytes=67_043_328
        ),
        name="layer",
    )(tok, cot, seg[None], frequency, lax.reduce_precision(gain, 8, 7)[None], *weights, *moments)


gain_rate = 0.2


def on_device(
    tokens,
    segments,
    cotangent,
    gain,
    w_query,
    w_key,
    w_value,
    w_outproj,
    moment_gain,
    moment_query,
    moment_key,
    moment_value,
    moment_outproj,
):
    n_rep, n_shard = lax.axis_size("rep"), lax.axis_size("shard")
    total_tokens = tokens.shape[0] * tokens.shape[1] * n_rep * n_shard
    weights = (w_query, w_key, w_value, w_outproj)
    moments = (moment_query, moment_key, moment_value, moment_outproj)
    result, grad_tokens, sum_in, sum_out, m_in, m_out, grad_gain = layer(
        tokens[0], cotangent[0], segments[0], gain, weights, moments, decay, n_rep, n_shard, 0
    )
    grad_gain = grad_gain[0]
    moment_gain_next = decay * moment_gain + grad_gain
    gain_next = gain - gain_rate / math.sqrt(total_tokens) * moment_gain_next
    own_out, cols_out = sum_out.shape[-2:]
    m_out = m_out.reshape(n_shard, n_rep, own_out, cols_out)
    all_in = sum_in.shape[-1]
    grads, moments_next, (result, grad_tokens), (mix, mix_kv, scales) = muon(
        m_in.reshape(-1, all_in),
        m_out,
        sum_in.reshape(-1, all_in),
        sum_out.reshape(n_rep, own_out, cols_out),
        moments,
        (result, grad_tokens),
    )
    updated = update(mix, mix_kv, scales, m_out, moments_next, weights, n_rep, 1)
    return (
        result[None],
        grad_tokens[None],
        grad_gain,
        *grads,
        gain_next,
        *updated,
        moment_gain_next,
        *moments_next,
    )


def solution(mesh):
    in_specs = (
        P(("rep", "shard"), None, None),
        P(("rep", "shard"), None),
        P(("rep", "shard"), None, None),
        P("shard"),
        P("shard", None),
        P("shard", None),
        P("shard", None),
        P("shard", None),
        P("shard"),
        P("shard", None),
        P("shard", None),
        P("shard", None),
        P("shard", None),
    )
    out_specs = (
        P(("rep", "shard"), None, None),
        P(("rep", "shard"), None, None),
        P("shard"),
        P("shard", None),
        P("shard", None),
        P("shard", None),
        P("shard", None),
        P("shard"),
        P("shard", "rep"),
        P("shard", "rep"),
        P("shard", "rep"),
        P("shard", "rep"),
        P("shard"),
        P("shard", None),
        P("shard", None),
        P("shard", None),
        P("shard", None),
    )
    return jax.shard_map(on_device, mesh=mesh, in_specs=in_specs, out_specs=out_specs, check_vma=False)
```

```python
import functools
import math

import jax
import jax.numpy as jnp
import numpy as np
from jax import lax
from jax.experimental import pallas as pl
from jax.experimental.pallas import tpu as pltpu
from jax.sharding import PartitionSpec as P

coef_a = 3.4445
coef_b = -4.775
coef_c = 2.0315
SWEEPS = 5
decay = 0.95
muon_rate = 0.02


def nt(left, right):
    return lax.dot_general(left, right, (((1,), (1,)), ((), ())), preferred_element_type=jnp.float32)


def tn(left, right):
    return lax.dot_general(left, right, (((0,), (0,)), ((), ())), preferred_element_type=jnp.float32)


def mm(left, right):
    return jnp.dot(left, right, preferred_element_type=jnp.float32)


def tiles(count, body):
    def one(i, carry):
        body(i)
        return carry

    lax.fori_loop(0, count, one, 0)


def span(i, size):
    return pl.ds(pl.multiple_of(i * size, size), size)


def total(x):
    return jnp.sum(jnp.sum(x, axis=1, keepdims=True), axis=0, keepdims=True)


class Iterate:
    def __init__(self, e, ebf, k, kbf, h, hbf, fbf):
        self.e, self.ebf, self.k, self.kbf, self.h, self.hbf, self.fbf = e, ebf, k, kbf, h, hbf, fbf
        self.n = n = e.shape[0]
        self.diag = min(256, n)
        self.squares = [slice(d, d + self.diag) for d in range(0, n, self.diag)]
        half = n // 2
        if n <= 256:
            self.blocks = [(slice(0, n), slice(0, n))]
        else:
            self.blocks = [(slice(0, n), slice(0, half)), (slice(half, n), slice(half, n))]

    def put(self, ref, at, value):
        r, c = at
        ref[r, c] = value.astype(jnp.bfloat16)
        if r != c:
            ref[c, c.stop : r.stop] = ref[c.stop : r.stop, c].T

    def eye(self):
        shape = (self.diag, self.diag)
        return lax.broadcasted_iota(jnp.int32, shape, 0) == lax.broadcasted_iota(jnp.int32, shape, 1)

    def trace(self, ref):
        mask = self.eye()
        return sum(total(jnp.where(mask, ref[d, d], 0.0)) for d in self.squares)

    def centre(self, s):
        shift = self.trace(self.e) * (1.0 / self.n)
        mask = self.eye()
        for d in self.squares:
            moved = self.e[d, d] - jnp.where(mask, shift, 0.0)
            self.e[d, d] = moved
            self.ebf[d, d] = moved.astype(jnp.bfloat16)
        return s + shift

    def start(self):
        norm = jnp.sqrt(self.trace(self.e)) + 1e-06
        scale = 1.0 / (norm * norm)
        for at in self.blocks:
            x = self.e[at] * scale
            self.e[at] = x
            self.put(self.ebf, at, x)
        return self.centre(jnp.zeros((1, 1), jnp.float32)), 1.0 / norm

    def polynomial(self, s, at):
        p1 = coef_b + 2.0 * coef_c * s
        self.put(self.fbf, at, p1 * self.e[at] + coef_c * mm(self.ebf[at[0], :], self.ebf[:, at[1]]))

    def first(self):
        for at in self.blocks:
            f = self.fbf[at].astype(jnp.float32)
            self.h[at] = f
            self.put(self.hbf.at[0], at, f)

    def grow(self, p0, q, at, now, later):
        new = p0 * self.h[at] + q * self.fbf[at].astype(jnp.float32) + mm(self.fbf[at[0], :], self.hbf[now, :, at[1]])
        self.h[at] = new
        self.put(self.hbf.at[later], at, new)

    def inner(self, p0, s, at):
        new = p0 * self.e[at] + s * self.fbf[at].astype(jnp.float32) + mm(self.fbf[at[0], :], self.ebf[:, at[1]])
        self.k[at] = new
        self.put(self.kbf, at, new)

    def outer(self, p0, beta, at):
        new = p0 * self.k[at] + beta * self.fbf[at].astype(jnp.float32) + mm(self.fbf[at[0], :], self.kbf[:, at[1]])
        self.e[at] = new
        self.put(self.ebf, at, new)


def muon_kernel(*refs):
    refs = list(refs)

    def take(count):
        return [refs.pop(0) for _ in range(count)]

    m_in, m_out, *passed = take(4)
    g_in, g_out, *moments = take(6)
    grads_out, moments_out, passed_out = take(4), take(4), take(2)
    h_out, hs_out, scal = take(3)
    grads, news, held = take(4), take(4), take(2)
    sums_in, sums_out, tall, lump, x, small_m = take(6)
    in_sem, own_sem, out_sem, pass_sem = take(4)
    big, small = Iterate(*take(7)), Iterate(*take(7))
    f32, b16 = jnp.float32, jnp.bfloat16
    core = lax.rem(lax.axis_index("rep"), 2)
    shard = lax.axis_index("shard")
    n, ns = big.n, small.n
    own_in = g_in.shape[0]
    n_rep, own_out, cols_out = g_out.shape
    chunk, q_part, kv_part = (n + 2 * ns) // 2, n // 2, ns // 2
    firsts = [(0, q_part), (q_part, kv_part), (q_part + kv_part, kv_part)]

    wide = [
        pltpu.make_async_copy(m_in.at[:, pl.ds(c * chunk, q_part)], tall.at[:, pl.ds(c * q_part, q_part)], in_sem.at[c])
        for c in range(2)
    ]
    flat = pltpu.make_async_copy(m_out, lump, in_sem.at[0])
    kv = [
        pltpu.make_async_copy(
            m_in.at[:, pl.ds(pl.multiple_of(c * chunk + q_part + core * kv_part, 128), kv_part)],
            small_m.at[:, pl.ds(c * kv_part, kv_part)],
            in_sem.at[2 + c],
        )
        for c in range(2)
    ]
    own = [pltpu.make_async_copy(a, b, own_sem.at[i]) for i, (a, b) in enumerate(zip(moments, news))]
    own_sums = [pltpu.make_async_copy(g_in, sums_in, own_sem.at[4]), pltpu.make_async_copy(g_out, sums_out, own_sem.at[5])]
    passing = [pltpu.make_async_copy(a, b, pass_sem.at[i]) for i, (a, b) in enumerate(zip(passed, held))]
    leaving = [pltpu.make_async_copy(a, b, pass_sem.at[i]) for i, (a, b) in enumerate(zip(held, passed_out))]

    @pl.when(core == 0)
    def _():
        for copy in wide:
            copy.start()

    @pl.when(core != 0)
    def _():
        flat.start()

    for copy in kv + own_sums + own:
        copy.start()

    mine = span(shard, own_in)
    rows = 64

    @pl.when(core == 0)
    def _():
        for copy in wide:
            copy.wait()
        tiles(tall.shape[0] // 256, lambda i: x.__setitem__((slice(None), span(i, 256)), tall[span(i, 256), :].T))

    @pl.when(core != 0)
    def _():
        flat.wait()
        for s in range(lump.shape[0]):
            tiles(n_rep, lambda r, s=s: x.__setitem__((slice(s * own_out, (s + 1) * own_out), span(r, cols_out)), lump[s, r]))

    for copy in kv + own_sums + own:
        copy.wait()
    for copy in passing:
        copy.start()
    for i in range(4):
        if i < 3:
            def update(j, i=i, first=firsts[i][0], width=firsts[i][1]):
                r = span(j, rows)
                for c in range(2):
                    at, to = c * chunk + first, slice(c * width, (c + 1) * width)
                    grad = sums_in[r, at : at + width].astype(f32)
                    grads[i][r, to] = grad
                    news[i][r, to] = decay * news[i][r, to] + grad

            tiles(own_in // rows, update)
        else:
            def update(r, i=i):
                at = span(r, cols_out)
                grad = sums_out[r].astype(f32)
                grads[i][:, at] = grad
                news[i][:, at] = decay * news[i][:, at] + grad

            tiles(n_rep, update)

    @pl.when(core == 0)
    def _():
        x[:, mine] = news[0][...].astype(b16).T
        small_m[mine, :] = news[1][...].astype(b16)

    @pl.when(core != 0)
    def _():
        x[span(shard, own_out), :] = news[3][...].astype(b16)
        small_m[mine, :] = news[2][...].astype(b16)

    copies = [
        pltpu.make_async_copy(a, b, out_sem.at[i])
        for i, (a, b) in enumerate(zip(grads + news, grads_out + moments_out))
    ]
    for copy in copies:
        copy.start()
    for a, b in zip(passing, leaving):
        a.wait()
        b.start()
    for r, c in big.blocks:
        big.e[r, c] = nt(x[r, :], x[c, :])
    small.e[...] = tn(small_m[...], small_m[...])
    s, inv = big.start()
    ss, sinv = small.start()

    def sweep(it, carry):
        s, q, ss, sq = carry
        now, later = lax.rem(it + 1, 2), lax.rem(it, 2)
        p0 = coef_a + s * (coef_b + coef_c * s)
        sp0 = coef_a + ss * (coef_b + coef_c * ss)

        def each(method, *args):
            for i, c in enumerate(big.blocks):
                getattr(big, method)(*[a[0] for a in args], c, *extra)
                if i == 0:
                    for d in small.blocks:
                        getattr(small, method)(*[a[1] for a in args], d, *extra)

        extra = ()
        each("polynomial", (s, ss))

        @pl.when(it == 0)
        def _():
            big.first()
            small.first()

        extra = (now, later)

        @pl.when(it > 0)
        def _():
            each("grow", (p0, sp0), (q, sq))

        extra = ()
        q, sq = p0 * q, sp0 * sq

        def advance():
            each("inner", (p0, sp0), (s, ss))
            beta, sbeta = p0 * s, sp0 * ss
            each("outer", (p0, sp0), (beta, sbeta))
            return big.centre(p0 * beta), small.centre(sp0 * sbeta)

        s, ss = lax.cond(it < SWEEPS - 1, advance, lambda: (s, ss))
        return s, q, ss, sq

    one = jnp.ones((1, 1), f32)
    s, q, ss, sq = lax.fori_loop(0, SWEEPS, sweep, (s, one, ss, one))
    last = (SWEEPS - 1) % 2
    h_out[...] = big.hbf[last]
    hs_out[...] = small.hbf[last]
    row = lax.broadcasted_iota(jnp.int32, (8, 128), 0)
    scal[...] = jnp.where(row == 0, q * inv, jnp.where(row == 1, inv, jnp.where(row == 2, sq * sinv, sinv)))
    for copy in copies + leaving:
        copy.wait()


def muon(m_in, m_out, g_in, g_out, moments, passed):
    f32, b16 = jnp.float32, jnp.bfloat16
    tall, n, kv = m_in.shape[0], m_out.shape[0] * m_out.shape[2], moments[1].shape[1]
    V = pltpu.VMEM
    sets = []
    for d in (n, kv):
        sets += [V((d, d), f32), V((d, d), b16), V((d, d), f32), V((d, d), b16), V((d, d), f32), V((2, d, d), b16), V((d, d), b16)]
    vmem, any_ = pl.BlockSpec(memory_space=pltpu.VMEM), pl.BlockSpec(memory_space=pl.ANY)
    own = [jax.ShapeDtypeStruct(m.shape, f32) for m in moments]
    out = pl.pallas_call(
        muon_kernel,
        out_shape=own
        + own
        + [jax.ShapeDtypeStruct(p.shape, p.dtype) for p in passed]
        + [
            jax.ShapeDtypeStruct((n, n), b16),
            jax.ShapeDtypeStruct((kv, kv), b16),
            jax.ShapeDtypeStruct((8, 128), f32),
        ],
        in_specs=[any_] * 10,
        out_specs=[any_] * 10 + [vmem] * 3,
        scratch_shapes=[V(m.shape, f32) for m in moments] * 2
        + [V(p.shape, p.dtype) for p in passed]
        + [
            V(g_in.shape, b16),
            V(g_out.shape, b16),
            V((tall, n), b16),
            V(m_out.shape, b16),
            V((n, m_out.shape[1] * m_out.shape[3]), b16),
            V((tall, kv), b16),
            pltpu.SemaphoreType.DMA((4,)),
            pltpu.SemaphoreType.DMA((6,)),
            pltpu.SemaphoreType.DMA((8,)),
            pltpu.SemaphoreType.DMA((2,)),
        ]
        + sets,
        compiler_params=pltpu.CompilerParams(vmem_limit_bytes=63 << 20),
        name="muon",
    )(m_in, m_out, *passed, g_in, g_out, *moments)
    return out[:4], out[4:8], out[8:10], out[10:]


def swap_kernel(n_rep, h, hs, scal, h_pair, hs_come, scal_come, send, recv):
    rep, shard = lax.axis_index("rep"), lax.axis_index("shard")
    core = lax.rem(rep, 2)
    other = rep + 1 - 2 * core
    sem = pltpu.get_barrier_semaphore()
    pl.semaphore_signal(sem, 1, device_id=(other, shard), device_id_type=pl.DeviceIdType.MESH)
    pl.semaphore_wait(sem, 1)

    def remote(src, dst, i):
        return pltpu.make_async_remote_copy(
            src, dst, send.at[i], recv.at[i], device_id=(other, shard), device_id_type=pl.DeviceIdType.MESH
        )

    count = h_pair.shape[0]
    at = jnp.where(core == 0, lax.div(rep, 2), shard)
    copies = [remote(h.at[span(at, count), :], h_pair, 0), remote(hs, hs_come, 1), remote(scal, scal_come, 2)]
    for c in copies:
        c.start()
    for c in copies:
        c.wait()


def swap(h, hs, scal, count, n_rep, collective_id):
    any_ = pl.BlockSpec(memory_space=pl.ANY)
    return pl.pallas_call(
        functools.partial(swap_kernel, n_rep),
        out_shape=[
            jax.ShapeDtypeStruct((count, h.shape[1]), h.dtype),
            jax.ShapeDtypeStruct(hs.shape, hs.dtype),
            jax.ShapeDtypeStruct(scal.shape, scal.dtype),
        ],
        in_specs=[any_] * 3,
        out_specs=[any_] * 3,
        scratch_shapes=[pltpu.SemaphoreType.DMA((3,)), pltpu.SemaphoreType.DMA((3,))],
        compiler_params=pltpu.CompilerParams(collective_id=collective_id, has_side_effects=True),
        name="swap",
    )(h, hs, scal)


def window(index, width):
    size = max(width, 128)
    start = lax.div(index * width, size) * size
    return pl.ds(pl.multiple_of(start, 128), size), size, index * width - start


def cut(x, size, offset, width):
    return x if size == width else pltpu.roll(x, lax.rem(size - offset, size), 1)[:, :width]


def update_kernel(h, h_pair, hs, hs_come, scal, scal_come, m_out, mq_hbm, mk_hbm, mv_hbm, mo, wq, wk, wv, wo, *refs):
    nexts, (hq, ho, flat, mo_win), weight_wins, (mq, mk, mv), (h_sem, sem) = (
        refs[:4], refs[4:8], refs[8:12], refs[12:15], refs[15:]
    )
    f32, b16 = jnp.float32, jnp.bfloat16
    rep, shard = lax.axis_index("rep"), lax.axis_index("shard")
    even = lax.rem(rep, 2) == 0
    widths = [nexts[0].shape[1], nexts[1].shape[0], nexts[2].shape[0], nexts[3].shape[1]]
    wins = [window(rep, w) for w in widths]
    own_out = ho.shape[0]
    copies = [
        pltpu.make_async_copy(m_out.at[:, rep], flat, sem.at[4]),
        pltpu.make_async_copy(mo.at[:, wins[3][0]], mo_win, sem.at[5]),
        pltpu.make_async_copy(mq_hbm, mq, sem.at[6]),
        pltpu.make_async_copy(mk_hbm, mk, sem.at[7]),
        pltpu.make_async_copy(mv_hbm, mv, sem.at[8]),
    ] + [pltpu.make_async_copy(w.at[:, wins[i][0]], weight_wins[i], sem.at[i]) for i, w in enumerate((wq, wk, wv, wo))]
    for copy in copies:
        copy.start()
    rows_q = h.at[span(rep, widths[0]), :], h_pair.at[pl.ds(h_pair.shape[0] - widths[0], widths[0]), :]
    rows_o = h_pair, h.at[span(shard, own_out), :]
    mixes = [[pltpu.make_async_copy(a, b, h_sem.at[i]) for i, (a, b) in enumerate(((q, hq), (o, ho)))] for q, o in zip(rows_q, rows_o)]
    for side, here in ((0, even), (1, jnp.logical_not(even))):
        @pl.when(here)
        def _():
            for copy in mixes[side]:
                copy.start()
            for copy in mixes[side]:
                copy.wait()
    for copy in copies:
        copy.wait()
    first = jnp.where(even, scal[...], scal_come[...])
    second = jnp.where(even, scal_come[...], scal[...])
    flat[shard] = mo_win[...].astype(b16)

    def rows_of(i):
        at = span(rep, widths[i])
        mine, theirs = hs[at, :].astype(f32), hs_come[at, :].astype(f32)
        return jnp.where(even == (i == 1), mine, theirs).astype(b16)

    parts = (
        (mq, lambda: nt(mq[...].astype(b16), hq[...]), first[0:1, 0:1], first[1:2, 0:1]),
        (mk, lambda: nt(rows_of(1), mk[...].astype(b16)), first[2:3, 0:1], first[3:4, 0:1]),
        (mv, lambda: nt(rows_of(2), mv[...].astype(b16)), second[2:3, 0:1], second[3:4, 0:1]),
        (None, lambda: mm(ho[...], flat[...].reshape(-1, flat.shape[2])), second[0:1, 0:1], second[1:2, 0:1]),
    )
    n_shard = lax.axis_size("shard")
    for i, (moment, product, straight, mixed) in enumerate(parts):
        at, size, offset = wins[i]

        def mine(x):
            x = cut(x, size, offset, widths[i])
            return x.T if i in (1, 2) else x

        here = mine(mo_win[...] if moment is None else moment[:, at])
        ortho = straight * here + mixed * product()
        whole = (weight_wins[i].shape[0] * n_shard, (wq, wk, wv, wo)[i].shape[1])
        nexts[i][...] = mine(weight_wins[i][...]) - muon_rate * math.sqrt(max(whole)) * ortho


def update(h, hs, scal, m_out, moments, weights, n_rep, collective_id):
    f32, b16 = jnp.float32, jnp.bfloat16
    widths = [w.shape[1] // n_rep for w in weights]
    own_out = weights[3].shape[0]
    assert 2 * widths[0] == own_out and m_out.shape[3] == widths[3]
    h_pair, hs_come, scal_come = swap(h, hs, scal, own_out, n_rep, collective_id)
    vmem, any_ = pl.BlockSpec(memory_space=pltpu.VMEM), pl.BlockSpec(memory_space=pl.ANY)
    V = pltpu.VMEM
    sizes = [max(w, 128) for w in widths]
    shapes = [(w.shape[0], width) for w, width in zip(weights, widths)]
    out = pl.pallas_call(
        update_kernel,
        out_shape=[jax.ShapeDtypeStruct(s[::-1] if i in (1, 2) else s, f32) for i, s in enumerate(shapes)],
        in_specs=[any_] * 2 + [vmem] * 4 + [any_] * 9,
        out_specs=[vmem] * 4,
        scratch_shapes=[
            V((widths[0], h.shape[1]), b16),
            V((own_out, h.shape[1]), b16),
            V((m_out.shape[0],) + m_out.shape[2:], b16),
            V((own_out, sizes[3]), f32),
        ]
        + [V((w.shape[0], size), f32) for w, size in zip(weights, sizes)]
        + [V(m.shape, f32) for m in moments[:3]]
        + [pltpu.SemaphoreType.DMA((2,)), pltpu.SemaphoreType.DMA((9,))],
        name="update",
    )(h, h_pair, hs, hs_come, scal, scal_come, m_out, *moments, *weights)
    return out[0], out[1].T, out[2].T, out[3]


HEAD_SIZE = 64
TILE = 256
norm_eps = 1e-05
rope_base = 500000.0
F32, B16 = jnp.float32, jnp.bfloat16
MESH = pl.DeviceIdType.MESH
WAYS = (1, -1)


class Links:
    def __init__(self, n_rep, n_shard, send, recv):
        self.n_bits, self.n_shard = n_rep.bit_length() - 1, n_shard
        self.rep, self.shard = lax.axis_index("rep"), lax.axis_index("shard")
        self.bits = [lax.rem(lax.div(self.rep, 1 << b), 2) for b in range(self.n_bits)]
        far = list(range(1, self.n_bits))
        self.orders = (far, far[::-1])
        self.send, self.recv, self.names = send, recv, {}

    def flip(self, bit):
        return self.rep + (1 << bit) * (1 - 2 * self.bits[bit])

    def barrier(self):
        sem = pltpu.get_barrier_semaphore()
        for b in range(self.n_bits):
            pl.semaphore_signal(sem, 1, device_id=(self.flip(b), self.shard), device_id_type=MESH)
        for k in range(1, self.n_shard):
            there = lax.rem(self.shard + k, self.n_shard)
            pl.semaphore_signal(sem, 1, device_id=(self.rep, there), device_id_type=MESH)
        pl.semaphore_wait(sem, self.n_bits + self.n_shard - 1)

    def where(self, free=()):
        return tuple(slice(None) if b in free else self.bits[b] for b in reversed(range(self.n_bits)))

    def remote(self, src, dst, name, rep, shard):
        i = self.names.setdefault(name, len(self.names))
        return pltpu.make_async_remote_copy(
            src, dst, self.send.at[i], self.recv.at[i], device_id=(rep, shard), device_id_type=MESH
        )

    def goes(self, way, k):
        q, there = self.shard - way * k, self.shard + way
        return (q >= 0) & (q < self.n_shard) & (there >= 0) & (there < self.n_shard)

    def comes(self, way, k):
        q = self.shard - way * (k + 1)
        return (q >= 0) & (q < self.n_shard)


class Gather:
    def __init__(self, links, name, full, half, first=None):
        self.links, self.name, self.full, self.half, self.first = links, name, full, half, first

    def line(self, way, k, h):
        at = self.full.at[(self.links.shard - way * k,) + self.links.where() + self.half[h]]
        src = self.first.at[self.half[h]] if k == 0 and self.first is not None else at
        return self.links.remote(src, at, (self.name, "l", way, k, h), self.links.rep, self.links.shard + way)

    def came(self, way, k, h):
        at = self.full.at[(self.links.shard - way * (k + 1),) + self.links.where() + self.half[h]]
        return self.links.remote(at, at, (self.name, "l", way, k, h), self.links.rep, self.links.shard)

    def plane(self, way, k, h, step):
        links = self.links
        order = links.orders[h] + [0]
        view = self.full.at[(links.shard - way * (k + 1),) + links.where(order[:step]) + self.half[h]]
        return links.remote(view, view, (self.name, "p", way, k, h, step), links.flip(order[step]), links.shard)

    def start(self):
        for way in WAYS:
            @pl.when(self.links.goes(way, 0))
            def _():
                for h in range(2):
                    self.line(way, 0, h).start()

    def arrive(self, k):
        links = self.links
        for way in WAYS:
            @pl.when(links.comes(way, k))
            def _():
                for h in range(2):
                    self.came(way, k, h).wait_recv()
                    if k + 1 < links.n_shard - 1:
                        @pl.when(links.goes(way, k + 1))
                        def _():
                            self.line(way, k + 1, h).start()

    def event(self, k, step, then=None):
        links = self.links
        for way in WAYS:
            @pl.when(links.comes(way, k))
            def _():
                for h in range(2):
                    if step > 0:
                        self.plane(way, k, h, step - 1).wait_recv()
                    if step < links.n_bits:
                        self.plane(way, k, h, step).start()
                if step == links.n_bits and then is not None:
                    then(links.shard - way * (k + 1))

    def drain(self):
        links = self.links
        for way in WAYS:
            for k in range(links.n_shard - 1):
                @pl.when(links.goes(way, k))
                def _():
                    for h in range(2):
                        self.line(way, k, h).wait_send()

                @pl.when(links.comes(way, k))
                def _():
                    for h in range(2):
                        for step in range(links.n_bits):
                            self.plane(way, k, h, step).wait_send()


class Reduce:
    def __init__(self, links, name, refs, region, half, keep_sem):
        self.links, self.name, self.region, self.half = links, name, region, half
        self.part, self.bufs, self.zbuf, self.gpiece, self.mpiece, self.moment, self.sums, wholes = refs
        self.whole = Gather(links, name + "m", wholes, half, self.mpiece)
        self.keep = lambda: pltpu.make_async_copy(
            self.gpiece.at[region], self.sums.at[links.where() + region], keep_sem
        )

    def dest(self, k):
        return lax.rem(self.links.shard + 1 + k, self.links.n_shard)

    def origin(self, k):
        return lax.rem(self.links.shard + self.links.n_shard - 1 - k, self.links.n_shard)

    def order(self, h):
        return [0] + self.links.orders[h]

    def cut(self, h, step):
        return self.region if step == 0 else self.half[h]

    def send(self, k, h, step):
        links, o = self.links, self.order(h)
        bit = o[step]
        src = self.part if step == 0 else self.bufs[step - 1]
        left = sorted(o[step:], reverse=True)
        pick = tuple(1 - links.bits[bit] if b == bit else slice(None) for b in left)
        d, cut = self.dest(k), self.cut(h, step)
        into = self.bufs[step].at[(d,) + (slice(None),) * (links.n_bits - 1 - step) + cut]
        return links.remote(src.at[(d,) + pick + cut], into, (self.name, "r", k, h, step), links.flip(bit), links.shard)

    def add(self, k, h, step):
        links, o = self.links, self.order(h)
        src = self.part if step == 0 else self.bufs[step - 1]
        left = sorted(o[step:], reverse=True)
        others = [b for b in left if b != o[step]]
        d, cut = self.dest(k), self.cut(h, step)

        def one(i):
            at = {b: lax.rem(lax.div(i, 1 << (len(others) - 1 - n)), 2) for n, b in enumerate(others)}
            here = (d,) + tuple(at[b] for b in others) + cut
            there = (d,) + tuple(links.bits[b] if b == o[step] else at[b] for b in left) + cut
            both = src[there].astype(F32) + self.bufs[step][here].astype(F32)
            self.bufs[step][here] = both.astype(B16)

        if others:
            tiles(1 << len(others), one)
        else:
            one(0)

    def send_line(self, k):
        links, d = self.links, self.dest(k)
        src, into = self.bufs[-1].at[(d,) + self.region], self.zbuf.at[(links.shard,) + self.region]
        return links.remote(src, into, (self.name, "z", k), links.rep, d)

    def come_line(self, k):
        links, at = self.links, self.zbuf.at[(self.origin(k),) + self.region]
        return links.remote(at, at, (self.name, "z", k), links.rep, links.shard)

    def start(self, k):
        self.send(k, 0, 0).start()

    def event(self, k, step):
        last = self.links.n_bits - 1
        for h in range(1 if step == 0 else 2):
            self.send(k, h, step).wait_recv()
            self.add(k, h, step)
            if step == 0 and last > 0:
                self.send(k, 0, 1).start()
                self.send(k, 1, 1).start()
            elif step < last:
                self.send(k, h, step + 1).start()
        if step == last and k < self.links.n_shard - 1:
            self.send_line(k).start()

    def gather_sum(self, h, step):
        links = self.links
        order = links.orders[h] + [0]
        into = self.sums.at[links.where(order[:step]) + self.half[h]]
        src = self.gpiece.at[self.half[h]] if step == 0 else into
        return links.remote(src, into, (self.name, "g", h, step), links.flip(order[step]), links.shard)

    def finish(self, decay):
        links = self.links
        for k in range(links.n_shard - 1):
            self.come_line(k).wait_recv()
        acc = self.bufs[-1][(links.shard,) + self.region].astype(F32)
        for k in range(links.n_shard - 1):
            acc = acc + self.zbuf[(self.origin(k),) + self.region].astype(F32)
        g = acc.astype(B16)
        self.gpiece[self.region] = g
        self.mpiece[self.region] = (decay * self.moment[self.region] + g.astype(F32)).astype(B16)
        self.whole.start()
        for h in range(2):
            self.gather_sum(h, 0).start()
        self.keep().start()

    def gather_event(self, i, step):
        if i > 0:
            self.whole.event(i - 1, step)
            return
        if step == 0:
            self.keep().wait()
        if step < self.links.n_bits:
            for h in range(2):
                self.gather_sum(h, step).wait_recv()
                if step + 1 < self.links.n_bits:
                    self.gather_sum(h, step + 1).start()

    def drain(self):
        links = self.links
        for k in range(links.n_shard):
            for step in range(links.n_bits):
                for h in range(1 if step == 0 else 2):
                    self.send(k, h, step).wait_send()
            if k < links.n_shard - 1:
                self.send_line(k).wait_send()
        for h in range(2):
            for step in range(links.n_bits):
                self.gather_sum(h, step).wait_send()
        self.whole.drain()


class GainSum:
    def __init__(self, links, acc, come, line):
        self.links, self.acc, self.come, self.line = links, acc, come, line

    def send(self, b):
        return self.links.remote(self.acc, self.come.at[b], ("gain", b), self.links.flip(b), self.links.shard)

    def send_line(self, k):
        links = self.links
        d = lax.rem(links.shard + 1 + k, links.n_shard)
        return links.remote(self.acc.at[d], self.line.at[links.shard], ("gainz", k), links.rep, d)

    def event(self, b):
        links = self.links
        self.send(b).wait()
        self.acc[...] = self.acc[...] + self.come[b]
        if b + 1 < links.n_bits:
            self.send(b + 1).start()
        else:
            for k in range(links.n_shard - 1):
                self.send_line(k).start()

    def end(self):
        links = self.links
        for k in range(links.n_shard - 1):
            self.send_line(k).wait_send()
            at = self.line.at[lax.rem(links.shard + links.n_shard - 1 - k, links.n_shard)]
            links.remote(at, at, ("gainz", k), links.rep, links.shard).wait_recv()
        acc = self.acc[links.shard]
        for q in range(links.n_shard):
            acc = jnp.where(links.shard == q, acc, acc + self.line[q])
        return acc


def swap_halves(x):
    half, width = HEAD_SIZE // 2, x.shape[1]
    lane = lax.rem(lax.broadcasted_iota(jnp.int32, x.shape, 1), HEAD_SIZE)
    return jnp.where(lane < half, pltpu.roll(x, width - half, 1), pltpu.roll(x, half, 1))


def flat(x):
    return x.reshape(-1, x.shape[-1])


def bits_of(r, n_bits):
    return tuple(lax.rem(lax.div(r, 1 << b), 2) if isinstance(r, jax.Array) else (r >> b) & 1 for b in reversed(range(n_bits)))


def layer_kernel(
    n_rep, n_shard, decay,
    tok_hbm, cot_hbm, seg_row, frequency, gain, w_query, w_key, w_value, w_outproj, m_query, m_key, m_value, m_outproj,
    out_hbm, grad_hbm, sums_in, sums_out, wholes_in, wholes_out, gain_out,
    out, grad_tok,    tok, cot, w_in, w_out, gain_full, xn, inv_ref, q, dattn, attn_t, attn, dqkv, dxn, row_acc, kx, vx, kxt, vxt, dk_acc, dv_acc,
    bias, cosine, sine, inv_l, part_in, part_out, gain_acc, gain_come, gain_line, moment_in, moment_out,
    zbuf_in, gp_in, mp_in, zbuf_out, gp_out, mp_out, load_sem, keep_sem, send, recv, *bufs,
):
    seq, width = tok.shape
    q_width, kv_width = w_query.shape[1], w_key.shape[1]
    kv_heads = kv_width // HEAD_SIZE
    pair = 2 * HEAD_SIZE
    pairs = q_width // pair
    per_group = pairs // kv_heads
    n_tok = seq // TILE
    scale = 1.0 / math.sqrt(HEAD_SIZE)
    rows = 64
    nb = n_rep.bit_length() - 1
    own_in, own_out = width // n_shard, q_width // n_shard
    rows_in, cols_out = own_in // n_rep, width // n_rep
    all_in = w_in.shape[-1]
    chunk, q_part, kv_part = all_in // 2, q_width // 2, kv_width // 2
    places = [
        (i, c * size, c * chunk + first, size)
        for c in range(2)
        for i, (first, size) in enumerate(((0, q_part), (q_part, kv_part), (q_part + kv_part, kv_part)))
    ]

    links = Links(n_rep, n_shard, send, recv)
    me, rep = links.shard, links.rep
    both = slice(None)
    part_cols = [(both, pl.ds(c * chunk, chunk)) for c in range(2)]
    half_cols = [[(both, pl.ds(c * chunk + h * (chunk // 2), chunk // 2)) for h in range(2)] for c in range(2)]
    half_in = [(both, pl.ds(h * chunk, chunk)) for h in range(2)]
    half_out = [(pl.ds(h * (own_out // 2), own_out // 2), both) for h in range(2)]
    get_in, get_out = Gather(links, "wi", w_in, half_in), Gather(links, "wo", w_out, half_out)
    refs_in = (part_in, bufs[:nb], zbuf_in, gp_in, mp_in, moment_in, sums_in, wholes_in)
    refs_out = (part_out, bufs[nb:], zbuf_out, gp_out, mp_out, moment_out, sums_out, wholes_out)
    sum_in = [Reduce(links, f"i{c}", refs_in, part_cols[c], half_cols[c], keep_sem.at[c]) for c in range(2)]
    sum_out = Reduce(links, "o", refs_out, (both, both), half_out, keep_sem.at[2])
    sum_gain = GainSum(links, gain_acc, gain_come, gain_line)

    ws, ms = (w_query, w_key, w_value), (m_query, m_key, m_value)
    loads = [
        pltpu.make_async_copy(ws[i].at[:, pl.ds(at, size)], dxn.at[pl.ds(0, own_in), pl.ds(to, size)], load_sem.at[n])
        for n, (i, at, to, size) in enumerate(places)
    ]
    first = [
        pltpu.make_async_copy(ws[i].at[span(rep, rows_in), pl.ds(at, size)], moment_in.at[:, pl.ds(to, size)], load_sem.at[9 + n])
        for n, (i, at, to, size) in enumerate(places)
    ] + [pltpu.make_async_copy(w_outproj.at[:, span(rep, cols_out)], moment_out, load_sem.at[15])]
    early = [pltpu.make_async_copy(a, b, load_sem.at[7 + i]) for i, (a, b) in enumerate(((tok_hbm, tok), (cot_hbm, cot)))]
    for load in first + loads + early:
        load.start()
    gain_full[me] = gain[...].astype(B16).astype(F32)
    links.barrier()

    def gain_line_copy(way, k):
        at = gain_full.at[me - way * k]
        return links.remote(at, at, ("gf", way, k), rep, me + way)

    def gain_came(way, k):
        at = gain_full.at[me - way * (k + 1)]
        return links.remote(at, at, ("gf", way, k), rep, me)

    for way in WAYS:
        @pl.when(links.goes(way, 0))
        def _():
            gain_line_copy(way, 0).start()
    for load in first:
        load.wait()
    here = (me,) + links.where()
    w_in[here] = moment_in[...].astype(B16)
    get_in.start()
    w_out[here] = moment_out[...].astype(B16)
    for load in loads:
        load.wait()
    for r in range(n_rep):
        @pl.when(rep != r)
        def _():
            w_in[(me,) + bits_of(r, nb)] = dxn[r * rows_in : (r + 1) * rows_in, :all_in].astype(B16)

    load_out = pltpu.make_async_copy(w_outproj, dxn.at[pl.ds(0, own_out), :], load_sem.at[6])
    load_out.start()
    load_out.wait()
    for r in range(n_rep):
        @pl.when(rep != r)
        def _():
            w_out[(me,) + bits_of(r, nb)] = dxn[:own_out, r * cols_out : (r + 1) * cols_out].astype(B16)

    loads = [
        pltpu.make_async_copy(ms[i].at[span(rep, rows_in), pl.ds(at, size)], moment_in.at[:, pl.ds(to, size)], load_sem.at[n])
        for n, (i, at, to, size) in enumerate(places)
    ] + [pltpu.make_async_copy(m_outproj.at[:, span(rep, cols_out)], moment_out, load_sem.at[6])]
    for load in loads:
        load.start()

    row_acc[...] = jnp.broadcast_to(seg_row[...].astype(F32), (row_acc.shape[1], seq)).T
    own_seg = seg_row[...].astype(F32)

    def masks(i):
        r = span(i, rows)
        seg_col = row_acc[r, :1]
        key = lax.broadcasted_iota(jnp.int32, (rows, seq), 0) + i * rows
        query = lax.broadcasted_iota(jnp.int32, (rows, seq), 1)
        seen = (key <= query) & (seg_col == own_seg)
        bias[r, :] = jnp.where(seen, 0.0, -1e30)
        start = jnp.sum(jnp.where(own_seg < seg_col, 1.0, 0.0), 1, keepdims=True)
        at = lax.broadcasted_iota(jnp.int32, (rows, 1), 0) + i * rows
        angle = (at.astype(F32) - start) * frequency[...]
        lane = lax.rem(lax.broadcasted_iota(jnp.int32, (rows, pair), 1), HEAD_SIZE)
        cosine[r, :] = jnp.cos(angle)
        s = jnp.sin(angle)
        sine[r, :] = jnp.where(lane < HEAD_SIZE // 2, -s, s)
        x = tok[r, :].astype(F32)
        inv = lax.rsqrt(jnp.mean(x * x, -1, keepdims=True) + norm_eps)
        inv_ref[r, :] = jnp.broadcast_to(inv, (rows, 128))

    early[0].wait()
    tiles(seq // rows, masks)
    early[1].wait()

    for k in range(n_shard - 1):
        for way in WAYS:
            @pl.when(links.comes(way, k))
            def _():
                gain_came(way, k).wait_recv()
                if k + 1 < n_shard - 1:
                    @pl.when(links.goes(way, k + 1))
                    def _():
                        gain_line_copy(way, k + 1).start()

    def gains():
        return jnp.concatenate([gain_full[s] for s in range(n_shard)], 1)

    def norm(i):
        r = span(i, rows)
        xn[r, :] = (tok[r, :].astype(F32) * inv_ref[r, :1] * gains()).astype(B16)

    tiles(seq // rows, norm)

    def project(s, fresh=False):
        x = xn[:, span(s, own_in)]

        def columns(c):
            part = mm(x, flat(w_in[(s,) + (slice(None),) * (nb + 1) + (span(c, TILE),)]))
            at = span(c, TILE)
            dxn[:, at] = part if fresh else dxn[:, at] + part

        tiles(all_in // TILE, columns)

    project(me, True)
    items = [(get_in, k, k) for k in range(n_shard - 1)] + [(get_out, k, n_shard - 1 + k) for k in range(n_shard - 1)]

    def gather_time(t):
        for gather, k, at in items:
            if t == (k if gather is get_in else k + 1):
                gather.arrive(k)
        for gather, k, at in items:
            if 0 <= t - at <= nb:
                gather.event(k, t - at, project if gather is get_in else None)

    first_phase = n_shard - 1 + nb
    get_out.start()
    for t in range(first_phase):
        gather_time(t)
    later = list(range(first_phase, items[-1][2] + nb + 1))

    def tables():
        c, s = cosine[...], sine[...]
        return jnp.concatenate([c] * (TILE // pair), 1), jnp.concatenate([s] * (TILE // pair), 1)

    def query_tile(i):
        per = q_part // TILE
        x = dxn[:, pl.ds(pl.multiple_of(lax.div(i, per) * chunk + lax.rem(i, per) * TILE, TILE), TILE)]
        c, s = tables()
        q[:, span(i, TILE)] = (x * c + swap_halves(x) * s).astype(B16) * B16(scale)

    tiles(q_width // TILE, query_tile)
    low = lax.broadcasted_iota(jnp.int32, (seq, pair), 1) < HEAD_SIZE

    def split(x, into, into_t, shrink):
        for g in range(kv_heads):
            two = x[:, (g // 2) * pair : (g // 2 + 1) * pair].astype(B16).astype(F32)
            other = pltpu.roll(two, HEAD_SIZE, 1)
            first, second = (two, other) if g % 2 == 0 else (other, two)
            sides = jnp.where(low, first, 0.0).astype(B16), jnp.where(low, 0.0, second).astype(B16)
            for b in range(n_tok):
                for side in range(2):
                    at = slice((2 * b + side) * TILE, (2 * b + side + 1) * TILE)
                    part = sides[side][b * TILE : (b + 1) * TILE]
                    into[g, at, :] = part
                    into_t[g, :, at] = part.T * B16(shrink)

    for first, into, into_t, turned in ((q_part, kx, kxt, True), (q_part + kv_part, vx, vxt, False)):
        x = jnp.concatenate([dxn[:, c * chunk + first : c * chunk + first + kv_part] for c in range(2)], 1)
        if turned:
            c, s = tables()
            x = x * c + swap_halves(x) * s
        split(x, into, into_t, scale if turned else 1.0)

    def blocks():
        for b in range(n_tok):
            first = max(b - 1, 0)
            yield b, slice(b * TILE, (b + 1) * TILE), slice(2 * first * TILE, 2 * (b + 1) * TILE), range(first, b + 1)

    def tile_of(x, j):
        return x[j * TILE : (j + 1) * TILE]

    together = 2

    def forward(i):
        for n, t in enumerate(later):
            @pl.when(i == min(1 + n, pairs // together))
            def _():
                gather_time(t)

        here = [(i * together + u, *block) for u in range(together) for block in blocks()]
        scores = [nt(kx[lax.div(p, per_group), rs, :], q[qs, span(p, pair)]) for p, b, qs, rs, keys in here]
        probs = []
        for (p, b, qs, rs, keys), score in zip(here, scores):
            grown = [
                jnp.exp(tile_of(score, 2 * j + side) + bias[key * TILE : (key + 1) * TILE, qs])
                for j, key in enumerate(keys)
                for side in range(2)
            ]
            inv = []
            for side in range(2):
                inv.append(1.0 / sum(jnp.sum(x, 0, keepdims=True) for x in grown[side::2]))
                inv_l[p, side, :, qs] = inv[side]
            probs.append(jnp.concatenate([(x * inv[j % 2]).astype(B16) for j, x in enumerate(grown)], 0))
        for (p, b, qs, rs, keys), prob in zip(here, probs):
            a_t = mm(vxt[lax.div(p, per_group), :, rs], prob)
            attn_t[span(p, pair), qs] = a_t.astype(B16)
            attn[qs, span(p, pair)] = a_t.T.astype(B16)

    tiles(pairs // together, forward)

    def out_grad(r):
        x = mm(attn_t[...], cot[:, span(r, cols_out)]).astype(B16)
        part_out[(slice(None),) + bits_of(r, nb)] = x.reshape(n_shard, own_out, cols_out)

    tiles(n_rep, out_grad)
    for k in range(n_shard):
        sum_out.start(k)
    for t in later[max(pairs // together - 1, 0) :]:
        gather_time(t)

    def head_grad(s):
        x = None
        for r in range(n_rep):
            part = nt(cot[:, r * cols_out : (r + 1) * cols_out], w_out[(s,) + bits_of(r, nb)])
            x = part if x is None else x + part
        dattn[:, span(s, own_out)] = x.astype(B16)

    tiles(n_shard, head_grad)

    def reduce_time(who, t):
        for step in reversed(range(nb)):
            if 0 <= t - step < n_shard:
                who.event(t - step, step)

    def weight_grad(c):
        cols = dqkv[:, c * chunk : (c + 1) * chunk]

        def one(k):
            s = sum_in[c].dest(k)
            x = tn(xn[:, span(s, own_in)], cols).astype(B16)
            part_in[(s,) + (both,) * nb + part_cols[c]] = x.reshape((2,) * nb + (rows_in, chunk))

        tiles(n_shard, one)
        for k in range(n_shard):
            sum_in[c].start(k)

    n_reduce, n_gather = n_shard + nb - 1, n_shard + nb

    in_loop = (2 * n_reduce) // 3

    def backward(p):
        for t in range(in_loop):
            @pl.when(p == 1 + (t * (pairs - 2)) // max(in_loop - 1, 1))
            def _():
                reduce_time(sum_out, t)

        @pl.when(p == pairs // 2)
        def _():
            weight_grad(0)

        g = lax.div(p, per_group)
        lanes = span(p, pair)

        @pl.when(lax.rem(p, per_group) == 0)
        def _():
            dk_acc[...] = jnp.zeros_like(dk_acc)
            dv_acc[...] = jnp.zeros_like(dv_acc)

        scores = [(nt(kx[g, rs, :], q[qs, lanes]), nt(vx[g, rs, :], dattn[qs, lanes])) for b, qs, rs, keys in blocks()]
        grads = []
        for (b, qs, rs, keys), (score, dp) in zip(blocks(), scores):
            prob = [
                jnp.exp(tile_of(score, 2 * j + side) + bias[key * TILE : (key + 1) * TILE, qs]) * inv_l[p, side, :, qs]
                for j, key in enumerate(keys)
                for side in range(2)
            ]
            inner = [
                sum(jnp.sum(x * tile_of(dp, 2 * j + side), 0, keepdims=True) for j, x in enumerate(prob[side::2]))
                for side in range(2)
            ]
            ds = [(x * (tile_of(dp, j) - inner[j % 2])).astype(B16) for j, x in enumerate(prob)]
            grads.append((jnp.concatenate([x.astype(B16) for x in prob], 0), jnp.concatenate(ds, 0)))
        for (b, qs, rs, keys), (prob, ds) in zip(blocks(), grads):
            dv_acc[rs, :] += mm(prob, dattn[qs, lanes])
            dk_acc[rs, :] += mm(ds, q[qs, lanes])
            x = mm(kxt[g, :, rs], ds).T
            half_pairs = pairs // 2
            to = lax.div(p, half_pairs) * chunk + lax.rem(p, half_pairs) * pair
            dqkv[qs, pl.ds(pl.multiple_of(to, pair), pair)] = (x * cosine[qs, :] - swap_halves(x) * sine[qs, :]).astype(B16)

        @pl.when(lax.rem(p, per_group) == per_group - 1)
        def _():
            def joined(acc):
                both = [acc[j * TILE : (j + 1) * TILE, :] for j in range(2 * n_tok)]
                return jnp.concatenate([both[2 * b] + pltpu.roll(both[2 * b + 1], HEAD_SIZE, 1) for b in range(n_tok)], 0)

            dk, dv = joined(dk_acc), joined(dv_acc)
            dk = dk * cosine[...] - swap_halves(dk) * sine[...]
            for x, first in ((dk, q_part), (dv, q_part + kv_part)):
                half_groups = kv_heads // 2
                to = lax.div(g, half_groups) * chunk + first + lax.div(lax.rem(g, half_groups), 2) * pair
                at = pl.ds(pl.multiple_of(to, pair), pair)
                odd = lax.rem(g, 2)

                @pl.when(odd == 0)
                def _():
                    dqkv[:, at] = x.astype(B16)

                @pl.when(odd == 1)
                def _():
                    high = pltpu.roll(x, HEAD_SIZE, 1)
                    dqkv[:, at] = jnp.where(low, dqkv[:, at].astype(F32), high).astype(B16)

    tiles(pairs, backward)

    weight_grad(1)
    for load in loads:
        load.wait()

    row_acc[...] = jnp.zeros_like(row_acc)

    def input_grad(s):
        c = slice(s * own_in, (s + 1) * own_in)
        d = nt(dqkv[...], flat(w_in[s]))
        normed = tok[:, c].astype(F32) * inv_ref[:, :1]
        gain_acc[s] = jnp.sum(d * normed, 0, keepdims=True)
        d = d * gain_full[s]
        dxn[:, c] = d
        row_acc[...] += jnp.broadcast_to(jnp.sum(d * normed, 1, keepdims=True), row_acc.shape)

    def token_grad(i):
        r = span(i, rows)
        inv = inv_ref[r, :1]
        normed = tok[r, :].astype(F32) * inv
        mean = row_acc[r, :1] * (1.0 / width)
        grad_tok[r, :] = (cot[r, :].astype(F32) + inv * (dxn[r, :] - normed * mean)).astype(B16)

    def output(r):
        c = span(r, cols_out)
        x = mm(attn[...], flat(w_out[(slice(None),) + bits_of(r, nb)]))
        out[:, c] = (tok[:, c].astype(F32) + x).astype(B16)

    def gather_sums_time(who, t):
        if t < n_shard - 1:
            who.whole.arrive(t)
        for i in range(n_shard):
            if 0 <= t - i <= nb:
                who.gather_event(i, t - i)

    todo = []

    def then(method, *args):
        todo.append(functools.partial(method, *args))

    def gain_end():
        gain_out[...] = sum_gain.end()

    out_end = n_reduce - in_loop
    for u in range(3 * n_gather + n_reduce):
        if u < out_end:
            then(reduce_time, sum_out, in_loop + u)
        if u < n_reduce:
            then(reduce_time, sum_in[0], u)
        if u == n_reduce:
            then(sum_in[0].finish, decay)
        if 0 <= u - 2 < n_reduce:
            then(reduce_time, sum_in[1], u - 2)
        if u == out_end + 1:
            then(sum_out.finish, decay)
        if u == n_reduce + 2:
            then(sum_in[1].finish, decay)
        for who, lag in ((sum_in[0], n_reduce + 1), (sum_in[1], n_reduce + 3), (sum_out, out_end + 2)):
            if 0 <= u - lag < n_gather:
                then(gather_sums_time, who, u - lag)
        if 0 <= u - n_reduce - 3 < nb:
            then(sum_gain.event, u - n_reduce - 3)
        if u == n_reduce + nb + 4:
            then(gain_end)

    def advance():
        todo.pop(0)()

    for s in range(n_shard):
        advance()
        input_grad(s)
    sum_gain.send(0).start()
    advance()
    tiles(seq // rows, token_grad)
    gone = [pltpu.make_async_copy(grad_tok, grad_hbm, load_sem.at[16]), pltpu.make_async_copy(out, out_hbm, load_sem.at[17])]
    gone[0].start()
    advance()
    tiles(n_rep // 2, output)
    advance()
    tiles(n_rep // 2, lambda r: output(r + n_rep // 2))
    gone[1].start()
    while todo:
        advance()

    for who in (get_in, get_out, sum_out, *sum_in):
        who.drain()
    for copy in gone:
        copy.wait()
    for way in WAYS:
        for k in range(n_shard - 1):
            @pl.when(links.goes(way, k))
            def _():
                gain_line_copy(way, k).wait_send()
    assert len(links.names) <= send.shape[0]


def layer(tok, cot, seg, gain, weights, moments, decay, n_rep, n_shard, collective_id):
    seq, width = tok.shape
    w_query, w_key, _, w_outproj = weights
    q_width, kv_width = w_query.shape[1], w_key.shape[1]
    all_in = q_width + 2 * kv_width
    kv_heads, pair = kv_width // HEAD_SIZE, 2 * HEAD_SIZE
    nb = n_rep.bit_length() - 1
    bits = (2,) * nb
    own_in, own_out = width // n_shard, q_width // n_shard
    piece_in, piece_out = (own_in // n_rep, all_in), (own_out, width // n_rep)
    half = HEAD_SIZE // 2
    frequency = np.tile((rope_base ** (-2.0 * np.arange(half) / HEAD_SIZE)).astype(np.float32), pair // half)[None]
    vmem, any_ = pl.BlockSpec(memory_space=pltpu.VMEM), pl.BlockSpec(memory_space=pl.ANY)
    V, D = pltpu.VMEM, pltpu.SemaphoreType.DMA
    n_sems = (
        5 * 2 * (n_shard - 1) * (2 + 2 * nb) + 3 * (n_shard * (1 + 2 * (nb - 1)) + n_shard - 1 + 2 * nb) + nb + 3 * n_shard
    )
    bufs = [V((n_shard,) + (2,) * (nb - 1 - j) + piece, B16) for piece in (piece_in, piece_out) for j in range(nb)]
    shape = jax.ShapeDtypeStruct
    return pl.pallas_call(
        functools.partial(layer_kernel, n_rep, n_shard, decay),
        out_shape=[
            shape((seq, width), B16),
            shape((seq, width), B16),
            shape(bits + piece_in, B16),
            shape(bits + piece_out, B16),
            shape((n_shard,) + bits + piece_in, B16),
            shape((n_shard,) + bits + piece_out, B16),
            shape((1, own_in), F32),
        ],
        in_specs=[any_] * 2 + [vmem] * 3 + [any_] * 8,
        out_specs=[any_] * 6 + [vmem],
        scratch_shapes=[
            V((seq, width), B16),
            V((seq, width), B16),
            V((seq, width), B16),
            V((seq, width), B16),
            V((n_shard,) + bits + piece_in, B16),
            V((n_shard,) + bits + piece_out, B16),
            V((n_shard, 1, own_in), F32),
            V((seq, width), B16),
            V((seq, 128), F32),
            V((seq, q_width), B16),
            V((seq, q_width), B16),
            V((q_width, seq), B16),
            V((seq, q_width), B16),
            V((seq, all_in), B16),
            V((seq, width), F32),
            V((seq, 128), F32),
            V((kv_heads, 2 * seq, pair), B16),
            V((kv_heads, 2 * seq, pair), B16),
            V((kv_heads, pair, 2 * seq), B16),
            V((kv_heads, pair, 2 * seq), B16),
            V((2 * seq, pair), F32),
            V((2 * seq, pair), F32),
            V((seq, seq), F32),
            V((seq, pair), F32),
            V((seq, pair), F32),
            V((q_width // pair, 2, 1, seq), F32),
            V((n_shard,) + bits + piece_in, B16),
            V((n_shard,) + bits + piece_out, B16),
            V((n_shard, 1, own_in), F32),
            V((nb, n_shard, 1, own_in), F32),
            V((n_shard, 1, own_in), F32),
            V(piece_in, F32),
            V(piece_out, F32),
            V((n_shard,) + piece_in, B16),
            V(piece_in, B16),
            V(piece_in, B16),
            V((n_shard,) + piece_out, B16),
            V(piece_out, B16),
            V(piece_out, B16),
            D((18,)),
            D((3,)),
            D((n_sems,)),
            D((n_sems,)),
        ]
        + bufs,
        compiler_params=pltpu.CompilerParams(
            collective_id=collective_id, has_side_effects=True, vmem_limit_bytes=67_043_328
        ),
        name="layer",
    )(tok, cot, seg[None], frequency, gain[None], *weights, *moments)


gain_rate = 0.2


def on_device(
    tokens,
    segments,
    cotangent,
    gain,
    w_query,
    w_key,
    w_value,
    w_outproj,
    moment_gain,
    moment_query,
    moment_key,
    moment_value,
    moment_outproj,
):
    n_rep, n_shard = lax.axis_size("rep"), lax.axis_size("shard")
    total_tokens = tokens.shape[0] * tokens.shape[1] * n_rep * n_shard
    weights = (w_query, w_key, w_value, w_outproj)
    moments = (moment_query, moment_key, moment_value, moment_outproj)
    result, grad_tokens, sum_in, sum_out, m_in, m_out, grad_gain = layer(
        tokens[0], cotangent[0], segments[0], gain, weights, moments, decay, n_rep, n_shard, 0
    )
    grad_gain = grad_gain[0]
    moment_gain_next = decay * moment_gain + grad_gain
    gain_next = gain - gain_rate / math.sqrt(total_tokens) * moment_gain_next
    own_out, cols_out = sum_out.shape[-2:]
    m_out = m_out.reshape(n_shard, n_rep, own_out, cols_out)
    all_in = sum_in.shape[-1]
    grads, moments_next, (result, grad_tokens), (mix, mix_kv, scales) = muon(
        m_in.reshape(-1, all_in),
        m_out,
        sum_in.reshape(-1, all_in),
        sum_out.reshape(n_rep, own_out, cols_out),
        moments,
        (result, grad_tokens),
    )
    updated = update(mix, mix_kv, scales, m_out, moments_next, weights, n_rep, 1)
    return (
        result[None],
        grad_tokens[None],
        grad_gain,
        *grads,
        gain_next,
        *updated,
        moment_gain_next,
        *moments_next,
    )


def solution(mesh):
    in_specs = (
        P(("rep", "shard"), None, None),
        P(("rep", "shard"), None),
        P(("rep", "shard"), None, None),
        P("shard"),
        P("shard", None),
        P("shard", None),
        P("shard", None),
        P("shard", None),
        P("shard"),
        P("shard", None),
        P("shard", None),
        P("shard", None),
        P("shard", None),
    )
    out_specs = (
        P(("rep", "shard"), None, None),
        P(("rep", "shard"), None, None),
        P("shard"),
        P("shard", None),
        P("shard", None),
        P("shard", None),
        P("shard", None),
        P("shard"),
        P("shard", "rep"),
        P("shard", "rep"),
        P("shard", "rep"),
        P("shard", "rep"),
        P("shard"),
        P("shard", None),
        P("shard", None),
        P("shard", None),
        P("shard", None),
    )
    return jax.shard_map(on_device, mesh=mesh, in_specs=in_specs, out_specs=out_specs, check_vma=False)
```

```python
import functools
import math

import jax
import jax.numpy as jnp
import numpy as np
from jax import lax
from jax.experimental import pallas as pl
from jax.experimental.pallas import tpu as pltpu
from jax.sharding import PartitionSpec as P

coef_a = 3.4445
coef_b = -4.775
coef_c = 2.0315
SWEEPS = 5
decay = 0.95
muon_rate = 0.02


def nt(left, right):
    return lax.dot_general(left, right, (((1,), (1,)), ((), ())), preferred_element_type=jnp.float32)


def tn(left, right):
    return lax.dot_general(left, right, (((0,), (0,)), ((), ())), preferred_element_type=jnp.float32)


def mm(left, right):
    return jnp.dot(left, right, preferred_element_type=jnp.float32)


def tiles(count, body):
    def one(i, carry):
        body(i)
        return carry

    lax.fori_loop(0, count, one, 0)


def span(i, size):
    return pl.ds(pl.multiple_of(i * size, size), size)


def total(x):
    return jnp.sum(jnp.sum(x, axis=1, keepdims=True), axis=0, keepdims=True)


class Iterate:
    def __init__(self, e, ebf, k, kbf, h, hbf, fbf):
        self.e, self.ebf, self.k, self.kbf, self.h, self.hbf, self.fbf = e, ebf, k, kbf, h, hbf, fbf
        self.n = n = e.shape[0]
        self.diag = min(256, n)
        self.squares = [slice(d, d + self.diag) for d in range(0, n, self.diag)]
        half = n // 2
        if n <= 256:
            self.blocks = [(slice(0, n), slice(0, n))]
        else:
            self.blocks = [(slice(0, n), slice(0, half)), (slice(half, n), slice(half, n))]

    def put(self, ref, at, value):
        r, c = at
        ref[r, c] = value.astype(jnp.bfloat16)
        if r != c:
            ref[c, c.stop : r.stop] = ref[c.stop : r.stop, c].T

    def eye(self):
        shape = (self.diag, self.diag)
        return lax.broadcasted_iota(jnp.int32, shape, 0) == lax.broadcasted_iota(jnp.int32, shape, 1)

    def trace(self, ref):
        mask = self.eye()
        return sum(total(jnp.where(mask, ref[d, d], 0.0)) for d in self.squares)

    def centre(self, s):
        shift = self.trace(self.e) * (1.0 / self.n)
        mask = self.eye()
        for d in self.squares:
            moved = self.e[d, d] - jnp.where(mask, shift, 0.0)
            self.e[d, d] = moved
            self.ebf[d, d] = moved.astype(jnp.bfloat16)
        return s + shift

    def start(self):
        norm = jnp.sqrt(self.trace(self.e)) + 1e-06
        scale = 1.0 / (norm * norm)
        for at in self.blocks:
            x = self.e[at] * scale
            self.e[at] = x
            self.put(self.ebf, at, x)
        return self.centre(jnp.zeros((1, 1), jnp.float32)), 1.0 / norm

    def polynomial(self, s, at):
        p1 = coef_b + 2.0 * coef_c * s
        self.put(self.fbf, at, p1 * self.e[at] + coef_c * mm(self.ebf[at[0], :], self.ebf[:, at[1]]))

    def first(self):
        for at in self.blocks:
            f = self.fbf[at].astype(jnp.float32)
            self.h[at] = f
            self.put(self.hbf.at[0], at, f)

    def grow(self, p0, q, at, now, later):
        new = p0 * self.h[at] + q * self.fbf[at].astype(jnp.float32) + mm(self.fbf[at[0], :], self.hbf[now, :, at[1]])
        self.h[at] = new
        self.put(self.hbf.at[later], at, new)

    def inner(self, p0, s, at):
        new = p0 * self.e[at] + s * self.fbf[at].astype(jnp.float32) + mm(self.fbf[at[0], :], self.ebf[:, at[1]])
        self.k[at] = new
        self.put(self.kbf, at, new)

    def outer(self, p0, beta, at):
        new = p0 * self.k[at] + beta * self.fbf[at].astype(jnp.float32) + mm(self.fbf[at[0], :], self.kbf[:, at[1]])
        self.e[at] = new
        self.put(self.ebf, at, new)


def muon_kernel(*refs):
    refs = list(refs)

    def take(count):
        return [refs.pop(0) for _ in range(count)]

    m_in, m_out, *passed = take(4)
    g_in, g_out, *moments = take(6)
    grads_out, moments_out, passed_out = take(4), take(4), take(2)
    h_out, hs_out, scal = take(3)
    grads, news, held = take(4), take(4), take(2)
    sums_in, sums_out, tall, lump, x, small_m = take(6)
    in_sem, own_sem, out_sem, pass_sem = take(4)
    big, small = Iterate(*take(7)), Iterate(*take(7))
    f32, b16 = jnp.float32, jnp.bfloat16
    core = lax.rem(lax.axis_index("rep"), 2)
    shard = lax.axis_index("shard")
    n, ns = big.n, small.n
    own_in = g_in.shape[0]
    n_rep, own_out, cols_out = g_out.shape
    chunk, q_part, kv_part = (n + 2 * ns) // 2, n // 2, ns // 2
    firsts = [(0, q_part), (q_part, kv_part), (q_part + kv_part, kv_part)]

    wide = [
        pltpu.make_async_copy(m_in.at[:, pl.ds(c * chunk, q_part)], tall.at[:, pl.ds(c * q_part, q_part)], in_sem.at[c])
        for c in range(2)
    ]
    flat = pltpu.make_async_copy(m_out, lump, in_sem.at[0])
    kv = [
        pltpu.make_async_copy(
            m_in.at[:, pl.ds(pl.multiple_of(c * chunk + q_part + core * kv_part, 128), kv_part)],
            small_m.at[:, pl.ds(c * kv_part, kv_part)],
            in_sem.at[2 + c],
        )
        for c in range(2)
    ]
    own = [pltpu.make_async_copy(a, b, own_sem.at[i]) for i, (a, b) in enumerate(zip(moments, news))]
    own_sums = [pltpu.make_async_copy(g_in, sums_in, own_sem.at[4]), pltpu.make_async_copy(g_out, sums_out, own_sem.at[5])]
    passing = [pltpu.make_async_copy(a, b, pass_sem.at[i]) for i, (a, b) in enumerate(zip(passed, held))]
    leaving = [pltpu.make_async_copy(a, b, pass_sem.at[i]) for i, (a, b) in enumerate(zip(held, passed_out))]

    @pl.when(core == 0)
    def _():
        for copy in wide:
            copy.start()

    @pl.when(core != 0)
    def _():
        flat.start()

    for copy in kv + own_sums + own:
        copy.start()

    mine = span(shard, own_in)
    rows = 64

    @pl.when(core == 0)
    def _():
        for copy in wide:
            copy.wait()
        tiles(tall.shape[0] // 256, lambda i: x.__setitem__((slice(None), span(i, 256)), tall[span(i, 256), :].T))

    @pl.when(core != 0)
    def _():
        flat.wait()
        for s in range(lump.shape[0]):
            tiles(n_rep, lambda r, s=s: x.__setitem__((slice(s * own_out, (s + 1) * own_out), span(r, cols_out)), lump[s, r]))

    for copy in kv + own_sums + own:
        copy.wait()
    for copy in passing:
        copy.start()
    for i in range(4):
        if i < 3:
            def update(j, i=i, first=firsts[i][0], width=firsts[i][1]):
                r = span(j, rows)
                for c in range(2):
                    at, to = c * chunk + first, slice(c * width, (c + 1) * width)
                    grad = sums_in[r, at : at + width].astype(f32)
                    grads[i][r, to] = grad
                    news[i][r, to] = decay * news[i][r, to] + grad

            tiles(own_in // rows, update)
        else:
            def update(r, i=i):
                at = span(r, cols_out)
                grad = sums_out[r].astype(f32)
                grads[i][:, at] = grad
                news[i][:, at] = decay * news[i][:, at] + grad

            tiles(n_rep, update)

    @pl.when(core == 0)
    def _():
        x[:, mine] = news[0][...].astype(b16).T
        small_m[mine, :] = news[1][...].astype(b16)

    @pl.when(core != 0)
    def _():
        x[span(shard, own_out), :] = news[3][...].astype(b16)
        small_m[mine, :] = news[2][...].astype(b16)

    copies = [
        pltpu.make_async_copy(a, b, out_sem.at[i])
        for i, (a, b) in enumerate(zip(grads + news, grads_out + moments_out))
    ]
    for copy in copies:
        copy.start()
    for a, b in zip(passing, leaving):
        a.wait()
        b.start()
    for r, c in big.blocks:
        big.e[r, c] = nt(x[r, :], x[c, :])
    small.e[...] = tn(small_m[...], small_m[...])
    s, inv = big.start()
    ss, sinv = small.start()

    def sweep(it, carry):
        s, q, ss, sq = carry
        now, later = lax.rem(it + 1, 2), lax.rem(it, 2)
        p0 = coef_a + s * (coef_b + coef_c * s)
        sp0 = coef_a + ss * (coef_b + coef_c * ss)

        def each(method, *args):
            for i, c in enumerate(big.blocks):
                getattr(big, method)(*[a[0] for a in args], c, *extra)
                if i == 0:
                    for d in small.blocks:
                        getattr(small, method)(*[a[1] for a in args], d, *extra)

        extra = ()
        each("polynomial", (s, ss))

        @pl.when(it == 0)
        def _():
            big.first()
            small.first()

        extra = (now, later)

        @pl.when(it > 0)
        def _():
            each("grow", (p0, sp0), (q, sq))

        extra = ()
        q, sq = p0 * q, sp0 * sq

        def advance():
            each("inner", (p0, sp0), (s, ss))
            beta, sbeta = p0 * s, sp0 * ss
            each("outer", (p0, sp0), (beta, sbeta))
            return big.centre(p0 * beta), small.centre(sp0 * sbeta)

        s, ss = lax.cond(it < SWEEPS - 1, advance, lambda: (s, ss))
        return s, q, ss, sq

    one = jnp.ones((1, 1), f32)
    s, q, ss, sq = lax.fori_loop(0, SWEEPS, sweep, (s, one, ss, one))
    last = (SWEEPS - 1) % 2
    h_out[...] = big.hbf[last]
    hs_out[...] = small.hbf[last]
    row = lax.broadcasted_iota(jnp.int32, (8, 128), 0)
    scal[...] = jnp.where(row == 0, q * inv, jnp.where(row == 1, inv, jnp.where(row == 2, sq * sinv, sinv)))
    for copy in copies + leaving:
        copy.wait()


def muon(m_in, m_out, g_in, g_out, moments, passed):
    f32, b16 = jnp.float32, jnp.bfloat16
    tall, n, kv = m_in.shape[0], m_out.shape[0] * m_out.shape[2], moments[1].shape[1]
    V = pltpu.VMEM
    sets = []
    for d in (n, kv):
        sets += [V((d, d), f32), V((d, d), b16), V((d, d), f32), V((d, d), b16), V((d, d), f32), V((2, d, d), b16), V((d, d), b16)]
    vmem, any_ = pl.BlockSpec(memory_space=pltpu.VMEM), pl.BlockSpec(memory_space=pl.ANY)
    own = [jax.ShapeDtypeStruct(m.shape, f32) for m in moments]
    out = pl.pallas_call(
        muon_kernel,
        out_shape=own
        + own
        + [jax.ShapeDtypeStruct(p.shape, p.dtype) for p in passed]
        + [
            jax.ShapeDtypeStruct((n, n), b16),
            jax.ShapeDtypeStruct((kv, kv), b16),
            jax.ShapeDtypeStruct((8, 128), f32),
        ],
        in_specs=[any_] * 10,
        out_specs=[any_] * 10 + [vmem] * 3,
        scratch_shapes=[V(m.shape, f32) for m in moments] * 2
        + [V(p.shape, p.dtype) for p in passed]
        + [
            V(g_in.shape, b16),
            V(g_out.shape, b16),
            V((tall, n), b16),
            V(m_out.shape, b16),
            V((n, m_out.shape[1] * m_out.shape[3]), b16),
            V((tall, kv), b16),
            pltpu.SemaphoreType.DMA((4,)),
            pltpu.SemaphoreType.DMA((6,)),
            pltpu.SemaphoreType.DMA((8,)),
            pltpu.SemaphoreType.DMA((2,)),
        ]
        + sets,
        compiler_params=pltpu.CompilerParams(vmem_limit_bytes=63 << 20),
        name="muon",
    )(m_in, m_out, *passed, g_in, g_out, *moments)
    return out[:4], out[4:8], out[8:10], out[10:]


def swap_kernel(n_rep, h, hs, scal, h_pair, hs_come, scal_come, send, recv):
    rep, shard = lax.axis_index("rep"), lax.axis_index("shard")
    core = lax.rem(rep, 2)
    other = rep + 1 - 2 * core
    sem = pltpu.get_barrier_semaphore()
    pl.semaphore_signal(sem, 1, device_id=(other, shard), device_id_type=pl.DeviceIdType.MESH)
    pl.semaphore_wait(sem, 1)

    def remote(src, dst, i):
        return pltpu.make_async_remote_copy(
            src, dst, send.at[i], recv.at[i], device_id=(other, shard), device_id_type=pl.DeviceIdType.MESH
        )

    count = h_pair.shape[0]
    at = jnp.where(core == 0, lax.div(rep, 2), shard)
    copies = [remote(h.at[span(at, count), :], h_pair, 0), remote(hs, hs_come, 1), remote(scal, scal_come, 2)]
    for c in copies:
        c.start()
    for c in copies:
        c.wait()


def swap(h, hs, scal, count, n_rep, collective_id):
    any_ = pl.BlockSpec(memory_space=pl.ANY)
    return pl.pallas_call(
        functools.partial(swap_kernel, n_rep),
        out_shape=[
            jax.ShapeDtypeStruct((count, h.shape[1]), h.dtype),
            jax.ShapeDtypeStruct(hs.shape, hs.dtype),
            jax.ShapeDtypeStruct(scal.shape, scal.dtype),
        ],
        in_specs=[any_] * 3,
        out_specs=[any_] * 3,
        scratch_shapes=[pltpu.SemaphoreType.DMA((3,)), pltpu.SemaphoreType.DMA((3,))],
        compiler_params=pltpu.CompilerParams(collective_id=collective_id, has_side_effects=True),
        name="swap",
    )(h, hs, scal)


def window(index, width):
    size = max(width, 128)
    start = lax.div(index * width, size) * size
    return pl.ds(pl.multiple_of(start, 128), size), size, index * width - start


def cut(x, size, offset, width):
    return x if size == width else pltpu.roll(x, lax.rem(size - offset, size), 1)[:, :width]


def update_kernel(h, h_pair, hs, hs_come, scal, scal_come, m_out, mq_hbm, mk_hbm, mv_hbm, mo, wq, wk, wv, wo, *refs):
    nexts, (hq, ho, flat, mo_win), weight_wins, (mq, mk, mv), (h_sem, sem) = (
        refs[:4], refs[4:8], refs[8:12], refs[12:15], refs[15:]
    )
    f32, b16 = jnp.float32, jnp.bfloat16
    rep, shard = lax.axis_index("rep"), lax.axis_index("shard")
    even = lax.rem(rep, 2) == 0
    widths = [nexts[0].shape[1], nexts[1].shape[0], nexts[2].shape[0], nexts[3].shape[1]]
    wins = [window(rep, w) for w in widths]
    own_out = ho.shape[0]
    copies = [
        pltpu.make_async_copy(m_out.at[:, rep], flat, sem.at[4]),
        pltpu.make_async_copy(mo.at[:, wins[3][0]], mo_win, sem.at[5]),
        pltpu.make_async_copy(mq_hbm, mq, sem.at[6]),
        pltpu.make_async_copy(mk_hbm, mk, sem.at[7]),
        pltpu.make_async_copy(mv_hbm, mv, sem.at[8]),
    ] + [pltpu.make_async_copy(w.at[:, wins[i][0]], weight_wins[i], sem.at[i]) for i, w in enumerate((wq, wk, wv, wo))]
    for copy in copies:
        copy.start()
    rows_q = h.at[span(rep, widths[0]), :], h_pair.at[pl.ds(h_pair.shape[0] - widths[0], widths[0]), :]
    rows_o = h_pair, h.at[span(shard, own_out), :]
    mixes = [[pltpu.make_async_copy(a, b, h_sem.at[i]) for i, (a, b) in enumerate(((q, hq), (o, ho)))] for q, o in zip(rows_q, rows_o)]
    for side, here in ((0, even), (1, jnp.logical_not(even))):
        @pl.when(here)
        def _():
            for copy in mixes[side]:
                copy.start()
            for copy in mixes[side]:
                copy.wait()
    for copy in copies:
        copy.wait()
    first = jnp.where(even, scal[...], scal_come[...])
    second = jnp.where(even, scal_come[...], scal[...])
    flat[shard] = mo_win[...].astype(b16)

    def rows_of(i):
        at = span(rep, widths[i])
        mine, theirs = hs[at, :].astype(f32), hs_come[at, :].astype(f32)
        return jnp.where(even == (i == 1), mine, theirs).astype(b16)

    parts = (
        (mq, lambda: nt(mq[...].astype(b16), hq[...]), first[0:1, 0:1], first[1:2, 0:1]),
        (mk, lambda: nt(rows_of(1), mk[...].astype(b16)), first[2:3, 0:1], first[3:4, 0:1]),
        (mv, lambda: nt(rows_of(2), mv[...].astype(b16)), second[2:3, 0:1], second[3:4, 0:1]),
        (None, lambda: mm(ho[...], flat[...].reshape(-1, flat.shape[2])), second[0:1, 0:1], second[1:2, 0:1]),
    )
    n_shard = lax.axis_size("shard")
    for i, (moment, product, straight, mixed) in enumerate(parts):
        at, size, offset = wins[i]

        def mine(x):
            x = cut(x, size, offset, widths[i])
            return x.T if i in (1, 2) else x

        here = mine(mo_win[...] if moment is None else moment[:, at])
        ortho = straight * here + mixed * product()
        whole = (weight_wins[i].shape[0] * n_shard, (wq, wk, wv, wo)[i].shape[1])
        nexts[i][...] = mine(weight_wins[i][...]) - muon_rate * math.sqrt(max(whole)) * ortho


def update(h, hs, scal, m_out, moments, weights, n_rep, collective_id):
    f32, b16 = jnp.float32, jnp.bfloat16
    widths = [w.shape[1] // n_rep for w in weights]
    own_out = weights[3].shape[0]
    assert 2 * widths[0] == own_out and m_out.shape[3] == widths[3]
    h_pair, hs_come, scal_come = swap(h, hs, scal, own_out, n_rep, collective_id)
    vmem, any_ = pl.BlockSpec(memory_space=pltpu.VMEM), pl.BlockSpec(memory_space=pl.ANY)
    V = pltpu.VMEM
    sizes = [max(w, 128) for w in widths]
    shapes = [(w.shape[0], width) for w, width in zip(weights, widths)]
    out = pl.pallas_call(
        update_kernel,
        out_shape=[jax.ShapeDtypeStruct(s[::-1] if i in (1, 2) else s, f32) for i, s in enumerate(shapes)],
        in_specs=[any_] * 2 + [vmem] * 4 + [any_] * 9,
        out_specs=[vmem] * 4,
        scratch_shapes=[
            V((widths[0], h.shape[1]), b16),
            V((own_out, h.shape[1]), b16),
            V((m_out.shape[0],) + m_out.shape[2:], b16),
            V((own_out, sizes[3]), f32),
        ]
        + [V((w.shape[0], size), f32) for w, size in zip(weights, sizes)]
        + [V(m.shape, f32) for m in moments[:3]]
        + [pltpu.SemaphoreType.DMA((2,)), pltpu.SemaphoreType.DMA((9,))],
        name="update",
    )(h, h_pair, hs, hs_come, scal, scal_come, m_out, *moments, *weights)
    return out[0], out[1].T, out[2].T, out[3]


HEAD_SIZE = 64
TILE = 256
norm_eps = 1e-05
rope_base = 500000.0
F32, B16 = jnp.float32, jnp.bfloat16
MESH = pl.DeviceIdType.MESH
WAYS = (1, -1)


class Links:
    def __init__(self, n_rep, n_shard, send, recv):
        self.n_bits, self.n_shard = n_rep.bit_length() - 1, n_shard
        self.rep, self.shard = lax.axis_index("rep"), lax.axis_index("shard")
        self.bits = [lax.rem(lax.div(self.rep, 1 << b), 2) for b in range(self.n_bits)]
        far = list(range(1, self.n_bits))
        self.orders = (far, far[::-1])
        self.send, self.recv, self.names = send, recv, {}

    def flip(self, bit):
        return self.rep + (1 << bit) * (1 - 2 * self.bits[bit])

    def barrier(self):
        sem = pltpu.get_barrier_semaphore()
        for b in range(self.n_bits):
            pl.semaphore_signal(sem, 1, device_id=(self.flip(b), self.shard), device_id_type=MESH)
        for k in range(1, self.n_shard):
            there = lax.rem(self.shard + k, self.n_shard)
            pl.semaphore_signal(sem, 1, device_id=(self.rep, there), device_id_type=MESH)
        pl.semaphore_wait(sem, self.n_bits + self.n_shard - 1)

    def where(self, free=()):
        return tuple(slice(None) if b in free else self.bits[b] for b in reversed(range(self.n_bits)))

    def remote(self, src, dst, name, rep, shard):
        i = self.names.setdefault(name, len(self.names))
        return pltpu.make_async_remote_copy(
            src, dst, self.send.at[i], self.recv.at[i], device_id=(rep, shard), device_id_type=MESH
        )

    def goes(self, way, k):
        q, there = self.shard - way * k, self.shard + way
        return (q >= 0) & (q < self.n_shard) & (there >= 0) & (there < self.n_shard)

    def comes(self, way, k):
        q = self.shard - way * (k + 1)
        return (q >= 0) & (q < self.n_shard)


class Gather:
    def __init__(self, links, name, full, half, first=None):
        self.links, self.name, self.full, self.half, self.first = links, name, full, half, first

    def line(self, way, k, h):
        at = self.full.at[(self.links.shard - way * k,) + self.links.where() + self.half[h]]
        src = self.first.at[self.half[h]] if k == 0 and self.first is not None else at
        return self.links.remote(src, at, (self.name, "l", way, k, h), self.links.rep, self.links.shard + way)

    def came(self, way, k, h):
        at = self.full.at[(self.links.shard - way * (k + 1),) + self.links.where() + self.half[h]]
        return self.links.remote(at, at, (self.name, "l", way, k, h), self.links.rep, self.links.shard)

    def plane(self, way, k, h, step):
        links = self.links
        order = links.orders[h] + [0]
        view = self.full.at[(links.shard - way * (k + 1),) + links.where(order[:step]) + self.half[h]]
        return links.remote(view, view, (self.name, "p", way, k, h, step), links.flip(order[step]), links.shard)

    def start(self):
        for way in WAYS:
            @pl.when(self.links.goes(way, 0))
            def _():
                for h in range(2):
                    self.line(way, 0, h).start()

    def arrive(self, k):
        links = self.links
        for way in WAYS:
            @pl.when(links.comes(way, k))
            def _():
                for h in range(2):
                    self.came(way, k, h).wait_recv()
                    if k + 1 < links.n_shard - 1:
                        @pl.when(links.goes(way, k + 1))
                        def _():
                            self.line(way, k + 1, h).start()

    def times(self):
        return self.links.n_shard + self.links.n_bits

    def time(self, t):
        if t < self.links.n_shard - 1:
            self.arrive(t)
        for k in range(self.links.n_shard - 1):
            if 0 <= t - 1 - k <= self.links.n_bits:
                self.event(k, t - 1 - k)

    def event(self, k, step, then=None):
        links = self.links
        for way in WAYS:
            @pl.when(links.comes(way, k))
            def _():
                for h in range(2):
                    if step > 0:
                        self.plane(way, k, h, step - 1).wait_recv()
                    if step < links.n_bits:
                        self.plane(way, k, h, step).start()
                if step == links.n_bits and then is not None:
                    then(links.shard - way * (k + 1))

    def drain(self):
        links = self.links
        for way in WAYS:
            for k in range(links.n_shard - 1):
                @pl.when(links.goes(way, k))
                def _():
                    for h in range(2):
                        self.line(way, k, h).wait_send()

                @pl.when(links.comes(way, k))
                def _():
                    for h in range(2):
                        for step in range(links.n_bits):
                            self.plane(way, k, h, step).wait_send()


class Spread:
    def __init__(self, links, name, full, half, first):
        self.links, self.name, self.full, self.half, self.first = links, name, full, half, first

    def line(self, k, h):
        links = self.links
        d = lax.rem(links.shard + 1 + k, links.n_shard)
        into = self.full.at[(links.shard,) + links.where() + self.half[h]]
        return links.remote(self.first.at[self.half[h]], into, (self.name, "l", k, h), links.rep, d)

    def origin(self, k):
        return lax.rem(self.links.shard + self.links.n_shard - 1 - k, self.links.n_shard)

    def came(self, k, h):
        links = self.links
        at = self.full.at[(self.origin(k),) + links.where() + self.half[h]]
        return links.remote(at, at, (self.name, "l", k, h), links.rep, links.shard)

    def plane(self, k, h, step):
        links = self.links
        order = links.orders[h] + [0]
        view = self.full.at[(self.origin(k),) + links.where(order[:step]) + self.half[h]]
        return links.remote(view, view, (self.name, "p", k, h, step), links.flip(order[step]), links.shard)

    def start(self):
        for k in range(self.links.n_shard - 1):
            for h in range(2):
                self.line(k, h).start()

    def times(self):
        return self.links.n_bits + 1

    def time(self, step):
        for k in range(self.links.n_shard - 1):
            for h in range(2):
                if step == 0:
                    self.came(k, h).wait_recv()
                else:
                    self.plane(k, h, step - 1).wait_recv()
                if step < self.links.n_bits:
                    self.plane(k, h, step).start()

    def drain(self):
        for k in range(self.links.n_shard - 1):
            for h in range(2):
                self.line(k, h).wait_send()
                for step in range(self.links.n_bits):
                    self.plane(k, h, step).wait_send()


class Reduce:
    def __init__(self, links, name, refs, region, half, keep_sem, way_of_whole):
        self.links, self.name, self.region, self.half = links, name, region, half
        self.part, self.bufs, self.zbuf, self.gpiece, self.mpiece, self.moment, self.sums, wholes = refs
        self.whole = way_of_whole(links, name + "m", wholes, half, self.mpiece)
        self.keep = lambda: pltpu.make_async_copy(
            self.gpiece.at[region], self.sums.at[links.where() + region], keep_sem
        )

    def dest(self, k):
        return lax.rem(self.links.shard + 1 + k, self.links.n_shard)

    def origin(self, k):
        return lax.rem(self.links.shard + self.links.n_shard - 1 - k, self.links.n_shard)

    def order(self, h):
        return [0] + self.links.orders[h]

    def cut(self, h, step):
        return self.region if step == 0 else self.half[h]

    def send(self, k, h, step):
        links, o = self.links, self.order(h)
        bit = o[step]
        src = self.part if step == 0 else self.bufs[step - 1]
        left = sorted(o[step:], reverse=True)
        pick = tuple(1 - links.bits[bit] if b == bit else slice(None) for b in left)
        d, cut = self.dest(k), self.cut(h, step)
        into = self.bufs[step].at[(d,) + (slice(None),) * (links.n_bits - 1 - step) + cut]
        return links.remote(src.at[(d,) + pick + cut], into, (self.name, "r", k, h, step), links.flip(bit), links.shard)

    def add(self, k, h, step):
        links, o = self.links, self.order(h)
        src = self.part if step == 0 else self.bufs[step - 1]
        left = sorted(o[step:], reverse=True)
        others = [b for b in left if b != o[step]]
        d, cut = self.dest(k), self.cut(h, step)

        def one(i):
            at = {b: lax.rem(lax.div(i, 1 << (len(others) - 1 - n)), 2) for n, b in enumerate(others)}
            here = (d,) + tuple(at[b] for b in others) + cut
            there = (d,) + tuple(links.bits[b] if b == o[step] else at[b] for b in left) + cut
            both = src[there].astype(F32) + self.bufs[step][here].astype(F32)
            self.bufs[step][here] = both.astype(B16)

        if others:
            tiles(1 << len(others), one)
        else:
            one(0)

    def send_line(self, k):
        links, d = self.links, self.dest(k)
        src, into = self.bufs[-1].at[(d,) + self.region], self.zbuf.at[(links.shard,) + self.region]
        return links.remote(src, into, (self.name, "z", k), links.rep, d)

    def come_line(self, k):
        links, at = self.links, self.zbuf.at[(self.origin(k),) + self.region]
        return links.remote(at, at, (self.name, "z", k), links.rep, links.shard)

    def start(self, k):
        self.send(k, 0, 0).start()

    def event(self, k, step):
        last = self.links.n_bits - 1
        for h in range(1 if step == 0 else 2):
            self.send(k, h, step).wait_recv()
            self.add(k, h, step)
            if step == 0 and last > 0:
                self.send(k, 0, 1).start()
                self.send(k, 1, 1).start()
            elif step < last:
                self.send(k, h, step + 1).start()
        if step == last and k < self.links.n_shard - 1:
            self.send_line(k).start()

    def gather_sum(self, h, step):
        links = self.links
        order = links.orders[h] + [0]
        into = self.sums.at[links.where(order[:step]) + self.half[h]]
        src = self.gpiece.at[self.half[h]] if step == 0 else into
        return links.remote(src, into, (self.name, "g", h, step), links.flip(order[step]), links.shard)

    def finish(self, decay):
        links = self.links
        for k in range(links.n_shard - 1):
            self.come_line(k).wait_recv()
        acc = self.bufs[-1][(links.shard,) + self.region].astype(F32)
        for k in range(links.n_shard - 1):
            acc = acc + self.zbuf[(self.origin(k),) + self.region].astype(F32)
        g = acc.astype(B16)
        self.gpiece[self.region] = g
        self.mpiece[self.region] = (decay * self.moment[self.region] + g.astype(F32)).astype(B16)
        self.whole.start()
        for h in range(2):
            self.gather_sum(h, 0).start()
        self.keep().start()

    def gather_event(self, step):
        if step == 0:
            self.keep().wait()
        if step < self.links.n_bits:
            for h in range(2):
                self.gather_sum(h, step).wait_recv()
                if step + 1 < self.links.n_bits:
                    self.gather_sum(h, step + 1).start()
        self.whole.time(step)

    def drain(self):
        links = self.links
        for k in range(links.n_shard):
            for step in range(links.n_bits):
                for h in range(1 if step == 0 else 2):
                    self.send(k, h, step).wait_send()
            if k < links.n_shard - 1:
                self.send_line(k).wait_send()
        for h in range(2):
            for step in range(links.n_bits):
                self.gather_sum(h, step).wait_send()
        self.whole.drain()


class GainSum:
    def __init__(self, links, acc, come, line):
        self.links, self.acc, self.come, self.line = links, acc, come, line

    def send(self, b):
        return self.links.remote(self.acc, self.come.at[b], ("gain", b), self.links.flip(b), self.links.shard)

    def send_line(self, k):
        links = self.links
        d = lax.rem(links.shard + 1 + k, links.n_shard)
        return links.remote(self.acc.at[d], self.line.at[links.shard], ("gainz", k), links.rep, d)

    def event(self, b):
        links = self.links
        self.send(b).wait()
        self.acc[...] = self.acc[...] + self.come[b]
        if b + 1 < links.n_bits:
            self.send(b + 1).start()
        else:
            for k in range(links.n_shard - 1):
                self.send_line(k).start()

    def end(self):
        links = self.links
        for k in range(links.n_shard - 1):
            self.send_line(k).wait_send()
            at = self.line.at[lax.rem(links.shard + links.n_shard - 1 - k, links.n_shard)]
            links.remote(at, at, ("gainz", k), links.rep, links.shard).wait_recv()
        acc = self.acc[links.shard]
        for q in range(links.n_shard):
            acc = jnp.where(links.shard == q, acc, acc + self.line[q])
        return acc


def swap_halves(x):
    half, width = HEAD_SIZE // 2, x.shape[1]
    lane = lax.rem(lax.broadcasted_iota(jnp.int32, x.shape, 1), HEAD_SIZE)
    return jnp.where(lane < half, pltpu.roll(x, width - half, 1), pltpu.roll(x, half, 1))


def flat(x):
    return x.reshape(-1, x.shape[-1])


def bits_of(r, n_bits):
    return tuple(lax.rem(lax.div(r, 1 << b), 2) if isinstance(r, jax.Array) else (r >> b) & 1 for b in reversed(range(n_bits)))


def layer_kernel(
    n_rep, n_shard, decay,
    tok_hbm, cot_hbm, seg_row, frequency, gain, w_query, w_key, w_value, w_outproj, m_query, m_key, m_value, m_outproj,
    out_hbm, grad_hbm, sums_in, sums_out, wholes_in, wholes_out, gain_out,
    out, grad_tok,    tok, cot, w_in, w_out, gain_full, xn, inv_ref, q, dattn, attn_t, attn, dqkv, dxn, row_acc, kx, vx, kxt, vxt, dk_acc, dv_acc,
    bias, cosine, sine, inv_l, part_in, part_out, gain_acc, gain_come, gain_line, moment_in, moment_out,
    zbuf_in, gp_in, mp_in, zbuf_out, gp_out, mp_out, load_sem, keep_sem, send, recv, *bufs,
):
    seq, width = tok.shape
    q_width, kv_width = w_query.shape[1], w_key.shape[1]
    kv_heads = kv_width // HEAD_SIZE
    pair = 2 * HEAD_SIZE
    pairs = q_width // pair
    per_group = pairs // kv_heads
    n_tok = seq // TILE
    scale = 1.0 / math.sqrt(HEAD_SIZE)
    rows = 64
    nb = n_rep.bit_length() - 1
    own_in, own_out = width // n_shard, q_width // n_shard
    rows_in, cols_out = own_in // n_rep, width // n_rep
    all_in = w_in.shape[-1]
    chunk, q_part, kv_part = all_in // 2, q_width // 2, kv_width // 2
    places = [
        (i, c * size, c * chunk + first, size)
        for c in range(2)
        for i, (first, size) in enumerate(((0, q_part), (q_part, kv_part), (q_part + kv_part, kv_part)))
    ]

    links = Links(n_rep, n_shard, send, recv)
    me, rep = links.shard, links.rep
    both = slice(None)
    part_cols = [(both, pl.ds(c * chunk, chunk)) for c in range(2)]
    half_cols = [[(both, pl.ds(c * chunk + h * (chunk // 2), chunk // 2)) for h in range(2)] for c in range(2)]
    half_in = [(both, pl.ds(h * chunk, chunk)) for h in range(2)]
    half_out = [(pl.ds(h * (own_out // 2), own_out // 2), both) for h in range(2)]
    get_in, get_out = Gather(links, "wi", w_in, half_in), Gather(links, "wo", w_out, half_out)
    refs_in = (part_in, bufs[:nb], zbuf_in, gp_in, mp_in, moment_in, sums_in, wholes_in)
    refs_out = (part_out, bufs[nb:], zbuf_out, gp_out, mp_out, moment_out, sums_out, wholes_out)
    sum_in = [Reduce(links, f"i{c}", refs_in, part_cols[c], half_cols[c], keep_sem.at[c], Spread) for c in range(2)]
    sum_out = Reduce(links, "o", refs_out, (both, both), half_out, keep_sem.at[2], Gather)
    sum_gain = GainSum(links, gain_acc, gain_come, gain_line)

    ws, ms = (w_query, w_key, w_value), (m_query, m_key, m_value)
    loads = [
        pltpu.make_async_copy(ws[i].at[:, pl.ds(at, size)], dxn.at[pl.ds(0, own_in), pl.ds(to, size)], load_sem.at[n])
        for n, (i, at, to, size) in enumerate(places)
    ]
    first = [
        pltpu.make_async_copy(ws[i].at[span(rep, rows_in), pl.ds(at, size)], moment_in.at[:, pl.ds(to, size)], load_sem.at[9 + n])
        for n, (i, at, to, size) in enumerate(places)
    ] + [pltpu.make_async_copy(w_outproj.at[:, span(rep, cols_out)], moment_out, load_sem.at[15])]
    early = [pltpu.make_async_copy(a, b, load_sem.at[7 + i]) for i, (a, b) in enumerate(((tok_hbm, tok), (cot_hbm, cot)))]
    for load in first + loads + early:
        load.start()
    gain_full[me] = gain[...].astype(B16).astype(F32)
    links.barrier()

    def gain_line_copy(way, k):
        at = gain_full.at[me - way * k]
        return links.remote(at, at, ("gf", way, k), rep, me + way)

    def gain_came(way, k):
        at = gain_full.at[me - way * (k + 1)]
        return links.remote(at, at, ("gf", way, k), rep, me)

    for way in WAYS:
        @pl.when(links.goes(way, 0))
        def _():
            gain_line_copy(way, 0).start()
    for load in first:
        load.wait()
    here = (me,) + links.where()
    w_in[here] = moment_in[...].astype(B16)
    get_in.start()
    w_out[here] = moment_out[...].astype(B16)
    for load in loads:
        load.wait()
    for r in range(n_rep):
        @pl.when(rep != r)
        def _():
            w_in[(me,) + bits_of(r, nb)] = dxn[r * rows_in : (r + 1) * rows_in, :all_in].astype(B16)

    load_out = pltpu.make_async_copy(w_outproj, dxn.at[pl.ds(0, own_out), :], load_sem.at[6])
    load_out.start()
    load_out.wait()
    for r in range(n_rep):
        @pl.when(rep != r)
        def _():
            w_out[(me,) + bits_of(r, nb)] = dxn[:own_out, r * cols_out : (r + 1) * cols_out].astype(B16)

    loads = [
        pltpu.make_async_copy(ms[i].at[span(rep, rows_in), pl.ds(at, size)], moment_in.at[:, pl.ds(to, size)], load_sem.at[n])
        for n, (i, at, to, size) in enumerate(places)
    ] + [pltpu.make_async_copy(m_outproj.at[:, span(rep, cols_out)], moment_out, load_sem.at[6])]
    for load in loads:
        load.start()

    row_acc[...] = jnp.broadcast_to(seg_row[...].astype(F32), (row_acc.shape[1], seq)).T
    own_seg = seg_row[...].astype(F32)

    def masks(i):
        r = span(i, rows)
        seg_col = row_acc[r, :1]
        key = lax.broadcasted_iota(jnp.int32, (rows, seq), 0) + i * rows
        query = lax.broadcasted_iota(jnp.int32, (rows, seq), 1)
        seen = (key <= query) & (seg_col == own_seg)
        bias[r, :] = jnp.where(seen, 0.0, -1e30)
        start = jnp.sum(jnp.where(own_seg < seg_col, 1.0, 0.0), 1, keepdims=True)
        at = lax.broadcasted_iota(jnp.int32, (rows, 1), 0) + i * rows
        angle = (at.astype(F32) - start) * frequency[...]
        lane = lax.rem(lax.broadcasted_iota(jnp.int32, (rows, pair), 1), HEAD_SIZE)
        cosine[r, :] = jnp.cos(angle)
        s = jnp.sin(angle)
        sine[r, :] = jnp.where(lane < HEAD_SIZE // 2, -s, s)
        x = tok[r, :].astype(F32)
        inv = lax.rsqrt(jnp.mean(x * x, -1, keepdims=True) + norm_eps)
        inv_ref[r, :] = jnp.broadcast_to(inv, (rows, 128))

    early[0].wait()
    tiles(seq // rows, masks)
    early[1].wait()

    for k in range(n_shard - 1):
        for way in WAYS:
            @pl.when(links.comes(way, k))
            def _():
                gain_came(way, k).wait_recv()
                if k + 1 < n_shard - 1:
                    @pl.when(links.goes(way, k + 1))
                    def _():
                        gain_line_copy(way, k + 1).start()

    def gains():
        return jnp.concatenate([gain_full[s] for s in range(n_shard)], 1)

    def norm(i):
        r = span(i, rows)
        xn[r, :] = (tok[r, :].astype(F32) * inv_ref[r, :1] * gains()).astype(B16)

    tiles(seq // rows, norm)

    def project(s, fresh=False):
        x = xn[:, span(s, own_in)]

        def columns(c):
            part = mm(x, flat(w_in[(s,) + (slice(None),) * (nb + 1) + (span(c, TILE),)]))
            at = span(c, TILE)
            dxn[:, at] = part if fresh else dxn[:, at] + part

        tiles(all_in // TILE, columns)

    project(me, True)
    items = [(get_in, k, k) for k in range(n_shard - 1)] + [(get_out, k, n_shard - 1 + k) for k in range(n_shard - 1)]

    def gather_time(t):
        for gather, k, at in items:
            if t == (k if gather is get_in else k + 1):
                gather.arrive(k)
        for gather, k, at in items:
            if 0 <= t - at <= nb:
                gather.event(k, t - at, project if gather is get_in else None)

    first_phase = n_shard - 1 + nb
    get_out.start()
    for t in range(first_phase):
        gather_time(t)
    later = list(range(first_phase, items[-1][2] + nb + 1))

    def tables():
        c, s = cosine[...], sine[...]
        return jnp.concatenate([c] * (TILE // pair), 1), jnp.concatenate([s] * (TILE // pair), 1)

    def query_tile(i):
        per = q_part // TILE
        x = dxn[:, pl.ds(pl.multiple_of(lax.div(i, per) * chunk + lax.rem(i, per) * TILE, TILE), TILE)]
        c, s = tables()
        q[:, span(i, TILE)] = (x * c + swap_halves(x) * s).astype(B16) * B16(scale)

    tiles(q_width // TILE, query_tile)
    low = lax.broadcasted_iota(jnp.int32, (seq, pair), 1) < HEAD_SIZE

    def split(x, into, into_t, shrink):
        for g in range(kv_heads):
            two = x[:, (g // 2) * pair : (g // 2 + 1) * pair].astype(B16).astype(F32)
            other = pltpu.roll(two, HEAD_SIZE, 1)
            first, second = (two, other) if g % 2 == 0 else (other, two)
            sides = jnp.where(low, first, 0.0).astype(B16), jnp.where(low, 0.0, second).astype(B16)
            for b in range(n_tok):
                for side in range(2):
                    at = slice((2 * b + side) * TILE, (2 * b + side + 1) * TILE)
                    part = sides[side][b * TILE : (b + 1) * TILE]
                    into[g, at, :] = part
                    into_t[g, :, at] = part.T * B16(shrink)

    for first, into, into_t, turned in ((q_part, kx, kxt, True), (q_part + kv_part, vx, vxt, False)):
        x = jnp.concatenate([dxn[:, c * chunk + first : c * chunk + first + kv_part] for c in range(2)], 1)
        if turned:
            c, s = tables()
            x = x * c + swap_halves(x) * s
        split(x, into, into_t, scale if turned else 1.0)

    def blocks():
        for b in range(n_tok):
            first = max(b - 1, 0)
            yield b, slice(b * TILE, (b + 1) * TILE), slice(2 * first * TILE, 2 * (b + 1) * TILE), range(first, b + 1)

    def tile_of(x, j):
        return x[j * TILE : (j + 1) * TILE]

    together = 2

    def forward(i):
        for n, t in enumerate(later):
            @pl.when(i == min(1 + n, pairs // together))
            def _():
                gather_time(t)

        here = [(i * together + u, *block) for u in range(together) for block in blocks()]
        scores = [nt(kx[lax.div(p, per_group), rs, :], q[qs, span(p, pair)]) for p, b, qs, rs, keys in here]
        probs = []
        for (p, b, qs, rs, keys), score in zip(here, scores):
            grown = [
                jnp.exp(tile_of(score, 2 * j + side) + bias[key * TILE : (key + 1) * TILE, qs])
                for j, key in enumerate(keys)
                for side in range(2)
            ]
            inv = []
            for side in range(2):
                inv.append(1.0 / sum(jnp.sum(x, 0, keepdims=True) for x in grown[side::2]))
                inv_l[p, side, :, qs] = inv[side]
            probs.append(jnp.concatenate([(x * inv[j % 2]).astype(B16) for j, x in enumerate(grown)], 0))
        for (p, b, qs, rs, keys), prob in zip(here, probs):
            a_t = mm(vxt[lax.div(p, per_group), :, rs], prob)
            attn_t[span(p, pair), qs] = a_t.astype(B16)
            attn[qs, span(p, pair)] = a_t.T.astype(B16)

    tiles(pairs // together, forward)

    def out_grad(r):
        x = mm(attn_t[...], cot[:, span(r, cols_out)]).astype(B16)
        part_out[(slice(None),) + bits_of(r, nb)] = x.reshape(n_shard, own_out, cols_out)

    tiles(n_rep, out_grad)
    for k in range(n_shard):
        sum_out.start(k)
    for t in later[max(pairs // together - 1, 0) :]:
        gather_time(t)

    def head_grad(s):
        x = None
        for r in range(n_rep):
            part = nt(cot[:, r * cols_out : (r + 1) * cols_out], w_out[(s,) + bits_of(r, nb)])
            x = part if x is None else x + part
        dattn[:, span(s, own_out)] = x.astype(B16)

    tiles(n_shard, head_grad)

    def reduce_time(who, t):
        for step in reversed(range(nb)):
            if 0 <= t - step < n_shard:
                who.event(t - step, step)

    def weight_grad(c):
        cols = dqkv[:, c * chunk : (c + 1) * chunk]

        def one(k):
            s = sum_in[c].dest(k)
            x = tn(xn[:, span(s, own_in)], cols).astype(B16)
            part_in[(s,) + (both,) * nb + part_cols[c]] = x.reshape((2,) * nb + (rows_in, chunk))

        tiles(n_shard, one)
        for k in range(n_shard):
            sum_in[c].start(k)

    n_reduce = n_shard + nb - 1

    in_loop = (2 * n_reduce) // 3

    def backward(p):
        for t in range(in_loop):
            @pl.when(p == 1 + (t * (pairs - 2)) // max(in_loop - 1, 1))
            def _():
                reduce_time(sum_out, t)

        @pl.when(p == pairs // 2)
        def _():
            weight_grad(0)

        g = lax.div(p, per_group)
        lanes = span(p, pair)

        @pl.when(lax.rem(p, per_group) == 0)
        def _():
            dk_acc[...] = jnp.zeros_like(dk_acc)
            dv_acc[...] = jnp.zeros_like(dv_acc)

        scores = [(nt(kx[g, rs, :], q[qs, lanes]), nt(vx[g, rs, :], dattn[qs, lanes])) for b, qs, rs, keys in blocks()]
        grads = []
        for (b, qs, rs, keys), (score, dp) in zip(blocks(), scores):
            prob = [
                jnp.exp(tile_of(score, 2 * j + side) + bias[key * TILE : (key + 1) * TILE, qs]) * inv_l[p, side, :, qs]
                for j, key in enumerate(keys)
                for side in range(2)
            ]
            inner = [
                sum(jnp.sum(x * tile_of(dp, 2 * j + side), 0, keepdims=True) for j, x in enumerate(prob[side::2]))
                for side in range(2)
            ]
            ds = [(x * (tile_of(dp, j) - inner[j % 2])).astype(B16) for j, x in enumerate(prob)]
            grads.append((jnp.concatenate([x.astype(B16) for x in prob], 0), jnp.concatenate(ds, 0)))
        for (b, qs, rs, keys), (prob, ds) in zip(blocks(), grads):
            dv_acc[rs, :] += mm(prob, dattn[qs, lanes])
            dk_acc[rs, :] += mm(ds, q[qs, lanes])
            x = mm(kxt[g, :, rs], ds).T
            half_pairs = pairs // 2
            to = lax.div(p, half_pairs) * chunk + lax.rem(p, half_pairs) * pair
            dqkv[qs, pl.ds(pl.multiple_of(to, pair), pair)] = (x * cosine[qs, :] - swap_halves(x) * sine[qs, :]).astype(B16)

        @pl.when(lax.rem(p, per_group) == per_group - 1)
        def _():
            def joined(acc):
                both = [acc[j * TILE : (j + 1) * TILE, :] for j in range(2 * n_tok)]
                return jnp.concatenate([both[2 * b] + pltpu.roll(both[2 * b + 1], HEAD_SIZE, 1) for b in range(n_tok)], 0)

            dk, dv = joined(dk_acc), joined(dv_acc)
            dk = dk * cosine[...] - swap_halves(dk) * sine[...]
            for x, first in ((dk, q_part), (dv, q_part + kv_part)):
                half_groups = kv_heads // 2
                to = lax.div(g, half_groups) * chunk + first + lax.div(lax.rem(g, half_groups), 2) * pair
                at = pl.ds(pl.multiple_of(to, pair), pair)
                odd = lax.rem(g, 2)

                @pl.when(odd == 0)
                def _():
                    dqkv[:, at] = x.astype(B16)

                @pl.when(odd == 1)
                def _():
                    high = pltpu.roll(x, HEAD_SIZE, 1)
                    dqkv[:, at] = jnp.where(low, dqkv[:, at].astype(F32), high).astype(B16)

    tiles(pairs, backward)

    weight_grad(1)
    for load in loads:
        load.wait()

    row_acc[...] = jnp.zeros_like(row_acc)

    def input_grad(s):
        c = slice(s * own_in, (s + 1) * own_in)
        d = nt(dqkv[...], flat(w_in[s]))
        normed = tok[:, c].astype(F32) * inv_ref[:, :1]
        gain_acc[s] = jnp.sum(d * normed, 0, keepdims=True)
        d = d * gain_full[s]
        dxn[:, c] = d
        row_acc[...] += jnp.broadcast_to(jnp.sum(d * normed, 1, keepdims=True), row_acc.shape)

    def token_grad(i):
        r = span(i, rows)
        inv = inv_ref[r, :1]
        normed = tok[r, :].astype(F32) * inv
        mean = row_acc[r, :1] * (1.0 / width)
        grad_tok[r, :] = (cot[r, :].astype(F32) + inv * (dxn[r, :] - normed * mean)).astype(B16)

    def output(r):
        c = span(r, cols_out)
        x = mm(attn[...], flat(w_out[(slice(None),) + bits_of(r, nb)]))
        out[:, c] = (tok[:, c].astype(F32) + x).astype(B16)

    def gather_sums_time(who, t):
        who.gather_event(t)

    todo = []

    def then(method, *args):
        todo.append(functools.partial(method, *args))

    def gain_end():
        gain_out[...] = sum_gain.end()

    out_end = n_reduce - in_loop
    for u in range(3 * (n_shard + nb) + n_reduce):
        if u < out_end:
            then(reduce_time, sum_out, in_loop + u)
        if u < n_reduce:
            then(reduce_time, sum_in[0], u)
        if u == n_reduce:
            then(sum_in[0].finish, decay)
        if 0 <= u - 2 < n_reduce:
            then(reduce_time, sum_in[1], u - 2)
        if u == out_end + 1:
            then(sum_out.finish, decay)
        if u == n_reduce + 2:
            then(sum_in[1].finish, decay)
        for who, lag in ((sum_in[0], n_reduce + 1), (sum_in[1], n_reduce + 3), (sum_out, out_end + 2)):
            if 0 <= u - lag < who.whole.times():
                then(gather_sums_time, who, u - lag)
        if 0 <= u - 3 < nb:
            then(sum_gain.event, u - 3)
        if u == n_reduce + nb:
            then(gain_end)

    def advance():
        todo.pop(0)()

    for s in range(n_shard):
        advance()
        input_grad(s)
    sum_gain.send(0).start()
    advance()
    tiles(seq // rows, token_grad)
    gone = [pltpu.make_async_copy(grad_tok, grad_hbm, load_sem.at[16]), pltpu.make_async_copy(out, out_hbm, load_sem.at[17])]
    gone[0].start()
    advance()
    tiles(n_rep // 2, output)
    advance()
    tiles(n_rep // 2, lambda r: output(r + n_rep // 2))
    gone[1].start()
    while todo:
        advance()

    for who in (get_in, get_out, sum_out, *sum_in):
        who.drain()
    for copy in gone:
        copy.wait()
    for way in WAYS:
        for k in range(n_shard - 1):
            @pl.when(links.goes(way, k))
            def _():
                gain_line_copy(way, k).wait_send()
    assert len(links.names) <= send.shape[0]


def layer(tok, cot, seg, gain, weights, moments, decay, n_rep, n_shard, collective_id):
    seq, width = tok.shape
    w_query, w_key, _, w_outproj = weights
    q_width, kv_width = w_query.shape[1], w_key.shape[1]
    all_in = q_width + 2 * kv_width
    kv_heads, pair = kv_width // HEAD_SIZE, 2 * HEAD_SIZE
    nb = n_rep.bit_length() - 1
    bits = (2,) * nb
    own_in, own_out = width // n_shard, q_width // n_shard
    piece_in, piece_out = (own_in // n_rep, all_in), (own_out, width // n_rep)
    half = HEAD_SIZE // 2
    frequency = np.tile((rope_base ** (-2.0 * np.arange(half) / HEAD_SIZE)).astype(np.float32), pair // half)[None]
    vmem, any_ = pl.BlockSpec(memory_space=pltpu.VMEM), pl.BlockSpec(memory_space=pl.ANY)
    V, D = pltpu.VMEM, pltpu.SemaphoreType.DMA
    n_sems = (
        5 * 2 * (n_shard - 1) * (2 + 2 * nb) + 3 * (n_shard * (1 + 2 * (nb - 1)) + n_shard - 1 + 2 * nb) + nb + 3 * n_shard
    )
    bufs = [V((n_shard,) + (2,) * (nb - 1 - j) + piece, B16) for piece in (piece_in, piece_out) for j in range(nb)]
    shape = jax.ShapeDtypeStruct
    return pl.pallas_call(
        functools.partial(layer_kernel, n_rep, n_shard, decay),
        out_shape=[
            shape((seq, width), B16),
            shape((seq, width), B16),
            shape(bits + piece_in, B16),
            shape(bits + piece_out, B16),
            shape((n_shard,) + bits + piece_in, B16),
            shape((n_shard,) + bits + piece_out, B16),
            shape((1, own_in), F32),
        ],
        in_specs=[any_] * 2 + [vmem] * 3 + [any_] * 8,
        out_specs=[any_] * 6 + [vmem],
        scratch_shapes=[
            V((seq, width), B16),
            V((seq, width), B16),
            V((seq, width), B16),
            V((seq, width), B16),
            V((n_shard,) + bits + piece_in, B16),
            V((n_shard,) + bits + piece_out, B16),
            V((n_shard, 1, own_in), F32),
            V((seq, width), B16),
            V((seq, 128), F32),
            V((seq, q_width), B16),
            V((seq, q_width), B16),
            V((q_width, seq), B16),
            V((seq, q_width), B16),
            V((seq, all_in), B16),
            V((seq, width), F32),
            V((seq, 128), F32),
            V((kv_heads, 2 * seq, pair), B16),
            V((kv_heads, 2 * seq, pair), B16),
            V((kv_heads, pair, 2 * seq), B16),
            V((kv_heads, pair, 2 * seq), B16),
            V((2 * seq, pair), F32),
            V((2 * seq, pair), F32),
            V((seq, seq), F32),
            V((seq, pair), F32),
            V((seq, pair), F32),
            V((q_width // pair, 2, 1, seq), F32),
            V((n_shard,) + bits + piece_in, B16),
            V((n_shard,) + bits + piece_out, B16),
            V((n_shard, 1, own_in), F32),
            V((nb, n_shard, 1, own_in), F32),
            V((n_shard, 1, own_in), F32),
            V(piece_in, F32),
            V(piece_out, F32),
            V((n_shard,) + piece_in, B16),
            V(piece_in, B16),
            V(piece_in, B16),
            V((n_shard,) + piece_out, B16),
            V(piece_out, B16),
            V(piece_out, B16),
            D((18,)),
            D((3,)),
            D((n_sems,)),
            D((n_sems,)),
        ]
        + bufs,
        compiler_params=pltpu.CompilerParams(
            collective_id=collective_id, has_side_effects=True, vmem_limit_bytes=67_043_328
        ),
        name="layer",
    )(tok, cot, seg[None], frequency, gain[None], *weights, *moments)


gain_rate = 0.2


def on_device(
    tokens,
    segments,
    cotangent,
    gain,
    w_query,
    w_key,
    w_value,
    w_outproj,
    moment_gain,
    moment_query,
    moment_key,
    moment_value,
    moment_outproj,
):
    n_rep, n_shard = lax.axis_size("rep"), lax.axis_size("shard")
    total_tokens = tokens.shape[0] * tokens.shape[1] * n_rep * n_shard
    weights = (w_query, w_key, w_value, w_outproj)
    moments = (moment_query, moment_key, moment_value, moment_outproj)
    result, grad_tokens, sum_in, sum_out, m_in, m_out, grad_gain = layer(
        tokens[0], cotangent[0], segments[0], gain, weights, moments, decay, n_rep, n_shard, 0
    )
    grad_gain = grad_gain[0]
    moment_gain_next = decay * moment_gain + grad_gain
    gain_next = gain - gain_rate / math.sqrt(total_tokens) * moment_gain_next
    own_out, cols_out = sum_out.shape[-2:]
    m_out = m_out.reshape(n_shard, n_rep, own_out, cols_out)
    all_in = sum_in.shape[-1]
    grads, moments_next, (result, grad_tokens), (mix, mix_kv, scales) = muon(
        m_in.reshape(-1, all_in),
        m_out,
        sum_in.reshape(-1, all_in),
        sum_out.reshape(n_rep, own_out, cols_out),
        moments,
        (result, grad_tokens),
    )
    updated = update(mix, mix_kv, scales, m_out, moments_next, weights, n_rep, 1)
    return (
        result[None],
        grad_tokens[None],
        grad_gain,
        *grads,
        gain_next,
        *updated,
        moment_gain_next,
        *moments_next,
    )


def solution(mesh):
    in_specs = (
        P(("rep", "shard"), None, None),
        P(("rep", "shard"), None),
        P(("rep", "shard"), None, None),
        P("shard"),
        P("shard", None),
        P("shard", None),
        P("shard", None),
        P("shard", None),
        P("shard"),
        P("shard", None),
        P("shard", None),
        P("shard", None),
        P("shard", None),
    )
    out_specs = (
        P(("rep", "shard"), None, None),
        P(("rep", "shard"), None, None),
        P("shard"),
        P("shard", None),
        P("shard", None),
        P("shard", None),
        P("shard", None),
        P("shard"),
        P("shard", "rep"),
        P("shard", "rep"),
        P("shard", "rep"),
        P("shard", "rep"),
        P("shard"),
        P("shard", None),
        P("shard", None),
        P("shard", None),
        P("shard", None),
    )
    return jax.shard_map(on_device, mesh=mesh, in_specs=in_specs, out_specs=out_specs, check_vma=False)
```

```python
import functools
import math

import jax
import jax.numpy as jnp
import numpy as np
from jax import lax
from jax.experimental import pallas as pl
from jax.experimental.pallas import tpu as pltpu
from jax.sharding import PartitionSpec as P

coef_a = 3.4445
coef_b = -4.775
coef_c = 2.0315
SWEEPS = 5
decay = 0.95
muon_rate = 0.02


def nt(left, right):
    return lax.dot_general(left, right, (((1,), (1,)), ((), ())), preferred_element_type=jnp.float32)


def tn(left, right):
    return lax.dot_general(left, right, (((0,), (0,)), ((), ())), preferred_element_type=jnp.float32)


def mm(left, right):
    return jnp.dot(left, right, preferred_element_type=jnp.float32)


def tiles(count, body):
    def one(i, carry):
        body(i)
        return carry

    lax.fori_loop(0, count, one, 0)


def span(i, size):
    return pl.ds(pl.multiple_of(i * size, size), size)


def total(x):
    return jnp.sum(jnp.sum(x, axis=1, keepdims=True), axis=0, keepdims=True)


class Iterate:
    def __init__(self, e, ebf, k, kbf, h, hbf, fbf):
        self.e, self.ebf, self.k, self.kbf, self.h, self.hbf, self.fbf = e, ebf, k, kbf, h, hbf, fbf
        self.n = n = e.shape[0]
        self.diag = min(256, n)
        self.squares = [slice(d, d + self.diag) for d in range(0, n, self.diag)]
        half = n // 2
        if n <= 256:
            self.blocks = [(slice(0, n), slice(0, n))]
        else:
            self.blocks = [(slice(0, n), slice(0, half)), (slice(half, n), slice(half, n))]

    def put(self, ref, at, value):
        r, c = at
        ref[r, c] = value.astype(jnp.bfloat16)
        if r != c:
            ref[c, c.stop : r.stop] = ref[c.stop : r.stop, c].T

    def eye(self):
        shape = (self.diag, self.diag)
        return lax.broadcasted_iota(jnp.int32, shape, 0) == lax.broadcasted_iota(jnp.int32, shape, 1)

    def trace(self, ref):
        mask = self.eye()
        return sum(total(jnp.where(mask, ref[d, d], 0.0)) for d in self.squares)

    def centre(self, s):
        shift = self.trace(self.e) * (1.0 / self.n)
        mask = self.eye()
        for d in self.squares:
            moved = self.e[d, d] - jnp.where(mask, shift, 0.0)
            self.e[d, d] = moved
            self.ebf[d, d] = moved.astype(jnp.bfloat16)
        return s + shift

    def start(self):
        norm = jnp.sqrt(self.trace(self.e)) + 1e-06
        scale = 1.0 / (norm * norm)
        for at in self.blocks:
            x = self.e[at] * scale
            self.e[at] = x
            self.put(self.ebf, at, x)
        return self.centre(jnp.zeros((1, 1), jnp.float32)), 1.0 / norm

    def polynomial(self, s, at):
        p1 = coef_b + 2.0 * coef_c * s
        self.put(self.fbf, at, p1 * self.e[at] + coef_c * mm(self.ebf[at[0], :], self.ebf[:, at[1]]))

    def first(self):
        for at in self.blocks:
            f = self.fbf[at].astype(jnp.float32)
            self.h[at] = f
            self.put(self.hbf.at[0], at, f)

    def grow(self, p0, q, at, now, later):
        new = p0 * self.h[at] + q * self.fbf[at].astype(jnp.float32) + mm(self.fbf[at[0], :], self.hbf[now, :, at[1]])
        self.h[at] = new
        self.put(self.hbf.at[later], at, new)

    def inner(self, p0, s, at):
        new = p0 * self.e[at] + s * self.fbf[at].astype(jnp.float32) + mm(self.fbf[at[0], :], self.ebf[:, at[1]])
        self.k[at] = new
        self.put(self.kbf, at, new)

    def outer(self, p0, beta, at):
        new = p0 * self.k[at] + beta * self.fbf[at].astype(jnp.float32) + mm(self.fbf[at[0], :], self.kbf[:, at[1]])
        self.e[at] = new
        self.put(self.ebf, at, new)


def muon_kernel(*refs):
    refs = list(refs)

    def take(count):
        return [refs.pop(0) for _ in range(count)]

    m_in, m_out, *passed = take(4)
    g_in, g_out, *moments = take(6)
    grads_out, moments_out, passed_out = take(4), take(4), take(2)
    h_out, hs_out, scal = take(3)
    grads, news, held = take(4), take(4), take(2)
    sums_in, sums_out, tall, lump, x, small_m = take(6)
    in_sem, own_sem, out_sem, pass_sem = take(4)
    big, small = Iterate(*take(7)), Iterate(*take(7))
    f32, b16 = jnp.float32, jnp.bfloat16
    core = lax.rem(lax.axis_index("rep"), 2)
    shard = lax.axis_index("shard")
    n, ns = big.n, small.n
    own_in = g_in.shape[0]
    n_rep, own_out, cols_out = g_out.shape
    chunk, q_part, kv_part = (n + 2 * ns) // 2, n // 2, ns // 2
    firsts = [(0, q_part), (q_part, kv_part), (q_part + kv_part, kv_part)]

    wide = [
        pltpu.make_async_copy(m_in.at[:, pl.ds(c * chunk, q_part)], tall.at[:, pl.ds(c * q_part, q_part)], in_sem.at[c])
        for c in range(2)
    ]
    flat = pltpu.make_async_copy(m_out, lump, in_sem.at[0])
    kv = [
        pltpu.make_async_copy(
            m_in.at[:, pl.ds(pl.multiple_of(c * chunk + q_part + core * kv_part, 128), kv_part)],
            small_m.at[:, pl.ds(c * kv_part, kv_part)],
            in_sem.at[2 + c],
        )
        for c in range(2)
    ]
    own = [pltpu.make_async_copy(a, b, own_sem.at[i]) for i, (a, b) in enumerate(zip(moments, news))]
    own_sums = [pltpu.make_async_copy(g_in, sums_in, own_sem.at[4]), pltpu.make_async_copy(g_out, sums_out, own_sem.at[5])]
    passing = [pltpu.make_async_copy(a, b, pass_sem.at[i]) for i, (a, b) in enumerate(zip(passed, held))]
    leaving = [pltpu.make_async_copy(a, b, pass_sem.at[i]) for i, (a, b) in enumerate(zip(held, passed_out))]

    @pl.when(core == 0)
    def _():
        for copy in wide:
            copy.start()

    @pl.when(core != 0)
    def _():
        flat.start()

    for copy in kv + own_sums + own:
        copy.start()

    mine = span(shard, own_in)
    rows = 64

    @pl.when(core == 0)
    def _():
        for copy in wide:
            copy.wait()
        tiles(tall.shape[0] // 256, lambda i: x.__setitem__((slice(None), span(i, 256)), tall[span(i, 256), :].T))

    @pl.when(core != 0)
    def _():
        flat.wait()
        for s in range(lump.shape[0]):
            tiles(n_rep, lambda r, s=s: x.__setitem__((slice(s * own_out, (s + 1) * own_out), span(r, cols_out)), lump[s, r]))

    for copy in kv + own_sums + own:
        copy.wait()
    for copy in passing:
        copy.start()
    for i in range(4):
        if i < 3:
            def update(j, i=i, first=firsts[i][0], width=firsts[i][1]):
                r = span(j, rows)
                for c in range(2):
                    at, to = c * chunk + first, slice(c * width, (c + 1) * width)
                    grad = sums_in[r, at : at + width].astype(f32)
                    grads[i][r, to] = grad
                    news[i][r, to] = decay * news[i][r, to] + grad

            tiles(own_in // rows, update)
        else:
            def update(r, i=i):
                at = span(r, cols_out)
                grad = sums_out[r].astype(f32)
                grads[i][:, at] = grad
                news[i][:, at] = decay * news[i][:, at] + grad

            tiles(n_rep, update)

    @pl.when(core == 0)
    def _():
        x[:, mine] = news[0][...].astype(b16).T
        small_m[mine, :] = news[1][...].astype(b16)

    @pl.when(core != 0)
    def _():
        x[span(shard, own_out), :] = news[3][...].astype(b16)
        small_m[mine, :] = news[2][...].astype(b16)

    copies = [
        pltpu.make_async_copy(a, b, out_sem.at[i])
        for i, (a, b) in enumerate(zip(grads + news, grads_out + moments_out))
    ]
    for copy in copies:
        copy.start()
    for a, b in zip(passing, leaving):
        a.wait()
        b.start()
    for r, c in big.blocks:
        big.e[r, c] = nt(x[r, :], x[c, :])
    small.e[...] = tn(small_m[...], small_m[...])
    s, inv = big.start()
    ss, sinv = small.start()

    def sweep(it, carry):
        s, q, ss, sq = carry
        now, later = lax.rem(it + 1, 2), lax.rem(it, 2)
        p0 = coef_a + s * (coef_b + coef_c * s)
        sp0 = coef_a + ss * (coef_b + coef_c * ss)

        def each(method, *args):
            for i, c in enumerate(big.blocks):
                getattr(big, method)(*[a[0] for a in args], c, *extra)
                if i == 0:
                    for d in small.blocks:
                        getattr(small, method)(*[a[1] for a in args], d, *extra)

        extra = ()
        each("polynomial", (s, ss))

        @pl.when(it == 0)
        def _():
            big.first()
            small.first()

        extra = (now, later)

        @pl.when(it > 0)
        def _():
            each("grow", (p0, sp0), (q, sq))

        extra = ()
        q, sq = p0 * q, sp0 * sq

        def advance():
            each("inner", (p0, sp0), (s, ss))
            beta, sbeta = p0 * s, sp0 * ss
            each("outer", (p0, sp0), (beta, sbeta))
            return big.centre(p0 * beta), small.centre(sp0 * sbeta)

        s, ss = lax.cond(it < SWEEPS - 1, advance, lambda: (s, ss))
        return s, q, ss, sq

    one = jnp.ones((1, 1), f32)
    s, q, ss, sq = lax.fori_loop(0, SWEEPS, sweep, (s, one, ss, one))
    last = (SWEEPS - 1) % 2
    h_out[...] = big.hbf[last]
    hs_out[...] = small.hbf[last]
    row = lax.broadcasted_iota(jnp.int32, (8, 128), 0)
    scal[...] = jnp.where(row == 0, q * inv, jnp.where(row == 1, inv, jnp.where(row == 2, sq * sinv, sinv)))
    for copy in copies + leaving:
        copy.wait()


def muon(m_in, m_out, g_in, g_out, moments, passed):
    f32, b16 = jnp.float32, jnp.bfloat16
    tall, n, kv = m_in.shape[0], m_out.shape[0] * m_out.shape[2], moments[1].shape[1]
    V = pltpu.VMEM
    sets = []
    for d in (n, kv):
        sets += [V((d, d), f32), V((d, d), b16), V((d, d), f32), V((d, d), b16), V((d, d), f32), V((2, d, d), b16), V((d, d), b16)]
    vmem, any_ = pl.BlockSpec(memory_space=pltpu.VMEM), pl.BlockSpec(memory_space=pl.ANY)
    own = [jax.ShapeDtypeStruct(m.shape, f32) for m in moments]
    out = pl.pallas_call(
        muon_kernel,
        out_shape=own
        + own
        + [jax.ShapeDtypeStruct(p.shape, p.dtype) for p in passed]
        + [
            jax.ShapeDtypeStruct((n, n), b16),
            jax.ShapeDtypeStruct((kv, kv), b16),
            jax.ShapeDtypeStruct((8, 128), f32),
        ],
        in_specs=[any_] * 10,
        out_specs=[any_] * 10 + [vmem] * 3,
        scratch_shapes=[V(m.shape, f32) for m in moments] * 2
        + [V(p.shape, p.dtype) for p in passed]
        + [
            V(g_in.shape, b16),
            V(g_out.shape, b16),
            V((tall, n), b16),
            V(m_out.shape, b16),
            V((n, m_out.shape[1] * m_out.shape[3]), b16),
            V((tall, kv), b16),
            pltpu.SemaphoreType.DMA((4,)),
            pltpu.SemaphoreType.DMA((6,)),
            pltpu.SemaphoreType.DMA((8,)),
            pltpu.SemaphoreType.DMA((2,)),
        ]
        + sets,
        compiler_params=pltpu.CompilerParams(vmem_limit_bytes=63 << 20),
        name="muon",
    )(m_in, m_out, *passed, g_in, g_out, *moments)
    return out[:4], out[4:8], out[8:10], out[10:]


def swap_kernel(n_rep, h, hs, scal, h_pair, hs_come, scal_come, send, recv):
    rep, shard = lax.axis_index("rep"), lax.axis_index("shard")
    core = lax.rem(rep, 2)
    other = rep + 1 - 2 * core
    sem = pltpu.get_barrier_semaphore()
    pl.semaphore_signal(sem, 1, device_id=(other, shard), device_id_type=pl.DeviceIdType.MESH)
    pl.semaphore_wait(sem, 1)

    def remote(src, dst, i):
        return pltpu.make_async_remote_copy(
            src, dst, send.at[i], recv.at[i], device_id=(other, shard), device_id_type=pl.DeviceIdType.MESH
        )

    count = h_pair.shape[0]
    at = jnp.where(core == 0, lax.div(rep, 2), shard)
    copies = [remote(h.at[span(at, count), :], h_pair, 0), remote(hs, hs_come, 1), remote(scal, scal_come, 2)]
    for c in copies:
        c.start()
    for c in copies:
        c.wait()


def swap(h, hs, scal, count, n_rep, collective_id):
    any_ = pl.BlockSpec(memory_space=pl.ANY)
    return pl.pallas_call(
        functools.partial(swap_kernel, n_rep),
        out_shape=[
            jax.ShapeDtypeStruct((count, h.shape[1]), h.dtype),
            jax.ShapeDtypeStruct(hs.shape, hs.dtype),
            jax.ShapeDtypeStruct(scal.shape, scal.dtype),
        ],
        in_specs=[any_] * 3,
        out_specs=[any_] * 3,
        scratch_shapes=[pltpu.SemaphoreType.DMA((3,)), pltpu.SemaphoreType.DMA((3,))],
        compiler_params=pltpu.CompilerParams(collective_id=collective_id, has_side_effects=True),
        name="swap",
    )(h, hs, scal)


def window(index, width):
    size = max(width, 128)
    start = lax.div(index * width, size) * size
    return pl.ds(pl.multiple_of(start, 128), size), size, index * width - start


def cut(x, size, offset, width):
    return x if size == width else pltpu.roll(x, lax.rem(size - offset, size), 1)[:, :width]


def update_kernel(h, h_pair, hs, hs_come, scal, scal_come, m_out, mq_hbm, mk_hbm, mv_hbm, mo, wq, wk, wv, wo, *refs):
    nexts, (hq, ho, flat, mo_win), weight_wins, (mq, mk, mv), (h_sem, sem) = (
        refs[:4], refs[4:8], refs[8:12], refs[12:15], refs[15:]
    )
    f32, b16 = jnp.float32, jnp.bfloat16
    rep, shard = lax.axis_index("rep"), lax.axis_index("shard")
    even = lax.rem(rep, 2) == 0
    widths = [nexts[0].shape[1], nexts[1].shape[0], nexts[2].shape[0], nexts[3].shape[1]]
    wins = [window(rep, w) for w in widths]
    own_out = ho.shape[0]
    copies = [
        pltpu.make_async_copy(m_out.at[:, rep], flat, sem.at[4]),
        pltpu.make_async_copy(mo.at[:, wins[3][0]], mo_win, sem.at[5]),
        pltpu.make_async_copy(mq_hbm, mq, sem.at[6]),
        pltpu.make_async_copy(mk_hbm, mk, sem.at[7]),
        pltpu.make_async_copy(mv_hbm, mv, sem.at[8]),
    ] + [pltpu.make_async_copy(w.at[:, wins[i][0]], weight_wins[i], sem.at[i]) for i, w in enumerate((wq, wk, wv, wo))]
    for copy in copies:
        copy.start()
    rows_q = h.at[span(rep, widths[0]), :], h_pair.at[pl.ds(h_pair.shape[0] - widths[0], widths[0]), :]
    rows_o = h_pair, h.at[span(shard, own_out), :]
    mixes = [[pltpu.make_async_copy(a, b, h_sem.at[i]) for i, (a, b) in enumerate(((q, hq), (o, ho)))] for q, o in zip(rows_q, rows_o)]
    for side, here in ((0, even), (1, jnp.logical_not(even))):
        @pl.when(here)
        def _():
            for copy in mixes[side]:
                copy.start()
            for copy in mixes[side]:
                copy.wait()
    for copy in copies:
        copy.wait()
    first = jnp.where(even, scal[...], scal_come[...])
    second = jnp.where(even, scal_come[...], scal[...])
    flat[shard] = mo_win[...].astype(b16)

    def rows_of(i):
        at = span(rep, widths[i])
        mine, theirs = hs[at, :].astype(f32), hs_come[at, :].astype(f32)
        return jnp.where(even == (i == 1), mine, theirs).astype(b16)

    parts = (
        (mq, lambda: nt(mq[...].astype(b16), hq[...]), first[0:1, 0:1], first[1:2, 0:1]),
        (mk, lambda: nt(rows_of(1), mk[...].astype(b16)), first[2:3, 0:1], first[3:4, 0:1]),
        (mv, lambda: nt(rows_of(2), mv[...].astype(b16)), second[2:3, 0:1], second[3:4, 0:1]),
        (None, lambda: mm(ho[...], flat[...].reshape(-1, flat.shape[2])), second[0:1, 0:1], second[1:2, 0:1]),
    )
    n_shard = lax.axis_size("shard")
    for i, (moment, product, straight, mixed) in enumerate(parts):
        at, size, offset = wins[i]

        def mine(x):
            x = cut(x, size, offset, widths[i])
            return x.T if i in (1, 2) else x

        here = mine(mo_win[...] if moment is None else moment[:, at])
        ortho = straight * here + mixed * product()
        whole = (weight_wins[i].shape[0] * n_shard, (wq, wk, wv, wo)[i].shape[1])
        nexts[i][...] = mine(weight_wins[i][...]) - muon_rate * math.sqrt(max(whole)) * ortho


def update(h, hs, scal, m_out, moments, weights, n_rep, collective_id):
    f32, b16 = jnp.float32, jnp.bfloat16
    widths = [w.shape[1] // n_rep for w in weights]
    own_out = weights[3].shape[0]
    assert 2 * widths[0] == own_out and m_out.shape[3] == widths[3]
    h_pair, hs_come, scal_come = swap(h, hs, scal, own_out, n_rep, collective_id)
    vmem, any_ = pl.BlockSpec(memory_space=pltpu.VMEM), pl.BlockSpec(memory_space=pl.ANY)
    V = pltpu.VMEM
    sizes = [max(w, 128) for w in widths]
    shapes = [(w.shape[0], width) for w, width in zip(weights, widths)]
    out = pl.pallas_call(
        update_kernel,
        out_shape=[jax.ShapeDtypeStruct(s[::-1] if i in (1, 2) else s, f32) for i, s in enumerate(shapes)],
        in_specs=[any_] * 2 + [vmem] * 4 + [any_] * 9,
        out_specs=[vmem] * 4,
        scratch_shapes=[
            V((widths[0], h.shape[1]), b16),
            V((own_out, h.shape[1]), b16),
            V((m_out.shape[0],) + m_out.shape[2:], b16),
            V((own_out, sizes[3]), f32),
        ]
        + [V((w.shape[0], size), f32) for w, size in zip(weights, sizes)]
        + [V(m.shape, f32) for m in moments[:3]]
        + [pltpu.SemaphoreType.DMA((2,)), pltpu.SemaphoreType.DMA((9,))],
        name="update",
    )(h, h_pair, hs, hs_come, scal, scal_come, m_out, *moments, *weights)
    return out[0], out[1].T, out[2].T, out[3]


HEAD_SIZE = 64
TILE = 256
norm_eps = 1e-05
rope_base = 500000.0
F32, B16 = jnp.float32, jnp.bfloat16
MESH = pl.DeviceIdType.MESH
WAYS = (1, -1)


class Links:
    def __init__(self, n_rep, n_shard, send, recv):
        self.n_bits, self.n_shard = n_rep.bit_length() - 1, n_shard
        self.rep, self.shard = lax.axis_index("rep"), lax.axis_index("shard")
        self.bits = [lax.rem(lax.div(self.rep, 1 << b), 2) for b in range(self.n_bits)]
        far = list(range(1, self.n_bits))
        self.orders = (far, far[::-1])
        self.send, self.recv, self.names = send, recv, {}

    def flip(self, bit):
        return self.rep + (1 << bit) * (1 - 2 * self.bits[bit])

    def barrier(self):
        sem = pltpu.get_barrier_semaphore()
        for b in range(self.n_bits):
            pl.semaphore_signal(sem, 1, device_id=(self.flip(b), self.shard), device_id_type=MESH)
        for k in range(1, self.n_shard):
            there = lax.rem(self.shard + k, self.n_shard)
            pl.semaphore_signal(sem, 1, device_id=(self.rep, there), device_id_type=MESH)
        pl.semaphore_wait(sem, self.n_bits + self.n_shard - 1)

    def where(self, free=()):
        return tuple(slice(None) if b in free else self.bits[b] for b in reversed(range(self.n_bits)))

    def remote(self, src, dst, name, rep, shard):
        i = self.names.setdefault(name, len(self.names))
        return pltpu.make_async_remote_copy(
            src, dst, self.send.at[i], self.recv.at[i], device_id=(rep, shard), device_id_type=MESH
        )

    def goes(self, way, k):
        q, there = self.shard - way * k, self.shard + way
        return (q >= 0) & (q < self.n_shard) & (there >= 0) & (there < self.n_shard)

    def comes(self, way, k):
        q = self.shard - way * (k + 1)
        return (q >= 0) & (q < self.n_shard)


class Gather:
    def __init__(self, links, name, full, half, first=None):
        self.links, self.name, self.full, self.half, self.first = links, name, full, half, first

    def line(self, way, k, h):
        at = self.full.at[(self.links.shard - way * k,) + self.links.where() + self.half[h]]
        src = self.first.at[self.half[h]] if k == 0 and self.first is not None else at
        return self.links.remote(src, at, (self.name, "l", way, k, h), self.links.rep, self.links.shard + way)

    def came(self, way, k, h):
        at = self.full.at[(self.links.shard - way * (k + 1),) + self.links.where() + self.half[h]]
        return self.links.remote(at, at, (self.name, "l", way, k, h), self.links.rep, self.links.shard)

    def plane(self, way, k, h, step):
        links = self.links
        order = links.orders[h] + [0]
        view = self.full.at[(links.shard - way * (k + 1),) + links.where(order[:step]) + self.half[h]]
        return links.remote(view, view, (self.name, "p", way, k, h, step), links.flip(order[step]), links.shard)

    def start(self):
        for way in WAYS:
            @pl.when(self.links.goes(way, 0))
            def _():
                for h in range(2):
                    self.line(way, 0, h).start()

    def arrive(self, k):
        links = self.links
        for way in WAYS:
            @pl.when(links.comes(way, k))
            def _():
                for h in range(2):
                    self.came(way, k, h).wait_recv()
                    if k + 1 < links.n_shard - 1:
                        @pl.when(links.goes(way, k + 1))
                        def _():
                            self.line(way, k + 1, h).start()

    def times(self):
        return self.links.n_shard + self.links.n_bits

    def time(self, t):
        if t < self.links.n_shard - 1:
            self.arrive(t)
        for k in range(self.links.n_shard - 1):
            if 0 <= t - 1 - k <= self.links.n_bits:
                self.event(k, t - 1 - k)

    def event(self, k, step, then=None):
        links = self.links
        for way in WAYS:
            @pl.when(links.comes(way, k))
            def _():
                for h in range(2):
                    if step > 0:
                        self.plane(way, k, h, step - 1).wait_recv()
                    if step < links.n_bits:
                        self.plane(way, k, h, step).start()
                if step == links.n_bits and then is not None:
                    then(links.shard - way * (k + 1))

    def drain(self):
        links = self.links
        for way in WAYS:
            for k in range(links.n_shard - 1):
                @pl.when(links.goes(way, k))
                def _():
                    for h in range(2):
                        self.line(way, k, h).wait_send()

                @pl.when(links.comes(way, k))
                def _():
                    for h in range(2):
                        for step in range(links.n_bits):
                            self.plane(way, k, h, step).wait_send()


class Spread:
    def __init__(self, links, name, full, half, first):
        self.links, self.name, self.full, self.half, self.first = links, name, full, half, first

    def line(self, k, h):
        links = self.links
        d = lax.rem(links.shard + 1 + k, links.n_shard)
        into = self.full.at[(links.shard,) + links.where() + self.half[h]]
        return links.remote(self.first.at[self.half[h]], into, (self.name, "l", k, h), links.rep, d)

    def origin(self, k):
        return lax.rem(self.links.shard + self.links.n_shard - 1 - k, self.links.n_shard)

    def came(self, k, h):
        links = self.links
        at = self.full.at[(self.origin(k),) + links.where() + self.half[h]]
        return links.remote(at, at, (self.name, "l", k, h), links.rep, links.shard)

    def plane(self, k, h, step):
        links = self.links
        order = links.orders[h] + [0]
        view = self.full.at[(self.origin(k),) + links.where(order[:step]) + self.half[h]]
        return links.remote(view, view, (self.name, "p", k, h, step), links.flip(order[step]), links.shard)

    def start(self):
        for k in range(self.links.n_shard - 1):
            for h in range(2):
                self.line(k, h).start()

    def times(self):
        return self.links.n_bits + 1

    def time(self, step):
        for k in range(self.links.n_shard - 1):
            for h in range(2):
                if step == 0:
                    self.came(k, h).wait_recv()
                else:
                    self.plane(k, h, step - 1).wait_recv()
                if step < self.links.n_bits:
                    self.plane(k, h, step).start()

    def drain(self):
        for k in range(self.links.n_shard - 1):
            for h in range(2):
                self.line(k, h).wait_send()
                for step in range(self.links.n_bits):
                    self.plane(k, h, step).wait_send()


class Reduce:
    def __init__(self, links, name, refs, region, half, keep_sem, way_of_whole):
        self.links, self.name, self.region, self.half = links, name, region, half
        self.part, self.bufs, self.zbuf, self.gpiece, self.mpiece, self.moment, self.sums, wholes = refs
        self.whole = way_of_whole(links, name + "m", wholes, half, self.mpiece)
        self.keep = lambda: pltpu.make_async_copy(
            self.gpiece.at[region], self.sums.at[links.where() + region], keep_sem
        )

    def dest(self, k):
        return lax.rem(self.links.shard + 1 + k, self.links.n_shard)

    def origin(self, k):
        return lax.rem(self.links.shard + self.links.n_shard - 1 - k, self.links.n_shard)

    def order(self, h):
        return [0] + self.links.orders[h]

    def cut(self, h, step):
        return self.region if step == 0 else self.half[h]

    def send(self, k, h, step):
        links, o = self.links, self.order(h)
        bit = o[step]
        src = self.part if step == 0 else self.bufs[step - 1]
        left = sorted(o[step:], reverse=True)
        pick = tuple(1 - links.bits[bit] if b == bit else slice(None) for b in left)
        d, cut = self.dest(k), self.cut(h, step)
        into = self.bufs[step].at[(d,) + (slice(None),) * (links.n_bits - 1 - step) + cut]
        return links.remote(src.at[(d,) + pick + cut], into, (self.name, "r", k, h, step), links.flip(bit), links.shard)

    def add(self, k, h, step):
        links, o = self.links, self.order(h)
        src = self.part if step == 0 else self.bufs[step - 1]
        left = sorted(o[step:], reverse=True)
        others = [b for b in left if b != o[step]]
        d, cut = self.dest(k), self.cut(h, step)

        def one(i):
            at = {b: lax.rem(lax.div(i, 1 << (len(others) - 1 - n)), 2) for n, b in enumerate(others)}
            here = (d,) + tuple(at[b] for b in others) + cut
            there = (d,) + tuple(links.bits[b] if b == o[step] else at[b] for b in left) + cut
            both = src[there].astype(F32) + self.bufs[step][here].astype(F32)
            self.bufs[step][here] = both.astype(B16)

        if others:
            tiles(1 << len(others), one)
        else:
            one(0)

    def send_line(self, k):
        links, d = self.links, self.dest(k)
        src, into = self.bufs[-1].at[(d,) + self.region], self.zbuf.at[(links.shard,) + self.region]
        return links.remote(src, into, (self.name, "z", k), links.rep, d)

    def come_line(self, k):
        links, at = self.links, self.zbuf.at[(self.origin(k),) + self.region]
        return links.remote(at, at, (self.name, "z", k), links.rep, links.shard)

    def start(self, k):
        self.send(k, 0, 0).start()

    def event(self, k, step):
        last = self.links.n_bits - 1
        for h in range(1 if step == 0 else 2):
            self.send(k, h, step).wait_recv()
            self.add(k, h, step)
            if step == 0 and last > 0:
                self.send(k, 0, 1).start()
                self.send(k, 1, 1).start()
            elif step < last:
                self.send(k, h, step + 1).start()
        if step == last and k < self.links.n_shard - 1:
            self.send_line(k).start()

    def gather_sum(self, h, step):
        links = self.links
        order = links.orders[h] + [0]
        into = self.sums.at[links.where(order[:step]) + self.half[h]]
        src = self.gpiece.at[self.half[h]] if step == 0 else into
        return links.remote(src, into, (self.name, "g", h, step), links.flip(order[step]), links.shard)

    def finish(self, decay):
        links = self.links
        for k in range(links.n_shard - 1):
            self.come_line(k).wait_recv()
        acc = self.bufs[-1][(links.shard,) + self.region].astype(F32)
        for k in range(links.n_shard - 1):
            acc = acc + self.zbuf[(self.origin(k),) + self.region].astype(F32)
        g = acc.astype(B16)
        self.gpiece[self.region] = g
        self.mpiece[self.region] = (decay * self.moment[self.region] + g.astype(F32)).astype(B16)
        self.whole.start()
        for h in range(2):
            self.gather_sum(h, 0).start()
        self.keep().start()

    def gather_event(self, step):
        if step == 0:
            self.keep().wait()
        if step < self.links.n_bits:
            for h in range(2):
                self.gather_sum(h, step).wait_recv()
                if step + 1 < self.links.n_bits:
                    self.gather_sum(h, step + 1).start()
        self.whole.time(step)

    def drain(self):
        links = self.links
        for k in range(links.n_shard):
            for step in range(links.n_bits):
                for h in range(1 if step == 0 else 2):
                    self.send(k, h, step).wait_send()
            if k < links.n_shard - 1:
                self.send_line(k).wait_send()
        for h in range(2):
            for step in range(links.n_bits):
                self.gather_sum(h, step).wait_send()
        self.whole.drain()


class GainSum:
    def __init__(self, links, acc, come, line):
        self.links, self.acc, self.come, self.line = links, acc, come, line

    def send(self, b):
        return self.links.remote(self.acc, self.come.at[b], ("gain", b), self.links.flip(b), self.links.shard)

    def send_line(self, k):
        links = self.links
        d = lax.rem(links.shard + 1 + k, links.n_shard)
        return links.remote(self.acc.at[d], self.line.at[links.shard], ("gainz", k), links.rep, d)

    def event(self, b):
        links = self.links
        self.send(b).wait()
        self.acc[...] = self.acc[...] + self.come[b]
        if b + 1 < links.n_bits:
            self.send(b + 1).start()
        else:
            for k in range(links.n_shard - 1):
                self.send_line(k).start()

    def end(self):
        links = self.links
        for k in range(links.n_shard - 1):
            self.send_line(k).wait_send()
            at = self.line.at[lax.rem(links.shard + links.n_shard - 1 - k, links.n_shard)]
            links.remote(at, at, ("gainz", k), links.rep, links.shard).wait_recv()
        acc = self.acc[links.shard]
        for q in range(links.n_shard):
            acc = jnp.where(links.shard == q, acc, acc + self.line[q])
        return acc


def swap_halves(x):
    half, width = HEAD_SIZE // 2, x.shape[1]
    lane = lax.rem(lax.broadcasted_iota(jnp.int32, x.shape, 1), HEAD_SIZE)
    return jnp.where(lane < half, pltpu.roll(x, width - half, 1), pltpu.roll(x, half, 1))


def flat(x):
    return x.reshape(-1, x.shape[-1])


def bits_of(r, n_bits):
    return tuple(lax.rem(lax.div(r, 1 << b), 2) if isinstance(r, jax.Array) else (r >> b) & 1 for b in reversed(range(n_bits)))


def layer_kernel(
    n_rep, n_shard, decay,
    tok_hbm, cot_hbm, seg_row, frequency, gain, w_query, w_key, w_value, w_outproj, m_query, m_key, m_value, m_outproj,
    out_hbm, grad_hbm, sums_in, sums_out, wholes_in, wholes_out, gain_out,
    out, grad_tok,    tok, cot, w_in, w_out, gain_full, xn, inv_ref, q, dattn, attn_t, attn, dqkv, dxn, row_acc, kx, vx, kxt, vxt, dk_acc, dv_acc,
    bias, cosine, sine, inv_l, part_in, part_out, gain_acc, gain_come, gain_line, moment_in, moment_out,
    zbuf_in, gp_in, mp_in, zbuf_out, gp_out, mp_out, load_sem, keep_sem, send, recv, *bufs,
):
    seq, width = tok.shape
    q_width, kv_width = w_query.shape[1], w_key.shape[1]
    kv_heads = kv_width // HEAD_SIZE
    pair = 2 * HEAD_SIZE
    pairs = q_width // pair
    per_group = pairs // kv_heads
    n_tok = seq // TILE
    scale = 1.0 / math.sqrt(HEAD_SIZE)
    rows = 64
    nb = n_rep.bit_length() - 1
    own_in, own_out = width // n_shard, q_width // n_shard
    rows_in, cols_out = own_in // n_rep, width // n_rep
    all_in = w_in.shape[-1]
    chunk, q_part, kv_part = all_in // 2, q_width // 2, kv_width // 2
    places = [
        (i, c * size, c * chunk + first, size)
        for c in range(2)
        for i, (first, size) in enumerate(((0, q_part), (q_part, kv_part), (q_part + kv_part, kv_part)))
    ]

    links = Links(n_rep, n_shard, send, recv)
    me, rep = links.shard, links.rep
    both = slice(None)
    part_cols = [(both, pl.ds(c * chunk, chunk)) for c in range(2)]
    half_cols = [[(both, pl.ds(c * chunk + h * (chunk // 2), chunk // 2)) for h in range(2)] for c in range(2)]
    half_in = [(both, pl.ds(h * chunk, chunk)) for h in range(2)]
    half_out = [(pl.ds(h * (own_out // 2), own_out // 2), both) for h in range(2)]
    get_in = Gather(links, "wi", w_in, half_in)
    get_out = Spread(links, "wo", w_out, half_out, w_out.at[(links.shard,) + links.where()])
    refs_in = (part_in, bufs[:nb], zbuf_in, gp_in, mp_in, moment_in, sums_in, wholes_in)
    refs_out = (part_out, bufs[nb:], zbuf_out, gp_out, mp_out, moment_out, sums_out, wholes_out)
    sum_in = [Reduce(links, f"i{c}", refs_in, part_cols[c], half_cols[c], keep_sem.at[c], Spread) for c in range(2)]
    sum_out = Reduce(links, "o", refs_out, (both, both), half_out, keep_sem.at[2], Gather)
    sum_gain = GainSum(links, gain_acc, gain_come, gain_line)

    ws, ms = (w_query, w_key, w_value), (m_query, m_key, m_value)
    loads = [
        pltpu.make_async_copy(ws[i].at[:, pl.ds(at, size)], dxn.at[pl.ds(0, own_in), pl.ds(to, size)], load_sem.at[n])
        for n, (i, at, to, size) in enumerate(places)
    ]
    first = [
        pltpu.make_async_copy(ws[i].at[span(rep, rows_in), pl.ds(at, size)], moment_in.at[:, pl.ds(to, size)], load_sem.at[9 + n])
        for n, (i, at, to, size) in enumerate(places)
    ] + [pltpu.make_async_copy(w_outproj.at[:, span(rep, cols_out)], moment_out, load_sem.at[15])]
    early = [pltpu.make_async_copy(a, b, load_sem.at[7 + i]) for i, (a, b) in enumerate(((tok_hbm, tok), (cot_hbm, cot)))]
    for load in first + loads + early:
        load.start()
    gain_full[me] = gain[...].astype(B16).astype(F32)
    links.barrier()

    def gain_line_copy(way, k):
        at = gain_full.at[me - way * k]
        return links.remote(at, at, ("gf", way, k), rep, me + way)

    def gain_came(way, k):
        at = gain_full.at[me - way * (k + 1)]
        return links.remote(at, at, ("gf", way, k), rep, me)

    for way in WAYS:
        @pl.when(links.goes(way, 0))
        def _():
            gain_line_copy(way, 0).start()
    for load in first:
        load.wait()
    here = (me,) + links.where()
    w_in[here] = moment_in[...].astype(B16)
    get_in.start()
    w_out[here] = moment_out[...].astype(B16)
    for load in loads:
        load.wait()
    for r in range(n_rep):
        @pl.when(rep != r)
        def _():
            w_in[(me,) + bits_of(r, nb)] = dxn[r * rows_in : (r + 1) * rows_in, :all_in].astype(B16)

    load_out = pltpu.make_async_copy(w_outproj, dxn.at[pl.ds(0, own_out), :], load_sem.at[6])
    load_out.start()
    load_out.wait()
    for r in range(n_rep):
        @pl.when(rep != r)
        def _():
            w_out[(me,) + bits_of(r, nb)] = dxn[:own_out, r * cols_out : (r + 1) * cols_out].astype(B16)

    loads = [
        pltpu.make_async_copy(ms[i].at[span(rep, rows_in), pl.ds(at, size)], moment_in.at[:, pl.ds(to, size)], load_sem.at[n])
        for n, (i, at, to, size) in enumerate(places)
    ] + [pltpu.make_async_copy(m_outproj.at[:, span(rep, cols_out)], moment_out, load_sem.at[6])]
    for load in loads:
        load.start()

    row_acc[...] = jnp.broadcast_to(seg_row[...].astype(F32), (row_acc.shape[1], seq)).T
    own_seg = seg_row[...].astype(F32)

    def masks(i):
        r = span(i, rows)
        seg_col = row_acc[r, :1]
        key = lax.broadcasted_iota(jnp.int32, (rows, seq), 0) + i * rows
        query = lax.broadcasted_iota(jnp.int32, (rows, seq), 1)
        seen = (key <= query) & (seg_col == own_seg)
        bias[r, :] = jnp.where(seen, 0.0, -1e30)
        start = jnp.sum(jnp.where(own_seg < seg_col, 1.0, 0.0), 1, keepdims=True)
        at = lax.broadcasted_iota(jnp.int32, (rows, 1), 0) + i * rows
        angle = (at.astype(F32) - start) * frequency[...]
        lane = lax.rem(lax.broadcasted_iota(jnp.int32, (rows, pair), 1), HEAD_SIZE)
        cosine[r, :] = jnp.cos(angle)
        s = jnp.sin(angle)
        sine[r, :] = jnp.where(lane < HEAD_SIZE // 2, -s, s)
        x = tok[r, :].astype(F32)
        inv = lax.rsqrt(jnp.mean(x * x, -1, keepdims=True) + norm_eps)
        inv_ref[r, :] = jnp.broadcast_to(inv, (rows, 128))

    early[0].wait()
    tiles(seq // rows, masks)
    early[1].wait()

    for k in range(n_shard - 1):
        for way in WAYS:
            @pl.when(links.comes(way, k))
            def _():
                gain_came(way, k).wait_recv()
                if k + 1 < n_shard - 1:
                    @pl.when(links.goes(way, k + 1))
                    def _():
                        gain_line_copy(way, k + 1).start()

    def gains():
        return jnp.concatenate([gain_full[s] for s in range(n_shard)], 1)

    def norm(i):
        r = span(i, rows)
        xn[r, :] = (tok[r, :].astype(F32) * inv_ref[r, :1] * gains()).astype(B16)

    tiles(seq // rows, norm)

    def project(s, fresh=False):
        x = xn[:, span(s, own_in)]

        def columns(c):
            part = mm(x, flat(w_in[(s,) + (slice(None),) * (nb + 1) + (span(c, TILE),)]))
            at = span(c, TILE)
            dxn[:, at] = part if fresh else dxn[:, at] + part

        tiles(all_in // TILE, columns)

    project(me, True)
    first_phase, lag = n_shard - 1 + nb, n_shard

    def gather_time(t):
        if t < n_shard - 1:
            get_in.arrive(t)
        for k in range(n_shard - 1):
            if 0 <= t - k <= nb:
                get_in.event(k, t - k, project)
        if t == n_shard - 2:
            get_out.start()
        if 0 <= t - lag < get_out.times():
            get_out.time(t - lag)

    for t in range(first_phase):
        gather_time(t)
    later = list(range(first_phase, lag + get_out.times()))

    def tables():
        c, s = cosine[...], sine[...]
        return jnp.concatenate([c] * (TILE // pair), 1), jnp.concatenate([s] * (TILE // pair), 1)

    def query_tile(i):
        per = q_part // TILE
        x = dxn[:, pl.ds(pl.multiple_of(lax.div(i, per) * chunk + lax.rem(i, per) * TILE, TILE), TILE)]
        c, s = tables()
        q[:, span(i, TILE)] = (x * c + swap_halves(x) * s).astype(B16) * B16(scale)

    tiles(q_width // TILE, query_tile)
    low = lax.broadcasted_iota(jnp.int32, (seq, pair), 1) < HEAD_SIZE

    def split(x, into, into_t, shrink):
        for g in range(kv_heads):
            two = x[:, (g // 2) * pair : (g // 2 + 1) * pair].astype(B16).astype(F32)
            other = pltpu.roll(two, HEAD_SIZE, 1)
            first, second = (two, other) if g % 2 == 0 else (other, two)
            sides = jnp.where(low, first, 0.0).astype(B16), jnp.where(low, 0.0, second).astype(B16)
            for b in range(n_tok):
                for side in range(2):
                    at = slice((2 * b + side) * TILE, (2 * b + side + 1) * TILE)
                    part = sides[side][b * TILE : (b + 1) * TILE]
                    into[g, at, :] = part
                    into_t[g, :, at] = part.T * B16(shrink)

    for first, into, into_t, turned in ((q_part, kx, kxt, True), (q_part + kv_part, vx, vxt, False)):
        x = jnp.concatenate([dxn[:, c * chunk + first : c * chunk + first + kv_part] for c in range(2)], 1)
        if turned:
            c, s = tables()
            x = x * c + swap_halves(x) * s
        split(x, into, into_t, scale if turned else 1.0)

    def blocks():
        for b in range(n_tok):
            first = max(b - 1, 0)
            yield b, slice(b * TILE, (b + 1) * TILE), slice(2 * first * TILE, 2 * (b + 1) * TILE), range(first, b + 1)

    def tile_of(x, j):
        return x[j * TILE : (j + 1) * TILE]

    together = 2

    def forward(i):
        for n, t in enumerate(later):
            @pl.when(i == min(1 + n, pairs // together))
            def _():
                gather_time(t)

        here = [(i * together + u, *block) for u in range(together) for block in blocks()]
        scores = [nt(kx[lax.div(p, per_group), rs, :], q[qs, span(p, pair)]) for p, b, qs, rs, keys in here]
        probs = []
        for (p, b, qs, rs, keys), score in zip(here, scores):
            grown = [
                jnp.exp(tile_of(score, 2 * j + side) + bias[key * TILE : (key + 1) * TILE, qs])
                for j, key in enumerate(keys)
                for side in range(2)
            ]
            inv = []
            for side in range(2):
                inv.append(1.0 / sum(jnp.sum(x, 0, keepdims=True) for x in grown[side::2]))
                inv_l[p, side, :, qs] = inv[side]
            probs.append(jnp.concatenate([(x * inv[j % 2]).astype(B16) for j, x in enumerate(grown)], 0))
        for (p, b, qs, rs, keys), prob in zip(here, probs):
            a_t = mm(vxt[lax.div(p, per_group), :, rs], prob)
            attn_t[span(p, pair), qs] = a_t.astype(B16)
            attn[qs, span(p, pair)] = a_t.T.astype(B16)

    tiles(pairs // together, forward)

    def out_grad(r):
        x = mm(attn_t[...], cot[:, span(r, cols_out)]).astype(B16)
        part_out[(slice(None),) + bits_of(r, nb)] = x.reshape(n_shard, own_out, cols_out)

    tiles(n_rep, out_grad)
    for k in range(n_shard):
        sum_out.start(k)
    for t in later[max(pairs // together - 1, 0) :]:
        gather_time(t)

    def head_grad(s):
        x = None
        for r in range(n_rep):
            part = nt(cot[:, r * cols_out : (r + 1) * cols_out], w_out[(s,) + bits_of(r, nb)])
            x = part if x is None else x + part
        dattn[:, span(s, own_out)] = x.astype(B16)

    tiles(n_shard, head_grad)

    def reduce_time(who, t):
        for step in reversed(range(nb)):
            if 0 <= t - step < n_shard:
                who.event(t - step, step)

    def weight_grad(c):
        cols = dqkv[:, c * chunk : (c + 1) * chunk]

        def one(k):
            s = sum_in[c].dest(k)
            x = tn(xn[:, span(s, own_in)], cols).astype(B16)
            part_in[(s,) + (both,) * nb + part_cols[c]] = x.reshape((2,) * nb + (rows_in, chunk))

        tiles(n_shard, one)
        for k in range(n_shard):
            sum_in[c].start(k)

    n_reduce = n_shard + nb - 1

    in_loop = (2 * n_reduce) // 3

    def backward(p):
        for t in range(in_loop):
            @pl.when(p == 1 + (t * (pairs - 2)) // max(in_loop - 1, 1))
            def _():
                reduce_time(sum_out, t)

        @pl.when(p == pairs // 2)
        def _():
            weight_grad(0)

        g = lax.div(p, per_group)
        lanes = span(p, pair)

        @pl.when(lax.rem(p, per_group) == 0)
        def _():
            dk_acc[...] = jnp.zeros_like(dk_acc)
            dv_acc[...] = jnp.zeros_like(dv_acc)

        scores = [(nt(kx[g, rs, :], q[qs, lanes]), nt(vx[g, rs, :], dattn[qs, lanes])) for b, qs, rs, keys in blocks()]
        grads = []
        for (b, qs, rs, keys), (score, dp) in zip(blocks(), scores):
            prob = [
                jnp.exp(tile_of(score, 2 * j + side) + bias[key * TILE : (key + 1) * TILE, qs]) * inv_l[p, side, :, qs]
                for j, key in enumerate(keys)
                for side in range(2)
            ]
            inner = [
                sum(jnp.sum(x * tile_of(dp, 2 * j + side), 0, keepdims=True) for j, x in enumerate(prob[side::2]))
                for side in range(2)
            ]
            ds = [(x * (tile_of(dp, j) - inner[j % 2])).astype(B16) for j, x in enumerate(prob)]
            grads.append((jnp.concatenate([x.astype(B16) for x in prob], 0), jnp.concatenate(ds, 0)))
        for (b, qs, rs, keys), (prob, ds) in zip(blocks(), grads):
            dv_acc[rs, :] += mm(prob, dattn[qs, lanes])
            dk_acc[rs, :] += mm(ds, q[qs, lanes])
            x = mm(kxt[g, :, rs], ds).T
            half_pairs = pairs // 2
            to = lax.div(p, half_pairs) * chunk + lax.rem(p, half_pairs) * pair
            dqkv[qs, pl.ds(pl.multiple_of(to, pair), pair)] = (x * cosine[qs, :] - swap_halves(x) * sine[qs, :]).astype(B16)

        @pl.when(lax.rem(p, per_group) == per_group - 1)
        def _():
            def joined(acc):
                both = [acc[j * TILE : (j + 1) * TILE, :] for j in range(2 * n_tok)]
                return jnp.concatenate([both[2 * b] + pltpu.roll(both[2 * b + 1], HEAD_SIZE, 1) for b in range(n_tok)], 0)

            dk, dv = joined(dk_acc), joined(dv_acc)
            dk = dk * cosine[...] - swap_halves(dk) * sine[...]
            for x, first in ((dk, q_part), (dv, q_part + kv_part)):
                half_groups = kv_heads // 2
                to = lax.div(g, half_groups) * chunk + first + lax.div(lax.rem(g, half_groups), 2) * pair
                at = pl.ds(pl.multiple_of(to, pair), pair)
                odd = lax.rem(g, 2)

                @pl.when(odd == 0)
                def _():
                    dqkv[:, at] = x.astype(B16)

                @pl.when(odd == 1)
                def _():
                    high = pltpu.roll(x, HEAD_SIZE, 1)
                    dqkv[:, at] = jnp.where(low, dqkv[:, at].astype(F32), high).astype(B16)

    tiles(pairs, backward)

    weight_grad(1)
    for load in loads:
        load.wait()

    row_acc[...] = jnp.zeros_like(row_acc)

    def input_grad(s):
        c = slice(s * own_in, (s + 1) * own_in)
        d = nt(dqkv[...], flat(w_in[s]))
        normed = tok[:, c].astype(F32) * inv_ref[:, :1]
        gain_acc[s] = jnp.sum(d * normed, 0, keepdims=True)
        d = d * gain_full[s]
        dxn[:, c] = d
        row_acc[...] += jnp.broadcast_to(jnp.sum(d * normed, 1, keepdims=True), row_acc.shape)

    def token_grad(i):
        r = span(i, rows)
        inv = inv_ref[r, :1]
        normed = tok[r, :].astype(F32) * inv
        mean = row_acc[r, :1] * (1.0 / width)
        grad_tok[r, :] = (cot[r, :].astype(F32) + inv * (dxn[r, :] - normed * mean)).astype(B16)

    def output(r):
        c = span(r, cols_out)
        x = mm(attn[...], flat(w_out[(slice(None),) + bits_of(r, nb)]))
        out[:, c] = (tok[:, c].astype(F32) + x).astype(B16)

    def gather_sums_time(who, t):
        who.gather_event(t)

    todo = []

    def then(method, *args):
        todo.append(functools.partial(method, *args))

    def gain_end():
        gain_out[...] = sum_gain.end()

    out_end = n_reduce - in_loop
    for u in range(3 * (n_shard + nb) + n_reduce):
        if u < out_end:
            then(reduce_time, sum_out, in_loop + u)
        if u < n_reduce:
            then(reduce_time, sum_in[0], u)
        if u == n_reduce:
            then(sum_in[0].finish, decay)
        if 0 <= u - 2 < n_reduce:
            then(reduce_time, sum_in[1], u - 2)
        if u == out_end + 1:
            then(sum_out.finish, decay)
        if u == n_reduce + 2:
            then(sum_in[1].finish, decay)
        for who, lag in ((sum_in[0], n_reduce + 1), (sum_in[1], n_reduce + 3), (sum_out, out_end + 2)):
            if 0 <= u - lag < who.whole.times():
                then(gather_sums_time, who, u - lag)
        if 0 <= u - 3 < nb:
            then(sum_gain.event, u - 3)
        if u == n_reduce + nb:
            then(gain_end)

    def advance():
        todo.pop(0)()

    for s in range(n_shard):
        advance()
        input_grad(s)
    sum_gain.send(0).start()
    advance()
    tiles(seq // rows, token_grad)
    gone = [pltpu.make_async_copy(grad_tok, grad_hbm, load_sem.at[16]), pltpu.make_async_copy(out, out_hbm, load_sem.at[17])]
    gone[0].start()
    advance()
    tiles(n_rep // 2, output)
    advance()
    tiles(n_rep // 2, lambda r: output(r + n_rep // 2))
    gone[1].start()
    while todo:
        advance()

    for who in (get_in, get_out, sum_out, *sum_in):
        who.drain()
    for copy in gone:
        copy.wait()
    for way in WAYS:
        for k in range(n_shard - 1):
            @pl.when(links.goes(way, k))
            def _():
                gain_line_copy(way, k).wait_send()
    assert len(links.names) <= send.shape[0]


def layer(tok, cot, seg, gain, weights, moments, decay, n_rep, n_shard, collective_id):
    seq, width = tok.shape
    w_query, w_key, _, w_outproj = weights
    q_width, kv_width = w_query.shape[1], w_key.shape[1]
    all_in = q_width + 2 * kv_width
    kv_heads, pair = kv_width // HEAD_SIZE, 2 * HEAD_SIZE
    nb = n_rep.bit_length() - 1
    bits = (2,) * nb
    own_in, own_out = width // n_shard, q_width // n_shard
    piece_in, piece_out = (own_in // n_rep, all_in), (own_out, width // n_rep)
    half = HEAD_SIZE // 2
    frequency = np.tile((rope_base ** (-2.0 * np.arange(half) / HEAD_SIZE)).astype(np.float32), pair // half)[None]
    vmem, any_ = pl.BlockSpec(memory_space=pltpu.VMEM), pl.BlockSpec(memory_space=pl.ANY)
    V, D = pltpu.VMEM, pltpu.SemaphoreType.DMA
    n_sems = (
        5 * 2 * (n_shard - 1) * (2 + 2 * nb) + 3 * (n_shard * (1 + 2 * (nb - 1)) + n_shard - 1 + 2 * nb) + nb + 3 * n_shard
    )
    bufs = [V((n_shard,) + (2,) * (nb - 1 - j) + piece, B16) for piece in (piece_in, piece_out) for j in range(nb)]
    shape = jax.ShapeDtypeStruct
    return pl.pallas_call(
        functools.partial(layer_kernel, n_rep, n_shard, decay),
        out_shape=[
            shape((seq, width), B16),
            shape((seq, width), B16),
            shape(bits + piece_in, B16),
            shape(bits + piece_out, B16),
            shape((n_shard,) + bits + piece_in, B16),
            shape((n_shard,) + bits + piece_out, B16),
            shape((1, own_in), F32),
        ],
        in_specs=[any_] * 2 + [vmem] * 3 + [any_] * 8,
        out_specs=[any_] * 6 + [vmem],
        scratch_shapes=[
            V((seq, width), B16),
            V((seq, width), B16),
            V((seq, width), B16),
            V((seq, width), B16),
            V((n_shard,) + bits + piece_in, B16),
            V((n_shard,) + bits + piece_out, B16),
            V((n_shard, 1, own_in), F32),
            V((seq, width), B16),
            V((seq, 128), F32),
            V((seq, q_width), B16),
            V((seq, q_width), B16),
            V((q_width, seq), B16),
            V((seq, q_width), B16),
            V((seq, all_in), B16),
            V((seq, width), F32),
            V((seq, 128), F32),
            V((kv_heads, 2 * seq, pair), B16),
            V((kv_heads, 2 * seq, pair), B16),
            V((kv_heads, pair, 2 * seq), B16),
            V((kv_heads, pair, 2 * seq), B16),
            V((2 * seq, pair), F32),
            V((2 * seq, pair), F32),
            V((seq, seq), F32),
            V((seq, pair), F32),
            V((seq, pair), F32),
            V((q_width // pair, 2, 1, seq), F32),
            V((n_shard,) + bits + piece_in, B16),
            V((n_shard,) + bits + piece_out, B16),
            V((n_shard, 1, own_in), F32),
            V((nb, n_shard, 1, own_in), F32),
            V((n_shard, 1, own_in), F32),
            V(piece_in, F32),
            V(piece_out, F32),
            V((n_shard,) + piece_in, B16),
            V(piece_in, B16),
            V(piece_in, B16),
            V((n_shard,) + piece_out, B16),
            V(piece_out, B16),
            V(piece_out, B16),
            D((18,)),
            D((3,)),
            D((n_sems,)),
            D((n_sems,)),
        ]
        + bufs,
        compiler_params=pltpu.CompilerParams(
            collective_id=collective_id, has_side_effects=True, vmem_limit_bytes=67_043_328
        ),
        name="layer",
    )(tok, cot, seg[None], frequency, gain[None], *weights, *moments)


gain_rate = 0.2


def on_device(
    tokens,
    segments,
    cotangent,
    gain,
    w_query,
    w_key,
    w_value,
    w_outproj,
    moment_gain,
    moment_query,
    moment_key,
    moment_value,
    moment_outproj,
):
    n_rep, n_shard = lax.axis_size("rep"), lax.axis_size("shard")
    total_tokens = tokens.shape[0] * tokens.shape[1] * n_rep * n_shard
    weights = (w_query, w_key, w_value, w_outproj)
    moments = (moment_query, moment_key, moment_value, moment_outproj)
    result, grad_tokens, sum_in, sum_out, m_in, m_out, grad_gain = layer(
        tokens[0], cotangent[0], segments[0], gain, weights, moments, decay, n_rep, n_shard, 0
    )
    grad_gain = grad_gain[0]
    moment_gain_next = decay * moment_gain + grad_gain
    gain_next = gain - gain_rate / math.sqrt(total_tokens) * moment_gain_next
    own_out, cols_out = sum_out.shape[-2:]
    m_out = m_out.reshape(n_shard, n_rep, own_out, cols_out)
    all_in = sum_in.shape[-1]
    grads, moments_next, (result, grad_tokens), (mix, mix_kv, scales) = muon(
        m_in.reshape(-1, all_in),
        m_out,
        sum_in.reshape(-1, all_in),
        sum_out.reshape(n_rep, own_out, cols_out),
        moments,
        (result, grad_tokens),
    )
    updated = update(mix, mix_kv, scales, m_out, moments_next, weights, n_rep, 1)
    return (
        result[None],
        grad_tokens[None],
        grad_gain,
        *grads,
        gain_next,
        *updated,
        moment_gain_next,
        *moments_next,
    )


def solution(mesh):
    in_specs = (
        P(("rep", "shard"), None, None),
        P(("rep", "shard"), None),
        P(("rep", "shard"), None, None),
        P("shard"),
        P("shard", None),
        P("shard", None),
        P("shard", None),
        P("shard", None),
        P("shard"),
        P("shard", None),
        P("shard", None),
        P("shard", None),
        P("shard", None),
    )
    out_specs = (
        P(("rep", "shard"), None, None),
        P(("rep", "shard"), None, None),
        P("shard"),
        P("shard", None),
        P("shard", None),
        P("shard", None),
        P("shard", None),
        P("shard"),
        P("shard", "rep"),
        P("shard", "rep"),
        P("shard", "rep"),
        P("shard", "rep"),
        P("shard"),
        P("shard", None),
        P("shard", None),
        P("shard", None),
        P("shard", None),
    )
    return jax.shard_map(on_device, mesh=mesh, in_specs=in_specs, out_specs=out_specs, check_vma=False)
```
